8 devices in a mesh: fsdp: 8 (over z, y, x, core).
Axes of the slice: x: 2, y: 2, z: 1, core: 2. Of those that a mesh axis runs over, the one named last changes fastest.
Arguments:
- tokens_x: bfloat16 [48, 256, 640], P('fsdp')
- context: bfloat16 [48, 77, 2048], P('fsdp')
- cot_out: bfloat16 [48, 256, 640], P('fsdp')
- w_qkv: bfloat16 [2, 1228800], P(None, 'fsdp')
- w_out: bfloat16 [2, 409600], P(None, 'fsdp')
- w_q2: bfloat16 [2, 409600], P(None, 'fsdp')
- w_kv2: bfloat16 [2, 2621440], P(None, 'fsdp')
- w_out2: bfloat16 [2, 409600], P(None, 'fsdp')
- w_ff1: bfloat16 [2, 3276800], P(None, 'fsdp')
- w_ff2: bfloat16 [2, 1638400], P(None, 'fsdp')
- w_vecs: bfloat16 [2, 10880], P(None, 'fsdp')
Outputs:
- output 1: bfloat16 [48, 256, 640], P('fsdp')
- output 2: bfloat16 [48, 256, 640], P('fsdp')
- output 3: float32 [2, 1228800], P(None, 'fsdp')
- output 4: float32 [2, 409600], P(None, 'fsdp')
- output 5: float32 [2, 409600], P(None, 'fsdp')
- output 6: float32 [2, 2621440], P(None, 'fsdp')
- output 7: float32 [2, 409600], P(None, 'fsdp')
- output 8: float32 [2, 3276800], P(None, 'fsdp')
- output 9: float32 [2, 1638400], P(None, 'fsdp')
- output 10: float32 [2, 10880], P(None, 'fsdp')
All inputs are finite; a program needn't handle non-finite values.
Results may differ from the reference program's by a relative error of at most 0.0199541.
Values are sent between devices in bfloat16 or wider.
A program may use at most 1 GiB of HBM per device.

```python
import math
import jax
import jax.numpy as jnp
from jax import lax

FSDP = 8
BATCH_DEV = 6
TOKENS = 256
D = 640
CTX_D = 2048
CTX_LEN = 77
HEAD = 64
BLOCKS = 2

BATCH = FSDP * BATCH_DEV
HEADS = D // HEAD
FF = 4 * D
SHAPES = ((D, 3 * D), (D, D), (D, D), (CTX_D, 2 * D), (D, D), (D, 2 * FF), (FF, D), (9 * D + 2 * FF,))
NAMES = ('w_qkv', 'w_out', 'w_q2', 'w_kv2', 'w_out2', 'w_ff1', 'w_ff2', 'w_vecs')


def padded_len(shape):
    return ((math.prod(shape) + FSDP - 1) // FSDP) * FSDP


def setup_inputs(seed: int = 0) -> dict:
    draws = jax.random.split(jax.random.key(seed), 11)
    tokens_x = jax.random.normal(draws[0], (BATCH, TOKENS, D), jnp.float32)
    context = jax.random.normal(draws[1], (BATCH, CTX_LEN, CTX_D), jnp.float32)
    cot_out = jax.random.normal(draws[2], (BATCH, TOKENS, D), jnp.float32)
    result = {'tokens_x': tokens_x.astype(jnp.bfloat16), 'context': context.astype(jnp.bfloat16), 'cot_out': cot_out.astype(jnp.bfloat16)}
    for index in range(7):
        shape = SHAPES[index]
        drawn = jax.random.normal(draws[3 + index], (BLOCKS, padded_len(shape)), jnp.float32) * shape[0] ** -0.5
        result[NAMES[index]] = drawn.astype(jnp.bfloat16)
    length = padded_len(SHAPES[7])
    position = jnp.arange(length)
    gain_mask = ((position < 6 * D) & ((position // D) % 2 == 0)).astype(jnp.float32)
    drawn = 0.3 * jax.random.normal(draws[10], (BLOCKS, length), jnp.float32) + gain_mask
    result['w_vecs'] = drawn.astype(jnp.bfloat16)
    return result


def matmul(lhs, rhs):
    return jnp.dot(lhs, rhs, preferred_element_type=jnp.float32)


def layer_norm(residual, gain, shift):
    average = jnp.mean(residual, axis=-1, keepdims=True)
    centered = residual - average
    variance = jnp.mean(centered * centered, axis=-1, keepdims=True)
    return centered * lax.rsqrt(variance + 1e-5) * gain + shift


def attend(query, keys, values):
    scores = jnp.einsum('qhe,khe->hqk', query.astype(jnp.float32), keys.astype(jnp.float32)) * HEAD ** -0.5
    probabilities = jax.nn.softmax(scores, axis=-1).astype(jnp.bfloat16)
    mixed = jnp.einsum('hqk,khe->qhe', probabilities.astype(jnp.float32), values.astype(jnp.float32))
    return mixed.astype(jnp.bfloat16)


def batched_attend(query, keys, values):
    return lax.map(lambda trio: attend(trio[0], trio[1], trio[2]), (query, keys, values))


def block_forward(residual, ctx_rows, flats):
    matrices = [flat[:math.prod(shape)].reshape(shape).astype(jnp.bfloat16) for flat, shape in zip(flats[:7], SHAPES[:7])]
    w_qkv, w_out, w_q2, w_kv2, w_out2, w_ff1, w_ff2 = matrices
    rows = flats[7][:9 * D].reshape(9, D)
    bias_ff1 = flats[7][9 * D:9 * D + 2 * FF]
    norm1 = layer_norm(residual, rows[0], rows[1]).astype(jnp.bfloat16)
    qkv_heads = matmul(norm1, w_qkv).astype(jnp.bfloat16).reshape(BATCH, TOKENS, 3, HEADS, HEAD)
    self_out = batched_attend(qkv_heads[:, :, 0], qkv_heads[:, :, 1], qkv_heads[:, :, 2]).reshape(BATCH * TOKENS, D)
    residual = residual + matmul(self_out, w_out) + rows[6]
    norm2 = layer_norm(residual, rows[2], rows[3]).astype(jnp.bfloat16)
    query = matmul(norm2, w_q2).astype(jnp.bfloat16).reshape(BATCH, TOKENS, HEADS, HEAD)
    kv_heads = matmul(ctx_rows, w_kv2).astype(jnp.bfloat16).reshape(BATCH, CTX_LEN, 2, HEADS, HEAD)
    cross_out = batched_attend(query, kv_heads[:, :, 0], kv_heads[:, :, 1]).reshape(BATCH * TOKENS, D)
    residual = residual + matmul(cross_out, w_out2) + rows[7]
    norm3 = layer_norm(residual, rows[4], rows[5]).astype(jnp.bfloat16)
    hidden = matmul(norm3, w_ff1) + bias_ff1
    gated = (hidden[:, :FF] * jax.nn.gelu(hidden[:, FF:], approximate=False)).astype(jnp.bfloat16)
    return residual + matmul(gated, w_ff2) + rows[8]


def forward(tokens_x, context, flats):
    residual = tokens_x.reshape(BATCH * TOKENS, D).astype(jnp.float32)
    ctx_rows = context.reshape(BATCH * CTX_LEN, CTX_D)

    def step(carry, block_flats):
        return block_forward(carry, ctx_rows, block_flats), None

    residual, unused = lax.scan(step, residual, flats)
    return residual.astype(jnp.bfloat16).reshape(BATCH, TOKENS, D)


def reference(tokens_x, context, cot_out, w_qkv, w_out, w_q2, w_kv2, w_out2, w_ff1, w_ff2, w_vecs):
    flats = tuple(param.astype(jnp.float32) for param in (w_qkv, w_out, w_q2, w_kv2, w_out2, w_ff1, w_ff2, w_vecs))
    out_tokens, pullback = jax.vjp(lambda tok_in, param_set: forward(tok_in, context, param_set), tokens_x, flats)
    grad_x, grads = pullback(cot_out)
    scaled = [grad_item / BATCH for grad_item in grads]
    return (out_tokens, grad_x, scaled[0], scaled[1], scaled[2], scaled[3], scaled[4], scaled[5], scaled[6], scaled[7])
```

```python
import functools
import math
import jax
import jax.numpy as jnp
from jax import lax
from jax.experimental import pallas as pl
from jax.experimental.pallas import tpu as pltpu
from jax.sharding import PartitionSpec as P

HEAD = 64
AXIS = 'fsdp'
CHUNK = 512
STEP = 512
VMEM_LIMIT = 60 * 1024 * 1024

F32 = jnp.float32
BF16 = jnp.bfloat16


def first_bit(core):
    return 4 - 2 * core


def gather_perms(n_dev):
    near = [(i, i ^ (4 if i % 2 == 0 else 2)) for i in range(n_dev)]
    far = [(i, i ^ (2 if i % 2 == 0 else 4)) for i in range(n_dev)]
    core = [(i, i ^ 1) for i in range(n_dev)]
    return near, far, core


def gather_group(shard, n_dev):
    near, far, core = gather_perms(n_dev)
    first = lax.ppermute(shard, AXIS, near)
    mine = lax.ppermute(shard, AXIS, core)
    second = lax.ppermute(jnp.concatenate([shard, first], 0), AXIS, far)
    other_first = lax.ppermute(first, AXIS, core)
    other_second = lax.ppermute(second, AXIS, core)
    return [shard, first, second, mine, other_first, other_second]


def piece_table(me, rows):
    core = lax.rem(me, 2)
    one, two = 4 - 2 * core, 2 + 2 * core
    mate = jnp.bitwise_xor(me, 1)
    x = jnp.bitwise_xor
    return [(0, 0, me), (1, 0, x(me, one)), (2, 0, x(me, two)), (2, rows, x(me, 6)),
            (3, 0, mate), (4, 0, x(mate, two)), (5, 0, x(mate, one)), (5, rows, x(mate, 6))]


def start_loads(pieces, group_rows, width, targets, sems):
    me = lax.axis_index(AXIS)
    table = piece_table(me, group_rows)
    for which, (ref, offset) in enumerate(targets):
        depth = ref.shape[0] // 8
        for block in range(ref.shape[1] // width):
            for array, start, device in table:
                src = pieces[array].at[pl.ds(start + offset + block * depth, depth), :]
                dst = ref.at[pl.ds(pl.multiple_of(device * depth, 16), depth), pl.ds(block * width, width)]
                pltpu.make_async_copy(src, dst, sems.at[which]).start()


def wait_load(ref, sem):
    pltpu.make_async_copy(ref, ref, sem).wait()


def dot_nn(a, b):
    return lax.dot_general(a, b, (((1,), (0,)), ((), ())), preferred_element_type=F32)


def dot_nt(a, b):
    return lax.dot_general(a, b, (((1,), (1,)), ((), ())), preferred_element_type=F32)


def dot_tn(a, b):
    return lax.dot_general(a, b, (((0,), (0,)), ((), ())), preferred_element_type=F32)


def norm_stats(x):
    average = jnp.mean(x, axis=-1, keepdims=True)
    centered = x - average
    variance = jnp.mean(centered * centered, axis=-1, keepdims=True)
    scale = lax.rsqrt(variance + 1e-5)
    return centered * scale, scale


def norm_back(x, gain, d_norm):
    unit, scale = norm_stats(x)
    d_unit = d_norm * gain
    inner = d_unit - jnp.mean(d_unit, axis=-1, keepdims=True) - unit * jnp.mean(d_unit * unit, axis=-1, keepdims=True)
    return scale * inner, jnp.sum(d_norm * unit, axis=0, keepdims=True), jnp.sum(d_norm, axis=0, keepdims=True)


def softmax_rows(scores):
    top = jnp.max(scores, axis=-1, keepdims=True)
    raised = jnp.exp(scores - top)
    return raised * (1.0 / jnp.sum(raised, axis=-1, keepdims=True))


def lane_masks(rows):
    low = lax.broadcasted_iota(jnp.int32, (rows, 2 * HEAD), 1) < HEAD
    return low, jnp.logical_not(low)


def pair_scores(query, key, low, head, valid):
    q_head = jnp.where(low if head == 0 else jnp.logical_not(low), query, jnp.zeros_like(query))
    scores = dot_nt(q_head, key) * HEAD ** -0.5
    if valid is not None:
        column = lax.broadcasted_iota(jnp.int32, scores.shape, 1)
        scores = jnp.where(column < valid, scores, -1e30)
    return q_head, softmax_rows(scores)


def pair_forward(query, key, value, valid=None):
    low, _ = lane_masks(query.shape[0])
    mixed = []
    for head in range(2):
        _, probs = pair_scores(query, key, low, head, valid)
        mixed.append(dot_nn(probs.astype(BF16), value))
    return jnp.where(low, mixed[0], mixed[1]).astype(BF16)


def pair_backward(query, key, value, d_out, valid=None):
    low, _ = lane_masks(query.shape[0])
    d_query, d_key, d_value = [], None, None
    for head in range(2):
        q_head, probs = pair_scores(query, key, low, head, valid)
        d_head = jnp.where(low if head == 0 else jnp.logical_not(low), d_out, jnp.zeros_like(d_out))
        d_probs = dot_nt(d_head, value).astype(BF16).astype(F32)
        inner = jnp.sum(d_probs * probs, axis=-1, keepdims=True)
        d_scores = ((probs * (d_probs - inner)) * HEAD ** -0.5).astype(BF16)
        d_query.append(dot_nn(d_scores, key))
        dk, dv = dot_tn(d_scores, q_head), dot_tn(probs.astype(BF16), d_head)
        d_key = dk if d_key is None else d_key + dk
        d_value = dv if d_value is None else d_value + dv
    return jnp.where(low, d_query[0], d_query[1]).astype(BF16), d_key.astype(BF16), d_value.astype(BF16)


def add_rows(ref, step, rows):
    @pl.when(step == 0)
    def _():
        ref[...] = jnp.zeros_like(ref)
    for index, row in enumerate(rows):
        ref[pl.ds(index, 1), :] += row


def self_forward_kernel(samples, tokens, h_ref, rows_ref, *refs):
    pieces, (norm_ref, qkv_ref, mix_ref, out_ref, w_qkv, w_out, sems) = refs[:6], refs[6:]
    width = h_ref.shape[1]
    step = pl.program_id(0)

    @pl.when(step == 0)
    def _():
        depth = width // 8
        start_loads(pieces, pieces[0].shape[0], width, [(w_qkv, 0), (w_out, 3 * depth)], sems)

    x = h_ref[...].astype(F32)
    unit, _ = norm_stats(x)
    normed = (unit * rows_ref[0:1, :] + rows_ref[1:2, :]).astype(BF16)
    norm_ref[...] = normed

    @pl.when(step == 0)
    def _():
        wait_load(w_qkv, sems.at[0])
        wait_load(w_out, sems.at[1])

    qkv_ref[...] = dot_nn(normed, w_qkv[...]).astype(BF16)
    pairs = width // (2 * HEAD)

    def body(index, carry):
        row = pl.multiple_of((index // pairs) * tokens, tokens)
        col = pl.multiple_of((index % pairs) * 2 * HEAD, 2 * HEAD)
        part = lambda which: qkv_ref[pl.ds(row, tokens), pl.ds(which * width + col, 2 * HEAD)]
        mix_ref[pl.ds(row, tokens), pl.ds(col, 2 * HEAD)] = pair_forward(part(0), part(1), part(2))
        return carry

    lax.fori_loop(0, samples * pairs, body, 0)
    out_ref[...] = x + dot_nn(mix_ref[...], w_out[...]) + rows_ref[6:7, :]


def cross_forward_kernel(samples, tokens, valid, h_ref, rows_ref, ctx_ref, *refs):
    pieces, (norm_ref, query_ref, kv_ref, mix_ref, out_ref, w_kv, w_query, w_out, sems) = refs[:6], refs[6:]
    width = h_ref.shape[1]
    step = pl.program_id(0)
    padded = ctx_ref.shape[0] // (samples * pl.num_programs(0))

    @pl.when(step == 0)
    def _():
        deep, depth = w_kv.shape[0] // 8, width // 8
        start_loads(pieces, pieces[0].shape[0], width,
                    [(w_kv, 0), (w_query, 2 * deep), (w_out, 2 * deep + depth)], sems)

    x = h_ref[...]
    unit, _ = norm_stats(x)
    normed = (unit * rows_ref[2:3, :] + rows_ref[3:4, :]).astype(BF16)
    norm_ref[...] = normed

    @pl.when(step == 0)
    def _():
        wait_load(w_kv, sems.at[0])
        wait_load(w_query, sems.at[1])
        wait_load(w_out, sems.at[2])
        kv_ref[...] = dot_nn(ctx_ref[...], w_kv[...]).astype(BF16)

    query_ref[...] = dot_nn(normed, w_query[...]).astype(BF16)
    pairs = width // (2 * HEAD)

    def body(index, carry):
        sample = index // pairs
        row = pl.multiple_of(sample * tokens, tokens)
        kv_row = pl.multiple_of((step * samples + sample) * padded, 16)
        col = pl.multiple_of((index % pairs) * 2 * HEAD, 2 * HEAD)
        query = query_ref[pl.ds(row, tokens), pl.ds(col, 2 * HEAD)]
        key = kv_ref[pl.ds(kv_row, padded), pl.ds(col, 2 * HEAD)]
        value = kv_ref[pl.ds(kv_row, padded), pl.ds(width + col, 2 * HEAD)]
        mix_ref[pl.ds(row, tokens), pl.ds(col, 2 * HEAD)] = pair_forward(query, key, value, valid)
        return carry

    lax.fori_loop(0, samples * pairs, body, 0)
    out_ref[...] = x + dot_nn(mix_ref[...], w_out[...]) + rows_ref[7:8, :]


def ff_loads(pieces, w_ff1, w_ff2, sems):
    width = w_ff1.shape[0]
    start_loads(pieces, pieces[0].shape[0], width, [(w_ff1, 0), (w_ff2, w_ff1.shape[1] // width * (width // 8))], sems)


def ff_forward_kernel(h_ref, rows_ref, bias_ref, *refs):
    pieces, (norm_ref, gated_ref, save_a, save_g, out_ref, w_ff1, w_ff2, sems) = refs[:6], refs[6:]
    half = w_ff2.shape[0]
    step = pl.program_id(0)

    @pl.when(step == 0)
    def _():
        ff_loads(pieces, w_ff1, w_ff2, sems)

    x = h_ref[...]
    unit, _ = norm_stats(x)
    normed = (unit * rows_ref[4:5, :] + rows_ref[5:6, :]).astype(BF16)
    norm_ref[...] = normed

    @pl.when(step == 0)
    def _():
        wait_load(w_ff1, sems.at[0])
        wait_load(w_ff2, sems.at[1])

    total = x + rows_ref[8:9, :]
    for start in range(0, half, CHUNK):
        u_a = dot_nn(normed, w_ff1[:, start:start + CHUNK]) + bias_ref[:, start:start + CHUNK]
        u_g = dot_nn(normed, w_ff1[:, half + start:half + start + CHUNK]) + bias_ref[:, half + start:half + start + CHUNK]
        cumulative = 0.5 * (1.0 + lax.erf(u_g * math.sqrt(0.5)))
        gate = u_g * cumulative
        slope = cumulative + u_g * (jnp.exp(-0.5 * u_g * u_g) * (1.0 / math.sqrt(2.0 * math.pi)))
        gated = (u_a * gate).astype(BF16)
        gated_ref[:, start:start + CHUNK] = gated
        save_a[:, start:start + CHUNK] = gate
        save_g[:, start:start + CHUNK] = u_a * slope
        total = total + dot_nn(gated, w_ff2[start:start + CHUNK, :])
    out_ref[...] = total.astype(out_ref.dtype)


def ff_backward_kernel(grad_ref, save_a, save_g, h_ref, rows_ref, *refs):
    pieces, (grad_bf_ref, d_hidden_ref, out_ref, vec_ref, bias_ref, w_ff1, w_ff2, sems) = refs[:6], refs[6:]
    half = w_ff2.shape[0]
    step = pl.program_id(0)

    @pl.when(step == 0)
    def _():
        ff_loads(pieces, w_ff1, w_ff2, sems)
        bias_ref[...] = jnp.zeros_like(bias_ref)

    grad = grad_ref[...].astype(F32)
    grad_bf = grad.astype(BF16)
    grad_bf_ref[...] = grad_bf

    @pl.when(step == 0)
    def _():
        wait_load(w_ff1, sems.at[0])
        wait_load(w_ff2, sems.at[1])

    d_norm = jnp.zeros(grad.shape, F32)
    for start in range(0, half, CHUNK):
        d_gated = dot_nt(grad_bf, w_ff2[start:start + CHUNK, :]).astype(BF16).astype(F32)
        for base, saved in ((0, save_a), (half, save_g)):
            d_part = d_gated * saved[:, start:start + CHUNK]
            columns = slice(base + start, base + start + CHUNK)
            bias_ref[0:1, columns] += jnp.sum(d_part, axis=0, keepdims=True)
            d_part = d_part.astype(BF16)
            d_hidden_ref[:, columns] = d_part
            d_norm = d_norm + dot_nt(d_part, w_ff1[:, columns])
    d_res, g_gain, g_shift = norm_back(h_ref[...], rows_ref[4:5, :], d_norm)
    out_ref[...] = grad + d_res
    add_rows(vec_ref, step, [g_gain, g_shift, jnp.sum(grad, axis=0, keepdims=True)])


def cross_backward_kernel(samples, tokens, valid, grad_ref, query_ref, kv_ref, h_ref, rows_ref, *refs):
    pieces, (grad_bf_ref, d_query_ref, d_kv_ref, out_ref, vec_ref, d_mix, w_query, w_out, sems) = refs[:6], refs[6:]
    width = h_ref.shape[1]
    step = pl.program_id(0)
    padded = kv_ref.shape[0] // samples

    @pl.when(step == 0)
    def _():
        depth = width // 8
        base = pieces[0].shape[0] - 2 * depth
        start_loads(pieces, pieces[0].shape[0], width, [(w_query, base), (w_out, base + depth)], sems)

    grad = grad_ref[...]
    grad_bf = grad.astype(BF16)
    grad_bf_ref[...] = grad_bf

    @pl.when(step == 0)
    def _():
        wait_load(w_query, sems.at[0])
        wait_load(w_out, sems.at[1])

    d_mix[...] = dot_nt(grad_bf, w_out[...]).astype(BF16)
    pairs = width // (2 * HEAD)

    def body(index, carry):
        sample = index // pairs
        row = pl.multiple_of(sample * tokens, tokens)
        kv_row = pl.multiple_of(sample * padded, 16)
        col = pl.multiple_of((index % pairs) * 2 * HEAD, 2 * HEAD)
        at = (pl.ds(row, tokens), pl.ds(col, 2 * HEAD))
        at_key = (pl.ds(kv_row, padded), pl.ds(col, 2 * HEAD))
        at_value = (pl.ds(kv_row, padded), pl.ds(width + col, 2 * HEAD))
        dq, dk, dv = pair_backward(query_ref[at], kv_ref[at_key], kv_ref[at_value], d_mix[at], valid)
        d_query_ref[at] = dq
        d_kv_ref[at_key] = dk
        d_kv_ref[at_value] = dv
        return carry

    lax.fori_loop(0, samples * pairs, body, 0)
    d_norm = dot_nt(d_query_ref[...], w_query[...])
    d_res, g_gain, g_shift = norm_back(h_ref[...], rows_ref[2:3, :], d_norm)
    out_ref[...] = grad + d_res
    add_rows(vec_ref, step, [g_gain, g_shift, jnp.sum(grad, axis=0, keepdims=True)])


def self_backward_kernel(samples, tokens, grad_ref, qkv_ref, h_ref, rows_ref, *refs):
    pieces, (grad_bf_ref, d_qkv_ref, out_ref, vec_ref, d_mix, w_qkv, w_out, sems) = refs[:6], refs[6:]
    width = h_ref.shape[1]
    step = pl.program_id(0)

    @pl.when(step == 0)
    def _():
        depth = width // 8
        start_loads(pieces, pieces[0].shape[0], width, [(w_qkv, 0), (w_out, 3 * depth)], sems)

    grad = grad_ref[...]
    grad_bf = grad.astype(BF16)
    grad_bf_ref[...] = grad_bf

    @pl.when(step == 0)
    def _():
        wait_load(w_qkv, sems.at[0])
        wait_load(w_out, sems.at[1])

    d_mix[...] = dot_nt(grad_bf, w_out[...]).astype(BF16)
    pairs = width // (2 * HEAD)

    def body(index, carry):
        row = pl.multiple_of((index // pairs) * tokens, tokens)
        col = pl.multiple_of((index % pairs) * 2 * HEAD, 2 * HEAD)
        at = lambda which: (pl.ds(row, tokens), pl.ds(which * width + col, 2 * HEAD))
        d_parts = pair_backward(qkv_ref[at(0)], qkv_ref[at(1)], qkv_ref[at(2)], d_mix[at(0)])
        for which in range(3):
            d_qkv_ref[at(which)] = d_parts[which]
        return carry

    lax.fori_loop(0, samples * pairs, body, 0)
    d_norm = dot_nt(d_qkv_ref[...], w_qkv[...])
    d_res, g_gain, g_shift = norm_back(h_ref[...].astype(F32), rows_ref[0:1, :], d_norm)
    out_ref[...] = (grad + d_res).astype(out_ref.dtype)
    add_rows(vec_ref, step, [g_gain, g_shift, jnp.sum(grad, axis=0, keepdims=True)])


ANY = pl.BlockSpec(memory_space=pl.ANY)


def by_step(rows, columns):
    return pl.BlockSpec((rows, columns), lambda i: (i, 0))


def whole(rows, columns):
    return pl.BlockSpec((rows, columns), lambda i: (0, 0))


def shape(rows, columns, dtype):
    return jax.ShapeDtypeStruct((rows, columns), dtype)


def call(kernel, name, steps, in_specs, out_specs, out_shapes, scratch, flops, moved):
    return pl.pallas_call(
        kernel, grid=(steps,), in_specs=in_specs, out_specs=out_specs, out_shape=out_shapes, scratch_shapes=scratch,
        cost_estimate=pl.CostEstimate(flops=int(flops), bytes_accessed=int(moved), transcendentals=0),
        compiler_params=pltpu.CompilerParams(dimension_semantics=('arbitrary',), vmem_limit_bytes=VMEM_LIMIT), name=name)


def self_forward(h, rows, pieces, tokens):
    count, width = h.shape
    return call(
        functools.partial(self_forward_kernel, STEP // tokens, tokens), 'self_forward', count // STEP,
        [by_step(STEP, width), whole(*rows.shape)] + [ANY] * 6,
        [by_step(STEP, width), by_step(STEP, 3 * width), by_step(STEP, width), by_step(STEP, width)],
        [shape(count, width, BF16), shape(count, 3 * width, BF16), shape(count, width, BF16), shape(count, width, F32)],
        [pltpu.VMEM((width, 3 * width), BF16), pltpu.VMEM((width, width), BF16), pltpu.SemaphoreType.DMA((2,))],
        count * width * width * 8 + count * tokens * width * 4, 2e7)(h, rows, *pieces)


def cross_forward(h, rows, ctx, pieces, tokens, valid):
    count, width = h.shape
    ctx_rows, ctx_width = ctx.shape
    return call(
        functools.partial(cross_forward_kernel, STEP // tokens, tokens, valid), 'cross_forward', count // STEP,
        [by_step(STEP, width), whole(*rows.shape), whole(ctx_rows, ctx_width)] + [ANY] * 6,
        [by_step(STEP, width), by_step(STEP, width), whole(ctx_rows, 2 * width), by_step(STEP, width), by_step(STEP, width)],
        [shape(count, width, BF16), shape(count, width, BF16), shape(ctx_rows, 2 * width, BF16), shape(count, width, BF16),
         shape(count, width, F32)],
        [pltpu.VMEM((ctx_width, 2 * width), BF16), pltpu.VMEM((width, width), BF16), pltpu.VMEM((width, width), BF16),
         pltpu.SemaphoreType.DMA((3,))],
        count * width * width * 4 + ctx_rows * ctx_width * width * 4 + count * 128 * width * 4, 2e7)(h, rows, ctx, *pieces)


def ff_forward(h, rows, bias, pieces, out_dtype):
    count, width = h.shape
    half = bias.shape[1] // 2
    return call(
        ff_forward_kernel, 'ff_forward', count // STEP,
        [by_step(STEP, width), whole(*rows.shape), whole(1, 2 * half)] + [ANY] * 6,
        [by_step(STEP, width), by_step(STEP, half), by_step(STEP, half), by_step(STEP, half), by_step(STEP, width)],
        [shape(count, width, BF16), shape(count, half, BF16), shape(count, half, F32), shape(count, half, F32),
         shape(count, width, out_dtype)],
        [pltpu.VMEM((width, 2 * half), BF16), pltpu.VMEM((half, width), BF16), pltpu.SemaphoreType.DMA((2,))],
        count * width * half * 6, 6e7)(h, rows, bias, *pieces)


def ff_backward(grad, save_a, save_g, h, rows, pieces):
    count, width = h.shape
    half = save_a.shape[1]
    return call(
        ff_backward_kernel, 'ff_backward', count // STEP,
        [by_step(STEP, width), by_step(STEP, half), by_step(STEP, half), by_step(STEP, width), whole(*rows.shape)] + [ANY] * 6,
        [by_step(STEP, width), by_step(STEP, 2 * half), by_step(STEP, width), whole(8, width), whole(8, 2 * half)],
        [shape(count, width, BF16), shape(count, 2 * half, BF16), shape(count, width, F32), shape(8, width, F32),
         shape(8, 2 * half, F32)],
        [pltpu.VMEM((width, 2 * half), BF16), pltpu.VMEM((half, width), BF16), pltpu.SemaphoreType.DMA((2,))],
        count * width * half * 6, 6e7)(grad, save_a, save_g, h, rows, *pieces)


def cross_backward(grad, query, kv, h, rows, pieces, tokens, valid):
    count, width = h.shape
    ctx_rows = kv.shape[0]
    steps = count // STEP
    return call(
        functools.partial(cross_backward_kernel, STEP // tokens, tokens, valid), 'cross_backward', steps,
        [by_step(STEP, width), by_step(STEP, width), by_step(ctx_rows // steps, 2 * width), by_step(STEP, width),
         whole(*rows.shape)] + [ANY] * 6,
        [by_step(STEP, width), by_step(STEP, width), by_step(ctx_rows // steps, 2 * width), by_step(STEP, width), whole(8, width)],
        [shape(count, width, BF16), shape(count, width, BF16), shape(ctx_rows, 2 * width, BF16), shape(count, width, F32),
         shape(8, width, F32)],
        [pltpu.VMEM((STEP, width), BF16), pltpu.VMEM((width, width), BF16), pltpu.VMEM((width, width), BF16),
         pltpu.SemaphoreType.DMA((2,))],
        count * width * width * 4 + count * 128 * width * 10, 2e7)(grad, query, kv, h, rows, *pieces)


def self_backward(grad, qkv, h, rows, pieces, tokens, out_dtype):
    count, width = h.shape
    return call(
        functools.partial(self_backward_kernel, STEP // tokens, tokens), 'self_backward', count // STEP,
        [by_step(STEP, width), by_step(STEP, 3 * width), by_step(STEP, width), whole(*rows.shape)] + [ANY] * 6,
        [by_step(STEP, width), by_step(STEP, 3 * width), by_step(STEP, width), whole(8, width)],
        [shape(count, width, BF16), shape(count, 3 * width, BF16), shape(count, width, out_dtype), shape(8, width, F32)],
        [pltpu.VMEM((STEP, width), BF16), pltpu.VMEM((width, 3 * width), BF16), pltpu.VMEM((width, width), BF16),
         pltpu.SemaphoreType.DMA((2,))],
        count * width * width * 8 + count * tokens * width * 10, 3e7)(grad, qkv, h, rows, *pieces)


def scatter_sum(full, n_dev):
    near, far, core_perm = gather_perms(n_dev)
    me = lax.axis_index(AXIS)
    core, chip = me % 2, me // 2
    one, two = 1 + core, 2 - core
    by_chip = full.reshape((n_dev // 2, 2) + full.shape[1:])
    pick = lambda array, index: lax.dynamic_index_in_dim(array, index, 0, keepdims=False)
    ours = lambda index: lax.dynamic_slice(by_chip, (index, core) + (0,) * (full.ndim - 1),
                                           (1, 1) + full.shape[1:]).reshape(full.shape[1:])
    got = lax.ppermute(lax.dynamic_index_in_dim(by_chip, 1 - core, 1, keepdims=False), AXIS, core_perm)
    part = lambda index: ours(index) + pick(got, index)
    x = jnp.bitwise_xor
    second = lax.ppermute(jnp.stack([part(x(chip, one)), part(x(x(chip, one), two))]), AXIS, far)
    third = lax.ppermute(part(x(chip, two)) + second[1], AXIS, near)
    return part(chip) + second[0] + third


def weight_grad(inputs, grads):
    grad = lax.dot_general(inputs, grads, (((0,), (0,)), ((), ())), preferred_element_type=F32)
    return grad.reshape(8, grad.shape[0] // 8, grad.shape[1])


def solution(mesh):
    n_dev = mesh.shape[AXIS]

    def local(tokens_x, context, cot_out, *shards):
        batch, tokens, width = tokens_x.shape
        _, valid, ctx_width = context.shape
        blocks = shards[0].shape[0]
        total = batch * n_dev
        depth = width // n_dev
        count = batch * tokens
        half = 4 * width

        views = []
        for shard, rows in zip(shards[:7], (depth, depth, depth, ctx_width // n_dev, depth, depth, half // n_dev)):
            views.append(shard.reshape(blocks, rows, -1))
        views = lax.optimization_barrier(views)
        cut = lambda view, layer: [view[layer][:, c:c + width] for c in range(0, view.shape[2], width)]
        qkv_s, out_s, q2_s, kv2_s, out2_s, ff1_s, ff2_s = views
        vec_len = shards[7].shape[1]
        vec_rows = 16
        vec_block = jnp.pad(shards[7].reshape(-1), (0, vec_rows * width - blocks * vec_len)).reshape(vec_rows, width)

        groups = []
        for layer in range(blocks):
            extra = [vec_block] if layer == 0 else []
            groups.append([gather_group(jnp.concatenate(cut(qkv_s, layer) + cut(out_s, layer) + extra, 0), n_dev),
                           gather_group(jnp.concatenate(cut(kv2_s, layer) + cut(q2_s, layer) + cut(out2_s, layer), 0), n_dev),
                           gather_group(jnp.concatenate(cut(ff1_s, layer) + cut(ff2_s, layer), 0), n_dev)])

        me = lax.axis_index(AXIS)
        first = groups[0][0]
        group_rows = first[0].shape[0]
        table = piece_table(me, group_rows)
        vecs = jnp.zeros((n_dev, vec_rows, width), BF16)
        for array, start, device in table:
            block = first[array][start + group_rows - vec_rows:start + group_rows]
            vecs = lax.dynamic_update_slice(vecs, block[None], (device, 0, 0))
        vecs = vecs.reshape(n_dev, -1)[:, :blocks * vec_len].reshape(n_dev, blocks, vec_len)
        vecs = jnp.swapaxes(vecs, 0, 1).reshape(blocks, n_dev * vec_len).astype(F32)
        rows_all = jnp.pad(vecs[:, :9 * width].reshape(blocks, 9, width), ((0, 0), (0, 7), (0, 0)))
        bias_all = vecs[:, None, 9 * width:17 * width]

        padded = (valid + 15) // 16 * 16
        ctx = jnp.pad(context, ((0, 0), (0, padded - valid), (0, 0))).reshape(batch * padded, ctx_width)

        h = tokens_x.reshape(count, width)
        saved = []
        for layer in range(blocks):
            rows, bias = rows_all[layer], bias_all[layer]
            group = groups[layer]
            norm1, qkv, mix1, h1 = self_forward(h, rows, group[0], tokens)
            norm2, query, kv, mix2, h2 = cross_forward(h1, rows, ctx, group[1], tokens, valid)
            last = layer == blocks - 1
            norm3, gated, save_a, save_g, h3 = ff_forward(h2, rows, bias, group[2], BF16 if last else F32)
            saved.append((h, norm1, qkv, mix1, h1, norm2, query, kv, mix2, h2, norm3, gated, save_a, save_g))
            h = h3
        out_tokens = h

        grad = cot_out.reshape(count, width)
        results, vec_grads = [None] * blocks, [None] * blocks
        scatter = lambda full: scatter_sum(full, n_dev)
        for layer in reversed(range(blocks)):
            rows, group = rows_all[layer], groups[layer]
            h0, norm1, qkv, mix1, h1, norm2, query, kv, mix2, h2, norm3, gated, save_a, save_g = saved[layer]
            grad_bf, d_hidden, grad, vec3, vec_b1 = ff_backward(grad, save_a, save_g, h2, rows, group[2])
            g_ff2 = scatter(weight_grad(gated, grad_bf))
            g_ff1 = scatter(weight_grad(norm3, d_hidden))
            grad_bf, d_query, d_kv, grad, vec2 = cross_backward(grad, query, kv, h1, rows, group[1], tokens, valid)
            g_out2 = scatter(weight_grad(mix2, grad_bf))
            g_q2 = scatter(weight_grad(norm2, d_query))
            g_kv2 = scatter(weight_grad(ctx, d_kv))
            grad_bf, d_qkv, grad, vec1 = self_backward(grad, qkv, h0, rows, group[0], tokens, BF16 if layer == 0 else F32)
            g_out = scatter(weight_grad(mix1, grad_bf))
            g_qkv = scatter(weight_grad(norm1, d_qkv))
            results[layer] = [g_qkv, g_out, g_q2, g_kv2, g_out2, g_ff1, g_ff2]
            vec_grads[layer] = jnp.concatenate([vec1[0], vec1[1], vec2[0], vec2[1], vec3[0], vec3[1],
                                                vec1[2], vec2[2], vec3[2], vec_b1[0]])
        vec_full = jnp.stack([jnp.pad(g, (0, vec_len * n_dev - g.shape[0])).reshape(n_dev, vec_len) for g in vec_grads], 1)
        vec_out = scatter(vec_full)
        outs = []
        for index in range(7):
            stacked = jnp.stack([results[layer][index] for layer in range(blocks)]) / total
            stacked = lax.optimization_barrier(stacked)
            outs.append(stacked.reshape(blocks, -1))
        outs.append(vec_out / total)
        return tuple([out_tokens.reshape(tokens_x.shape), grad.reshape(tokens_x.shape)] + outs)

    param_spec = P(None, AXIS)
    in_specs = (P(AXIS), P(AXIS), P(AXIS)) + (param_spec,) * 8
    out_specs = (P(AXIS), P(AXIS)) + (param_spec,) * 8
    return jax.shard_map(local, mesh=mesh, in_specs=in_specs, out_specs=out_specs, check_vma=False)
```

```python
import functools
import math
import jax
import jax.numpy as jnp
from jax import lax
from jax.experimental import pallas as pl
from jax.experimental.pallas import tpu as pltpu
from jax.sharding import PartitionSpec as P


HEAD = 64
AXIS = 'fsdp'
CHUNK = 512
STEP = 512
VMEM_LIMIT = 60 * 1024 * 1024
FORWARD_UNROLL = 10
BACKWARD_UNROLL = 5

F32 = jnp.float32
BF16 = jnp.bfloat16


def gather_perms(n_dev):
    near = [(i, i ^ (4 if i % 2 == 0 else 2)) for i in range(n_dev)]
    far = [(i, i ^ (2 if i % 2 == 0 else 4)) for i in range(n_dev)]
    core = [(i, i ^ 1) for i in range(n_dev)]
    return near, far, core


def pack_kernel(*refs):
    ins, out = refs[:-1], refs[-1]
    width, row = out.shape[1], 0
    for ref in ins:
        depth = ref.shape[-2]
        for col in range(0, ref.shape[-1], width):
            piece = ref[0, :, col:col + width] if len(ref.shape) == 3 else ref[:, col:col + width]
            out[row:row + depth, :] = piece
            row += depth


def pack(views, layer, extra, width):
    rows = sum(v.shape[1] * v.shape[2] // width for v in views) + sum(e.shape[0] for e in extra)
    specs = [pl.BlockSpec((1,) + v.shape[1:], lambda i: (layer, 0, 0)) for v in views]
    specs += [pl.BlockSpec(e.shape, lambda i: (0, 0)) for e in extra]
    return pl.pallas_call(
        pack_kernel, grid=(1,), in_specs=specs, out_specs=pl.BlockSpec((rows, width), lambda i: (0, 0)),
        out_shape=jax.ShapeDtypeStruct((rows, width), BF16),
        cost_estimate=pl.CostEstimate(flops=rows * width, bytes_accessed=rows * width * 4, transcendentals=0),
        name='pack')(*views, *extra)


def permute(array, perm):
    return lax.ppermute(array, AXIS, perm)


def gather_group(shard, n_dev):
    near, far, core = gather_perms(n_dev)
    first = permute(shard, near)
    mine = permute(shard, core)
    second = permute(jnp.concatenate([shard, first], 0), far)
    other_first = permute(first, core)
    other_second = permute(second, core)
    return [shard, first, second, mine, other_first, other_second]


def piece_table(me, rows):
    core = lax.rem(me, 2)
    one, two = 4 - 2 * core, 2 + 2 * core
    mate = jnp.bitwise_xor(me, 1)
    x = jnp.bitwise_xor
    return [(0, 0, me), (1, 0, x(me, one)), (2, 0, x(me, two)), (2, rows, x(me, 6)),
            (3, 0, mate), (4, 0, x(mate, two)), (5, 0, x(mate, one)), (5, rows, x(mate, 6))]


def start_loads(pieces, group_rows, width, targets, sems):
    me = lax.axis_index(AXIS)
    table = piece_table(me, group_rows)
    for which, (ref, offset) in enumerate(targets):
        depth = ref.shape[0] // 8
        for block in range(ref.shape[1] // width):
            for array, start, device in table:
                src = pieces[array].at[pl.ds(start + offset + block * depth, depth), :]
                dst = ref.at[pl.ds(pl.multiple_of(device * depth, 16), depth), pl.ds(block * width, width)]
                pltpu.make_async_copy(src, dst, sems.at[which]).start()


def wait_load(ref, sem):
    pltpu.make_async_copy(ref, ref, sem).wait()


def dot_nn(a, b):
    return lax.dot_general(a, b, (((1,), (0,)), ((), ())), preferred_element_type=F32)


def dot_nt(a, b):
    return lax.dot_general(a, b, (((1,), (1,)), ((), ())), preferred_element_type=F32)


def norm_stats(x):
    average = jnp.mean(x, axis=-1, keepdims=True)
    centered = x - average
    variance = jnp.mean(centered * centered, axis=-1, keepdims=True)
    scale = lax.rsqrt(variance + 1e-5)
    return centered * scale, scale


def norm_back(x, gain, d_norm):
    unit, scale = norm_stats(x)
    d_unit = d_norm * gain
    inner = d_unit - jnp.mean(d_unit, axis=-1, keepdims=True) - unit * jnp.mean(d_unit * unit, axis=-1, keepdims=True)
    return scale * inner, jnp.sum(d_norm * unit, axis=0, keepdims=True), jnp.sum(d_norm, axis=0, keepdims=True)


def softmax_rows(scores):
    top = jnp.max(scores, axis=-1, keepdims=True)
    raised = jnp.exp(scores - top)
    return raised * (1.0 / jnp.sum(raised, axis=-1, keepdims=True))


def low_lanes(rows):
    return lax.broadcasted_iota(jnp.int32, (rows, 2 * HEAD), 1) < HEAD


def pair_scores(query, key, low, head, valid):
    q_head = jnp.where(low if head == 0 else jnp.logical_not(low), query, jnp.zeros_like(query))
    scores = dot_nt(q_head, key) * HEAD ** -0.5
    if valid is not None:
        column = lax.broadcasted_iota(jnp.int32, scores.shape, 1)
        scores = jnp.where(column < valid, scores, -1e30)
    return q_head, softmax_rows(scores)


def pair_forward(query, key, value, valid=None):
    low = low_lanes(query.shape[0])
    mixed = []
    for head in range(2):
        _, probs = pair_scores(query, key, low, head, valid)
        mixed.append(dot_nn(probs.astype(BF16), value))
    return jnp.where(low, mixed[0], mixed[1]).astype(BF16)


def pair_probs(key, query, low, head, valid):
    q_head = jnp.where(low if head == 0 else jnp.logical_not(low), query, jnp.zeros_like(query))
    scores = dot_nt(key, q_head) * HEAD ** -0.5
    if valid is not None:
        row = lax.broadcasted_iota(jnp.int32, scores.shape, 0)
        scores = jnp.where(row < valid, scores, -1e30)
    top = jnp.max(scores, axis=0, keepdims=True)
    raised = jnp.exp(scores - top)
    return q_head, raised * (1.0 / jnp.sum(raised, axis=0, keepdims=True))


def pair_backward(query, key, value, d_out, valid=None):
    low = low_lanes(query.shape[0])
    turned = key.T
    d_query, d_key, d_value = [], None, None
    for head in range(2):
        q_head, probs = pair_probs(key, query, low, head, valid)
        d_head = jnp.where(low if head == 0 else jnp.logical_not(low), d_out, jnp.zeros_like(d_out))
        d_probs = dot_nt(value, d_head).astype(BF16).astype(F32)
        inner = jnp.sum(d_probs * probs, axis=0, keepdims=True)
        d_scores = ((probs * (d_probs - inner)) * HEAD ** -0.5).astype(BF16)
        d_query.append(dot_nn(turned[head * HEAD:(head + 1) * HEAD, :], d_scores))
        dk, dv = dot_nn(d_scores, q_head), dot_nn(probs.astype(BF16), d_head)
        d_key = dk if d_key is None else d_key + dk
        d_value = dv if d_value is None else d_value + dv
    return jnp.concatenate(d_query, 0).T.astype(BF16), d_key.astype(BF16), d_value.astype(BF16)


def add_rows(ref, step, rows):
    @pl.when(step == 0)
    def _():
        ref[...] = jnp.zeros_like(ref)

    for index, row in enumerate(rows):
        ref[pl.ds(index, 1), :] += row


def self_forward_kernel(samples, tokens, h_ref, rows_ref, *refs):
    pieces, (norm_ref, qkv_ref, mix_ref, out_ref, w_qkv, w_out, sems) = refs[:6], refs[6:]
    width = h_ref.shape[1]
    step = pl.program_id(0)

    @pl.when(step == 0)
    def _():
        depth = width // 8
        start_loads(pieces, pieces[0].shape[0], width, [(w_qkv, 0), (w_out, 3 * depth)], sems)

    x = h_ref[...].astype(F32)
    unit, _ = norm_stats(x)
    normed = (unit * rows_ref[0:1, :] + rows_ref[1:2, :]).astype(BF16)
    norm_ref[...] = normed

    @pl.when(step == 0)
    def _():
        wait_load(w_qkv, sems.at[0])
        wait_load(w_out, sems.at[1])

    qkv_ref[...] = dot_nn(normed, w_qkv[...]).astype(BF16)
    pairs = width // (2 * HEAD)

    def body(index, carry):
        row = pl.multiple_of((index // pairs) * tokens, tokens)
        col = pl.multiple_of((index % pairs) * 2 * HEAD, 2 * HEAD)
        part = lambda which: qkv_ref[pl.ds(row, tokens), pl.ds(which * width + col, 2 * HEAD)]
        mix_ref[pl.ds(row, tokens), pl.ds(col, 2 * HEAD)] = pair_forward(part(0), part(1), part(2))
        return carry

    lax.fori_loop(0, samples * pairs, body, 0, unroll=FORWARD_UNROLL)
    out_ref[...] = x + dot_nn(mix_ref[...], w_out[...]) + rows_ref[6:7, :]


def cross_forward_kernel(samples, tokens, valid, h_ref, rows_ref, ctx_ref, *refs):
    pieces, (norm_ref, query_ref, kv_ref, mix_ref, out_ref, w_kv, w_query, w_out, sems) = refs[:6], refs[6:]
    width = h_ref.shape[1]
    step = pl.program_id(0)
    padded = ctx_ref.shape[0] // (samples * pl.num_programs(0))

    @pl.when(step == 0)
    def _():
        deep, depth = w_kv.shape[0] // 8, width // 8
        start_loads(pieces, pieces[0].shape[0], width,
                    [(w_kv, 0), (w_query, 2 * deep), (w_out, 2 * deep + depth)], sems)

    x = h_ref[...]
    unit, _ = norm_stats(x)
    normed = (unit * rows_ref[2:3, :] + rows_ref[3:4, :]).astype(BF16)
    norm_ref[...] = normed

    @pl.when(step == 0)
    def _():
        wait_load(w_kv, sems.at[0])
        wait_load(w_query, sems.at[1])
        wait_load(w_out, sems.at[2])
        kv_ref[...] = dot_nn(ctx_ref[...], w_kv[...]).astype(BF16)

    query_ref[...] = dot_nn(normed, w_query[...]).astype(BF16)
    pairs = width // (2 * HEAD)

    def body(index, carry):
        sample = index // pairs
        row = pl.multiple_of(sample * tokens, tokens)
        kv_row = pl.multiple_of((step * samples + sample) * padded, 16)
        col = pl.multiple_of((index % pairs) * 2 * HEAD, 2 * HEAD)
        query = query_ref[pl.ds(row, tokens), pl.ds(col, 2 * HEAD)]
        key = kv_ref[pl.ds(kv_row, padded), pl.ds(col, 2 * HEAD)]
        value = kv_ref[pl.ds(kv_row, padded), pl.ds(width + col, 2 * HEAD)]
        mix_ref[pl.ds(row, tokens), pl.ds(col, 2 * HEAD)] = pair_forward(query, key, value, valid)
        return carry

    lax.fori_loop(0, samples * pairs, body, 0, unroll=FORWARD_UNROLL)
    out_ref[...] = x + dot_nn(mix_ref[...], w_out[...]) + rows_ref[7:8, :]


def ff_loads(pieces, w_ff1, w_ff2, sems):
    width = w_ff1.shape[0]
    start_loads(pieces, pieces[0].shape[0], width, [(w_ff1, 0), (w_ff2, w_ff1.shape[1] // width * (width // 8))], sems)


def ff_forward_kernel(h_ref, rows_ref, bias_ref, *refs):
    pieces, (norm_ref, gated_ref, save_a, save_g, out_ref, w_ff1, w_ff2, sems) = refs[:6], refs[6:]
    half = w_ff2.shape[0]
    step = pl.program_id(0)

    @pl.when(step == 0)
    def _():
        ff_loads(pieces, w_ff1, w_ff2, sems)

    x = h_ref[...]
    unit, _ = norm_stats(x)
    normed = (unit * rows_ref[4:5, :] + rows_ref[5:6, :]).astype(BF16)
    norm_ref[...] = normed

    @pl.when(step == 0)
    def _():
        wait_load(w_ff1, sems.at[0])
        wait_load(w_ff2, sems.at[1])

    total = x + rows_ref[8:9, :]
    for start in range(0, half, CHUNK):
        u_a = dot_nn(normed, w_ff1[:, start:start + CHUNK]) + bias_ref[:, start:start + CHUNK]
        u_g = dot_nn(normed, w_ff1[:, half + start:half + start + CHUNK]) + bias_ref[:, half + start:half + start + CHUNK]
        cumulative = 0.5 * (1.0 + lax.erf(u_g * math.sqrt(0.5)))
        gate = u_g * cumulative
        slope = cumulative + u_g * (jnp.exp(-0.5 * u_g * u_g) * (1.0 / math.sqrt(2.0 * math.pi)))
        gated = (u_a * gate).astype(BF16)
        gated_ref[:, start:start + CHUNK] = gated
        save_a[:, start:start + CHUNK] = gate
        save_g[:, start:start + CHUNK] = u_a * slope
        total = total + dot_nn(gated, w_ff2[start:start + CHUNK, :])
    out_ref[...] = total.astype(out_ref.dtype)


def ff_backward_kernel(grad_ref, save_a, save_g, h_ref, rows_ref, *refs):
    pieces, (d_hidden_ref, out_ref, vec_ref, bias_ref, w_ff1, w_ff2, sems) = refs[:6], refs[6:]
    half = w_ff2.shape[0]
    step = pl.program_id(0)

    @pl.when(step == 0)
    def _():
        ff_loads(pieces, w_ff1, w_ff2, sems)
        bias_ref[...] = jnp.zeros_like(bias_ref)

    grad = grad_ref[...].astype(F32)
    grad_bf = grad.astype(BF16)

    @pl.when(step == 0)
    def _():
        wait_load(w_ff1, sems.at[0])
        wait_load(w_ff2, sems.at[1])

    d_norm = jnp.zeros(grad.shape, F32)
    for start in range(0, half, CHUNK):
        d_gated = dot_nt(grad_bf, w_ff2[start:start + CHUNK, :]).astype(BF16).astype(F32)
        for base, saved in ((0, save_a), (half, save_g)):
            d_part = d_gated * saved[:, start:start + CHUNK]
            columns = slice(base + start, base + start + CHUNK)
            bias_ref[0:1, columns] += jnp.sum(d_part, axis=0, keepdims=True)
            d_part = d_part.astype(BF16)
            d_hidden_ref[:, columns] = d_part
            d_norm = d_norm + dot_nt(d_part, w_ff1[:, columns])
    d_res, g_gain, g_shift = norm_back(h_ref[...], rows_ref[4:5, :], d_norm)
    out_ref[...] = grad + d_res
    add_rows(vec_ref, step, [g_gain, g_shift, jnp.sum(grad, axis=0, keepdims=True)])


def cross_backward_kernel(samples, tokens, valid, grad_ref, query_ref, kv_ref, h_ref, rows_ref, *refs):
    pieces, (grad_bf_ref, d_query_ref, d_kv_ref, out_ref, vec_ref, d_mix, w_query, w_out, sems) = refs[:6], refs[6:]
    width = h_ref.shape[1]
    step = pl.program_id(0)
    padded = kv_ref.shape[0] // samples

    @pl.when(step == 0)
    def _():
        depth = width // 8
        base = pieces[0].shape[0] - 2 * depth
        start_loads(pieces, pieces[0].shape[0], width, [(w_query, base), (w_out, base + depth)], sems)

    grad = grad_ref[...]
    grad_bf = grad.astype(BF16)
    grad_bf_ref[...] = grad_bf

    @pl.when(step == 0)
    def _():
        wait_load(w_query, sems.at[0])
        wait_load(w_out, sems.at[1])

    d_mix[...] = dot_nt(grad_bf, w_out[...]).astype(BF16)
    pairs = width // (2 * HEAD)

    def body(index, carry):
        sample = index // pairs
        row = pl.multiple_of(sample * tokens, tokens)
        kv_row = pl.multiple_of(sample * padded, 16)
        col = pl.multiple_of((index % pairs) * 2 * HEAD, 2 * HEAD)
        at = (pl.ds(row, tokens), pl.ds(col, 2 * HEAD))
        at_key = (pl.ds(kv_row, padded), pl.ds(col, 2 * HEAD))
        at_value = (pl.ds(kv_row, padded), pl.ds(width + col, 2 * HEAD))
        dq, dk, dv = pair_backward(query_ref[at], kv_ref[at_key], kv_ref[at_value], d_mix[at], valid)
        d_query_ref[at] = dq
        d_kv_ref[at_key] = dk
        d_kv_ref[at_value] = dv
        return carry

    lax.fori_loop(0, samples * pairs, body, 0, unroll=BACKWARD_UNROLL)
    d_norm = dot_nt(d_query_ref[...], w_query[...])
    d_res, g_gain, g_shift = norm_back(h_ref[...], rows_ref[2:3, :], d_norm)
    out_ref[...] = grad + d_res
    add_rows(vec_ref, step, [g_gain, g_shift, jnp.sum(grad, axis=0, keepdims=True)])


def self_backward_kernel(samples, tokens, grad_ref, qkv_ref, h_ref, rows_ref, *refs):
    pieces, (grad_bf_ref, d_qkv_ref, out_ref, vec_ref, d_mix, w_qkv, w_out, sems) = refs[:6], refs[6:]
    width = h_ref.shape[1]
    step = pl.program_id(0)

    @pl.when(step == 0)
    def _():
        depth = width // 8
        start_loads(pieces, pieces[0].shape[0], width, [(w_qkv, 0), (w_out, 3 * depth)], sems)

    grad = grad_ref[...]
    grad_bf = grad.astype(BF16)
    grad_bf_ref[...] = grad_bf

    @pl.when(step == 0)
    def _():
        wait_load(w_qkv, sems.at[0])
        wait_load(w_out, sems.at[1])

    d_mix[...] = dot_nt(grad_bf, w_out[...]).astype(BF16)
    pairs = width // (2 * HEAD)

    def body(index, carry):
        row = pl.multiple_of((index // pairs) * tokens, tokens)
        col = pl.multiple_of((index % pairs) * 2 * HEAD, 2 * HEAD)
        at = lambda which: (pl.ds(row, tokens), pl.ds(which * width + col, 2 * HEAD))
        d_parts = pair_backward(qkv_ref[at(0)], qkv_ref[at(1)], qkv_ref[at(2)], d_mix[at(0)])
        for which in range(3):
            d_qkv_ref[at(which)] = d_parts[which]
        return carry

    lax.fori_loop(0, samples * pairs, body, 0, unroll=BACKWARD_UNROLL)
    d_norm = dot_nt(d_qkv_ref[...], w_qkv[...])
    d_res, g_gain, g_shift = norm_back(h_ref[...].astype(F32), rows_ref[0:1, :], d_norm)
    out_ref[...] = (grad + d_res).astype(out_ref.dtype)
    add_rows(vec_ref, step, [g_gain, g_shift, jnp.sum(grad, axis=0, keepdims=True)])


ANY = pl.BlockSpec(memory_space=pl.ANY)


def by_step(rows, columns):
    return pl.BlockSpec((rows, columns), lambda i: (i, 0))


def whole(rows, columns):
    return pl.BlockSpec((rows, columns), lambda i: (0, 0))


def shape(rows, columns, dtype):
    return jax.ShapeDtypeStruct((rows, columns), dtype)


def call(kernel, steps, in_specs, out_specs, out_shapes, scratch, flops, moved):
    return pl.pallas_call(
        kernel, grid=(steps,), in_specs=in_specs, out_specs=out_specs, out_shape=out_shapes, scratch_shapes=scratch,
        cost_estimate=pl.CostEstimate(flops=int(flops), bytes_accessed=int(moved), transcendentals=0),
        compiler_params=pltpu.CompilerParams(dimension_semantics=('arbitrary',), vmem_limit_bytes=VMEM_LIMIT))


def self_forward(h, rows, pieces, tokens):
    count, width = h.shape
    return call(
        functools.partial(self_forward_kernel, STEP // tokens, tokens), count // STEP,
        [by_step(STEP, width), whole(*rows.shape)] + [ANY] * 6,
        [by_step(STEP, width), by_step(STEP, 3 * width), by_step(STEP, width), by_step(STEP, width)],
        [shape(count, width, BF16), shape(count, 3 * width, BF16), shape(count, width, BF16), shape(count, width, F32)],
        [pltpu.VMEM((width, 3 * width), BF16), pltpu.VMEM((width, width), BF16), pltpu.SemaphoreType.DMA((2,))],
        count * width * width * 8 + count * tokens * width * 4, 2e7)(h, rows, *pieces)


def cross_forward(h, rows, ctx, pieces, tokens, valid):
    count, width = h.shape
    ctx_rows, ctx_width = ctx.shape
    return call(
        functools.partial(cross_forward_kernel, STEP // tokens, tokens, valid), count // STEP,
        [by_step(STEP, width), whole(*rows.shape), whole(ctx_rows, ctx_width)] + [ANY] * 6,
        [by_step(STEP, width), by_step(STEP, width), whole(ctx_rows, 2 * width), by_step(STEP, width), by_step(STEP, width)],
        [shape(count, width, BF16), shape(count, width, BF16), shape(ctx_rows, 2 * width, BF16), shape(count, width, BF16),
         shape(count, width, F32)],
        [pltpu.VMEM((ctx_width, 2 * width), BF16), pltpu.VMEM((width, width), BF16), pltpu.VMEM((width, width), BF16),
         pltpu.SemaphoreType.DMA((3,))],
        count * width * width * 4 + ctx_rows * ctx_width * width * 4 + count * 128 * width * 4, 2e7)(h, rows, ctx, *pieces)


def ff_forward(h, rows, bias, pieces, out_dtype):
    count, width = h.shape
    half = bias.shape[1] // 2
    return call(
        ff_forward_kernel, count // STEP,
        [by_step(STEP, width), whole(*rows.shape), whole(1, 2 * half)] + [ANY] * 6,
        [by_step(STEP, width), by_step(STEP, half), by_step(STEP, half), by_step(STEP, half), by_step(STEP, width)],
        [shape(count, width, BF16), shape(count, half, BF16), shape(count, half, F32), shape(count, half, F32),
         shape(count, width, out_dtype)],
        [pltpu.VMEM((width, 2 * half), BF16), pltpu.VMEM((half, width), BF16), pltpu.SemaphoreType.DMA((2,))],
        count * width * half * 6, 6e7)(h, rows, bias, *pieces)


def ff_backward(grad, save_a, save_g, h, rows, pieces):
    count, width = h.shape
    half = save_a.shape[1]
    return call(
        ff_backward_kernel, count // STEP,
        [by_step(STEP, width), by_step(STEP, half), by_step(STEP, half), by_step(STEP, width), whole(*rows.shape)] + [ANY] * 6,
        [by_step(STEP, 2 * half), by_step(STEP, width), whole(8, width), whole(8, 2 * half)],
        [shape(count, 2 * half, BF16), shape(count, width, F32), shape(8, width, F32),
         shape(8, 2 * half, F32)],
        [pltpu.VMEM((width, 2 * half), BF16), pltpu.VMEM((half, width), BF16), pltpu.SemaphoreType.DMA((2,))],
        count * width * half * 6, 6e7)(grad, save_a, save_g, h, rows, *pieces)


def cross_backward(grad, query, kv, h, rows, pieces, tokens, valid):
    count, width = h.shape
    ctx_rows = kv.shape[0]
    steps = count // STEP
    return call(
        functools.partial(cross_backward_kernel, STEP // tokens, tokens, valid), steps,
        [by_step(STEP, width), by_step(STEP, width), by_step(ctx_rows // steps, 2 * width), by_step(STEP, width),
         whole(*rows.shape)] + [ANY] * 6,
        [by_step(STEP, width), by_step(STEP, width), by_step(ctx_rows // steps, 2 * width), by_step(STEP, width), whole(8, width)],
        [shape(count, width, BF16), shape(count, width, BF16), shape(ctx_rows, 2 * width, BF16), shape(count, width, F32),
         shape(8, width, F32)],
        [pltpu.VMEM((STEP, width), BF16), pltpu.VMEM((width, width), BF16), pltpu.VMEM((width, width), BF16),
         pltpu.SemaphoreType.DMA((2,))],
        count * width * width * 4 + count * 128 * width * 10, 2e7)(grad, query, kv, h, rows, *pieces)


def self_backward(grad, qkv, h, rows, pieces, tokens, out_dtype):
    count, width = h.shape
    return call(
        functools.partial(self_backward_kernel, STEP // tokens, tokens), count // STEP,
        [by_step(STEP, width), by_step(STEP, 3 * width), by_step(STEP, width), whole(*rows.shape)] + [ANY] * 6,
        [by_step(STEP, width), by_step(STEP, 3 * width), by_step(STEP, width), whole(8, width)],
        [shape(count, width, BF16), shape(count, 3 * width, BF16), shape(count, width, out_dtype), shape(8, width, F32)],
        [pltpu.VMEM((STEP, width), BF16), pltpu.VMEM((width, 3 * width), BF16), pltpu.VMEM((width, width), BF16),
         pltpu.SemaphoreType.DMA((2,))],
        count * width * width * 8 + count * tokens * width * 10, 3e7)(grad, qkv, h, rows, *pieces)


def scatter_sum(full, n_dev):
    near, far, core_perm = gather_perms(n_dev)
    me = lax.axis_index(AXIS)
    core, chip = me % 2, me // 2
    one, two = 1 + core, 2 - core
    by_chip = full.reshape((n_dev // 2, 2) + full.shape[1:])
    pick = lambda array, index: lax.dynamic_index_in_dim(array, index, 0, keepdims=False)
    ours = lambda index: lax.dynamic_slice(by_chip, (index, core) + (0,) * (full.ndim - 1),
                                           (1, 1) + full.shape[1:]).reshape(full.shape[1:])
    got = permute(lax.dynamic_index_in_dim(by_chip, 1 - core, 1, keepdims=False), core_perm)
    part = lambda index: ours(index) + pick(got, index)
    x = jnp.bitwise_xor
    second = permute(jnp.stack([part(x(chip, one)), part(x(x(chip, one), two))]), far)
    third = permute(part(x(chip, two)) + second[1], near)
    return part(chip) + second[0] + third


def weight_grad(inputs, grads):
    grad = lax.dot_general(inputs, grads, (((0,), (0,)), ((), ())), preferred_element_type=F32)
    return grad.reshape(8, grad.shape[0] // 8, grad.shape[1])


def solution(mesh):
    n_dev = mesh.shape[AXIS]

    def inner(tokens_x, context, cot_out, *shards):
        batch, tokens, width = tokens_x.shape
        _, valid, ctx_width = context.shape
        blocks = shards[0].shape[0]
        total = batch * n_dev
        depth = width // n_dev
        count = batch * tokens
        half = 4 * width

        views = []
        for shard, rows in zip(shards[:7], (depth, depth, depth, ctx_width // n_dev, depth, depth, half // n_dev)):
            views.append(shard.reshape(blocks, rows, -1))
        qkv_s, out_s, q2_s, kv2_s, out2_s, ff1_s, ff2_s = lax.optimization_barrier(views)
        me = lax.axis_index(AXIS)
        vec_len = shards[7].shape[1]
        vec_each = 17
        vec_rows = (blocks * vec_each + 15) // 16 * 16
        vec_block = lax.dynamic_update_slice(jnp.zeros((blocks, n_dev * vec_len), BF16), shards[7], (0, me * vec_len))
        vec_block = vec_block[:, :vec_each * width].reshape(blocks * vec_each, width)
        vec_block = jnp.pad(vec_block, ((0, vec_rows - blocks * vec_each), (0, 0)))

        groups = []
        for layer in range(blocks):
            extra = [vec_block] if layer == 0 else []
            for index, members in enumerate(([qkv_s, out_s], [kv2_s, q2_s, out2_s], [ff1_s, ff2_s])):
                block = pack(members, layer, extra if index == 0 else [], width)
                groups.append(gather_group(block, n_dev))

        group_rows = groups[0][0].shape[0]
        vecs = jnp.zeros((vec_rows, width), F32)
        for array, start, _ in piece_table(me, group_rows):
            vecs = vecs + groups[0][array][start + group_rows - vec_rows:start + group_rows].astype(F32)
        vecs = vecs[:blocks * vec_each].reshape(blocks, vec_each, width)
        rows_all = jnp.pad(vecs[:, :9], ((0, 0), (0, 7), (0, 0)))
        bias_all = vecs[:, 9:].reshape(blocks, 1, 8 * width)

        padded = (valid + 15) // 16 * 16
        ctx = jnp.pad(context, ((0, 0), (0, padded - valid), (0, 0))).reshape(batch * padded, ctx_width)

        h = tokens_x.reshape(count, width)
        saved = []
        for layer in range(blocks):
            rows, bias = rows_all[layer], bias_all[layer]
            group = groups[3 * layer:3 * layer + 3]
            norm1, qkv, mix1, h1 = self_forward(h, rows, group[0], tokens)
            norm2, query, kv, mix2, h2 = cross_forward(h1, rows, ctx, group[1], tokens, valid)
            last = layer == blocks - 1
            norm3, gated, save_a, save_g, h3 = ff_forward(h2, rows, bias, group[2], BF16 if last else F32)
            saved.append((h, norm1, qkv, mix1, h1, norm2, query, kv, mix2, h2, norm3, gated, save_a, save_g))
            h = h3
        out_tokens = h

        grad = cot_out.reshape(count, width)
        results, vec_grads = [None] * blocks, [None] * blocks
        for layer in reversed(range(blocks)):
            rows, group = rows_all[layer], groups[3 * layer:3 * layer + 3]
            h0, norm1, qkv, mix1, h1, norm2, query, kv, mix2, h2, norm3, gated, save_a, save_g = saved[layer]
            g_ff2 = scatter_sum(weight_grad(gated, grad.astype(BF16)), n_dev)
            d_hidden, grad, vec3, vec_b1 = ff_backward(grad, save_a, save_g, h2, rows, group[2])
            g_ff1 = scatter_sum(weight_grad(norm3, d_hidden), n_dev)
            grad_bf, d_query, d_kv, grad, vec2 = cross_backward(grad, query, kv, h1, rows, group[1], tokens, valid)
            g_out2 = scatter_sum(weight_grad(mix2, grad_bf), n_dev)
            g_q2 = scatter_sum(weight_grad(norm2, d_query), n_dev)
            g_kv2 = scatter_sum(weight_grad(ctx, d_kv), n_dev)
            grad_bf, d_qkv, grad, vec1 = self_backward(grad, qkv, h0, rows, group[0], tokens, BF16 if layer == 0 else F32)
            g_out = scatter_sum(weight_grad(mix1, grad_bf), n_dev)
            g_qkv = scatter_sum(weight_grad(norm1, d_qkv), n_dev)
            results[layer] = [g_qkv, g_out, g_q2, g_kv2, g_out2, g_ff1, g_ff2]
            vec_grads[layer] = jnp.concatenate([vec1[0], vec1[1], vec2[0], vec2[1], vec3[0], vec3[1],
                                                vec1[2], vec2[2], vec3[2], vec_b1[0]])
        vec_full = jnp.stack([jnp.pad(g, (0, vec_len * n_dev - g.shape[0])).reshape(n_dev, vec_len) for g in vec_grads], 1)
        vec_out = scatter_sum(vec_full, n_dev)
        outs = []
        for index in range(7):
            stacked = jnp.stack([results[layer][index] for layer in range(blocks)]) / total
            stacked = lax.optimization_barrier(stacked)
            outs.append(stacked.reshape(blocks, -1))
        outs.append(vec_out / total)
        return tuple([out_tokens.reshape(tokens_x.shape), grad.reshape(tokens_x.shape)] + outs)

    param_spec = P(None, AXIS)
    in_specs = (P(AXIS), P(AXIS), P(AXIS)) + (param_spec,) * 8
    out_specs = (P(AXIS), P(AXIS)) + (param_spec,) * 8
    return jax.shard_map(inner, mesh=mesh, in_specs=in_specs, out_specs=out_specs, check_vma=False)
```

```python
import functools
import math
import jax
import jax.numpy as jnp
from jax import lax
from jax.experimental import pallas as pl
from jax.experimental.pallas import tpu as pltpu
from jax.sharding import PartitionSpec as P


HEAD = 64
AXIS = 'fsdp'
CHUNK = 1280
FF_STEP = 256
STEP = 512
VMEM_LIMIT = 60 * 1024 * 1024
FORWARD_UNROLL = 10
BACKWARD_UNROLL = 5

F32 = jnp.float32
BF16 = jnp.bfloat16


def gather_perms(n_dev):
    near = [(i, i ^ (4 if i % 2 == 0 else 2)) for i in range(n_dev)]
    far = [(i, i ^ (2 if i % 2 == 0 else 4)) for i in range(n_dev)]
    core = [(i, i ^ 1) for i in range(n_dev)]
    return near, far, core


def pack_kernel(*refs):
    ins, out = refs[:-1], refs[-1]
    width, row = out.shape[1], 0
    for ref in ins:
        depth = ref.shape[-2]
        for col in range(0, ref.shape[-1], width):
            piece = ref[0, :, col:col + width] if len(ref.shape) == 3 else ref[:, col:col + width]
            out[row:row + depth, :] = piece
            row += depth


def pack(views, layer, extra, width):
    rows = sum(v.shape[1] * v.shape[2] // width for v in views) + sum(e.shape[0] for e in extra)
    specs = [pl.BlockSpec((1,) + v.shape[1:], lambda i: (layer, 0, 0)) for v in views]
    specs += [pl.BlockSpec(e.shape, lambda i: (0, 0)) for e in extra]
    return pl.pallas_call(
        pack_kernel, grid=(1,), in_specs=specs, out_specs=pl.BlockSpec((rows, width), lambda i: (0, 0)),
        out_shape=jax.ShapeDtypeStruct((rows, width), BF16),
        cost_estimate=pl.CostEstimate(flops=rows * width, bytes_accessed=rows * width * 4, transcendentals=0),
        name='pack')(*views, *extra)


def permute(array, perm):
    return lax.ppermute(array, AXIS, perm)


def gather_group(shard, n_dev):
    near, far, core = gather_perms(n_dev)
    first = permute(shard, near)
    second = permute(shard, far)
    third = permute(first, far)
    mine = [shard, first, second, third]
    return mine + [permute(piece, core) for piece in mine]


def piece_devices(me):
    core = lax.rem(me, 2)
    one, two = 4 - 2 * core, 2 + 2 * core
    x = jnp.bitwise_xor
    mate = x(me, 1)
    return [me, x(me, one), x(me, two), x(me, 6), mate, x(mate, two), x(mate, one), x(mate, 6)]


def start_load(pieces, offset, ref, sem):
    width = pieces[0].shape[1]
    depth = ref.shape[0] // 8
    devices = piece_devices(lax.axis_index(AXIS))
    for block in range(ref.shape[1] // width):
        for piece, device in zip(pieces, devices):
            src = piece.at[pl.ds(offset + block * depth, depth), :]
            dst = ref.at[pl.ds(pl.multiple_of(device * depth, 16), depth), pl.ds(block * width, width)]
            pltpu.make_async_copy(src, dst, sem).start()


def wait_load(ref, sem):
    pltpu.make_async_copy(ref, ref, sem).wait()


def dot_nn(a, b):
    return lax.dot_general(a, b, (((1,), (0,)), ((), ())), preferred_element_type=F32)


def dot_nt(a, b):
    return lax.dot_general(a, b, (((1,), (1,)), ((), ())), preferred_element_type=F32)


def norm_stats(x):
    average = jnp.mean(x, axis=-1, keepdims=True)
    centered = x - average
    variance = jnp.mean(centered * centered, axis=-1, keepdims=True)
    scale = lax.rsqrt(variance + 1e-5)
    return centered * scale, scale


def norm_back(x, gain, d_norm):
    unit, scale = norm_stats(x)
    d_unit = d_norm * gain
    inner = d_unit - jnp.mean(d_unit, axis=-1, keepdims=True) - unit * jnp.mean(d_unit * unit, axis=-1, keepdims=True)
    return scale * inner, jnp.sum(d_norm * unit, axis=0, keepdims=True), jnp.sum(d_norm, axis=0, keepdims=True)


def softmax_rows(scores):
    top = jnp.max(scores, axis=-1, keepdims=True)
    raised = jnp.exp(scores - top)
    return raised * (1.0 / jnp.sum(raised, axis=-1, keepdims=True))


def low_lanes(rows):
    return lax.broadcasted_iota(jnp.int32, (rows, 2 * HEAD), 1) < HEAD


def pair_scores(query, key, low, head, valid):
    q_head = jnp.where(low if head == 0 else jnp.logical_not(low), query, jnp.zeros_like(query))
    scores = dot_nt(q_head, key) * HEAD ** -0.5
    if valid is not None:
        column = lax.broadcasted_iota(jnp.int32, scores.shape, 1)
        scores = jnp.where(column < valid, scores, -1e30)
    return q_head, softmax_rows(scores)


def pair_forward(query, key, value, valid=None):
    low = low_lanes(query.shape[0])
    mixed = []
    for head in range(2):
        _, probs = pair_scores(query, key, low, head, valid)
        mixed.append(dot_nn(probs.astype(BF16), value))
    return jnp.where(low, mixed[0], mixed[1]).astype(BF16)


def pair_probs(key, query, low, head, valid):
    q_head = jnp.where(low if head == 0 else jnp.logical_not(low), query, jnp.zeros_like(query))
    scores = dot_nt(key, q_head) * HEAD ** -0.5
    if valid is not None:
        row = lax.broadcasted_iota(jnp.int32, scores.shape, 0)
        scores = jnp.where(row < valid, scores, -1e30)
    top = jnp.max(scores, axis=0, keepdims=True)
    raised = jnp.exp(scores - top)
    return q_head, raised * (1.0 / jnp.sum(raised, axis=0, keepdims=True))


def pair_backward(query, key, value, d_out, valid=None):
    low = low_lanes(query.shape[0])
    turned = key.T
    d_query, d_key, d_value = [], None, None
    for head in range(2):
        q_head, probs = pair_probs(key, query, low, head, valid)
        d_head = jnp.where(low if head == 0 else jnp.logical_not(low), d_out, jnp.zeros_like(d_out))
        d_probs = dot_nt(value, d_head).astype(BF16).astype(F32)
        inner = jnp.sum(d_probs * probs, axis=0, keepdims=True)
        d_scores = ((probs * (d_probs - inner)) * HEAD ** -0.5).astype(BF16)
        d_query.append(dot_nn(turned[head * HEAD:(head + 1) * HEAD, :], d_scores))
        dk, dv = dot_nn(d_scores, q_head), dot_nn(probs.astype(BF16), d_head)
        d_key = dk if d_key is None else d_key + dk
        d_value = dv if d_value is None else d_value + dv
    return jnp.concatenate(d_query, 0).T.astype(BF16), d_key.astype(BF16), d_value.astype(BF16)


def add_rows(ref, step, rows):
    @pl.when(step == 0)
    def _():
        ref[...] = jnp.zeros_like(ref)

    for index, row in enumerate(rows):
        ref[pl.ds(index, 1), :] += row


def self_forward_kernel(samples, tokens, h_ref, rows_ref, *refs):
    pieces, (norm_ref, qkv_ref, mix_ref, out_ref, w_qkv, w_out, sems) = refs[:8], refs[8:]
    width = h_ref.shape[1]
    step = pl.program_id(0)

    @pl.when(step == 0)
    def _():
        start_load(pieces, 0, w_qkv, sems.at[0])
        start_load(pieces, 3 * (width // 8), w_out, sems.at[1])

    x = h_ref[...].astype(F32)
    unit, _ = norm_stats(x)
    normed = (unit * rows_ref[0:1, :] + rows_ref[1:2, :]).astype(BF16)
    norm_ref[...] = normed

    @pl.when(step == 0)
    def _():
        wait_load(w_qkv, sems.at[0])
        wait_load(w_out, sems.at[1])

    qkv_ref[...] = dot_nn(normed, w_qkv[...]).astype(BF16)
    pairs = width // (2 * HEAD)

    def body(index, carry):
        row = pl.multiple_of((index // pairs) * tokens, tokens)
        col = pl.multiple_of((index % pairs) * 2 * HEAD, 2 * HEAD)
        part = lambda which: qkv_ref[pl.ds(row, tokens), pl.ds(which * width + col, 2 * HEAD)]
        mix_ref[pl.ds(row, tokens), pl.ds(col, 2 * HEAD)] = pair_forward(part(0), part(1), part(2))
        return carry

    lax.fori_loop(0, samples * pairs, body, 0, unroll=FORWARD_UNROLL)
    out_ref[...] = x + dot_nn(mix_ref[...], w_out[...]) + rows_ref[6:7, :]


def cross_forward_kernel(samples, tokens, valid, h_ref, rows_ref, ctx_ref, *refs):
    pieces, (norm_ref, query_ref, kv_ref, mix_ref, out_ref, w_kv, w_query, w_out, sems) = refs[:8], refs[8:]
    width = h_ref.shape[1]
    step = pl.program_id(0)
    padded = ctx_ref.shape[0] // (samples * pl.num_programs(0))

    @pl.when(step == 0)
    def _():
        deep, depth = w_kv.shape[0] // 8, width // 8
        start_load(pieces, 0, w_kv, sems.at[0])
        start_load(pieces, 2 * deep, w_query, sems.at[1])
        start_load(pieces, 2 * deep + depth, w_out, sems.at[2])

    x = h_ref[...]
    unit, _ = norm_stats(x)
    normed = (unit * rows_ref[2:3, :] + rows_ref[3:4, :]).astype(BF16)
    norm_ref[...] = normed

    @pl.when(step == 0)
    def _():
        wait_load(w_kv, sems.at[0])
        wait_load(w_query, sems.at[1])
        wait_load(w_out, sems.at[2])
        kv_ref[...] = dot_nn(ctx_ref[...], w_kv[...]).astype(BF16)

    query_ref[...] = dot_nn(normed, w_query[...]).astype(BF16)
    pairs = width // (2 * HEAD)

    def body(index, carry):
        sample = index // pairs
        row = pl.multiple_of(sample * tokens, tokens)
        kv_row = pl.multiple_of((step * samples + sample) * padded, 16)
        col = pl.multiple_of((index % pairs) * 2 * HEAD, 2 * HEAD)
        query = query_ref[pl.ds(row, tokens), pl.ds(col, 2 * HEAD)]
        key = kv_ref[pl.ds(kv_row, padded), pl.ds(col, 2 * HEAD)]
        value = kv_ref[pl.ds(kv_row, padded), pl.ds(width + col, 2 * HEAD)]
        mix_ref[pl.ds(row, tokens), pl.ds(col, 2 * HEAD)] = pair_forward(query, key, value, valid)
        return carry

    lax.fori_loop(0, samples * pairs, body, 0, unroll=FORWARD_UNROLL)
    out_ref[...] = x + dot_nn(mix_ref[...], w_out[...]) + rows_ref[7:8, :]


def ff_loads(pieces, offset, w_ff1, w_ff2, sems):
    start_load(pieces[:8], 0, w_ff1, sems.at[0])
    start_load(pieces[8:], offset, w_ff2, sems.at[1])


def ff_up(normed, bias_ref, w_ff1, half, start, gated_ref, save_a, save_g):
    u_a = dot_nn(normed, w_ff1[:, start:start + CHUNK]) + bias_ref[:, start:start + CHUNK]
    u_g = dot_nn(normed, w_ff1[:, half + start:half + start + CHUNK]) + bias_ref[:, half + start:half + start + CHUNK]
    cumulative = 0.5 * (1.0 + lax.erf(u_g * math.sqrt(0.5)))
    gate = u_g * cumulative
    slope = cumulative + u_g * (jnp.exp(-0.5 * u_g * u_g) * (1.0 / math.sqrt(2.0 * math.pi)))
    gated = (u_a * gate).astype(BF16)
    gated_ref[:, start:start + CHUNK] = gated
    save_a[:, start:start + CHUNK] = gate
    save_g[:, start:start + CHUNK] = u_a * slope
    return gated


def ff_forward_kernel(offset, h_ref, rows_ref, bias_ref, *refs):
    pieces, (norm_ref, gated_ref, save_a, save_g, out_ref, w_ff1, w_ff2, sems) = refs[:16], refs[16:]
    half = w_ff2.shape[0]
    step = pl.program_id(0)

    @pl.when(step == 0)
    def _():
        ff_loads(pieces, offset, w_ff1, w_ff2, sems)

    x = h_ref[...]
    unit, _ = norm_stats(x)
    normed = (unit * rows_ref[4:5, :] + rows_ref[5:6, :]).astype(BF16)
    norm_ref[...] = normed

    @pl.when(step == 0)
    def _():
        wait_load(w_ff1, sems.at[0])
        wait_load(w_ff2, sems.at[1])

    total = x + rows_ref[8:9, :]
    for start in range(0, half, CHUNK):
        gated = ff_up(normed, bias_ref, w_ff1, half, start, gated_ref, save_a, save_g)
        total = total + dot_nn(gated, w_ff2[start:start + CHUNK, :])
    out_ref[...] = total


def ff_up_kernel(h_ref, rows_ref, bias_ref, *refs):
    pieces, (norm_ref, gated_ref, save_a, save_g, w_ff1, sems) = refs[:8], refs[8:]
    half = w_ff1.shape[1] // 2
    step = pl.program_id(0)

    @pl.when(step == 0)
    def _():
        start_load(pieces, 0, w_ff1, sems.at[0])

    unit, _ = norm_stats(h_ref[...])
    normed = (unit * rows_ref[4:5, :] + rows_ref[5:6, :]).astype(BF16)
    norm_ref[...] = normed

    @pl.when(step == 0)
    def _():
        wait_load(w_ff1, sems.at[0])

    for start in range(0, half, CHUNK):
        ff_up(normed, bias_ref, w_ff1, half, start, gated_ref, save_a, save_g)


def ff_down_kernel(h_ref, rows_ref, gated_ref, *refs):
    pieces, (out_ref, w_ff2, sems) = refs[:8], refs[8:]
    step = pl.program_id(0)

    @pl.when(step == 0)
    def _():
        start_load(pieces, 0, w_ff2, sems.at[0])
        wait_load(w_ff2, sems.at[0])

    out_ref[...] = (h_ref[...] + rows_ref[8:9, :] + dot_nn(gated_ref[...], w_ff2[...])).astype(BF16)


def ff_backward_kernel(offset, grad_ref, save_a, save_g, h_ref, rows_ref, *refs):
    pieces, (d_hidden_ref, out_ref, vec_ref, bias_ref, w_ff1, w_ff2, sems) = refs[:16], refs[16:]
    half = w_ff2.shape[0]
    step = pl.program_id(0)

    @pl.when(step == 0)
    def _():
        ff_loads(pieces, offset, w_ff1, w_ff2, sems)
        bias_ref[...] = jnp.zeros_like(bias_ref)

    grad = grad_ref[...].astype(F32)
    grad_bf = grad.astype(BF16)

    @pl.when(step == 0)
    def _():
        wait_load(w_ff1, sems.at[0])
        wait_load(w_ff2, sems.at[1])

    d_norm = jnp.zeros(grad.shape, F32)
    for start in range(0, half, CHUNK):
        d_gated = dot_nt(grad_bf, w_ff2[start:start + CHUNK, :]).astype(BF16).astype(F32)
        for base, saved in ((0, save_a), (half, save_g)):
            d_part = d_gated * saved[:, start:start + CHUNK]
            columns = slice(base + start, base + start + CHUNK)
            bias_ref[0:1, columns] += jnp.sum(d_part, axis=0, keepdims=True)
            d_part = d_part.astype(BF16)
            d_hidden_ref[:, columns] = d_part
            d_norm = d_norm + dot_nt(d_part, w_ff1[:, columns])
    d_res, g_gain, g_shift = norm_back(h_ref[...], rows_ref[4:5, :], d_norm)
    out_ref[...] = grad + d_res
    add_rows(vec_ref, step, [g_gain, g_shift, jnp.sum(grad, axis=0, keepdims=True)])


def cross_backward_kernel(samples, tokens, valid, grad_ref, query_ref, kv_ref, h_ref, rows_ref, *refs):
    pieces, (grad_bf_ref, d_query_ref, d_kv_ref, out_ref, vec_ref, d_mix, w_query, w_out, sems) = refs[:8], refs[8:]
    width = h_ref.shape[1]
    step = pl.program_id(0)
    padded = kv_ref.shape[0] // samples

    @pl.when(step == 0)
    def _():
        depth = width // 8
        base = pieces[0].shape[0] - 2 * depth
        start_load(pieces, base, w_query, sems.at[0])
        start_load(pieces, base + depth, w_out, sems.at[1])

    grad = grad_ref[...]
    grad_bf = grad.astype(BF16)
    grad_bf_ref[...] = grad_bf

    @pl.when(step == 0)
    def _():
        wait_load(w_query, sems.at[0])
        wait_load(w_out, sems.at[1])

    d_mix[...] = dot_nt(grad_bf, w_out[...]).astype(BF16)
    pairs = width // (2 * HEAD)

    def body(index, carry):
        sample = index // pairs
        row = pl.multiple_of(sample * tokens, tokens)
        kv_row = pl.multiple_of(sample * padded, 16)
        col = pl.multiple_of((index % pairs) * 2 * HEAD, 2 * HEAD)
        at = (pl.ds(row, tokens), pl.ds(col, 2 * HEAD))
        at_key = (pl.ds(kv_row, padded), pl.ds(col, 2 * HEAD))
        at_value = (pl.ds(kv_row, padded), pl.ds(width + col, 2 * HEAD))
        dq, dk, dv = pair_backward(query_ref[at], kv_ref[at_key], kv_ref[at_value], d_mix[at], valid)
        d_query_ref[at] = dq
        d_kv_ref[at_key] = dk
        d_kv_ref[at_value] = dv
        return carry

    lax.fori_loop(0, samples * pairs, body, 0, unroll=BACKWARD_UNROLL)
    d_norm = dot_nt(d_query_ref[...], w_query[...])
    d_res, g_gain, g_shift = norm_back(h_ref[...], rows_ref[2:3, :], d_norm)
    out_ref[...] = grad + d_res
    add_rows(vec_ref, step, [g_gain, g_shift, jnp.sum(grad, axis=0, keepdims=True)])


def self_backward_kernel(samples, tokens, grad_ref, qkv_ref, h_ref, rows_ref, *refs):
    pieces, (grad_bf_ref, d_qkv_ref, out_ref, vec_ref, d_mix, w_qkv, w_out, sems) = refs[:8], refs[8:]
    width = h_ref.shape[1]
    step = pl.program_id(0)

    @pl.when(step == 0)
    def _():
        start_load(pieces, 0, w_qkv, sems.at[0])
        start_load(pieces, 3 * (width // 8), w_out, sems.at[1])

    grad = grad_ref[...]
    grad_bf = grad.astype(BF16)
    grad_bf_ref[...] = grad_bf

    @pl.when(step == 0)
    def _():
        wait_load(w_qkv, sems.at[0])
        wait_load(w_out, sems.at[1])

    d_mix[...] = dot_nt(grad_bf, w_out[...]).astype(BF16)
    pairs = width // (2 * HEAD)

    def body(index, carry):
        row = pl.multiple_of((index // pairs) * tokens, tokens)
        col = pl.multiple_of((index % pairs) * 2 * HEAD, 2 * HEAD)
        at = lambda which: (pl.ds(row, tokens), pl.ds(which * width + col, 2 * HEAD))
        d_parts = pair_backward(qkv_ref[at(0)], qkv_ref[at(1)], qkv_ref[at(2)], d_mix[at(0)])
        for which in range(3):
            d_qkv_ref[at(which)] = d_parts[which]
        return carry

    lax.fori_loop(0, samples * pairs, body, 0, unroll=BACKWARD_UNROLL)
    d_norm = dot_nt(d_qkv_ref[...], w_qkv[...])
    d_res, g_gain, g_shift = norm_back(h_ref[...].astype(F32), rows_ref[0:1, :], d_norm)
    out_ref[...] = (grad + d_res).astype(out_ref.dtype)
    add_rows(vec_ref, step, [g_gain, g_shift, jnp.sum(grad, axis=0, keepdims=True)])


ANY = pl.BlockSpec(memory_space=pl.ANY)


def by_step(rows, columns):
    return pl.BlockSpec((rows, columns), lambda i: (i, 0))


def whole(rows, columns):
    return pl.BlockSpec((rows, columns), lambda i: (0, 0))


def shape(rows, columns, dtype):
    return jax.ShapeDtypeStruct((rows, columns), dtype)


def call(kernel, steps, in_specs, out_specs, out_shapes, scratch, flops, moved):
    return pl.pallas_call(
        kernel, grid=(steps,), in_specs=in_specs, out_specs=out_specs, out_shape=out_shapes, scratch_shapes=scratch,
        cost_estimate=pl.CostEstimate(flops=int(flops), bytes_accessed=int(moved), transcendentals=0),
        compiler_params=pltpu.CompilerParams(dimension_semantics=('arbitrary',), vmem_limit_bytes=VMEM_LIMIT))


def self_forward(h, rows, pieces, tokens):
    count, width = h.shape
    return call(
        functools.partial(self_forward_kernel, STEP // tokens, tokens), count // STEP,
        [by_step(STEP, width), whole(*rows.shape)] + [ANY] * 8,
        [by_step(STEP, width), by_step(STEP, 3 * width), by_step(STEP, width), by_step(STEP, width)],
        [shape(count, width, BF16), shape(count, 3 * width, BF16), shape(count, width, BF16), shape(count, width, F32)],
        [pltpu.VMEM((width, 3 * width), BF16), pltpu.VMEM((width, width), BF16), pltpu.SemaphoreType.DMA((2,))],
        count * width * width * 8 + count * tokens * width * 4, 2e7)(h, rows, *pieces)


def cross_forward(h, rows, ctx, pieces, tokens, valid):
    count, width = h.shape
    ctx_rows, ctx_width = ctx.shape
    return call(
        functools.partial(cross_forward_kernel, STEP // tokens, tokens, valid), count // STEP,
        [by_step(STEP, width), whole(*rows.shape), whole(ctx_rows, ctx_width)] + [ANY] * 8,
        [by_step(STEP, width), by_step(STEP, width), whole(ctx_rows, 2 * width), by_step(STEP, width), by_step(STEP, width)],
        [shape(count, width, BF16), shape(count, width, BF16), shape(ctx_rows, 2 * width, BF16), shape(count, width, BF16),
         shape(count, width, F32)],
        [pltpu.VMEM((ctx_width, 2 * width), BF16), pltpu.VMEM((width, width), BF16), pltpu.VMEM((width, width), BF16),
         pltpu.SemaphoreType.DMA((3,))],
        count * width * width * 4 + ctx_rows * ctx_width * width * 4 + count * 128 * width * 4, 2e7)(h, rows, ctx, *pieces)


def ff_forward(h, rows, bias, pieces, offset):
    count, width = h.shape
    half = bias.shape[1] // 2
    return call(
        functools.partial(ff_forward_kernel, offset), count // FF_STEP,
        [by_step(FF_STEP, width), whole(*rows.shape), whole(1, 2 * half)] + [ANY] * 16,
        [by_step(FF_STEP, width), by_step(FF_STEP, half), by_step(FF_STEP, half), by_step(FF_STEP, half), by_step(FF_STEP, width)],
        [shape(count, width, BF16), shape(count, half, BF16), shape(count, half, F32), shape(count, half, F32),
         shape(count, width, F32)],
        [pltpu.VMEM((width, 2 * half), BF16), pltpu.VMEM((half, width), BF16), pltpu.SemaphoreType.DMA((2,))],
        count * width * half * 6, 6e7)(h, rows, bias, *pieces)


def ff_up_forward(h, rows, bias, pieces):
    count, width = h.shape
    half = bias.shape[1] // 2
    return call(
        ff_up_kernel, count // FF_STEP,
        [by_step(FF_STEP, width), whole(*rows.shape), whole(1, 2 * half)] + [ANY] * 8,
        [by_step(FF_STEP, width), by_step(FF_STEP, half), by_step(FF_STEP, half), by_step(FF_STEP, half)],
        [shape(count, width, BF16), shape(count, half, BF16), shape(count, half, F32), shape(count, half, F32)],
        [pltpu.VMEM((width, 2 * half), BF16), pltpu.SemaphoreType.DMA((1,))],
        count * width * half * 4, 5e7)(h, rows, bias, *pieces)


def ff_down_forward(h, rows, gated, pieces):
    count, width = h.shape
    half = gated.shape[1]
    return call(
        ff_down_kernel, count // STEP,
        [by_step(STEP, width), whole(*rows.shape), by_step(STEP, half)] + [ANY] * 8,
        by_step(STEP, width), shape(count, width, BF16),
        [pltpu.VMEM((half, width), BF16), pltpu.SemaphoreType.DMA((1,))],
        count * width * half * 2, 2e7)(h, rows, gated, *pieces)


def ff_backward(grad, save_a, save_g, h, rows, pieces, offset):
    count, width = h.shape
    half = save_a.shape[1]
    return call(
        functools.partial(ff_backward_kernel, offset), count // FF_STEP,
        [by_step(FF_STEP, width), by_step(FF_STEP, half), by_step(FF_STEP, half), by_step(FF_STEP, width), whole(*rows.shape)]
        + [ANY] * 16,
        [by_step(FF_STEP, 2 * half), by_step(FF_STEP, width), whole(8, width), whole(8, 2 * half)],
        [shape(count, 2 * half, BF16), shape(count, width, F32), shape(8, width, F32), shape(8, 2 * half, F32)],
        [pltpu.VMEM((width, 2 * half), BF16), pltpu.VMEM((half, width), BF16), pltpu.SemaphoreType.DMA((2,))],
        count * width * half * 6, 6e7)(grad, save_a, save_g, h, rows, *pieces)


def cross_backward(grad, query, kv, h, rows, pieces, tokens, valid):
    count, width = h.shape
    ctx_rows = kv.shape[0]
    steps = count // STEP
    return call(
        functools.partial(cross_backward_kernel, STEP // tokens, tokens, valid), steps,
        [by_step(STEP, width), by_step(STEP, width), by_step(ctx_rows // steps, 2 * width), by_step(STEP, width),
         whole(*rows.shape)] + [ANY] * 8,
        [by_step(STEP, width), by_step(STEP, width), by_step(ctx_rows // steps, 2 * width), by_step(STEP, width), whole(8, width)],
        [shape(count, width, BF16), shape(count, width, BF16), shape(ctx_rows, 2 * width, BF16), shape(count, width, F32),
         shape(8, width, F32)],
        [pltpu.VMEM((STEP, width), BF16), pltpu.VMEM((width, width), BF16), pltpu.VMEM((width, width), BF16),
         pltpu.SemaphoreType.DMA((2,))],
        count * width * width * 4 + count * 128 * width * 10, 2e7)(grad, query, kv, h, rows, *pieces)


def self_backward(grad, qkv, h, rows, pieces, tokens, out_dtype):
    count, width = h.shape
    return call(
        functools.partial(self_backward_kernel, STEP // tokens, tokens), count // STEP,
        [by_step(STEP, width), by_step(STEP, 3 * width), by_step(STEP, width), whole(*rows.shape)] + [ANY] * 8,
        [by_step(STEP, width), by_step(STEP, 3 * width), by_step(STEP, width), whole(8, width)],
        [shape(count, width, BF16), shape(count, 3 * width, BF16), shape(count, width, out_dtype), shape(8, width, F32)],
        [pltpu.VMEM((STEP, width), BF16), pltpu.VMEM((width, 3 * width), BF16), pltpu.VMEM((width, width), BF16),
         pltpu.SemaphoreType.DMA((2,))],
        count * width * width * 8 + count * tokens * width * 10, 3e7)(grad, qkv, h, rows, *pieces)


def scatter_sum(full, n_dev):
    near, far, core_perm = gather_perms(n_dev)
    me = lax.axis_index(AXIS)
    core, chip = me % 2, me // 2
    one, two = 1 + core, 2 - core
    by_chip = full.reshape((n_dev // 2, 2) + full.shape[1:])
    pick = lambda array, index: lax.dynamic_index_in_dim(array, index, 0, keepdims=False)
    ours = lambda index: lax.dynamic_slice(by_chip, (index, core) + (0,) * (full.ndim - 1),
                                           (1, 1) + full.shape[1:]).reshape(full.shape[1:])
    got = permute(lax.dynamic_index_in_dim(by_chip, 1 - core, 1, keepdims=False), core_perm)
    part = lambda index: ours(index) + pick(got, index)
    x = jnp.bitwise_xor
    second = permute(jnp.stack([part(x(chip, one)), part(x(x(chip, one), two))]), far)
    third = permute(part(x(chip, two)) + second[1], near)
    return part(chip) + second[0] + third


def grad_kernel(tiles, group_rows, inputs, *refs):
    ins, (far_ref, keep_ref, x_buf, turned, y_buf, tile, own, recv, x_sem, y_sem, send_sem, recv_sem) = refs[:inputs], refs[inputs:]
    width = tile.shape[1]
    me = lax.axis_index(AXIS)
    core, chip = lax.rem(me, 2), me // 2
    mate = me + 1 - 2 * core
    chip_x, chip_y = lax.rem(chip, 2), chip // 2

    xs, ys, x_of, y_of = [], [], [], []
    for x, x_col, y, y_col, *_ in tiles:
        if not xs or xs[-1] != (x, x_col):
            xs.append((x, x_col))
        if not ys or ys[-1] != (y, y_col):
            ys.append((y, y_col))
        x_of.append(len(xs) - 1)
        y_of.append(len(ys) - 1)

    def load(which, sequence, buf, sem):
        array, col = sequence[which]
        return pltpu.make_async_copy(ins[array].at[:, pl.ds(col, width)], buf.at[which % 2], sem.at[which % 2])

    for which in range(2):
        if which < len(xs):
            load(which, xs, x_buf, x_sem).start()
        if which < len(ys):
            load(which, ys, y_buf, y_sem).start()

    barrier = pltpu.get_barrier_semaphore()
    pl.semaphore_signal(barrier, inc=1, device_id=(mate,), device_id_type=pl.DeviceIdType.MESH)
    pl.semaphore_wait(barrier, 1)

    def sends(q):
        *_, first_row, rows, chips = tiles[q]
        copies = []
        for index, other in enumerate(chips):
            d_x, d_y = lax.rem(chip_x + other % 2, 2), lax.rem(chip_y + other // 2, 2)
            slot = d_x + 2 * d_y + core * (d_x - d_y)
            start = pl.multiple_of((2 * index + 1 - core) * rows, 16)
            copies.append(pltpu.make_async_remote_copy(
                src_ref=tile.at[q % 3, pl.ds(start, rows), :], dst_ref=recv.at[slot, pl.ds(first_row, rows), :],
                send_sem=send_sem.at[q % 3, index], recv_sem=recv_sem.at[q, index],
                device_id=(mate,), device_id_type=pl.DeviceIdType.MESH))
        return copies

    for q, (x, x_col, y, y_col, first_row, rows, chips) in enumerate(tiles):
        if q == 0 or x_of[q] != x_of[q - 1]:
            which = x_of[q]
            load(which, xs, x_buf, x_sem).wait()
            turned[...] = x_buf[which % 2].T
            if which + 2 < len(xs):
                load(which + 2, xs, x_buf, x_sem).start()
        if q == 0 or y_of[q] != y_of[q - 1]:
            load(y_of[q], ys, y_buf, y_sem).wait()
        if q >= 3:
            for copy in sends(q - 3):
                copy.wait_send()
        tile[q % 3] = dot_nn(turned[...], y_buf[y_of[q] % 2])
        if (q + 1 == len(tiles) or y_of[q + 1] != y_of[q]) and y_of[q] + 2 < len(ys):
            load(y_of[q] + 2, ys, y_buf, y_sem).start()
        for index, other in enumerate(chips):
            d_x, d_y = lax.rem(chip_x + other % 2, 2), lax.rem(chip_y + other // 2, 2)
            slot = 2 * d_x + d_y + core * (d_y - d_x)
            start = pl.multiple_of((2 * index + core) * rows, 16)
            own[slot, first_row:first_row + rows, :] = tile[q % 3, pl.ds(start, rows), :]
        if q >= 1:
            for copy in sends(q - 1):
                copy.start()
    last = len(tiles) - 1
    for copy in sends(last):
        copy.start()
    for q in range(max(0, last - 2), last + 1):
        for copy in sends(q):
            copy.wait_send()
    for q in range(last + 1):
        for copy in sends(q):
            copy.wait_recv()
    for slot in range(4):
        ref = keep_ref if slot < 2 else far_ref
        ref[(slot % 2) * group_rows:(slot % 2 + 1) * group_rows, :] = own[slot] + recv[slot]


def weight_grads(kind, arrays, tiles, group_rows):
    count, width = arrays[0].shape[0], 640
    chips = max(len(t[-1]) for t in tiles)
    out = jax.ShapeDtypeStruct((2 * group_rows, width), F32)
    return pl.pallas_call(
        functools.partial(grad_kernel, tiles, group_rows, len(arrays)), in_specs=[ANY] * len(arrays),
        out_specs=[pl.BlockSpec(memory_space=pltpu.VMEM)] * 2, out_shape=[out, out],
        scratch_shapes=[pltpu.VMEM((2, count, width), BF16), pltpu.VMEM((width, count), BF16), pltpu.VMEM((2, count, width), BF16),
                        pltpu.VMEM((3, width, width), F32), pltpu.VMEM((4, group_rows, width), F32),
                        pltpu.VMEM((4, group_rows, width), F32), pltpu.SemaphoreType.DMA((2,)), pltpu.SemaphoreType.DMA((2,)),
                        pltpu.SemaphoreType.DMA((3, chips)), pltpu.SemaphoreType.DMA((len(tiles), chips))],
        cost_estimate=pl.CostEstimate(flops=2 * count * width * width * len(tiles), bytes_accessed=int(2e7), transcendentals=0),
        compiler_params=pltpu.CompilerParams(collective_id=kind, has_side_effects=True, vmem_limit_bytes=VMEM_LIMIT))(*arrays)


def context_grad_kernel(ctx_ref, mine_ref, other_ref, far_ref, keep_ref, d_kv):
    rows, width = mine_ref.shape[0], far_ref.shape[1]
    d_kv[0:rows, :] = mine_ref[...]
    d_kv[rows:2 * rows, :] = other_ref[...]
    depth = ctx_ref.shape[0] // 4
    for slot in range(4):
        ref = keep_ref if slot < 2 else far_ref
        for block in range(2):
            start = ((slot % 2) * 2 + block) * depth
            ref[start:start + depth, :] = dot_nn(ctx_ref[slot * depth:(slot + 1) * depth, :], d_kv[:, block * width:(block + 1) * width])


def context_grad(turned, mine, other):
    width = mine.shape[1] // 2
    out = jax.ShapeDtypeStruct((turned.shape[0], width), F32)
    vmem = pl.BlockSpec(memory_space=pltpu.VMEM)
    return pl.pallas_call(
        context_grad_kernel, in_specs=[vmem] * 3, out_specs=[vmem] * 2, out_shape=[out, out],
        scratch_shapes=[pltpu.VMEM((2 * mine.shape[0], 2 * width), BF16)],
        cost_estimate=pl.CostEstimate(flops=2 * turned.size * 2 * width, bytes_accessed=int(2e7), transcendentals=0),
        compiler_params=pltpu.CompilerParams(vmem_limit_bytes=VMEM_LIMIT), name='context_grad')(turned, mine, other)


def context_columns(ctx, n_dev):
    _, _, core_perm = gather_perms(n_dev)
    me = lax.axis_index(AXIS)
    core, chip = me % 2, me // 2
    each = ctx.shape[1] // n_dev
    x = jnp.bitwise_xor

    def columns(of_core):
        one, two = 1 + of_core, 2 - of_core
        chips = [chip, x(chip, two), x(chip, one), x(chip, 3)]
        return jnp.concatenate([lax.dynamic_slice(ctx, (0, (2 * c + of_core) * each), (ctx.shape[0], each)) for c in chips], 1)

    other = permute(columns(1 - core), core_perm)
    return jnp.concatenate([columns(core), other], 0).T


def finish_scatter(far, keep, n_dev):
    near_perm, far_perm, _ = gather_perms(n_dev)
    rows = keep.shape[0] // 2
    second = permute(far, far_perm)
    third = permute(keep[rows:] + second[rows:], near_perm)
    return keep[:rows] + second[:rows] + third


def solution(mesh):
    n_dev = mesh.shape[AXIS]

    def inner(tokens_x, context, cot_out, *shards):
        batch, tokens, width = tokens_x.shape
        _, valid, ctx_width = context.shape
        blocks = shards[0].shape[0]
        total = batch * n_dev
        depth = width // n_dev
        count = batch * tokens
        half = 4 * width

        views = []
        for shard, rows in zip(shards[:7], (depth, depth, depth, ctx_width // n_dev, depth, depth, half // n_dev)):
            views.append(shard.reshape(blocks, rows, -1))
        qkv_s, out_s = lax.optimization_barrier(views[:2])
        q2_s, kv2_s, out2_s = lax.optimization_barrier(views[2:5])
        ff1_s, ff2_s = lax.optimization_barrier(views[5:])
        me = lax.axis_index(AXIS)
        vec_len = shards[7].shape[1]
        vec_each = 17
        vec_rows = (blocks * vec_each + 15) // 16 * 16
        vec_block = lax.dynamic_update_slice(jnp.zeros((blocks, n_dev * vec_len), BF16), shards[7], (0, me * vec_len))
        vec_block = vec_block[:, :vec_each * width].reshape(blocks * vec_each, width)
        vec_block = jnp.pad(vec_block, ((0, vec_rows - blocks * vec_each), (0, 0)))

        members = []
        for layer in range(blocks):
            members += [(layer, [qkv_s, out_s]), (layer, [kv2_s, q2_s, out2_s])]
            members += [(layer, [ff1_s, ff2_s])] if layer < blocks - 1 else [(layer, [ff1_s]), (layer, [ff2_s])]
        groups = []
        for index, (layer, parts) in enumerate(members):
            block = pack(parts, layer, [vec_block] if index == 0 else [], width)
            groups.append(gather_group(block, n_dev))
        ff_groups = [groups[3 * layer + 2] * 2 if layer < blocks - 1 else groups[-2] + groups[-1] for layer in range(blocks)]
        ff_offsets = [8 * depth if layer < blocks - 1 else 0 for layer in range(blocks)]

        group_rows = groups[0][0].shape[0]
        vecs = jnp.zeros((vec_rows, width), F32)
        for piece in groups[0]:
            vecs = vecs + piece[group_rows - vec_rows:].astype(F32)
        vecs = vecs[:blocks * vec_each].reshape(blocks, vec_each, width)
        rows_all = jnp.pad(vecs[:, :9], ((0, 0), (0, 7), (0, 0)))
        bias_all = vecs[:, 9:].reshape(blocks, 1, 8 * width)

        padded = (valid + 15) // 16 * 16
        ctx = jnp.pad(context, ((0, 0), (0, padded - valid), (0, 0))).reshape(batch * padded, ctx_width)

        turned_ctx = context_columns(ctx, n_dev)

        h = tokens_x.reshape(count, width)
        saved = []
        for layer in range(blocks):
            rows, bias = rows_all[layer], bias_all[layer]
            group = groups[3 * layer:3 * layer + 2]
            norm1, qkv, mix1, h1 = self_forward(h, rows, group[0], tokens)
            norm2, query, kv, mix2, h2 = cross_forward(h1, rows, ctx, group[1], tokens, valid)
            if layer < blocks - 1:
                norm3, gated, save_a, save_g, h3 = ff_forward(h2, rows, bias, ff_groups[layer], ff_offsets[layer])
            else:
                norm3, gated, save_a, save_g = ff_up_forward(h2, rows, bias, groups[-2])
                out_tokens = ff_down_forward(h2, rows, gated, groups[-1])
            saved.append((h, norm1, qkv, mix1, h1, norm2, query, kv, mix2, h2, norm3, gated, save_a, save_g))
            h = h3 if layer < blocks - 1 else None

        grad = cot_out.reshape(count, width)
        results, vec_grads = [None] * blocks, [None] * blocks
        every = tuple(range(n_dev // 2))
        by_column = lambda x, y, columns, first: [(x, 0, y, c * width, first + c * depth, depth, every) for c in range(columns)]
        _, _, core_perm = gather_perms(n_dev)
        for layer in reversed(range(blocks)):
            rows, group = rows_all[layer], groups[3 * layer:3 * layer + 2]
            h0, norm1, qkv, mix1, h1, norm2, query, kv, mix2, h2, norm3, gated, save_a, save_g = saved[layer]

            def reduce(pair):
                return finish_scatter(pair[0], pair[1], n_dev)

            r_ff2 = reduce(weight_grads(1, (gated, grad.astype(BF16)),
                                           [(0, c * width, 1, 0, 0, half // n_dev, (c,)) for c in range(half // width)], half // n_dev))
            d_hidden, grad, vec3, vec_b1 = ff_backward(grad, save_a, save_g, h2, rows, ff_groups[layer], ff_offsets[layer])
            r_ff1 = reduce(weight_grads(2, (norm3, d_hidden), by_column(0, 1, 8, 0), 8 * depth))
            grad_bf, d_query, d_kv, grad, vec2 = cross_backward(grad, query, kv, h1, rows, group[1], tokens, valid)
            d_kv_other = permute(d_kv, core_perm)
            r_cross = reduce(weight_grads(3, (norm2, d_query, mix2, grad_bf),
                                             by_column(0, 1, 1, 0) + by_column(2, 3, 1, depth), 2 * depth))
            r_kv = reduce(context_grad(turned_ctx, d_kv, d_kv_other))
            grad_bf, d_qkv, grad, vec1 = self_backward(grad, qkv, h0, rows, group[0], tokens, BF16 if layer == 0 else F32)
            r_self = reduce(weight_grads(4, (norm1, d_qkv, mix1, grad_bf),
                                            by_column(0, 1, 3, 0) + by_column(2, 3, 1, 3 * depth), 4 * depth))
            side = lambda array, blocks_of: jnp.concatenate(jnp.split(array, blocks_of, 0), 1)
            results[layer] = [side(r_self[:3 * depth], 3), r_self[3 * depth:], r_cross[:depth], side(r_kv, 2), r_cross[depth:],
                              side(r_ff1, 8), r_ff2]
            vec_grads[layer] = jnp.concatenate([vec1[0], vec1[1], vec2[0], vec2[1], vec3[0], vec3[1],
                                                vec1[2], vec2[2], vec3[2], vec_b1[0]])
        vec_full = jnp.stack([jnp.pad(g, (0, vec_len * n_dev - g.shape[0])).reshape(n_dev, vec_len) for g in vec_grads], 1)
        vec_out = scatter_sum(vec_full, n_dev)
        outs = []
        for index in range(7):
            stacked = jnp.stack([results[layer][index] for layer in range(blocks)]) / total
            stacked = lax.optimization_barrier(stacked)
            outs.append(stacked.reshape(blocks, -1))
        outs.append(vec_out / total)
        return tuple([out_tokens.reshape(tokens_x.shape), grad.reshape(tokens_x.shape)] + outs)

    param_spec = P(None, AXIS)
    in_specs = (P(AXIS), P(AXIS), P(AXIS)) + (param_spec,) * 8
    out_specs = (P(AXIS), P(AXIS)) + (param_spec,) * 8
    return jax.shard_map(inner, mesh=mesh, in_specs=in_specs, out_specs=out_specs, check_vma=False)
```

```python
import functools
import math
import jax
import jax.numpy as jnp
from jax import lax
from jax.experimental import pallas as pl
from jax.experimental.pallas import tpu as pltpu
from jax.sharding import PartitionSpec as P


HEAD = 64
AXIS = 'fsdp'
CHUNK = 1280
FF_STEP = 256
STEP = 512
VMEM_LIMIT = 60 * 1024 * 1024
VMEM_MOST = 67043328
FORWARD_UNROLL = 10
BACKWARD_UNROLL = 5

F32 = jnp.float32
BF16 = jnp.bfloat16


def gather_perms(n_dev):
    near = [(i, i ^ (4 if i % 2 == 0 else 2)) for i in range(n_dev)]
    far = [(i, i ^ (2 if i % 2 == 0 else 4)) for i in range(n_dev)]
    core = [(i, i ^ 1) for i in range(n_dev)]
    return near, far, core


def pack_kernel(*refs):
    ins, out = refs[:-1], refs[-1]
    width, row = out.shape[1], 0
    for ref in ins:
        depth = ref.shape[-2]
        for col in range(0, ref.shape[-1], width):
            piece = ref[0, :, col:col + width] if len(ref.shape) == 3 else ref[:, col:col + width]
            out[row:row + depth, :] = piece
            row += depth


def pack(views, layer, extra, width):
    rows = sum(v.shape[1] * v.shape[2] // width for v in views) + sum(e.shape[0] for e in extra)
    specs = [pl.BlockSpec((1,) + v.shape[1:], lambda i: (layer, 0, 0)) for v in views]
    specs += [pl.BlockSpec(e.shape, lambda i: (0, 0)) for e in extra]
    return pl.pallas_call(
        pack_kernel, grid=(1,), in_specs=specs, out_specs=pl.BlockSpec((rows, width), lambda i: (0, 0)),
        out_shape=jax.ShapeDtypeStruct((rows, width), BF16),
        cost_estimate=pl.CostEstimate(flops=rows * width, bytes_accessed=rows * width * 4, transcendentals=0),
        name='pack')(*views, *extra)


def permute(array, perm):
    return lax.ppermute(array, AXIS, perm)


def gather_group(shard, n_dev):
    near, far, core = gather_perms(n_dev)
    first = permute(shard, near)
    second = permute(shard, far)
    third = permute(first, far)
    mine = [shard, first, second, third]
    return mine + [permute(piece, core) for piece in mine]


def piece_devices(me):
    core = lax.rem(me, 2)
    one, two = 4 - 2 * core, 2 + 2 * core
    x = jnp.bitwise_xor
    mate = x(me, 1)
    return [me, x(me, one), x(me, two), x(me, 6), mate, x(mate, two), x(mate, one), x(mate, 6)]


def start_load(pieces, offset, ref, sem):
    width = pieces[0].shape[1]
    depth = ref.shape[0] // 8
    devices = piece_devices(lax.axis_index(AXIS))
    for block in range(ref.shape[1] // width):
        for piece, device in zip(pieces, devices):
            src = piece.at[pl.ds(offset + block * depth, depth), :]
            dst = ref.at[pl.ds(pl.multiple_of(device * depth, 16), depth), pl.ds(block * width, width)]
            pltpu.make_async_copy(src, dst, sem).start()


def wait_load(ref, sem):
    pltpu.make_async_copy(ref, ref, sem).wait()


def dot_nn(a, b):
    return lax.dot_general(a, b, (((1,), (0,)), ((), ())), preferred_element_type=F32)


def dot_nt(a, b):
    return lax.dot_general(a, b, (((1,), (1,)), ((), ())), preferred_element_type=F32)


def norm_stats(x):
    average = jnp.mean(x, axis=-1, keepdims=True)
    centered = x - average
    variance = jnp.mean(centered * centered, axis=-1, keepdims=True)
    scale = lax.rsqrt(variance + 1e-5)
    return centered * scale, scale


def norm_back(x, gain, d_norm):
    unit, scale = norm_stats(x)
    d_unit = d_norm * gain
    inner = d_unit - jnp.mean(d_unit, axis=-1, keepdims=True) - unit * jnp.mean(d_unit * unit, axis=-1, keepdims=True)
    return scale * inner, jnp.sum(d_norm * unit, axis=0, keepdims=True), jnp.sum(d_norm, axis=0, keepdims=True)


def softmax_rows(scores):
    top = jnp.max(scores, axis=-1, keepdims=True)
    raised = jnp.exp(scores - top)
    return raised * (1.0 / jnp.sum(raised, axis=-1, keepdims=True))


def low_lanes(rows):
    return lax.broadcasted_iota(jnp.int32, (rows, 2 * HEAD), 1) < HEAD


def pair_scores(query, key, low, head, valid):
    q_head = jnp.where(low if head == 0 else jnp.logical_not(low), query, jnp.zeros_like(query))
    scores = dot_nt(q_head, key) * HEAD ** -0.5
    if valid is not None:
        column = lax.broadcasted_iota(jnp.int32, scores.shape, 1)
        scores = jnp.where(column < valid, scores, -1e30)
    return q_head, softmax_rows(scores)


def pair_forward(query, key, value, valid=None):
    low = low_lanes(query.shape[0])
    mixed = []
    for head in range(2):
        _, probs = pair_scores(query, key, low, head, valid)
        mixed.append(dot_nn(probs.astype(BF16), value))
    return jnp.where(low, mixed[0], mixed[1]).astype(BF16)


def pair_probs(key, query, low, head, valid):
    q_head = jnp.where(low if head == 0 else jnp.logical_not(low), query, jnp.zeros_like(query))
    scores = dot_nt(key, q_head) * HEAD ** -0.5
    if valid is not None:
        row = lax.broadcasted_iota(jnp.int32, scores.shape, 0)
        scores = jnp.where(row < valid, scores, -1e30)
    top = jnp.max(scores, axis=0, keepdims=True)
    raised = jnp.exp(scores - top)
    return q_head, raised * (1.0 / jnp.sum(raised, axis=0, keepdims=True))


def pair_backward(query, key, value, d_out, valid=None):
    low = low_lanes(query.shape[0])
    turned = key.T
    d_query, d_key, d_value = [], None, None
    for head in range(2):
        q_head, probs = pair_probs(key, query, low, head, valid)
        d_head = jnp.where(low if head == 0 else jnp.logical_not(low), d_out, jnp.zeros_like(d_out))
        d_probs = dot_nt(value, d_head).astype(BF16).astype(F32)
        inner = jnp.sum(d_probs * probs, axis=0, keepdims=True)
        d_scores = ((probs * (d_probs - inner)) * HEAD ** -0.5).astype(BF16)
        d_query.append(dot_nn(turned[head * HEAD:(head + 1) * HEAD, :], d_scores))
        dk, dv = dot_nn(d_scores, q_head), dot_nn(probs.astype(BF16), d_head)
        d_key = dk if d_key is None else d_key + dk
        d_value = dv if d_value is None else d_value + dv
    return jnp.concatenate(d_query, 0).T.astype(BF16), d_key.astype(BF16), d_value.astype(BF16)


def add_rows(ref, step, rows):
    @pl.when(step == 0)
    def _():
        ref[...] = jnp.zeros_like(ref)

    for index, row in enumerate(rows):
        ref[pl.ds(index, 1), :] += row


def self_forward_kernel(samples, tokens, h_ref, rows_ref, *refs):
    pieces, (norm_ref, qkv_ref, mix_ref, out_ref, w_qkv, w_out, sems) = refs[:8], refs[8:]
    width = h_ref.shape[1]
    step = pl.program_id(0)

    @pl.when(step == 0)
    def _():
        start_load(pieces, 0, w_qkv, sems.at[0])
        start_load(pieces, 3 * (width // 8), w_out, sems.at[1])

    x = h_ref[...].astype(F32)
    unit, _ = norm_stats(x)
    normed = (unit * rows_ref[0:1, :] + rows_ref[1:2, :]).astype(BF16)
    norm_ref[...] = normed

    @pl.when(step == 0)
    def _():
        wait_load(w_qkv, sems.at[0])
        wait_load(w_out, sems.at[1])

    qkv_ref[...] = dot_nn(normed, w_qkv[...]).astype(BF16)
    pairs = width // (2 * HEAD)

    def body(index, carry):
        row = pl.multiple_of((index // pairs) * tokens, tokens)
        col = pl.multiple_of((index % pairs) * 2 * HEAD, 2 * HEAD)
        part = lambda which: qkv_ref[pl.ds(row, tokens), pl.ds(which * width + col, 2 * HEAD)]
        mix_ref[pl.ds(row, tokens), pl.ds(col, 2 * HEAD)] = pair_forward(part(0), part(1), part(2))
        return carry

    lax.fori_loop(0, samples * pairs, body, 0, unroll=FORWARD_UNROLL)
    out_ref[...] = x + dot_nn(mix_ref[...], w_out[...]) + rows_ref[6:7, :]


def cross_forward_kernel(samples, tokens, valid, h_ref, rows_ref, ctx_ref, *refs):
    pieces, (norm_ref, query_ref, kv_ref, mix_ref, out_ref, w_kv, w_query, w_out, sems) = refs[:8], refs[8:]
    width = h_ref.shape[1]
    step = pl.program_id(0)
    padded = ctx_ref.shape[0] // (samples * pl.num_programs(0))

    @pl.when(step == 0)
    def _():
        deep, depth = w_kv.shape[0] // 8, width // 8
        start_load(pieces, 0, w_kv, sems.at[0])
        start_load(pieces, 2 * deep, w_query, sems.at[1])
        start_load(pieces, 2 * deep + depth, w_out, sems.at[2])

    x = h_ref[...]
    unit, _ = norm_stats(x)
    normed = (unit * rows_ref[2:3, :] + rows_ref[3:4, :]).astype(BF16)
    norm_ref[...] = normed

    @pl.when(step == 0)
    def _():
        wait_load(w_kv, sems.at[0])
        wait_load(w_query, sems.at[1])
        wait_load(w_out, sems.at[2])
        kv_ref[...] = dot_nn(ctx_ref[...], w_kv[...]).astype(BF16)

    query_ref[...] = dot_nn(normed, w_query[...]).astype(BF16)
    pairs = width // (2 * HEAD)

    def body(index, carry):
        sample = index // pairs
        row = pl.multiple_of(sample * tokens, tokens)
        kv_row = pl.multiple_of((step * samples + sample) * padded, 16)
        col = pl.multiple_of((index % pairs) * 2 * HEAD, 2 * HEAD)
        query = query_ref[pl.ds(row, tokens), pl.ds(col, 2 * HEAD)]
        key = kv_ref[pl.ds(kv_row, padded), pl.ds(col, 2 * HEAD)]
        value = kv_ref[pl.ds(kv_row, padded), pl.ds(width + col, 2 * HEAD)]
        mix_ref[pl.ds(row, tokens), pl.ds(col, 2 * HEAD)] = pair_forward(query, key, value, valid)
        return carry

    lax.fori_loop(0, samples * pairs, body, 0, unroll=FORWARD_UNROLL)
    out_ref[...] = x + dot_nn(mix_ref[...], w_out[...]) + rows_ref[7:8, :]


def ff_loads(pieces, offset, w_ff1, w_ff2, sems):
    start_load(pieces[:8], 0, w_ff1, sems.at[0])
    start_load(pieces[8:], offset, w_ff2, sems.at[1])


def ff_up(normed, bias_ref, w_ff1, half, start, gated_ref, save_a, save_g):
    u_a = dot_nn(normed, w_ff1[:, start:start + CHUNK]) + bias_ref[:, start:start + CHUNK]
    u_g = dot_nn(normed, w_ff1[:, half + start:half + start + CHUNK]) + bias_ref[:, half + start:half + start + CHUNK]
    cumulative = 0.5 * (1.0 + lax.erf(u_g * math.sqrt(0.5)))
    gate = u_g * cumulative
    slope = cumulative + u_g * (jnp.exp(-0.5 * u_g * u_g) * (1.0 / math.sqrt(2.0 * math.pi)))
    gated = (u_a * gate).astype(BF16)
    gated_ref[:, start:start + CHUNK] = gated
    save_a[:, start:start + CHUNK] = gate
    save_g[:, start:start + CHUNK] = u_a * slope
    return gated


def ff_forward_kernel(offset, h_ref, rows_ref, bias_ref, *refs):
    pieces, (norm_ref, gated_ref, save_a, save_g, out_ref, w_ff1, w_ff2, sems) = refs[:16], refs[16:]
    half = w_ff2.shape[0]
    step = pl.program_id(0)

    @pl.when(step == 0)
    def _():
        ff_loads(pieces, offset, w_ff1, w_ff2, sems)

    x = h_ref[...]
    unit, _ = norm_stats(x)
    normed = (unit * rows_ref[4:5, :] + rows_ref[5:6, :]).astype(BF16)
    norm_ref[...] = normed

    @pl.when(step == 0)
    def _():
        wait_load(w_ff1, sems.at[0])
        wait_load(w_ff2, sems.at[1])

    total = x + rows_ref[8:9, :]
    for start in range(0, half, CHUNK):
        gated = ff_up(normed, bias_ref, w_ff1, half, start, gated_ref, save_a, save_g)
        total = total + dot_nn(gated, w_ff2[start:start + CHUNK, :])
    out_ref[...] = total


def ff_up_kernel(h_ref, rows_ref, bias_ref, *refs):
    pieces, (norm_ref, gated_ref, save_a, save_g, w_ff1, sems) = refs[:8], refs[8:]
    half = w_ff1.shape[1] // 2
    step = pl.program_id(0)

    @pl.when(step == 0)
    def _():
        start_load(pieces, 0, w_ff1, sems.at[0])

    unit, _ = norm_stats(h_ref[...])
    normed = (unit * rows_ref[4:5, :] + rows_ref[5:6, :]).astype(BF16)
    norm_ref[...] = normed

    @pl.when(step == 0)
    def _():
        wait_load(w_ff1, sems.at[0])

    for start in range(0, half, CHUNK):
        ff_up(normed, bias_ref, w_ff1, half, start, gated_ref, save_a, save_g)


def ff_down_kernel(h_ref, rows_ref, gated_ref, *refs):
    pieces, (out_ref, w_ff2, sems) = refs[:8], refs[8:]
    step = pl.program_id(0)

    @pl.when(step == 0)
    def _():
        start_load(pieces, 0, w_ff2, sems.at[0])
        wait_load(w_ff2, sems.at[0])

    out_ref[...] = (h_ref[...] + rows_ref[8:9, :] + dot_nn(gated_ref[...], w_ff2[...])).astype(BF16)


def cross_backward_kernel(samples, tokens, valid, grad_ref, query_ref, kv_ref, h_ref, rows_ref, *refs):
    pieces, (grad_bf_ref, d_query_ref, d_kv_ref, out_ref, vec_ref, d_mix, w_query, w_out, sems) = refs[:8], refs[8:]
    width = h_ref.shape[1]
    step = pl.program_id(0)
    padded = kv_ref.shape[0] // samples

    @pl.when(step == 0)
    def _():
        depth = width // 8
        base = pieces[0].shape[0] - 2 * depth
        start_load(pieces, base, w_query, sems.at[0])
        start_load(pieces, base + depth, w_out, sems.at[1])

    grad = grad_ref[...]
    grad_bf = grad.astype(BF16)
    grad_bf_ref[...] = grad_bf

    @pl.when(step == 0)
    def _():
        wait_load(w_query, sems.at[0])
        wait_load(w_out, sems.at[1])

    d_mix[...] = dot_nt(grad_bf, w_out[...]).astype(BF16)
    pairs = width // (2 * HEAD)

    def body(index, carry):
        sample = index // pairs
        row = pl.multiple_of(sample * tokens, tokens)
        kv_row = pl.multiple_of(sample * padded, 16)
        col = pl.multiple_of((index % pairs) * 2 * HEAD, 2 * HEAD)
        at = (pl.ds(row, tokens), pl.ds(col, 2 * HEAD))
        at_key = (pl.ds(kv_row, padded), pl.ds(col, 2 * HEAD))
        at_value = (pl.ds(kv_row, padded), pl.ds(width + col, 2 * HEAD))
        dq, dk, dv = pair_backward(query_ref[at], kv_ref[at_key], kv_ref[at_value], d_mix[at], valid)
        d_query_ref[at] = dq
        d_kv_ref[at_key] = dk
        d_kv_ref[at_value] = dv
        return carry

    lax.fori_loop(0, samples * pairs, body, 0, unroll=BACKWARD_UNROLL)
    d_norm = dot_nt(d_query_ref[...], w_query[...])
    d_res, g_gain, g_shift = norm_back(h_ref[...], rows_ref[2:3, :], d_norm)
    out_ref[...] = grad + d_res
    add_rows(vec_ref, step, [g_gain, g_shift, jnp.sum(grad, axis=0, keepdims=True)])


def self_backward_kernel(samples, tokens, grad_ref, qkv_ref, h_ref, rows_ref, *refs):
    pieces, (grad_bf_ref, d_qkv_ref, out_ref, vec_ref, d_mix, w_qkv, w_out, sems) = refs[:8], refs[8:]
    width = h_ref.shape[1]
    step = pl.program_id(0)

    @pl.when(step == 0)
    def _():
        start_load(pieces, 0, w_qkv, sems.at[0])
        start_load(pieces, 3 * (width // 8), w_out, sems.at[1])

    grad = grad_ref[...]
    grad_bf = grad.astype(BF16)
    grad_bf_ref[...] = grad_bf

    @pl.when(step == 0)
    def _():
        wait_load(w_qkv, sems.at[0])
        wait_load(w_out, sems.at[1])

    d_mix[...] = dot_nt(grad_bf, w_out[...]).astype(BF16)
    pairs = width // (2 * HEAD)

    def body(index, carry):
        row = pl.multiple_of((index // pairs) * tokens, tokens)
        col = pl.multiple_of((index % pairs) * 2 * HEAD, 2 * HEAD)
        at = lambda which: (pl.ds(row, tokens), pl.ds(which * width + col, 2 * HEAD))
        d_parts = pair_backward(qkv_ref[at(0)], qkv_ref[at(1)], qkv_ref[at(2)], d_mix[at(0)])
        for which in range(3):
            d_qkv_ref[at(which)] = d_parts[which]
        return carry

    lax.fori_loop(0, samples * pairs, body, 0, unroll=BACKWARD_UNROLL)
    d_norm = dot_nt(d_qkv_ref[...], w_qkv[...])
    d_res, g_gain, g_shift = norm_back(h_ref[...].astype(F32), rows_ref[0:1, :], d_norm)
    out_ref[...] = (grad + d_res).astype(out_ref.dtype)
    add_rows(vec_ref, step, [g_gain, g_shift, jnp.sum(grad, axis=0, keepdims=True)])


ANY = pl.BlockSpec(memory_space=pl.ANY)


def by_step(rows, columns):
    return pl.BlockSpec((rows, columns), lambda i: (i, 0))


def whole(rows, columns):
    return pl.BlockSpec((rows, columns), lambda i: (0, 0))


def shape(rows, columns, dtype):
    return jax.ShapeDtypeStruct((rows, columns), dtype)


def call(kernel, steps, in_specs, out_specs, out_shapes, scratch, flops, moved):
    return pl.pallas_call(
        kernel, grid=(steps,), in_specs=in_specs, out_specs=out_specs, out_shape=out_shapes, scratch_shapes=scratch,
        cost_estimate=pl.CostEstimate(flops=int(flops), bytes_accessed=int(moved), transcendentals=0),
        compiler_params=pltpu.CompilerParams(dimension_semantics=('arbitrary',), vmem_limit_bytes=VMEM_LIMIT))


def self_forward(h, rows, pieces, tokens):
    count, width = h.shape
    return call(
        functools.partial(self_forward_kernel, STEP // tokens, tokens), count // STEP,
        [by_step(STEP, width), whole(*rows.shape)] + [ANY] * 8,
        [by_step(STEP, width), by_step(STEP, 3 * width), by_step(STEP, width), by_step(STEP, width)],
        [shape(count, width, BF16), shape(count, 3 * width, BF16), shape(count, width, BF16), shape(count, width, F32)],
        [pltpu.VMEM((width, 3 * width), BF16), pltpu.VMEM((width, width), BF16), pltpu.SemaphoreType.DMA((2,))],
        count * width * width * 8 + count * tokens * width * 4, 2e7)(h, rows, *pieces)


def cross_forward(h, rows, ctx, pieces, tokens, valid):
    count, width = h.shape
    ctx_rows, ctx_width = ctx.shape
    return call(
        functools.partial(cross_forward_kernel, STEP // tokens, tokens, valid), count // STEP,
        [by_step(STEP, width), whole(*rows.shape), whole(ctx_rows, ctx_width)] + [ANY] * 8,
        [by_step(STEP, width), by_step(STEP, width), whole(ctx_rows, 2 * width), by_step(STEP, width), by_step(STEP, width)],
        [shape(count, width, BF16), shape(count, width, BF16), shape(ctx_rows, 2 * width, BF16), shape(count, width, BF16),
         shape(count, width, F32)],
        [pltpu.VMEM((ctx_width, 2 * width), BF16), pltpu.VMEM((width, width), BF16), pltpu.VMEM((width, width), BF16),
         pltpu.SemaphoreType.DMA((3,))],
        count * width * width * 4 + ctx_rows * ctx_width * width * 4 + count * 128 * width * 4, 2e7)(h, rows, ctx, *pieces)


def ff_forward(h, rows, bias, pieces, offset):
    count, width = h.shape
    half = bias.shape[1] // 2
    return call(
        functools.partial(ff_forward_kernel, offset), count // FF_STEP,
        [by_step(FF_STEP, width), whole(*rows.shape), whole(1, 2 * half)] + [ANY] * 16,
        [by_step(FF_STEP, width), by_step(FF_STEP, half), by_step(FF_STEP, half), by_step(FF_STEP, half), by_step(FF_STEP, width)],
        [shape(count, width, BF16), shape(count, half, BF16), shape(count, half, F32), shape(count, half, F32),
         shape(count, width, F32)],
        [pltpu.VMEM((width, 2 * half), BF16), pltpu.VMEM((half, width), BF16), pltpu.SemaphoreType.DMA((2,))],
        count * width * half * 6, 6e7)(h, rows, bias, *pieces)


def ff_up_forward(h, rows, bias, pieces):
    count, width = h.shape
    half = bias.shape[1] // 2
    return call(
        ff_up_kernel, count // FF_STEP,
        [by_step(FF_STEP, width), whole(*rows.shape), whole(1, 2 * half)] + [ANY] * 8,
        [by_step(FF_STEP, width), by_step(FF_STEP, half), by_step(FF_STEP, half), by_step(FF_STEP, half)],
        [shape(count, width, BF16), shape(count, half, BF16), shape(count, half, F32), shape(count, half, F32)],
        [pltpu.VMEM((width, 2 * half), BF16), pltpu.SemaphoreType.DMA((1,))],
        count * width * half * 4, 5e7)(h, rows, bias, *pieces)


def ff_down_forward(h, rows, gated, pieces):
    count, width = h.shape
    half = gated.shape[1]
    return call(
        ff_down_kernel, count // STEP,
        [by_step(STEP, width), whole(*rows.shape), by_step(STEP, half)] + [ANY] * 8,
        by_step(STEP, width), shape(count, width, BF16),
        [pltpu.VMEM((half, width), BF16), pltpu.SemaphoreType.DMA((1,))],
        count * width * half * 2, 2e7)(h, rows, gated, *pieces)


def cross_backward(grad, query, kv, h, rows, pieces, tokens, valid):
    count, width = h.shape
    ctx_rows = kv.shape[0]
    steps = count // STEP
    return call(
        functools.partial(cross_backward_kernel, STEP // tokens, tokens, valid), steps,
        [by_step(STEP, width), by_step(STEP, width), by_step(ctx_rows // steps, 2 * width), by_step(STEP, width),
         whole(*rows.shape)] + [ANY] * 8,
        [by_step(STEP, width), by_step(STEP, width), by_step(ctx_rows // steps, 2 * width), by_step(STEP, width), whole(8, width)],
        [shape(count, width, BF16), shape(count, width, BF16), shape(ctx_rows, 2 * width, BF16), shape(count, width, F32),
         shape(8, width, F32)],
        [pltpu.VMEM((STEP, width), BF16), pltpu.VMEM((width, width), BF16), pltpu.VMEM((width, width), BF16),
         pltpu.SemaphoreType.DMA((2,))],
        count * width * width * 4 + count * 128 * width * 10, 2e7)(grad, query, kv, h, rows, *pieces)


def self_backward(grad, qkv, h, rows, pieces, tokens, out_dtype):
    count, width = h.shape
    return call(
        functools.partial(self_backward_kernel, STEP // tokens, tokens), count // STEP,
        [by_step(STEP, width), by_step(STEP, 3 * width), by_step(STEP, width), whole(*rows.shape)] + [ANY] * 8,
        [by_step(STEP, width), by_step(STEP, 3 * width), by_step(STEP, width), whole(8, width)],
        [shape(count, width, BF16), shape(count, 3 * width, BF16), shape(count, width, out_dtype), shape(8, width, F32)],
        [pltpu.VMEM((STEP, width), BF16), pltpu.VMEM((width, 3 * width), BF16), pltpu.VMEM((width, width), BF16),
         pltpu.SemaphoreType.DMA((2,))],
        count * width * width * 8 + count * tokens * width * 10, 3e7)(grad, qkv, h, rows, *pieces)


def scatter_sum(full, n_dev):
    near, far, core_perm = gather_perms(n_dev)
    me = lax.axis_index(AXIS)
    core, chip = me % 2, me // 2
    one, two = 1 + core, 2 - core
    by_chip = full.reshape((n_dev // 2, 2) + full.shape[1:])
    pick = lambda array, index: lax.dynamic_index_in_dim(array, index, 0, keepdims=False)
    ours = lambda index: lax.dynamic_slice(by_chip, (index, core) + (0,) * (full.ndim - 1),
                                           (1, 1) + full.shape[1:]).reshape(full.shape[1:])
    got = permute(lax.dynamic_index_in_dim(by_chip, 1 - core, 1, keepdims=False), core_perm)
    part = lambda index: ours(index) + pick(got, index)
    x = jnp.bitwise_xor
    second = permute(jnp.stack([part(x(chip, one)), part(x(x(chip, one), two))]), far)
    third = permute(part(x(chip, two)) + second[1], near)
    return part(chip) + second[0] + third


def grad_kernel(tiles, group_rows, inputs, *refs):
    ins, (far_ref, keep_ref, x_buf, turned, y_buf, tile, own, recv, x_sem, y_sem, send_sem, recv_sem) = refs[:inputs], refs[inputs:]
    width = tile.shape[1]
    me = lax.axis_index(AXIS)
    core, chip = lax.rem(me, 2), me // 2
    mate = me + 1 - 2 * core
    chip_x, chip_y = lax.rem(chip, 2), chip // 2

    xs, ys, x_of, y_of = [], [], [], []
    for x, x_col, y, y_col, *_ in tiles:
        if not xs or xs[-1] != (x, x_col):
            xs.append((x, x_col))
        if not ys or ys[-1] != (y, y_col):
            ys.append((y, y_col))
        x_of.append(len(xs) - 1)
        y_of.append(len(ys) - 1)

    def load(which, sequence, buf, sem):
        array, col = sequence[which]
        return pltpu.make_async_copy(ins[array].at[:, pl.ds(col, width)], buf.at[which % 2], sem.at[which % 2])

    for which in range(2):
        if which < len(xs):
            load(which, xs, x_buf, x_sem).start()
        if which < len(ys):
            load(which, ys, y_buf, y_sem).start()

    barrier = pltpu.get_barrier_semaphore()
    pl.semaphore_signal(barrier, inc=1, device_id=(mate,), device_id_type=pl.DeviceIdType.MESH)
    pl.semaphore_wait(barrier, 1)

    def sends(q):
        *_, first_row, rows, chips = tiles[q]
        copies = []
        for index, other in enumerate(chips):
            d_x, d_y = lax.rem(chip_x + other % 2, 2), lax.rem(chip_y + other // 2, 2)
            slot = d_x + 2 * d_y + core * (d_x - d_y)
            start = pl.multiple_of((2 * index + 1 - core) * rows, 16)
            copies.append(pltpu.make_async_remote_copy(
                src_ref=tile.at[q % 3, pl.ds(start, rows), :], dst_ref=recv.at[slot, pl.ds(first_row, rows), :],
                send_sem=send_sem.at[q % 3, index], recv_sem=recv_sem.at[q, index],
                device_id=(mate,), device_id_type=pl.DeviceIdType.MESH))
        return copies

    for q, (x, x_col, y, y_col, first_row, rows, chips) in enumerate(tiles):
        if q == 0 or x_of[q] != x_of[q - 1]:
            which = x_of[q]
            load(which, xs, x_buf, x_sem).wait()
            turned[...] = x_buf[which % 2].T
            if which + 2 < len(xs):
                load(which + 2, xs, x_buf, x_sem).start()
        if q == 0 or y_of[q] != y_of[q - 1]:
            load(y_of[q], ys, y_buf, y_sem).wait()
        if q >= 3:
            for copy in sends(q - 3):
                copy.wait_send()
        tile[q % 3] = dot_nn(turned[...], y_buf[y_of[q] % 2])
        if (q + 1 == len(tiles) or y_of[q + 1] != y_of[q]) and y_of[q] + 2 < len(ys):
            load(y_of[q] + 2, ys, y_buf, y_sem).start()
        for index, other in enumerate(chips):
            d_x, d_y = lax.rem(chip_x + other % 2, 2), lax.rem(chip_y + other // 2, 2)
            slot = 2 * d_x + d_y + core * (d_y - d_x)
            start = pl.multiple_of((2 * index + core) * rows, 16)
            own[slot, first_row:first_row + rows, :] = tile[q % 3, pl.ds(start, rows), :]
        if q >= 1:
            for copy in sends(q - 1):
                copy.start()
    last = len(tiles) - 1
    for copy in sends(last):
        copy.start()
    for q in range(max(0, last - 2), last + 1):
        for copy in sends(q):
            copy.wait_send()
    for q in range(last + 1):
        for copy in sends(q):
            copy.wait_recv()
    for slot in range(4):
        ref = keep_ref if slot < 2 else far_ref
        ref[(slot % 2) * group_rows:(slot % 2 + 1) * group_rows, :] = own[slot] + recv[slot]


def weight_grads(kind, arrays, tiles, group_rows):
    count, width = arrays[0].shape[0], 640
    chips = max(len(t[-1]) for t in tiles)
    out = jax.ShapeDtypeStruct((2 * group_rows, width), F32)
    return pl.pallas_call(
        functools.partial(grad_kernel, tiles, group_rows, len(arrays)), in_specs=[ANY] * len(arrays),
        out_specs=[pl.BlockSpec(memory_space=pltpu.VMEM)] * 2, out_shape=[out, out],
        scratch_shapes=[pltpu.VMEM((2, count, width), BF16), pltpu.VMEM((width, count), BF16), pltpu.VMEM((2, count, width), BF16),
                        pltpu.VMEM((3, width, width), F32), pltpu.VMEM((4, group_rows, width), F32),
                        pltpu.VMEM((4, group_rows, width), F32), pltpu.SemaphoreType.DMA((2,)), pltpu.SemaphoreType.DMA((2,)),
                        pltpu.SemaphoreType.DMA((3, chips)), pltpu.SemaphoreType.DMA((len(tiles), chips))],
        cost_estimate=pl.CostEstimate(flops=2 * count * width * width * len(tiles), bytes_accessed=int(2e7), transcendentals=0),
        compiler_params=pltpu.CompilerParams(collective_id=kind, has_side_effects=True, vmem_limit_bytes=VMEM_LIMIT))(*arrays)


def ff_grad_kernel(offset, with_down, grad_ref, save_a, save_g, norm_ref, h_ref, rows_ref, *refs):
    gated_ref, refs = (refs[0], refs[1:]) if with_down else (None, refs)
    pieces, refs = refs[:16], refs[16:]
    out_ref, vec_ref, bias_ref, far1, keep1 = refs[:5]
    far2, keep2 = refs[5:7] if with_down else (None, None)
    (grad, grad_bf, turned, acc, part_a, part_g, d_a, d_g, w_ff1, w_ff2, tile, recv1, obuf,
     in_sem, part_sem, w1_sem, w2_sem, out_sem, send_sem, recv_sem1) = refs[7 if with_down else 5:][:20]
    if with_down:
        z_buf, z_turned, recv2, z_sem, recv_sem2 = refs[-5:]
    count, width = grad.shape
    half = w_ff2.shape[0]
    chunks, each = half // width, STEP
    steps = count // each
    depth, deep = width // 8, half // 8
    me = lax.axis_index(AXIS)
    core, chip = lax.rem(me, 2), me // 2
    mate = me + 1 - 2 * core
    chip_x, chip_y = lax.rem(chip, 2), chip // 2

    def slot_of(other, of_mate):
        d_x, d_y = lax.rem(chip_x + other % 2, 2), lax.rem(chip_y + other // 2, 2)
        return d_x + 2 * d_y + core * (d_x - d_y) if of_mate else 2 * d_x + d_y + core * (d_y - d_x)

    def chip_in(slot):
        one, two = slot // 2, slot % 2
        d_x, d_y = one + core * (two - one), two + core * (one - two)
        return 2 * lax.rem(chip_y + d_y, 2) + lax.rem(chip_x + d_x, 2)

    load_grad = pltpu.make_async_copy(grad_ref, grad, in_sem.at[0])
    load_norm = pltpu.make_async_copy(norm_ref, d_a, in_sem.at[1])
    load_grad.start()
    load_norm.start()
    start_load(pieces[8:], offset, w_ff2, w2_sem)

    def parts(index):
        chunk, step = divmod(index, steps)
        at = (pl.ds(step * each, each), pl.ds(chunk * width, width))
        return [pltpu.make_async_copy(ref.at[at], buf.at[index % 2], part_sem.at[which, index % 2])
                for which, (ref, buf) in enumerate(((save_a, part_a), (save_g, part_g)))]

    def load_h(step):
        return pltpu.make_async_copy(h_ref.at[pl.ds(step * each, each), :], part_a.at[step % 2], part_sem.at[0, step % 2])

    for copy in parts(0):
        copy.start()
    devices = piece_devices(me)
    for block in [b + k for b in range(chunks) for k in (0, chunks)]:
        for piece, device in zip(pieces[:8], devices):
            pltpu.make_async_copy(piece.at[pl.ds(block * depth, depth), :],
                                  w_ff1.at[pl.ds(pl.multiple_of(device * depth, 16), depth), pl.ds(block * width, width)],
                                  w1_sem.at[block]).start()
    for copy in parts(1):
        copy.start()

    barrier = pltpu.get_barrier_semaphore()
    pl.semaphore_signal(barrier, inc=1, device_id=(mate,), device_id_type=pl.DeviceIdType.MESH)
    pl.semaphore_wait(barrier, 1)

    def load_z(chunk):
        return pltpu.make_async_copy(gated_ref.at[:, pl.ds(chunk * width, width)], z_buf, z_sem)

    if with_down:
        load_z(0).start()

    tiles = []
    for chunk in range(chunks):
        tiles += [(1, chunk), (1, chunks + chunk)] + ([(2, chunk)] if with_down else [])
    ring = tile.shape[0]

    def sends(q):
        which, block = tiles[q]
        copies = []
        for index, other in enumerate(range(4) if which == 1 else (block,)):
            rows = depth if which == 1 else deep
            start = pl.multiple_of((2 * index + 1 - core) * rows, 16)
            slot = slot_of(other, True)
            dst = (recv1.at[block, pl.ds(pl.multiple_of(slot * rows, 16), rows), :] if which == 1 else recv2.at[block])
            copies.append(pltpu.make_async_remote_copy(
                src_ref=tile.at[q % ring, pl.ds(start, rows), :], dst_ref=dst, send_sem=send_sem.at[q % ring, index],
                recv_sem=recv_sem1.at[block, index] if which == 1 else recv_sem2.at[block],
                device_id=(mate,), device_id_type=pl.DeviceIdType.MESH))
        return copies

    def writes(q, branch=None):
        which, block = tiles[q]
        if which == 1:
            return [pltpu.make_async_copy(
                obuf.at[q % 2, pl.ds(slot * depth, depth), :],
                (keep1 if slot < 2 else far1).at[pl.ds((slot % 2) * 8 * depth + block * depth, depth), :],
                out_sem.at[q % 2]) for slot in range(4)]
        slot = slot_of(block, False)
        ref = keep2 if branch == 0 else far2
        return [pltpu.make_async_copy(obuf.at[q % 2], ref.at[pl.ds(pl.multiple_of(lax.rem(slot, 2) * deep, 16), deep), :],
                                      out_sem.at[q % 2])]

    def wait_writes(q):
        pltpu.make_async_copy(obuf.at[q % 2], obuf.at[q % 2], out_sem.at[q % 2]).wait()

    def finish(q):
        which, block = tiles[q]
        for copy in sends(q):
            copy.wait_recv()
        if q >= 2:
            wait_writes(q - 2)
        if which == 1:
            for slot in range(4):
                start = pl.multiple_of((2 * chip_in(slot) + core) * depth, 16)
                rows = slice(slot * depth, (slot + 1) * depth)
                obuf[q % 2, rows, :] = tile[q % ring, pl.ds(start, depth), :] + recv1[block, rows, :]
            for copy in writes(q):
                copy.start()
        else:
            obuf[q % 2] = tile[q % ring, pl.ds(pl.multiple_of(core * deep, 16), deep), :] + recv2[block]
            slot = slot_of(block, False)
            for branch in range(2):
                @pl.when(slot // 2 == branch)
                def _():
                    for copy in writes(q, branch):
                        copy.start()
        for copy in sends(q):
            copy.wait_send()

    load_grad.wait()
    grad_bf[...] = grad[...].astype(BF16)
    load_norm.wait()
    turned[...] = d_a[...].T
    acc[...] = jnp.zeros_like(acc)
    bias_ref[...] = jnp.zeros_like(bias_ref)
    vec_ref[...] = jnp.zeros_like(vec_ref)
    wait_load(w_ff2, w2_sem)

    q = 0
    for chunk in range(chunks):
        for block in (chunk, chunks + chunk):
            ref = w_ff1.at[:, pl.ds(block * width, width)]
            pltpu.make_async_copy(ref, ref, w1_sem.at[block]).wait()
        for step in range(steps):
            index = chunk * steps + step
            rows = slice(step * each, (step + 1) * each)
            d_gated = dot_nt(grad_bf[rows, :], w_ff2[chunk * width:(chunk + 1) * width, :]).astype(BF16).astype(F32)
            for copy in parts(index):
                copy.wait()
            total = acc[rows, :]
            for base, saved, kept in ((0, part_a, d_a), (half, part_g, d_g)):
                d_part = d_gated * saved[index % 2]
                columns = slice(base + chunk * width, base + (chunk + 1) * width)
                bias_ref[0:1, columns] += jnp.sum(d_part, axis=0, keepdims=True)
                d_part = d_part.astype(BF16)
                kept[rows, :] = d_part
                total = total + dot_nt(d_part, w_ff1[:, columns])
            acc[rows, :] = total
            if index + 2 < chunks * steps:
                for copy in parts(index + 2):
                    copy.start()
        for kept in (d_a, d_g):
            tile[q % ring] = dot_nn(turned[...], kept[...])
            if q >= 1:
                for copy in sends(q - 1):
                    copy.start()
            if q >= 3:
                finish(q - 3)
            q += 1
        if with_down:
            load_z(chunk).wait()
            z_turned[...] = z_buf[...].T
            if chunk + 1 < chunks:
                load_z(chunk + 1).start()
            tile[q % ring] = dot_nn(z_turned[...], grad_bf[...])
            for copy in sends(q - 1):
                copy.start()
            if q >= 3:
                finish(q - 3)
            q += 1
    load_h(0).start()
    load_h(1).start()
    for copy in sends(q - 1):
        copy.start()
    for step in range(steps):
        rows = slice(step * each, (step + 1) * each)
        load_h(step).wait()
        mine = grad[rows, :].astype(F32)
        d_res, g_gain, g_shift = norm_back(part_a[step % 2], rows_ref[4:5, :], acc[rows, :])
        if step + 2 < steps:
            load_h(step + 2).start()
        acc[rows, :] = mine + d_res
        pltpu.make_async_copy(acc.at[pl.ds(step * each, each), :], out_ref.at[pl.ds(step * each, each), :], in_sem.at[0]).start()
        for at, row in enumerate((g_gain, g_shift, jnp.sum(mine, axis=0, keepdims=True))):
            vec_ref[at:at + 1, :] += row
    for late in range(max(0, q - 3), q):
        finish(late)
    for late in range(max(0, q - 2), q):
        wait_writes(late)
    pltpu.make_async_copy(acc, out_ref, in_sem.at[0]).wait()


def ff_grads(kind, grad, save_a, save_g, norm, h, rows, gated, pieces, offset):
    count, width = h.shape
    half = save_a.shape[1]
    down = gated is not None
    vmem = pl.BlockSpec(memory_space=pltpu.VMEM)
    big, small = shape(2 * width, width, F32), shape(half // 4, width, F32)
    dma = pltpu.SemaphoreType.DMA
    scratch = [pltpu.VMEM((count, width), grad.dtype), pltpu.VMEM((count, width), BF16), pltpu.VMEM((width, count), BF16),
               pltpu.VMEM((count, width), F32), pltpu.VMEM((2, STEP, width), F32), pltpu.VMEM((2, STEP, width), F32),
               pltpu.VMEM((count, width), BF16), pltpu.VMEM((count, width), BF16), pltpu.VMEM((width, 2 * half), BF16),
               pltpu.VMEM((half, width), BF16), pltpu.VMEM((4, width, width), F32), pltpu.VMEM((8, width // 2, width), F32),
               pltpu.VMEM((2, width // 2, width), F32), dma((2,)), dma((2, 2)), dma((8,)), dma, dma((2,)), dma((4, 4)), dma((8, 4))]
    if down:
        scratch += [pltpu.VMEM((count, width), BF16), pltpu.VMEM((width, count), BF16), pltpu.VMEM((4, half // 8, width), F32),
                    dma, dma((4,))]
    return pl.pallas_call(
        functools.partial(ff_grad_kernel, offset, down),
        in_specs=[ANY] * 5 + [vmem] + [ANY] * (16 + down),
        out_specs=[ANY, vmem, vmem, ANY, ANY] + [ANY, ANY] * down,
        out_shape=[shape(count, width, F32), shape(8, width, F32), shape(8, 2 * half, F32), big, big] + [small, small] * down,
        scratch_shapes=scratch,
        cost_estimate=pl.CostEstimate(flops=count * width * half * (14 if down else 10), bytes_accessed=int(6e7), transcendentals=0),
        compiler_params=pltpu.CompilerParams(collective_id=kind, has_side_effects=True, vmem_limit_bytes=VMEM_MOST))(grad, save_a, save_g, norm, h, rows, *([gated] if down else []), *pieces)


def context_grad_kernel(ctx_ref, mine_ref, other_ref, far_ref, keep_ref, d_kv):
    rows, width = mine_ref.shape[0], far_ref.shape[1]
    d_kv[0:rows, :] = mine_ref[...]
    d_kv[rows:2 * rows, :] = other_ref[...]
    depth = ctx_ref.shape[0] // 4
    for slot in range(4):
        ref = keep_ref if slot < 2 else far_ref
        for block in range(2):
            start = ((slot % 2) * 2 + block) * depth
            ref[start:start + depth, :] = dot_nn(ctx_ref[slot * depth:(slot + 1) * depth, :], d_kv[:, block * width:(block + 1) * width])


def context_grad(turned, mine, other):
    width = mine.shape[1] // 2
    out = jax.ShapeDtypeStruct((turned.shape[0], width), F32)
    vmem = pl.BlockSpec(memory_space=pltpu.VMEM)
    return pl.pallas_call(
        context_grad_kernel, in_specs=[vmem] * 3, out_specs=[vmem] * 2, out_shape=[out, out],
        scratch_shapes=[pltpu.VMEM((2 * mine.shape[0], 2 * width), BF16)],
        cost_estimate=pl.CostEstimate(flops=2 * turned.size * 2 * width, bytes_accessed=int(2e7), transcendentals=0),
        compiler_params=pltpu.CompilerParams(vmem_limit_bytes=VMEM_LIMIT), name='context_grad')(turned, mine, other)


def context_columns(ctx, n_dev):
    _, _, core_perm = gather_perms(n_dev)
    me = lax.axis_index(AXIS)
    core, chip = me % 2, me // 2
    each = ctx.shape[1] // n_dev
    x = jnp.bitwise_xor

    def columns(of_core):
        one, two = 1 + of_core, 2 - of_core
        chips = [chip, x(chip, two), x(chip, one), x(chip, 3)]
        return jnp.concatenate([lax.dynamic_slice(ctx, (0, (2 * c + of_core) * each), (ctx.shape[0], each)) for c in chips], 1)

    other = permute(columns(1 - core), core_perm)
    return jnp.concatenate([columns(core), other], 0).T


def finish_scatter(far, keep, n_dev):
    near_perm, far_perm, _ = gather_perms(n_dev)
    rows = keep.shape[0] // 2
    second = permute(far, far_perm)
    third = permute(keep[rows:] + second[rows:], near_perm)
    return keep[:rows] + second[:rows] + third


def solution(mesh):
    n_dev = mesh.shape[AXIS]

    def inner(tokens_x, context, cot_out, *shards):
        batch, tokens, width = tokens_x.shape
        _, valid, ctx_width = context.shape
        blocks = shards[0].shape[0]
        total = batch * n_dev
        depth = width // n_dev
        count = batch * tokens
        half = 4 * width

        views = []
        for shard, rows in zip(shards[:7], (depth, depth, depth, ctx_width // n_dev, depth, depth, half // n_dev)):
            views.append(shard.reshape(blocks, rows, -1))
        qkv_s, out_s = lax.optimization_barrier(views[:2])
        q2_s, kv2_s, out2_s = lax.optimization_barrier(views[2:5])
        ff1_s, ff2_s = lax.optimization_barrier(views[5:])
        me = lax.axis_index(AXIS)
        vec_len = shards[7].shape[1]
        vec_each = 17
        vec_rows = (blocks * vec_each + 15) // 16 * 16
        vec_block = lax.dynamic_update_slice(jnp.zeros((blocks, n_dev * vec_len), BF16), shards[7], (0, me * vec_len))
        vec_block = vec_block[:, :vec_each * width].reshape(blocks * vec_each, width)
        vec_block = jnp.pad(vec_block, ((0, vec_rows - blocks * vec_each), (0, 0)))

        members = []
        for layer in range(blocks):
            members += [(layer, [qkv_s, out_s]), (layer, [kv2_s, q2_s, out2_s])]
            members += [(layer, [ff1_s, ff2_s])] if layer < blocks - 1 else [(layer, [ff1_s]), (layer, [ff2_s])]
        groups = []
        for index, (layer, parts) in enumerate(members):
            block = pack(parts, layer, [vec_block] if index == 0 else [], width)
            groups.append(gather_group(block, n_dev))
        ff_groups = [groups[3 * layer + 2] * 2 if layer < blocks - 1 else groups[-2] + groups[-1] for layer in range(blocks)]
        ff_offsets = [8 * depth if layer < blocks - 1 else 0 for layer in range(blocks)]

        group_rows = groups[0][0].shape[0]
        vecs = jnp.zeros((vec_rows, width), F32)
        for piece in groups[0]:
            vecs = vecs + piece[group_rows - vec_rows:].astype(F32)
        vecs = vecs[:blocks * vec_each].reshape(blocks, vec_each, width)
        rows_all = jnp.pad(vecs[:, :9], ((0, 0), (0, 7), (0, 0)))
        bias_all = vecs[:, 9:].reshape(blocks, 1, 8 * width)

        padded = (valid + 15) // 16 * 16
        ctx = jnp.pad(context, ((0, 0), (0, padded - valid), (0, 0))).reshape(batch * padded, ctx_width)

        turned_ctx = context_columns(ctx, n_dev)

        h = tokens_x.reshape(count, width)
        saved = []
        for layer in range(blocks):
            rows, bias = rows_all[layer], bias_all[layer]
            group = groups[3 * layer:3 * layer + 2]
            norm1, qkv, mix1, h1 = self_forward(h, rows, group[0], tokens)
            norm2, query, kv, mix2, h2 = cross_forward(h1, rows, ctx, group[1], tokens, valid)
            if layer < blocks - 1:
                norm3, gated, save_a, save_g, h3 = ff_forward(h2, rows, bias, ff_groups[layer], ff_offsets[layer])
            else:
                norm3, gated, save_a, save_g = ff_up_forward(h2, rows, bias, groups[-2])
                out_tokens = ff_down_forward(h2, rows, gated, groups[-1])
            saved.append((h, norm1, qkv, mix1, h1, norm2, query, kv, mix2, h2, norm3, gated, save_a, save_g))
            h = h3 if layer < blocks - 1 else None

        grad = cot_out.reshape(count, width)
        results, vec_grads = [None] * blocks, [None] * blocks
        every = tuple(range(n_dev // 2))
        by_column = lambda x, y, columns, first: [(x, 0, y, c * width, first + c * depth, depth, every) for c in range(columns)]
        _, _, core_perm = gather_perms(n_dev)
        for layer in reversed(range(blocks)):
            turn = blocks - 1 - layer
            rows, group = rows_all[layer], groups[3 * layer:3 * layer + 2]
            h0, norm1, qkv, mix1, h1, norm2, query, kv, mix2, h2, norm3, gated, save_a, save_g = saved[layer]

            def reduce(pair):
                return finish_scatter(pair[0], pair[1], n_dev)

            if turn == 0:
                r_ff2 = reduce(weight_grads(1, (gated, grad.astype(BF16)),
                                               [(0, c * width, 1, 0, 0, half // n_dev, (c,)) for c in range(half // width)], half // n_dev))
            grad, vec3, vec_b1, *pairs = ff_grads(5 + min(turn, 1), grad, save_a, save_g, norm3, h2, rows,
                                                  gated if turn > 0 else None, ff_groups[layer], ff_offsets[layer])
            r_ff1 = reduce(pairs[:2])
            if turn > 0:
                r_ff2 = reduce(pairs[2:])
            grad_bf, d_query, d_kv, grad, vec2 = cross_backward(grad, query, kv, h1, rows, group[1], tokens, valid)
            d_kv_other = permute(d_kv, core_perm)
            r_cross = reduce(weight_grads(3, (norm2, d_query, mix2, grad_bf),
                                             by_column(0, 1, 1, 0) + by_column(2, 3, 1, depth), 2 * depth))
            r_kv = reduce(context_grad(turned_ctx, d_kv, d_kv_other))
            grad_bf, d_qkv, grad, vec1 = self_backward(grad, qkv, h0, rows, group[0], tokens, BF16 if layer == 0 else F32)
            r_self = reduce(weight_grads(4, (norm1, d_qkv, mix1, grad_bf),
                                            by_column(0, 1, 3, 0) + by_column(2, 3, 1, 3 * depth), 4 * depth))
            side = lambda array, blocks_of: jnp.concatenate(jnp.split(array, blocks_of, 0), 1)
            results[layer] = [side(r_self[:3 * depth], 3), r_self[3 * depth:], r_cross[:depth], side(r_kv, 2), r_cross[depth:],
                              side(r_ff1, 8), r_ff2]
            vec_grads[layer] = jnp.concatenate([vec1[0], vec1[1], vec2[0], vec2[1], vec3[0], vec3[1],
                                                vec1[2], vec2[2], vec3[2], vec_b1[0]])
        vec_full = jnp.stack([jnp.pad(g, (0, vec_len * n_dev - g.shape[0])).reshape(n_dev, vec_len) for g in vec_grads], 1)
        vec_out = scatter_sum(vec_full, n_dev)
        outs = []
        for index in range(7):
            stacked = jnp.stack([results[layer][index] for layer in range(blocks)]) / total
            stacked = lax.optimization_barrier(stacked)
            outs.append(stacked.reshape(blocks, -1))
        outs.append(vec_out / total)
        return tuple([out_tokens.reshape(tokens_x.shape), grad.reshape(tokens_x.shape)] + outs)

    param_spec = P(None, AXIS)
    in_specs = (P(AXIS), P(AXIS), P(AXIS)) + (param_spec,) * 8
    out_specs = (P(AXIS), P(AXIS)) + (param_spec,) * 8
    return jax.shard_map(inner, mesh=mesh, in_specs=in_specs, out_specs=out_specs, check_vma=False)
```

```python
import functools
import math
import jax
import jax.numpy as jnp
from jax import lax
from jax.experimental import pallas as pl
from jax.experimental.pallas import tpu as pltpu
from jax.sharding import PartitionSpec as P


HEAD = 64
AXIS = 'fsdp'
CHUNK = 1280
FF_STEP = 256
STEP = 512
VMEM_LIMIT = 60 * 1024 * 1024
VMEM_MOST = 67043328
FORWARD_UNROLL = 10
BACKWARD_UNROLL = 5

F32 = jnp.float32
BF16 = jnp.bfloat16
ANY = pl.BlockSpec(memory_space=pl.ANY)


def gather_perms(n_dev):
    near = [(i, i ^ (4 if i % 2 == 0 else 2)) for i in range(n_dev)]
    far = [(i, i ^ (2 if i % 2 == 0 else 4)) for i in range(n_dev)]
    core = [(i, i ^ 1) for i in range(n_dev)]
    return near, far, core


def pack_kernel(*refs):
    ins, out = refs[:-1], refs[-1]
    width, row = out.shape[1], 0
    for ref in ins:
        depth = ref.shape[-2]
        for col in range(0, ref.shape[-1], width):
            piece = ref[0, :, col:col + width] if len(ref.shape) == 3 else ref[:, col:col + width]
            out[row:row + depth, :] = piece
            row += depth


def pack(views, layer, extra, width):
    rows = sum(v.shape[1] * v.shape[2] // width for v in views) + sum(e.shape[0] for e in extra)
    specs = [pl.BlockSpec((1,) + v.shape[1:], lambda i: (layer, 0, 0)) for v in views]
    specs += [pl.BlockSpec(e.shape, lambda i: (0, 0)) for e in extra]
    return pl.pallas_call(
        pack_kernel, grid=(1,), in_specs=specs, out_specs=pl.BlockSpec((rows, width), lambda i: (0, 0)),
        out_shape=jax.ShapeDtypeStruct((rows, width), BF16),
        cost_estimate=pl.CostEstimate(flops=rows * width, bytes_accessed=rows * width * 4, transcendentals=0),
        name='pack')(*views, *extra)


def vec_kernel(*refs):
    pieces, (out, buf, sem) = refs[:8], refs[8:]
    rows = out.shape[0]
    copies = [pltpu.make_async_copy(piece.at[pl.ds(piece.shape[0] - rows, rows), :], buf.at[index], sem.at[index])
              for index, piece in enumerate(pieces)]
    for copy in copies:
        copy.start()
    total = None
    for index, copy in enumerate(copies):
        copy.wait()
        total = buf[index].astype(F32) if total is None else total + buf[index].astype(F32)
    out[...] = total


def vec_sum(pieces, rows):
    width = pieces[0].shape[1]
    return pl.pallas_call(
        vec_kernel, in_specs=[ANY] * 8, out_specs=pl.BlockSpec(memory_space=pltpu.VMEM),
        out_shape=jax.ShapeDtypeStruct((rows, width), F32),
        scratch_shapes=[pltpu.VMEM((8, rows, width), BF16), pltpu.SemaphoreType.DMA((8,))],
        cost_estimate=pl.CostEstimate(flops=rows * width * 8, bytes_accessed=rows * width * 20, transcendentals=0),
        name='vec_sum')(*pieces)


def permute(array, perm):
    return lax.ppermute(array, AXIS, perm)


def gather_group(shard, n_dev):
    near, far, core = gather_perms(n_dev)
    first = permute(shard, near)
    second = permute(shard, far)
    third = permute(first, far)
    mine = [shard, first, second, third]
    return mine + [permute(piece, core) for piece in mine]


def piece_devices(me):
    core = lax.rem(me, 2)
    one, two = 4 - 2 * core, 2 + 2 * core
    x = jnp.bitwise_xor
    mate = x(me, 1)
    return [me, x(me, one), x(me, two), x(me, 6), mate, x(mate, two), x(mate, one), x(mate, 6)]


def start_load(pieces, offset, ref, sem):
    width = pieces[0].shape[1]
    depth = ref.shape[0] // 8
    devices = piece_devices(lax.axis_index(AXIS))
    for block in range(ref.shape[1] // width):
        for piece, device in zip(pieces, devices):
            src = piece.at[pl.ds(offset + block * depth, depth), :]
            dst = ref.at[pl.ds(pl.multiple_of(device * depth, 16), depth), pl.ds(block * width, width)]
            pltpu.make_async_copy(src, dst, sem).start()


def wait_load(ref, sem):
    pltpu.make_async_copy(ref, ref, sem).wait()


def dot_nn(a, b):
    return lax.dot_general(a, b, (((1,), (0,)), ((), ())), preferred_element_type=F32)


def dot_nt(a, b):
    return lax.dot_general(a, b, (((1,), (1,)), ((), ())), preferred_element_type=F32)


def norm_stats(x):
    average = jnp.mean(x, axis=-1, keepdims=True)
    centered = x - average
    variance = jnp.mean(centered * centered, axis=-1, keepdims=True)
    scale = lax.rsqrt(variance + 1e-5)
    return centered * scale, scale


def norm_back(x, gain, d_norm):
    unit, scale = norm_stats(x)
    d_unit = d_norm * gain
    inner = d_unit - jnp.mean(d_unit, axis=-1, keepdims=True) - unit * jnp.mean(d_unit * unit, axis=-1, keepdims=True)
    return scale * inner, jnp.sum(d_norm * unit, axis=0, keepdims=True), jnp.sum(d_norm, axis=0, keepdims=True)


def softmax_rows(scores):
    top = jnp.max(scores, axis=-1, keepdims=True)
    raised = jnp.exp(scores - top)
    return raised * (1.0 / jnp.sum(raised, axis=-1, keepdims=True))


def low_lanes(rows):
    return lax.broadcasted_iota(jnp.int32, (rows, 2 * HEAD), 1) < HEAD


def pair_scores(query, key, low, head, valid):
    q_head = jnp.where(low if head == 0 else jnp.logical_not(low), query, jnp.zeros_like(query))
    scores = dot_nt(q_head, key) * HEAD ** -0.5
    if valid is not None:
        column = lax.broadcasted_iota(jnp.int32, scores.shape, 1)
        scores = jnp.where(column < valid, scores, -1e30)
    return q_head, softmax_rows(scores)


def pair_forward(query, key, value, valid=None):
    low = low_lanes(query.shape[0])
    mixed = []
    for head in range(2):
        _, probs = pair_scores(query, key, low, head, valid)
        mixed.append(dot_nn(probs.astype(BF16), value))
    return jnp.where(low, mixed[0], mixed[1]).astype(BF16)


def pair_probs(key, query, low, head, valid):
    q_head = jnp.where(low if head == 0 else jnp.logical_not(low), query, jnp.zeros_like(query))
    scores = dot_nt(key, q_head) * HEAD ** -0.5
    if valid is not None:
        row = lax.broadcasted_iota(jnp.int32, scores.shape, 0)
        scores = jnp.where(row < valid, scores, -1e30)
    top = jnp.max(scores, axis=0, keepdims=True)
    raised = jnp.exp(scores - top)
    return q_head, raised * (1.0 / jnp.sum(raised, axis=0, keepdims=True))


def pair_backward(query, key, value, d_out, valid=None):
    low = low_lanes(query.shape[0])
    turned = key.T
    d_query, d_key, d_value = [], None, None
    for head in range(2):
        q_head, probs = pair_probs(key, query, low, head, valid)
        d_head = jnp.where(low if head == 0 else jnp.logical_not(low), d_out, jnp.zeros_like(d_out))
        d_probs = dot_nt(value, d_head).astype(BF16).astype(F32)
        inner = jnp.sum(d_probs * probs, axis=0, keepdims=True)
        d_scores = ((probs * (d_probs - inner)) * HEAD ** -0.5).astype(BF16)
        d_query.append(dot_nn(turned[head * HEAD:(head + 1) * HEAD, :], d_scores))
        dk, dv = dot_nn(d_scores, q_head), dot_nn(probs.astype(BF16), d_head)
        d_key = dk if d_key is None else d_key + dk
        d_value = dv if d_value is None else d_value + dv
    return jnp.concatenate(d_query, 0).T.astype(BF16), d_key.astype(BF16), d_value.astype(BF16)


def add_rows(ref, step, rows):
    @pl.when(step == 0)
    def _():
        ref[...] = jnp.zeros_like(ref)

    for index, row in enumerate(rows):
        ref[pl.ds(index, 1), :] += row


def self_forward_kernel(samples, tokens, h_ref, rows_ref, *refs):
    pieces, (norm_ref, qkv_ref, mix_ref, out_ref, w_qkv, w_out, sems) = refs[:8], refs[8:]
    width = h_ref.shape[1]
    step = pl.program_id(0)

    @pl.when(step == 0)
    def _():
        start_load(pieces, 0, w_qkv, sems.at[0])
        start_load(pieces, 3 * (width // 8), w_out, sems.at[1])

    x = h_ref[...].astype(F32)
    unit, _ = norm_stats(x)
    normed = (unit * rows_ref[0:1, :] + rows_ref[1:2, :]).astype(BF16)
    norm_ref[...] = normed

    @pl.when(step == 0)
    def _():
        wait_load(w_qkv, sems.at[0])
        wait_load(w_out, sems.at[1])

    qkv_ref[...] = dot_nn(normed, w_qkv[...]).astype(BF16)
    pairs = width // (2 * HEAD)

    def body(index, carry):
        row = pl.multiple_of((index // pairs) * tokens, tokens)
        col = pl.multiple_of((index % pairs) * 2 * HEAD, 2 * HEAD)
        part = lambda which: qkv_ref[pl.ds(row, tokens), pl.ds(which * width + col, 2 * HEAD)]
        mix_ref[pl.ds(row, tokens), pl.ds(col, 2 * HEAD)] = pair_forward(part(0), part(1), part(2))
        return carry

    lax.fori_loop(0, samples * pairs, body, 0, unroll=FORWARD_UNROLL)
    out_ref[...] = x + dot_nn(mix_ref[...], w_out[...]) + rows_ref[6:7, :]


def cross_forward_kernel(samples, tokens, valid, h_ref, rows_ref, ctx_ref, *refs):
    pieces, (norm_ref, query_ref, kv_ref, mix_ref, out_ref, w_kv, w_query, w_out, sems) = refs[:8], refs[8:]
    width = h_ref.shape[1]
    step = pl.program_id(0)
    padded = ctx_ref.shape[0] // (samples * pl.num_programs(0))

    @pl.when(step == 0)
    def _():
        deep, depth = w_kv.shape[0] // 8, width // 8
        start_load(pieces, 0, w_kv, sems.at[0])
        start_load(pieces, 2 * deep, w_query, sems.at[1])
        start_load(pieces, 2 * deep + depth, w_out, sems.at[2])

    x = h_ref[...]
    unit, _ = norm_stats(x)
    normed = (unit * rows_ref[2:3, :] + rows_ref[3:4, :]).astype(BF16)
    norm_ref[...] = normed

    @pl.when(step == 0)
    def _():
        wait_load(w_kv, sems.at[0])
        wait_load(w_query, sems.at[1])
        wait_load(w_out, sems.at[2])
        kv_ref[...] = dot_nn(ctx_ref[...], w_kv[...]).astype(BF16)

    query_ref[...] = dot_nn(normed, w_query[...]).astype(BF16)
    pairs = width // (2 * HEAD)

    def body(index, carry):
        sample = index // pairs
        row = pl.multiple_of(sample * tokens, tokens)
        kv_row = pl.multiple_of((step * samples + sample) * padded, 16)
        col = pl.multiple_of((index % pairs) * 2 * HEAD, 2 * HEAD)
        query = query_ref[pl.ds(row, tokens), pl.ds(col, 2 * HEAD)]
        key = kv_ref[pl.ds(kv_row, padded), pl.ds(col, 2 * HEAD)]
        value = kv_ref[pl.ds(kv_row, padded), pl.ds(width + col, 2 * HEAD)]
        mix_ref[pl.ds(row, tokens), pl.ds(col, 2 * HEAD)] = pair_forward(query, key, value, valid)
        return carry

    lax.fori_loop(0, samples * pairs, body, 0, unroll=FORWARD_UNROLL)
    out_ref[...] = x + dot_nn(mix_ref[...], w_out[...]) + rows_ref[7:8, :]


def ff_loads(pieces, offset, w_ff1, w_ff2, sems):
    start_load(pieces[:8], 0, w_ff1, sems.at[0])
    start_load(pieces[8:], offset, w_ff2, sems.at[1])


def ff_up(normed, bias_ref, w_ff1, half, start, gated_ref, save_a, save_g):
    u_a = dot_nn(normed, w_ff1[:, start:start + CHUNK]) + bias_ref[:, start:start + CHUNK]
    u_g = dot_nn(normed, w_ff1[:, half + start:half + start + CHUNK]) + bias_ref[:, half + start:half + start + CHUNK]
    cumulative = 0.5 * (1.0 + lax.erf(u_g * math.sqrt(0.5)))
    gate = u_g * cumulative
    slope = cumulative + u_g * (jnp.exp(-0.5 * u_g * u_g) * (1.0 / math.sqrt(2.0 * math.pi)))
    gated = (u_a * gate).astype(BF16)
    gated_ref[:, start:start + CHUNK] = gated
    save_a[:, start:start + CHUNK] = gate
    save_g[:, start:start + CHUNK] = u_a * slope
    return gated


def ff_forward_kernel(offset, h_ref, rows_ref, bias_ref, *refs):
    pieces, (norm_ref, gated_ref, save_a, save_g, out_ref, w_ff1, w_ff2, sems) = refs[:16], refs[16:]
    half = w_ff2.shape[0]
    step = pl.program_id(0)

    @pl.when(step == 0)
    def _():
        ff_loads(pieces, offset, w_ff1, w_ff2, sems)

    x = h_ref[...]
    unit, _ = norm_stats(x)
    normed = (unit * rows_ref[4:5, :] + rows_ref[5:6, :]).astype(BF16)
    norm_ref[...] = normed

    @pl.when(step == 0)
    def _():
        wait_load(w_ff1, sems.at[0])
        wait_load(w_ff2, sems.at[1])

    total = x + rows_ref[8:9, :]
    for start in range(0, half, CHUNK):
        gated = ff_up(normed, bias_ref, w_ff1, half, start, gated_ref, save_a, save_g)
        total = total + dot_nn(gated, w_ff2[start:start + CHUNK, :])
    out_ref[...] = total


def ff_up_kernel(h_ref, rows_ref, bias_ref, *refs):
    pieces, (norm_ref, gated_ref, save_a, save_g, w_ff1, sems) = refs[:8], refs[8:]
    half = w_ff1.shape[1] // 2
    step = pl.program_id(0)

    @pl.when(step == 0)
    def _():
        start_load(pieces, 0, w_ff1, sems.at[0])

    unit, _ = norm_stats(h_ref[...])
    normed = (unit * rows_ref[4:5, :] + rows_ref[5:6, :]).astype(BF16)
    norm_ref[...] = normed

    @pl.when(step == 0)
    def _():
        wait_load(w_ff1, sems.at[0])

    for start in range(0, half, CHUNK):
        ff_up(normed, bias_ref, w_ff1, half, start, gated_ref, save_a, save_g)


def ff_down_kernel(h_ref, rows_ref, gated_ref, *refs):
    pieces, (out_ref, w_ff2, sems) = refs[:8], refs[8:]
    step = pl.program_id(0)

    @pl.when(step == 0)
    def _():
        start_load(pieces, 0, w_ff2, sems.at[0])
        wait_load(w_ff2, sems.at[0])

    out_ref[...] = (h_ref[...] + rows_ref[8:9, :] + dot_nn(gated_ref[...], w_ff2[...])).astype(BF16)


def cross_backward_kernel(samples, tokens, valid, grad_ref, query_ref, kv_ref, h_ref, rows_ref, *refs):
    pieces, (grad_bf_ref, d_query_ref, d_kv_ref, out_ref, vec_ref, d_mix, w_query, w_out, sems) = refs[:8], refs[8:]
    width = h_ref.shape[1]
    step = pl.program_id(0)
    padded = kv_ref.shape[0] // samples

    @pl.when(step == 0)
    def _():
        depth = width // 8
        base = pieces[0].shape[0] - 2 * depth
        start_load(pieces, base, w_query, sems.at[0])
        start_load(pieces, base + depth, w_out, sems.at[1])

    grad = grad_ref[...]
    grad_bf = grad.astype(BF16)
    grad_bf_ref[...] = grad_bf

    @pl.when(step == 0)
    def _():
        wait_load(w_query, sems.at[0])
        wait_load(w_out, sems.at[1])

    d_mix[...] = dot_nt(grad_bf, w_out[...]).astype(BF16)
    pairs = width // (2 * HEAD)

    def body(index, carry):
        sample = index // pairs
        row = pl.multiple_of(sample * tokens, tokens)
        kv_row = pl.multiple_of(sample * padded, 16)
        col = pl.multiple_of((index % pairs) * 2 * HEAD, 2 * HEAD)
        at = (pl.ds(row, tokens), pl.ds(col, 2 * HEAD))
        at_key = (pl.ds(kv_row, padded), pl.ds(col, 2 * HEAD))
        at_value = (pl.ds(kv_row, padded), pl.ds(width + col, 2 * HEAD))
        dq, dk, dv = pair_backward(query_ref[at], kv_ref[at_key], kv_ref[at_value], d_mix[at], valid)
        d_query_ref[at] = dq
        d_kv_ref[at_key] = dk
        d_kv_ref[at_value] = dv
        return carry

    lax.fori_loop(0, samples * pairs, body, 0, unroll=BACKWARD_UNROLL)
    d_norm = dot_nt(d_query_ref[...], w_query[...])
    d_res, g_gain, g_shift = norm_back(h_ref[...], rows_ref[2:3, :], d_norm)
    out_ref[...] = grad + d_res
    add_rows(vec_ref, step, [g_gain, g_shift, jnp.sum(grad, axis=0, keepdims=True)])


def self_backward_kernel(samples, tokens, grad_ref, qkv_ref, h_ref, rows_ref, *refs):
    pieces, (grad_bf_ref, d_qkv_ref, out_ref, vec_ref, d_mix, w_qkv, w_out, sems) = refs[:8], refs[8:]
    width = h_ref.shape[1]
    step = pl.program_id(0)

    @pl.when(step == 0)
    def _():
        start_load(pieces, 0, w_qkv, sems.at[0])
        start_load(pieces, 3 * (width // 8), w_out, sems.at[1])

    grad = grad_ref[...]
    grad_bf = grad.astype(BF16)
    grad_bf_ref[...] = grad_bf

    @pl.when(step == 0)
    def _():
        wait_load(w_qkv, sems.at[0])
        wait_load(w_out, sems.at[1])

    d_mix[...] = dot_nt(grad_bf, w_out[...]).astype(BF16)
    pairs = width // (2 * HEAD)

    def body(index, carry):
        row = pl.multiple_of((index // pairs) * tokens, tokens)
        col = pl.multiple_of((index % pairs) * 2 * HEAD, 2 * HEAD)
        at = lambda which: (pl.ds(row, tokens), pl.ds(which * width + col, 2 * HEAD))
        d_parts = pair_backward(qkv_ref[at(0)], qkv_ref[at(1)], qkv_ref[at(2)], d_mix[at(0)])
        for which in range(3):
            d_qkv_ref[at(which)] = d_parts[which]
        return carry

    lax.fori_loop(0, samples * pairs, body, 0, unroll=BACKWARD_UNROLL)
    d_norm = dot_nt(d_qkv_ref[...], w_qkv[...])
    d_res, g_gain, g_shift = norm_back(h_ref[...].astype(F32), rows_ref[0:1, :], d_norm)
    out_ref[...] = (grad + d_res).astype(out_ref.dtype)
    add_rows(vec_ref, step, [g_gain, g_shift, jnp.sum(grad, axis=0, keepdims=True)])


def by_step(rows, columns):
    return pl.BlockSpec((rows, columns), lambda i: (i, 0))


def whole(rows, columns):
    return pl.BlockSpec((rows, columns), lambda i: (0, 0))


def shape(rows, columns, dtype):
    return jax.ShapeDtypeStruct((rows, columns), dtype)


def call(kernel, steps, in_specs, out_specs, out_shapes, scratch, flops, moved):
    return pl.pallas_call(
        kernel, grid=(steps,), in_specs=in_specs, out_specs=out_specs, out_shape=out_shapes, scratch_shapes=scratch,
        cost_estimate=pl.CostEstimate(flops=int(flops), bytes_accessed=int(moved), transcendentals=0),
        compiler_params=pltpu.CompilerParams(dimension_semantics=('arbitrary',), vmem_limit_bytes=VMEM_LIMIT))


def self_forward(h, rows, pieces, tokens):
    count, width = h.shape
    return call(
        functools.partial(self_forward_kernel, STEP // tokens, tokens), count // STEP,
        [by_step(STEP, width), whole(*rows.shape)] + [ANY] * 8,
        [by_step(STEP, width), by_step(STEP, 3 * width), by_step(STEP, width), by_step(STEP, width)],
        [shape(count, width, BF16), shape(count, 3 * width, BF16), shape(count, width, BF16), shape(count, width, F32)],
        [pltpu.VMEM((width, 3 * width), BF16), pltpu.VMEM((width, width), BF16), pltpu.SemaphoreType.DMA((2,))],
        count * width * width * 8 + count * tokens * width * 4, 2e7)(h, rows, *pieces)


def cross_forward(h, rows, ctx, pieces, tokens, valid):
    count, width = h.shape
    ctx_rows, ctx_width = ctx.shape
    return call(
        functools.partial(cross_forward_kernel, STEP // tokens, tokens, valid), count // STEP,
        [by_step(STEP, width), whole(*rows.shape), whole(ctx_rows, ctx_width)] + [ANY] * 8,
        [by_step(STEP, width), by_step(STEP, width), whole(ctx_rows, 2 * width), by_step(STEP, width), by_step(STEP, width)],
        [shape(count, width, BF16), shape(count, width, BF16), shape(ctx_rows, 2 * width, BF16), shape(count, width, BF16),
         shape(count, width, F32)],
        [pltpu.VMEM((ctx_width, 2 * width), BF16), pltpu.VMEM((width, width), BF16), pltpu.VMEM((width, width), BF16),
         pltpu.SemaphoreType.DMA((3,))],
        count * width * width * 4 + ctx_rows * ctx_width * width * 4 + count * 128 * width * 4, 2e7)(h, rows, ctx, *pieces)


def ff_forward(h, rows, bias, pieces, offset):
    count, width = h.shape
    half = bias.shape[1] // 2
    return call(
        functools.partial(ff_forward_kernel, offset), count // FF_STEP,
        [by_step(FF_STEP, width), whole(*rows.shape), whole(1, 2 * half)] + [ANY] * 16,
        [by_step(FF_STEP, width), by_step(FF_STEP, half), by_step(FF_STEP, half), by_step(FF_STEP, half), by_step(FF_STEP, width)],
        [shape(count, width, BF16), shape(count, half, BF16), shape(count, half, F32), shape(count, half, F32),
         shape(count, width, F32)],
        [pltpu.VMEM((width, 2 * half), BF16), pltpu.VMEM((half, width), BF16), pltpu.SemaphoreType.DMA((2,))],
        count * width * half * 6, 6e7)(h, rows, bias, *pieces)


def ff_up_forward(h, rows, bias, pieces):
    count, width = h.shape
    half = bias.shape[1] // 2
    return call(
        ff_up_kernel, count // FF_STEP,
        [by_step(FF_STEP, width), whole(*rows.shape), whole(1, 2 * half)] + [ANY] * 8,
        [by_step(FF_STEP, width), by_step(FF_STEP, half), by_step(FF_STEP, half), by_step(FF_STEP, half)],
        [shape(count, width, BF16), shape(count, half, BF16), shape(count, half, F32), shape(count, half, F32)],
        [pltpu.VMEM((width, 2 * half), BF16), pltpu.SemaphoreType.DMA((1,))],
        count * width * half * 4, 5e7)(h, rows, bias, *pieces)


def ff_down_forward(h, rows, gated, pieces):
    count, width = h.shape
    half = gated.shape[1]
    return call(
        ff_down_kernel, count // STEP,
        [by_step(STEP, width), whole(*rows.shape), by_step(STEP, half)] + [ANY] * 8,
        by_step(STEP, width), shape(count, width, BF16),
        [pltpu.VMEM((half, width), BF16), pltpu.SemaphoreType.DMA((1,))],
        count * width * half * 2, 2e7)(h, rows, gated, *pieces)


def cross_backward(grad, query, kv, h, rows, pieces, tokens, valid):
    count, width = h.shape
    ctx_rows = kv.shape[0]
    steps = count // STEP
    return call(
        functools.partial(cross_backward_kernel, STEP // tokens, tokens, valid), steps,
        [by_step(STEP, width), by_step(STEP, width), by_step(ctx_rows // steps, 2 * width), by_step(STEP, width),
         whole(*rows.shape)] + [ANY] * 8,
        [by_step(STEP, width), by_step(STEP, width), by_step(ctx_rows // steps, 2 * width), by_step(STEP, width), whole(8, width)],
        [shape(count, width, BF16), shape(count, width, BF16), shape(ctx_rows, 2 * width, BF16), shape(count, width, F32),
         shape(8, width, F32)],
        [pltpu.VMEM((STEP, width), BF16), pltpu.VMEM((width, width), BF16), pltpu.VMEM((width, width), BF16),
         pltpu.SemaphoreType.DMA((2,))],
        count * width * width * 4 + count * 128 * width * 10, 2e7)(grad, query, kv, h, rows, *pieces)


def self_backward(grad, qkv, h, rows, pieces, tokens, out_dtype):
    count, width = h.shape
    return call(
        functools.partial(self_backward_kernel, STEP // tokens, tokens), count // STEP,
        [by_step(STEP, width), by_step(STEP, 3 * width), by_step(STEP, width), whole(*rows.shape)] + [ANY] * 8,
        [by_step(STEP, width), by_step(STEP, 3 * width), by_step(STEP, width), whole(8, width)],
        [shape(count, width, BF16), shape(count, 3 * width, BF16), shape(count, width, out_dtype), shape(8, width, F32)],
        [pltpu.VMEM((STEP, width), BF16), pltpu.VMEM((width, 3 * width), BF16), pltpu.VMEM((width, width), BF16),
         pltpu.SemaphoreType.DMA((2,))],
        count * width * width * 8 + count * tokens * width * 10, 3e7)(grad, qkv, h, rows, *pieces)


def grad_kernel(tiles, group_rows, inputs, with_context, *refs):
    ins, refs = refs[:inputs], refs[inputs:]
    far_ref, keep_ref, x_buf, turned, y_buf, tile, own, recv, x_sem, y_sem, send_sem, recv_sem = refs[:12]
    width, summed = tile.shape[1], own.shape[1]
    me = lax.axis_index(AXIS)
    core, chip = lax.rem(me, 2), me // 2
    mate = me + 1 - 2 * core
    chip_x, chip_y = lax.rem(chip, 2), chip // 2

    xs, ys, x_of, y_of = [], [], [], []
    for x, x_col, y, y_col, *_ in tiles:
        if not xs or xs[-1] != (x, x_col):
            xs.append((x, x_col))
        if not ys or ys[-1] != (y, y_col):
            ys.append((y, y_col))
        x_of.append(len(xs) - 1)
        y_of.append(len(ys) - 1)

    def load(which, sequence, buf, sem):
        array, col = sequence[which]
        return pltpu.make_async_copy(ins[array].at[:, pl.ds(col, width)], buf.at[which % 2], sem.at[which % 2])

    for which in range(2):
        if which < len(xs):
            load(which, xs, x_buf, x_sem).start()
        if which < len(ys):
            load(which, ys, y_buf, y_sem).start()

    barrier = pltpu.get_barrier_semaphore()
    pl.semaphore_signal(barrier, inc=1, device_id=(mate,), device_id_type=pl.DeviceIdType.MESH)
    pl.semaphore_wait(barrier, 1)

    if with_context:
        kv_ref, ctx_refs = ins[-3], ins[-2:]
        kv_mine, kv_other, ctx_mine, ctx_other, kv_sem, kv_send, kv_recv = refs[12:]
        exchange = pltpu.make_async_remote_copy(
            src_ref=kv_ref, dst_ref=kv_other, send_sem=kv_send, recv_sem=kv_recv, device_id=(mate,),
            device_id_type=pl.DeviceIdType.MESH)
        exchange.start()
        kv_loads = [pltpu.make_async_copy(src, dst, kv_sem.at[index])
                    for index, (src, dst) in enumerate(((kv_ref, kv_mine), (ctx_refs[0], ctx_mine), (ctx_refs[1], ctx_other)))]
        for copy in kv_loads:
            copy.start()

    def sends(q):
        *_, first_row, rows, chips = tiles[q]
        copies = []
        for index, other in enumerate(chips):
            d_x, d_y = lax.rem(chip_x + other % 2, 2), lax.rem(chip_y + other // 2, 2)
            slot = d_x + 2 * d_y + core * (d_x - d_y)
            start = pl.multiple_of((2 * index + 1 - core) * rows, 16)
            copies.append(pltpu.make_async_remote_copy(
                src_ref=tile.at[q % 3, pl.ds(start, rows), :], dst_ref=recv.at[slot, pl.ds(first_row, rows), :],
                send_sem=send_sem.at[q % 3, index], recv_sem=recv_sem.at[q, index],
                device_id=(mate,), device_id_type=pl.DeviceIdType.MESH))
        return copies

    for q, (x, x_col, y, y_col, first_row, rows, chips) in enumerate(tiles):
        if q == 0 or x_of[q] != x_of[q - 1]:
            which = x_of[q]
            load(which, xs, x_buf, x_sem).wait()
            turned[...] = x_buf[which % 2].T
            if which + 2 < len(xs):
                load(which + 2, xs, x_buf, x_sem).start()
        if q == 0 or y_of[q] != y_of[q - 1]:
            load(y_of[q], ys, y_buf, y_sem).wait()
        if q >= 3:
            for copy in sends(q - 3):
                copy.wait_send()
        tile[q % 3] = dot_nn(turned[...], y_buf[y_of[q] % 2])
        if (q + 1 == len(tiles) or y_of[q + 1] != y_of[q]) and y_of[q] + 2 < len(ys):
            load(y_of[q] + 2, ys, y_buf, y_sem).start()
        for index, other in enumerate(chips):
            d_x, d_y = lax.rem(chip_x + other % 2, 2), lax.rem(chip_y + other // 2, 2)
            slot = 2 * d_x + d_y + core * (d_y - d_x)
            start = pl.multiple_of((2 * index + core) * rows, 16)
            own[slot, first_row:first_row + rows, :] = tile[q % 3, pl.ds(start, rows), :]
        if q >= 1:
            for copy in sends(q - 1):
                copy.start()
    last = len(tiles) - 1
    for copy in sends(last):
        copy.start()
    if with_context:
        for copy in kv_loads:
            copy.wait()
        depth = ctx_mine.shape[0] // 4
        at = lambda slot, block: slice((slot % 2) * group_rows + summed + block * depth, (slot % 2) * group_rows + summed + (block + 1) * depth)
        for pair, (ctx, kv) in enumerate(((ctx_mine, kv_mine), (ctx_other, kv_other))):
            if pair == 1:
                exchange.wait()
            for slot in range(4):
                ref = keep_ref if slot < 2 else far_ref
                for block in range(2):
                    part = dot_nn(ctx[slot * depth:(slot + 1) * depth, :], kv[:, block * width:(block + 1) * width])
                    ref[at(slot, block), :] = part if pair == 0 else ref[at(slot, block), :] + part
    for q in range(max(0, last - 2), last + 1):
        for copy in sends(q):
            copy.wait_send()
    for q in range(last + 1):
        for copy in sends(q):
            copy.wait_recv()
    for slot in range(4):
        ref = keep_ref if slot < 2 else far_ref
        ref[(slot % 2) * group_rows:(slot % 2) * group_rows + summed, :] = own[slot] + recv[slot]


def weight_grads(kind, arrays, tiles, summed, context=None):
    count, width = arrays[0].shape[0], 640
    chips = max(len(t[-1]) for t in tiles)
    extra, more, group_rows = [], [], summed
    dma = pltpu.SemaphoreType.DMA
    if context is not None:
        more = list(context)
        group_rows += context[1].shape[0] // 2
        extra = [pltpu.VMEM(context[0].shape, BF16)] * 2 + [pltpu.VMEM(context[1].shape, BF16)] * 2 + [dma((3,)), dma, dma]
    out = jax.ShapeDtypeStruct((2 * group_rows, width), F32)
    return pl.pallas_call(
        functools.partial(grad_kernel, tiles, group_rows, len(arrays) + len(more), context is not None),
        in_specs=[ANY] * (len(arrays) + len(more)),
        out_specs=[pl.BlockSpec(memory_space=pltpu.VMEM)] * 2, out_shape=[out, out],
        scratch_shapes=[pltpu.VMEM((2, count, width), BF16), pltpu.VMEM((width, count), BF16), pltpu.VMEM((2, count, width), BF16),
                        pltpu.VMEM((3, width, width), F32), pltpu.VMEM((4, summed, width), F32),
                        pltpu.VMEM((4, summed, width), F32), dma((2,)), dma((2,)), dma((3, chips)), dma((len(tiles), chips))]
        + extra,
        cost_estimate=pl.CostEstimate(flops=2 * count * width * width * (len(tiles) + 2 * (context is not None)),
                                      bytes_accessed=int(2e7), transcendentals=0),
        compiler_params=pltpu.CompilerParams(collective_id=kind, has_side_effects=True, vmem_limit_bytes=VMEM_LIMIT))(*arrays, *more)


def context_kernel(context_ref, ctx_ref, mine_ref, other_ref):
    batch, valid, _ = context_ref.shape
    padded = ctx_ref.shape[0] // batch
    me = lax.axis_index(AXIS)
    core, chip = lax.rem(me, 2), me // 2
    ctx_ref[...] = jnp.zeros_like(ctx_ref)
    for sample in range(batch):
        ctx_ref[sample * padded:sample * padded + valid, :] = context_ref[sample]
    each = mine_ref.shape[0] // 4
    x = jnp.bitwise_xor
    for of_core, ref in ((core, mine_ref), (1 - core, other_ref)):
        for slot, other in enumerate((chip, x(chip, 2 - of_core), x(chip, 1 + of_core), x(chip, 3))):
            column = pl.multiple_of((2 * other + of_core) * each, each)
            ref[slot * each:(slot + 1) * each, :] = ctx_ref[:, pl.ds(column, each)].T


def prepare_context(context, n_dev):
    batch, valid, ctx_width = context.shape
    rows = batch * ((valid + 15) // 16 * 16)
    vmem = pl.BlockSpec(memory_space=pltpu.VMEM)
    turned = shape(ctx_width // 2, rows, BF16)
    ctx, mine, other = pl.pallas_call(
        context_kernel, in_specs=[vmem], out_specs=[vmem] * 3, out_shape=[shape(rows, ctx_width, BF16), turned, turned],
        cost_estimate=pl.CostEstimate(flops=rows * ctx_width * 8, bytes_accessed=int(8e6), transcendentals=0),
        name='context')(context)
    return ctx, mine, permute(other, gather_perms(n_dev)[2])


def vec_pack_kernel(*refs):
    ins, out = refs[:-1], refs[-1]
    width = out.shape[1]
    out[...] = jnp.zeros_like(out)
    for layer in range(len(ins) // 4):
        first, second, third, bias = ins[4 * layer:4 * layer + 4]
        rows = [(first, 0), (first, 1), (second, 0), (second, 1), (third, 0), (third, 1), (first, 2), (second, 2), (third, 2)]
        for index, (ref, row) in enumerate(rows):
            out[17 * layer + index:17 * layer + index + 1, :] = ref[row:row + 1, :]
        for index in range(8):
            row = 17 * layer + 9 + index
            out[row:row + 1, :] = bias[0:1, index * width:(index + 1) * width]


def vec_total(parts, rows, n_dev):
    vmem = pl.BlockSpec(memory_space=pltpu.VMEM)
    width = parts[0].shape[1]
    total = pl.pallas_call(
        vec_pack_kernel, in_specs=[vmem] * len(parts), out_specs=vmem, out_shape=shape(rows, width, F32),
        cost_estimate=pl.CostEstimate(flops=rows * width, bytes_accessed=rows * width * 8, transcendentals=0),
        name='vec_pack')(*parts)
    near, far, core = gather_perms(n_dev)
    for perm in (core, far, near):
        total = total + permute(total, perm)
    return total


def ff_grad_kernel(offset, with_down, grad_ref, save_a, save_g, norm_ref, h_ref, rows_ref, *refs):
    gated_ref, refs = (refs[0], refs[1:]) if with_down else (None, refs)
    pieces, refs = refs[:16], refs[16:]
    out_ref, vec_ref, bias_ref, far1, keep1 = refs[:5]
    far2, keep2 = refs[5:7] if with_down else (None, None)
    (grad, grad_bf, turned, acc, part_a, part_g, d_a, d_g, w_ff1, w_ff2, tile, recv1, obuf,
     in_sem, part_sem, w1_sem, w2_sem, out_sem, send_sem, recv_sem1) = refs[7 if with_down else 5:][:20]
    if with_down:
        z_buf, z_turned, recv2, z_sem, recv_sem2 = refs[-5:]
    count, width = grad.shape
    half = w_ff2.shape[0]
    chunks, each = half // width, STEP
    steps = count // each
    depth, deep = width // 8, half // 8
    me = lax.axis_index(AXIS)
    core, chip = lax.rem(me, 2), me // 2
    mate = me + 1 - 2 * core
    chip_x, chip_y = lax.rem(chip, 2), chip // 2

    def slot_of(other, of_mate):
        d_x, d_y = lax.rem(chip_x + other % 2, 2), lax.rem(chip_y + other // 2, 2)
        return d_x + 2 * d_y + core * (d_x - d_y) if of_mate else 2 * d_x + d_y + core * (d_y - d_x)

    def chip_in(slot):
        one, two = slot // 2, slot % 2
        d_x, d_y = one + core * (two - one), two + core * (one - two)
        return 2 * lax.rem(chip_y + d_y, 2) + lax.rem(chip_x + d_x, 2)

    load_grad = pltpu.make_async_copy(grad_ref, grad, in_sem.at[0])
    load_norm = pltpu.make_async_copy(norm_ref, d_a, in_sem.at[1])
    load_grad.start()
    load_norm.start()
    start_load(pieces[8:], offset, w_ff2, w2_sem)

    def parts(index):
        chunk, step = index // steps, index % steps
        at = (pl.ds(pl.multiple_of(step * each, each), each), pl.ds(pl.multiple_of(chunk * width, width), width))
        return [pltpu.make_async_copy(ref.at[at], buf.at[index % 2], part_sem.at[which, index % 2])
                for which, (ref, buf) in enumerate(((save_a, part_a), (save_g, part_g)))]

    def load_h(step):
        return pltpu.make_async_copy(h_ref.at[pl.ds(step * each, each), :], part_a.at[step % 2], part_sem.at[0, step % 2])

    for copy in parts(0):
        copy.start()
    devices = piece_devices(me)
    for block in [b + k for b in range(chunks) for k in (0, chunks)]:
        for piece, device in zip(pieces[:8], devices):
            pltpu.make_async_copy(piece.at[pl.ds(block * depth, depth), :],
                                  w_ff1.at[pl.ds(pl.multiple_of(device * depth, 16), depth), pl.ds(block * width, width)],
                                  w1_sem.at[block]).start()
    for copy in parts(1):
        copy.start()

    barrier = pltpu.get_barrier_semaphore()
    pl.semaphore_signal(barrier, inc=1, device_id=(mate,), device_id_type=pl.DeviceIdType.MESH)
    pl.semaphore_wait(barrier, 1)

    def load_z(chunk):
        return pltpu.make_async_copy(gated_ref.at[:, pl.ds(pl.multiple_of(chunk * width, width), width)], z_buf, z_sem)

    if with_down:
        load_z(0).start()

    kinds = (0, 1, 2) if with_down else (0, 1)

    def sends(kind, chunk):
        copies = []
        for index in range(4 if kind < 2 else 1):
            rows = depth if kind < 2 else deep
            start = pl.multiple_of((2 * index + 1 - core) * rows, 16)
            if kind < 2:
                block = kind * chunks + chunk
                slot = slot_of(index, True)
                dst = recv1.at[block, pl.ds(pl.multiple_of(slot * rows, 16), rows), :]
            else:
                dst = recv2.at[chunk]
            copies.append(pltpu.make_async_remote_copy(
                src_ref=tile.at[kind, pl.ds(start, rows), :], dst_ref=dst, send_sem=send_sem.at[kind, index],
                recv_sem=recv_sem1.at[block, index] if kind < 2 else recv_sem2.at[chunk],
                device_id=(mate,), device_id_type=pl.DeviceIdType.MESH))
        return copies

    def wait_write(kind):
        pltpu.make_async_copy(obuf.at[kind], obuf.at[kind], out_sem.at[kind]).wait()

    def finish(kind, chunk, first):
        for copy in sends(kind, chunk):
            copy.wait_recv()

        @pl.when(jnp.logical_not(first))
        def _():
            wait_write(kind)

        if kind < 2:
            block = kind * chunks + chunk
            for slot in range(4):
                start = pl.multiple_of((2 * chip_in(slot) + core) * depth, 16)
                rows = slice(slot * depth, (slot + 1) * depth)
                obuf[kind, rows, :] = tile[kind, pl.ds(start, depth), :] + recv1[block, rows, :]
            for slot in range(4):
                ref = keep1 if slot < 2 else far1
                row = pl.multiple_of((slot % 2) * 8 * depth + block * depth, 16)
                pltpu.make_async_copy(obuf.at[kind, pl.ds(slot * depth, depth), :], ref.at[pl.ds(row, depth), :],
                                      out_sem.at[kind]).start()
        else:
            obuf[kind] = tile[kind, pl.ds(pl.multiple_of(core * deep, 16), deep), :] + recv2[chunk]
            slot = slot_of(chunk, False)
            row = pl.multiple_of(lax.rem(slot, 2) * deep, 16)
            for branch, ref in enumerate((keep2, far2)):
                @pl.when(slot // 2 == branch)
                def _():
                    pltpu.make_async_copy(obuf.at[kind], ref.at[pl.ds(row, deep), :], out_sem.at[kind]).start()
        for copy in sends(kind, chunk):
            copy.wait_send()

    load_grad.wait()
    grad_bf[...] = grad[...].astype(BF16)
    load_norm.wait()
    turned[...] = d_a[...].T
    acc[...] = jnp.zeros_like(acc)
    bias_ref[...] = jnp.zeros_like(bias_ref)
    vec_ref[...] = jnp.zeros_like(vec_ref)
    wait_load(w_ff2, w2_sem)

    def one_chunk(chunk, carry):
        for block in (chunk, chunks + chunk):
            ref = w_ff1.at[:, pl.ds(0, width)]
            pltpu.make_async_copy(ref, ref, w1_sem.at[block]).wait()
        hidden = pl.multiple_of(chunk * width, width)

        def one_step(step, carry):
            index = chunk * steps + step
            even = lax.rem(index, 2)
            rows = pl.ds(pl.multiple_of(step * each, each), each)
            d_gated = dot_nt(grad_bf[rows, :], w_ff2[pl.ds(hidden, width), :])
            for copy in parts(index):
                copy.wait()
            total = acc[rows, :]
            for base, saved, kept in ((0, part_a, d_a), (half, part_g, d_g)):
                columns = pl.ds(pl.multiple_of(base + hidden, 2 * HEAD), width)
                d_part = d_gated * saved[even]
                bias_ref[0:1, columns] += jnp.sum(d_part, axis=0, keepdims=True)
                d_part = d_part.astype(BF16)
                kept[rows, :] = d_part
                total = total + dot_nt(d_part, w_ff1[:, columns])
            acc[rows, :] = total

            @pl.when(index + 2 < chunks * steps)
            def _():
                for copy in parts(index + 2):
                    copy.start()

            return carry

        lax.fori_loop(0, steps, one_step, 0)
        before = jnp.maximum(chunk - 1, 0)
        for kind in kinds:
            @pl.when(chunk > 0)
            def _():
                finish(kind, before, chunk == 1)

            if kind < 2:
                tile[kind] = dot_nn(turned[...], (d_a, d_g)[kind][...])
            else:
                load_z(chunk).wait()
                z_turned[...] = z_buf[...].T

                @pl.when(chunk + 1 < chunks)
                def _():
                    load_z(chunk + 1).start()

                tile[kind] = dot_nn(z_turned[...], grad_bf[...])
            if kind > 0:
                for copy in sends(kind - 1, chunk):
                    copy.start()
        for copy in sends(kinds[-1], chunk):
            copy.start()
        return carry

    lax.fori_loop(0, chunks, one_chunk, 0)
    load_h(0).start()
    load_h(1).start()
    for step in range(steps):
        rows = slice(step * each, (step + 1) * each)
        load_h(step).wait()
        mine = grad[rows, :].astype(F32)
        d_res, g_gain, g_shift = norm_back(part_a[step % 2], rows_ref[4:5, :], acc[rows, :])
        if step + 2 < steps:
            load_h(step + 2).start()
        acc[rows, :] = mine + d_res
        pltpu.make_async_copy(acc.at[pl.ds(step * each, each), :], out_ref.at[pl.ds(step * each, each), :], in_sem.at[0]).start()
        for at, row in enumerate((g_gain, g_shift, jnp.sum(mine, axis=0, keepdims=True))):
            vec_ref[at:at + 1, :] += row
    for kind in kinds:
        finish(kind, chunks - 1, False)
    for kind in kinds:
        wait_write(kind)
    pltpu.make_async_copy(acc, out_ref, in_sem.at[0]).wait()


def ff_grads(kind, grad, save_a, save_g, norm, h, rows, gated, pieces, offset):
    count, width = h.shape
    half = save_a.shape[1]
    down = gated is not None
    vmem = pl.BlockSpec(memory_space=pltpu.VMEM)
    big, small = shape(2 * width, width, F32), shape(half // 4, width, F32)
    dma = pltpu.SemaphoreType.DMA
    scratch = [pltpu.VMEM((count, width), grad.dtype), pltpu.VMEM((count, width), BF16), pltpu.VMEM((width, count), BF16),
               pltpu.VMEM((count, width), F32), pltpu.VMEM((2, STEP, width), F32), pltpu.VMEM((2, STEP, width), F32),
               pltpu.VMEM((count, width), BF16), pltpu.VMEM((count, width), BF16), pltpu.VMEM((width, 2 * half), BF16),
               pltpu.VMEM((half, width), BF16), pltpu.VMEM((2 + down, width, width), F32), pltpu.VMEM((8, width // 2, width), F32),
               pltpu.VMEM((2 + down, width // 2, width), F32), dma((2,)), dma((2, 2)), dma((8,)), dma, dma((3,)), dma((3, 4)), dma((8, 4))]
    if down:
        scratch += [pltpu.VMEM((count, width), BF16), pltpu.VMEM((width, count), BF16), pltpu.VMEM((4, half // 8, width), F32),
                    dma, dma((4,))]
    return pl.pallas_call(
        functools.partial(ff_grad_kernel, offset, down),
        in_specs=[ANY] * 5 + [vmem] + [ANY] * (16 + down),
        out_specs=[ANY, vmem, vmem, ANY, ANY] + [ANY, ANY] * down,
        out_shape=[shape(count, width, F32), shape(8, width, F32), shape(8, 2 * half, F32), big, big] + [small, small] * down,
        scratch_shapes=scratch,
        cost_estimate=pl.CostEstimate(flops=count * width * half * (14 if down else 10), bytes_accessed=int(6e7), transcendentals=0),
        compiler_params=pltpu.CompilerParams(collective_id=kind, has_side_effects=True, vmem_limit_bytes=VMEM_MOST))(grad, save_a, save_g, norm, h, rows, *([gated] if down else []), *pieces)


def finish_scatter(far, keep, n_dev):
    near_perm, far_perm, _ = gather_perms(n_dev)
    rows = keep.shape[0] // 2
    second = permute(far, far_perm)
    third = permute(keep[rows:] + second[rows:], near_perm)
    return keep[:rows] + second[:rows] + third


def solution(mesh):
    n_dev = mesh.shape[AXIS]

    def inner(tokens_x, context, cot_out, *shards):
        batch, tokens, width = tokens_x.shape
        _, valid, ctx_width = context.shape
        blocks = shards[0].shape[0]
        total = batch * n_dev
        depth = width // n_dev
        count = batch * tokens
        half = 4 * width

        views = []
        for shard, rows in zip(shards[:7], (depth, depth, depth, ctx_width // n_dev, depth, depth, half // n_dev)):
            views.append(shard.reshape(blocks, rows, -1))
        qkv_s, out_s = lax.optimization_barrier(views[:2])
        q2_s, kv2_s, out2_s = lax.optimization_barrier(views[2:5])
        ff1_s, ff2_s = lax.optimization_barrier(views[5:])
        me = lax.axis_index(AXIS)
        vec_len = shards[7].shape[1]
        vec_each = 17
        vec_rows = (blocks * vec_each + 15) // 16 * 16
        vec_block = lax.dynamic_update_slice(jnp.zeros((blocks, n_dev * vec_len), BF16), shards[7], (0, me * vec_len))
        vec_block = vec_block[:, :vec_each * width].reshape(blocks * vec_each, width)
        vec_block = jnp.pad(vec_block, ((0, vec_rows - blocks * vec_each), (0, 0)))

        members = []
        for layer in range(blocks):
            members += [(layer, [qkv_s, out_s]), (layer, [kv2_s, q2_s, out2_s])]
            members += [(layer, [ff1_s, ff2_s])] if layer < blocks - 1 else [(layer, [ff1_s]), (layer, [ff2_s])]
        groups = []
        for index, (layer, parts) in enumerate(members):
            block = pack(parts, layer, [vec_block] if index == 0 else [], width)
            groups.append(gather_group(block, n_dev))
        ff_groups = [groups[3 * layer + 2] * 2 if layer < blocks - 1 else groups[-2] + groups[-1] for layer in range(blocks)]
        ff_offsets = [8 * depth if layer < blocks - 1 else 0 for layer in range(blocks)]

        vecs = vec_sum(groups[0], vec_rows)
        vecs = vecs[:blocks * vec_each].reshape(blocks, vec_each, width)
        rows_all = jnp.pad(vecs[:, :9], ((0, 0), (0, 7), (0, 0)))
        bias_all = vecs[:, 9:].reshape(blocks, 1, 8 * width)

        ctx, ctx_mine, ctx_other = prepare_context(context, n_dev)

        h = tokens_x.reshape(count, width)
        saved = []
        for layer in range(blocks):
            rows, bias = rows_all[layer], bias_all[layer]
            group = groups[3 * layer:3 * layer + 2]
            norm1, qkv, mix1, h1 = self_forward(h, rows, group[0], tokens)
            norm2, query, kv, mix2, h2 = cross_forward(h1, rows, ctx, group[1], tokens, valid)
            if layer < blocks - 1:
                norm3, gated, save_a, save_g, h3 = ff_forward(h2, rows, bias, ff_groups[layer], ff_offsets[layer])
            else:
                norm3, gated, save_a, save_g = ff_up_forward(h2, rows, bias, groups[-2])
                out_tokens = ff_down_forward(h2, rows, gated, groups[-1])
            saved.append((h, norm1, qkv, mix1, h1, norm2, query, kv, mix2, h2, norm3, gated, save_a, save_g))
            h = h3 if layer < blocks - 1 else None

        grad = cot_out.reshape(count, width)
        results, vec_grads = [None] * blocks, [None] * blocks
        every = tuple(range(n_dev // 2))
        by_column = lambda x, y, columns, first: [(x, 0, y, c * width, first + c * depth, depth, every) for c in range(columns)]
        for layer in reversed(range(blocks)):
            turn = blocks - 1 - layer
            rows, group = rows_all[layer], groups[3 * layer:3 * layer + 2]
            h0, norm1, qkv, mix1, h1, norm2, query, kv, mix2, h2, norm3, gated, save_a, save_g = saved[layer]

            def reduce(pair):
                return finish_scatter(pair[0], pair[1], n_dev)

            if turn == 0:
                r_ff2 = reduce(weight_grads(1, (gated, grad.astype(BF16)),
                                               [(0, c * width, 1, 0, 0, half // n_dev, (c,)) for c in range(half // width)], half // n_dev))
            grad, vec3, vec_b1, *pairs = ff_grads(5 + min(turn, 1), grad, save_a, save_g, norm3, h2, rows,
                                                  gated if turn > 0 else None, ff_groups[layer], ff_offsets[layer])
            r_ff1 = reduce(pairs[:2])
            if turn > 0:
                r_ff2 = reduce(pairs[2:])
            grad_bf, d_query, d_kv, grad, vec2 = cross_backward(grad, query, kv, h1, rows, group[1], tokens, valid)
            r_cross = reduce(weight_grads(3, (norm2, d_query, mix2, grad_bf),
                                             by_column(0, 1, 1, 0) + by_column(2, 3, 1, depth), 2 * depth, (d_kv, ctx_mine, ctx_other)))
            grad_bf, d_qkv, grad, vec1 = self_backward(grad, qkv, h0, rows, group[0], tokens, BF16 if layer == 0 else F32)
            r_self = reduce(weight_grads(4, (norm1, d_qkv, mix1, grad_bf),
                                            by_column(0, 1, 3, 0) + by_column(2, 3, 1, 3 * depth), 4 * depth))
            side = lambda array, blocks_of: jnp.concatenate(jnp.split(array, blocks_of, 0), 1)
            results[layer] = [side(r_self[:3 * depth], 3), r_self[3 * depth:], r_cross[:depth], side(r_cross[2 * depth:], 2), r_cross[depth:2 * depth],
                              side(r_ff1, 8), r_ff2]
            vec_grads[layer] = [vec1, vec2, vec3, vec_b1]
        vec_out = vec_total([part for parts in vec_grads for part in parts], vec_rows, n_dev)
        vec_out = vec_out[:blocks * vec_each].reshape(blocks, vec_each * width)
        vec_out = jnp.pad(vec_out, ((0, 0), (0, vec_len * n_dev - vec_each * width)))
        vec_out = lax.dynamic_slice(vec_out, (0, me * vec_len), (blocks, vec_len))
        outs = []
        for index in range(7):
            stacked = jnp.stack([results[layer][index] for layer in range(blocks)]) / total
            stacked = lax.optimization_barrier(stacked)
            outs.append(stacked.reshape(blocks, -1))
        outs.append(vec_out / total)
        return tuple([out_tokens.reshape(tokens_x.shape), grad.reshape(tokens_x.shape)] + outs)

    param_spec = P(None, AXIS)
    in_specs = (P(AXIS), P(AXIS), P(AXIS)) + (param_spec,) * 8
    out_specs = (P(AXIS), P(AXIS)) + (param_spec,) * 8
    return jax.shard_map(inner, mesh=mesh, in_specs=in_specs, out_specs=out_specs, check_vma=False)
```

```python
import functools
import math
import jax
import jax.numpy as jnp
from jax import lax
from jax.experimental import pallas as pl
from jax.experimental.pallas import tpu as pltpu
from jax.sharding import PartitionSpec as P


HEAD = 64
AXIS = 'fsdp'
CHUNK = 1280
FF_ROWS = 256
FF_STEP = 256
STEP = 512
VMEM_LIMIT = 60 * 1024 * 1024
VMEM_MOST = 67043328
FORWARD_UNROLL = 10

F32 = jnp.float32
BF16 = jnp.bfloat16
ANY = pl.BlockSpec(memory_space=pl.ANY)


def gather_perms(n_dev):
    near = [(i, i ^ (4 if i % 2 == 0 else 2)) for i in range(n_dev)]
    far = [(i, i ^ (2 if i % 2 == 0 else 4)) for i in range(n_dev)]
    core = [(i, i ^ 1) for i in range(n_dev)]
    return near, far, core


def pack_kernel(*refs):
    ins, out = refs[:-1], refs[-1]
    width, row = out.shape[1], 0
    for ref in ins:
        depth = ref.shape[-2]
        for col in range(0, ref.shape[-1], width):
            piece = ref[0, :, col:col + width] if len(ref.shape) == 3 else ref[:, col:col + width]
            out[row:row + depth, :] = piece
            row += depth


def pack(views, layer, extra, width):
    rows = sum(v.shape[1] * v.shape[2] // width for v in views) + sum(e.shape[0] for e in extra)
    specs = [pl.BlockSpec((1,) + v.shape[1:], lambda i: (layer, 0, 0)) for v in views]
    specs += [pl.BlockSpec(e.shape, lambda i: (0, 0)) for e in extra]
    return pl.pallas_call(
        pack_kernel, grid=(1,), in_specs=specs, out_specs=pl.BlockSpec((rows, width), lambda i: (0, 0)),
        out_shape=jax.ShapeDtypeStruct((rows, width), BF16),
        cost_estimate=pl.CostEstimate(flops=rows * width, bytes_accessed=rows * width * 4, transcendentals=0),
        name='pack')(*views, *extra)


def vec_kernel(*refs):
    pieces, (out, buf, sem) = refs[:8], refs[8:]
    rows = out.shape[0]
    copies = [pltpu.make_async_copy(piece.at[pl.ds(piece.shape[0] - rows, rows), :], buf.at[index], sem.at[index])
              for index, piece in enumerate(pieces)]
    for copy in copies:
        copy.start()
    total = None
    for index, copy in enumerate(copies):
        copy.wait()
        total = buf[index].astype(F32) if total is None else total + buf[index].astype(F32)
    out[...] = total


def vec_sum(pieces, rows):
    width = pieces[0].shape[1]
    return pl.pallas_call(
        vec_kernel, in_specs=[ANY] * 8, out_specs=pl.BlockSpec(memory_space=pltpu.VMEM),
        out_shape=jax.ShapeDtypeStruct((rows, width), F32),
        scratch_shapes=[pltpu.VMEM((8, rows, width), BF16), pltpu.SemaphoreType.DMA((8,))],
        cost_estimate=pl.CostEstimate(flops=rows * width * 8, bytes_accessed=rows * width * 20, transcendentals=0),
        name='vec_sum')(*pieces)


def permute(array, perm):
    return lax.ppermute(array, AXIS, perm)


def gather_group(shard, n_dev):
    near, far, core = gather_perms(n_dev)
    first = permute(shard, near)
    second = permute(shard, far)
    third = permute(first, far)
    mine = [shard, first, second, third]
    return mine + [permute(piece, core) for piece in mine]


def piece_devices(me):
    core = lax.rem(me, 2)
    one, two = 4 - 2 * core, 2 + 2 * core
    x = jnp.bitwise_xor
    mate = x(me, 1)
    return [me, x(me, one), x(me, two), x(me, 6), mate, x(mate, two), x(mate, one), x(mate, 6)]


def start_load(pieces, offset, ref, sem):
    width = pieces[0].shape[1]
    depth = ref.shape[0] // 8
    devices = piece_devices(lax.axis_index(AXIS))
    for block in range(ref.shape[1] // width):
        for piece, device in zip(pieces, devices):
            src = piece.at[pl.ds(offset + block * depth, depth), :]
            dst = ref.at[pl.ds(pl.multiple_of(device * depth, 16), depth), pl.ds(block * width, width)]
            pltpu.make_async_copy(src, dst, sem).start()


def wait_load(ref, sem):
    pltpu.make_async_copy(ref, ref, sem).wait()


def dot_nn(a, b):
    return lax.dot_general(a, b, (((1,), (0,)), ((), ())), preferred_element_type=F32)


def dot_nt(a, b):
    return lax.dot_general(a, b, (((1,), (1,)), ((), ())), preferred_element_type=F32)


def dot_tn(a, b):
    return lax.dot_general(a, b, (((0,), (0,)), ((), ())), preferred_element_type=F32)


def norm_stats(x):
    average = jnp.mean(x, axis=-1, keepdims=True)
    centered = x - average
    variance = jnp.mean(centered * centered, axis=-1, keepdims=True)
    scale = lax.rsqrt(variance + 1e-5)
    return centered * scale, scale


def norm_back(x, gain, d_norm):
    unit, scale = norm_stats(x)
    d_unit = d_norm * gain
    inner = d_unit - jnp.mean(d_unit, axis=-1, keepdims=True) - unit * jnp.mean(d_unit * unit, axis=-1, keepdims=True)
    return scale * inner, jnp.sum(d_norm * unit, axis=0, keepdims=True), jnp.sum(d_norm, axis=0, keepdims=True)


def softmax_rows(scores):
    top = jnp.max(scores, axis=-1, keepdims=True)
    raised = jnp.exp(scores - top)
    return raised * (1.0 / jnp.sum(raised, axis=-1, keepdims=True))


def low_lanes(rows):
    return lax.broadcasted_iota(jnp.int32, (rows, 2 * HEAD), 1) < HEAD


def heads_of(pair):
    low, zero = low_lanes(pair.shape[0]), jnp.zeros_like(pair)
    return jnp.where(low, pair, zero), jnp.where(low, zero, pair)


def pair_forward(query, key, value, valid=None):
    mixed = []
    for q_head in heads_of(query * HEAD ** -0.5):
        scores = dot_nt(q_head, key)
        if valid is not None:
            column = lax.broadcasted_iota(jnp.int32, scores.shape, 1)
            scores = jnp.where(column < valid, scores, -1e30)
        mixed.append(dot_nn(softmax_rows(scores).astype(BF16), value))
    return jnp.where(low_lanes(query.shape[0]), mixed[0], mixed[1]).astype(BF16)


def backward_scores(query, key, value, d_out):
    q_heads, d_heads = heads_of(query * HEAD ** -0.5), heads_of(d_out)
    return q_heads, d_heads, [dot_nt(key, q) for q in q_heads], [dot_nt(value, d) for d in d_heads]


def backward_probs(scores, d_probs, valid):
    if valid is not None:
        row = lax.broadcasted_iota(jnp.int32, scores.shape, 0)
        scores = jnp.where(row < valid, scores, -1e30)
    raised = jnp.exp(scores - jnp.max(scores, axis=0, keepdims=True))
    probs = raised * (1.0 / jnp.sum(raised, axis=0, keepdims=True))
    inner = jnp.sum(d_probs * probs, axis=0, keepdims=True)
    return probs.astype(BF16), (probs * (d_probs - inner)).astype(BF16)


def pairs_backward(pairs, load, store, valid=None):
    ahead = load(0)
    ahead = ahead, backward_scores(*ahead)
    for pair in range(pairs):
        (query, key, value, d_out), (q_heads, d_heads, scores, d_probs) = ahead
        if pair + 1 < pairs:
            ahead = load(pair + 1)
            ahead = ahead, backward_scores(*ahead)
        turned = key.T
        d_query, d_key, d_value = [], 0.0, 0.0
        for head in range(2):
            probs, d_scores = backward_probs(scores[head], d_probs[head], valid)
            d_query.append(dot_nn(turned[head * HEAD:(head + 1) * HEAD, :], d_scores))
            d_key = d_key + dot_nn(d_scores, q_heads[head])
            d_value = d_value + dot_nn(probs, d_heads[head])
        d_query = (jnp.concatenate(d_query, 0) * HEAD ** -0.5).T
        store(pair, d_query.astype(BF16), d_key.astype(BF16), d_value.astype(BF16))


def chip_places(me):
    core, chip = lax.rem(me, 2), me // 2
    chip_x, chip_y = lax.rem(chip, 2), chip // 2

    def mate_slot(other):
        d_x, d_y = lax.rem(chip_x + other % 2, 2), lax.rem(chip_y + other // 2, 2)
        return d_x + 2 * d_y + core * (d_x - d_y)

    def own_chip(slot):
        one, two = slot // 2, slot % 2
        d_x, d_y = one + core * (two - one), two + core * (one - two)
        return 2 * lax.rem(chip_y + d_y, 2) + lax.rem(chip_x + d_x, 2)

    return core, me + 1 - 2 * core, mate_slot, own_chip


def greet(mate):
    barrier = pltpu.get_barrier_semaphore()
    pl.semaphore_signal(barrier, inc=1, device_id=(mate,), device_id_type=pl.DeviceIdType.MESH)
    pl.semaphore_wait(barrier, 1)


def tile_sends(q, rows, tile, recv, send_sem, recv_sem):
    core, mate, mate_slot, _ = chip_places(lax.axis_index(AXIS))
    copies = []
    for other in range(4):
        start = pl.multiple_of((2 * other + 1 - core) * rows, 16)
        copies.append(pltpu.make_async_remote_copy(
            src_ref=tile.at[q, pl.ds(start, rows), :], dst_ref=recv.at[mate_slot(other), pl.ds(q * rows, rows), :],
            send_sem=send_sem.at[q, other], recv_sem=recv_sem.at[q, other],
            device_id=(mate,), device_id_type=pl.DeviceIdType.MESH))
    return copies


def finish_tiles(tiles, rows, group_rows, tile, recv, send_sem, recv_sem, far_ref, keep_ref):
    core, _, _, own_chip = chip_places(lax.axis_index(AXIS))
    for q in range(tiles):
        for copy in tile_sends(q, rows, tile, recv, send_sem, recv_sem):
            copy.wait()
        for slot in range(4):
            ref = keep_ref if slot < 2 else far_ref
            start = pl.multiple_of((2 * own_chip(slot) + core) * rows, 16)
            at = (slot % 2) * group_rows + q * rows
            ref[at:at + rows, :] = tile[q, pl.ds(start, rows), :] + recv[slot, q * rows:(q + 1) * rows, :]


def add_rows(ref, step, rows):
    @pl.when(step == 0)
    def _():
        ref[...] = jnp.zeros_like(ref)

    for index, row in enumerate(rows):
        ref[pl.ds(index, 1), :] += row


def self_forward_kernel(samples, tokens, h_ref, rows_ref, *refs):
    pieces, (norm_ref, qkv_ref, mix_ref, out_ref, w_qkv, w_out, sems) = refs[:8], refs[8:]
    width = h_ref.shape[1]
    step = pl.program_id(0)

    @pl.when(step == 0)
    def _():
        start_load(pieces, 0, w_qkv, sems.at[0])
        start_load(pieces, 3 * (width // 8), w_out, sems.at[1])

    x = h_ref[...].astype(F32)
    unit, _ = norm_stats(x)
    normed = (unit * rows_ref[0:1, :] + rows_ref[1:2, :]).astype(BF16)
    norm_ref[...] = normed

    @pl.when(step == 0)
    def _():
        wait_load(w_qkv, sems.at[0])
        wait_load(w_out, sems.at[1])

    qkv_ref[...] = dot_nn(normed, w_qkv[...]).astype(BF16)
    pairs = width // (2 * HEAD)

    def body(index, carry):
        row = pl.multiple_of((index // pairs) * tokens, tokens)
        col = pl.multiple_of((index % pairs) * 2 * HEAD, 2 * HEAD)
        part = lambda which: qkv_ref[pl.ds(row, tokens), pl.ds(which * width + col, 2 * HEAD)]
        mix_ref[pl.ds(row, tokens), pl.ds(col, 2 * HEAD)] = pair_forward(part(0), part(1), part(2))
        return carry

    lax.fori_loop(0, samples * pairs, body, 0, unroll=FORWARD_UNROLL)
    out_ref[...] = x + dot_nn(mix_ref[...], w_out[...]) + rows_ref[6:7, :]


def cross_forward_kernel(samples, tokens, valid, h_ref, rows_ref, ctx_ref, *refs):
    pieces, (norm_ref, query_ref, kv_ref, mix_ref, out_ref, w_kv, w_query, w_out, sems) = refs[:8], refs[8:]
    width = h_ref.shape[1]
    step = pl.program_id(0)
    padded = ctx_ref.shape[0] // (samples * pl.num_programs(0))

    @pl.when(step == 0)
    def _():
        deep, depth = w_kv.shape[0] // 8, width // 8
        start_load(pieces, 0, w_kv, sems.at[0])
        start_load(pieces, 2 * deep, w_query, sems.at[1])
        start_load(pieces, 2 * deep + depth, w_out, sems.at[2])

    x = h_ref[...]
    unit, _ = norm_stats(x)
    normed = (unit * rows_ref[2:3, :] + rows_ref[3:4, :]).astype(BF16)
    norm_ref[...] = normed

    @pl.when(step == 0)
    def _():
        wait_load(w_kv, sems.at[0])
        wait_load(w_query, sems.at[1])
        wait_load(w_out, sems.at[2])
        kv_ref[...] = dot_nn(ctx_ref[...], w_kv[...]).astype(BF16)

    query_ref[...] = dot_nn(normed, w_query[...]).astype(BF16)
    pairs = width // (2 * HEAD)

    def body(index, carry):
        sample = index // pairs
        row = pl.multiple_of(sample * tokens, tokens)
        kv_row = pl.multiple_of((step * samples + sample) * padded, 16)
        col = pl.multiple_of((index % pairs) * 2 * HEAD, 2 * HEAD)
        query = query_ref[pl.ds(row, tokens), pl.ds(col, 2 * HEAD)]
        key = kv_ref[pl.ds(kv_row, padded), pl.ds(col, 2 * HEAD)]
        value = kv_ref[pl.ds(kv_row, padded), pl.ds(width + col, 2 * HEAD)]
        mix_ref[pl.ds(row, tokens), pl.ds(col, 2 * HEAD)] = pair_forward(query, key, value, valid)
        return carry

    lax.fori_loop(0, samples * pairs, body, 0, unroll=FORWARD_UNROLL)
    out_ref[...] = x + dot_nn(mix_ref[...], w_out[...]) + rows_ref[7:8, :]


def ff_loads(pieces, offset, w_ff1, w_ff2, sems):
    start_load(pieces[:8], 0, w_ff1, sems.at[0])
    start_load(pieces[8:], offset, w_ff2, sems.at[1])


def ff_up(normed, bias_ref, w_ff1, half, start, gated_ref, save_a, save_g):
    u_a = dot_nn(normed, w_ff1[:, start:start + CHUNK]) + bias_ref[:, start:start + CHUNK]
    u_g = dot_nn(normed, w_ff1[:, half + start:half + start + CHUNK]) + bias_ref[:, half + start:half + start + CHUNK]
    cumulative = 0.5 * (1.0 + lax.erf(u_g * math.sqrt(0.5)))
    gate = u_g * cumulative
    slope = cumulative + u_g * (jnp.exp(-0.5 * u_g * u_g) * (1.0 / math.sqrt(2.0 * math.pi)))
    gated = (u_a * gate).astype(BF16)
    gated_ref[:, start:start + CHUNK] = gated
    save_a[:, start:start + CHUNK] = gate
    save_g[:, start:start + CHUNK] = u_a * slope
    return gated


def ff_forward_kernel(offset, h_ref, rows_ref, bias_ref, *refs):
    pieces, (norm_ref, gated_ref, save_a, save_g, out_ref, w_ff1, w_ff2, sems) = refs[:16], refs[16:]
    half = w_ff2.shape[0]
    step = pl.program_id(0)

    @pl.when(step == 0)
    def _():
        ff_loads(pieces, offset, w_ff1, w_ff2, sems)

    x = h_ref[...]
    unit, _ = norm_stats(x)
    normed = (unit * rows_ref[4:5, :] + rows_ref[5:6, :]).astype(BF16)
    norm_ref[...] = normed

    @pl.when(step == 0)
    def _():
        wait_load(w_ff1, sems.at[0])
        wait_load(w_ff2, sems.at[1])

    total = x + rows_ref[8:9, :]
    for start in range(0, half, CHUNK):
        gated = ff_up(normed, bias_ref, w_ff1, half, start, gated_ref, save_a, save_g)
        total = total + dot_nn(gated, w_ff2[start:start + CHUNK, :])
    out_ref[...] = total


def ff_up_kernel(h_ref, rows_ref, bias_ref, *refs):
    pieces, (norm_ref, gated_ref, save_a, save_g, w_ff1, sems) = refs[:8], refs[8:]
    half = w_ff1.shape[1] // 2
    step = pl.program_id(0)

    @pl.when(step == 0)
    def _():
        start_load(pieces, 0, w_ff1, sems.at[0])

    unit, _ = norm_stats(h_ref[...])
    normed = (unit * rows_ref[4:5, :] + rows_ref[5:6, :]).astype(BF16)
    norm_ref[...] = normed

    @pl.when(step == 0)
    def _():
        wait_load(w_ff1, sems.at[0])

    for start in range(0, half, CHUNK):
        ff_up(normed, bias_ref, w_ff1, half, start, gated_ref, save_a, save_g)


def ff_down_kernel(h_ref, rows_ref, gated_ref, *refs):
    pieces, (out_ref, w_ff2, sems) = refs[:8], refs[8:]
    step = pl.program_id(0)

    @pl.when(step == 0)
    def _():
        start_load(pieces, 0, w_ff2, sems.at[0])
        wait_load(w_ff2, sems.at[0])

    out_ref[...] = (h_ref[...] + rows_ref[8:9, :] + dot_nn(gated_ref[...], w_ff2[...])).astype(BF16)


def cross_backward_kernel(samples, tokens, valid, grad_ref, query_ref, kv_ref, h_ref, rows_ref, norm_ref, mix_ref, ctx_mine_ref,
                          ctx_other_ref, *refs):
    pieces, refs = refs[:8], refs[8:]
    (out_ref, vec_ref, far_ref, keep_ref, d_mix, w_query, w_out, d_query, grad_bf, d_kv, kv_other, x_norm, x_mix, ctx_mine, ctx_other,
     tile, recv, sems, load_sem, kv_send, kv_recv, send_sem, recv_sem) = refs
    width = h_ref.shape[1]
    depth = width // 8
    step, last = pl.program_id(0), pl.num_programs(0) - 1
    padded = kv_ref.shape[0] // samples
    context_rows = kv_ref.shape[0] * (last + 1)
    mate = chip_places(lax.axis_index(AXIS))[1]
    loads = [pltpu.make_async_copy(src, dst, load_sem.at[index]) for index, (src, dst) in enumerate(
        ((norm_ref, x_norm), (mix_ref, x_mix), (ctx_mine_ref, ctx_mine), (ctx_other_ref, ctx_other)))]
    exchange = pltpu.make_async_remote_copy(
        src_ref=d_kv.at[pl.ds(0, context_rows), :], dst_ref=kv_other.at[pl.ds(0, context_rows), :], send_sem=kv_send, recv_sem=kv_recv,
        device_id=(mate,), device_id_type=pl.DeviceIdType.MESH)

    @pl.when(step == 0)
    def _():
        base = pieces[0].shape[0] - 2 * depth
        start_load(pieces, base, w_query, sems.at[0])
        start_load(pieces, base + depth, w_out, sems.at[1])
        for copy in loads:
            copy.start()
        for ref in (d_kv, kv_other):
            ref[context_rows:, :] = jnp.zeros((ref.shape[0] - context_rows, ref.shape[1]), BF16)
        greet(mate)

    grad = grad_ref[...]
    mine = pl.ds(pl.multiple_of(step * grad.shape[0], grad.shape[0]), grad.shape[0])
    grad_bf[mine, :] = grad.astype(BF16)

    @pl.when(step == 0)
    def _():
        wait_load(w_query, sems.at[0])
        wait_load(w_out, sems.at[1])

    d_mix[...] = dot_nt(grad.astype(BF16), w_out[...]).astype(BF16)
    pairs = width // (2 * HEAD)

    at = lambda which, pair: slice(which * width + pair * 2 * HEAD, which * width + (pair + 1) * 2 * HEAD)

    def load(index):
        sample, pair = index // pairs, index % pairs
        row, here = slice(sample * tokens, (sample + 1) * tokens), slice(sample * padded, (sample + 1) * padded)
        return query_ref[row, at(0, pair)], kv_ref[here, at(0, pair)], kv_ref[here, at(1, pair)], d_mix[row, at(0, pair)]

    def store(index, d_q, d_key, d_value):
        sample, pair = index // pairs, index % pairs
        d_query[pl.ds(pl.multiple_of((step * samples + sample) * tokens, tokens), tokens), at(0, pair)] = d_q
        there = pl.ds(pl.multiple_of((step * samples + sample) * padded, 16), padded)
        d_kv[there, at(0, pair)] = d_key
        d_kv[there, at(1, pair)] = d_value

    pairs_backward(samples * pairs, load, store, valid)
    rows, summed = depth, 2 * depth
    group_rows = keep_ref.shape[0] // 2
    deep = ctx_mine.shape[0] // 4

    def context_part(ctx, kv, slot, block):
        return dot_nn(ctx[slot * deep:(slot + 1) * deep, :], kv[:, block * width:(block + 1) * width])

    def context_at(slot, block):
        start = (slot % 2) * group_rows + summed + block * deep
        return slice(start, start + deep)

    @pl.when(step == last)
    def _():
        for copy in loads:
            copy.wait()
        tile[0] = dot_tn(x_norm[...], d_query[...])
        exchange.start()
        tile[1] = dot_tn(x_mix[...], grad_bf[...])
        for copy in tile_sends(0, rows, tile, recv, send_sem, recv_sem):
            copy.start()
        for slot in range(4):
            for block in range(2):
                (keep_ref if slot < 2 else far_ref)[context_at(slot, block), :] = context_part(ctx_mine, d_kv, slot, block)
        for copy in tile_sends(1, rows, tile, recv, send_sem, recv_sem):
            copy.start()

    d_norm = dot_nt(d_query[mine, :], w_query[...])
    d_res, g_gain, g_shift = norm_back(h_ref[...], rows_ref[2:3, :], d_norm)
    out_ref[...] = grad + d_res
    add_rows(vec_ref, step, [g_gain, g_shift, jnp.sum(grad, axis=0, keepdims=True)])

    @pl.when(step == last)
    def _():
        exchange.wait()
        for slot in range(4):
            for block in range(2):
                (keep_ref if slot < 2 else far_ref)[context_at(slot, block), :] += context_part(ctx_other, kv_other, slot, block)
        finish_tiles(2, rows, group_rows, tile, recv, send_sem, recv_sem, far_ref, keep_ref)


def self_backward_kernel(samples, tokens, grad_ref, qkv_ref, h_ref, rows_ref, norm_ref, mix_ref, *refs):
    pieces, refs = refs[:8], refs[8:]
    (out_ref, vec_ref, far_ref, keep_ref, d_mix, w_qkv, w_out, d_qkv, grad_bf, x_norm, x_mix, tile, recv, sems, load_sem,
     send_sem, recv_sem) = refs
    width = h_ref.shape[1]
    depth = width // 8
    step, last = pl.program_id(0), pl.num_programs(0) - 1
    mate = chip_places(lax.axis_index(AXIS))[1]
    loads = [pltpu.make_async_copy(src, dst, load_sem.at[index]) for index, (src, dst) in enumerate(((norm_ref, x_norm), (mix_ref, x_mix)))]

    @pl.when(step == 0)
    def _():
        start_load(pieces, 0, w_qkv, sems.at[0])
        start_load(pieces, 3 * depth, w_out, sems.at[1])
        for copy in loads:
            copy.start()
        greet(mate)

    grad = grad_ref[...]
    mine = pl.ds(pl.multiple_of(step * grad.shape[0], grad.shape[0]), grad.shape[0])
    grad_bf[mine, :] = grad.astype(BF16)

    @pl.when(step == 0)
    def _():
        wait_load(w_qkv, sems.at[0])
        wait_load(w_out, sems.at[1])

    d_mix[...] = dot_nt(grad.astype(BF16), w_out[...]).astype(BF16)
    pairs = width // (2 * HEAD)

    at = lambda which, pair: slice(which * width + pair * 2 * HEAD, which * width + (pair + 1) * 2 * HEAD)
    rows_of = lambda sample: slice(sample * tokens, (sample + 1) * tokens)
    all_rows_of = lambda sample: pl.ds(pl.multiple_of((step * samples + sample) * tokens, tokens), tokens)

    def load(index):
        row, pair = rows_of(index // pairs), index % pairs
        return tuple(qkv_ref[row, at(which, pair)] for which in range(3)) + (d_mix[row, at(0, pair)],)

    def store(index, *parts):
        for which, part in enumerate(parts):
            d_qkv[all_rows_of(index // pairs), at(which, index % pairs)] = part

    pairs_backward(samples * pairs, load, store)

    @pl.when(step == last)
    def _():
        for copy in loads:
            copy.wait()
        for q in range(4):
            if q < 3:
                tile[q] = dot_tn(x_norm[...], d_qkv[:, q * width:(q + 1) * width])
            else:
                tile[q] = dot_tn(x_mix[...], grad_bf[...])
            if q > 0:
                for copy in tile_sends(q - 1, depth, tile, recv, send_sem, recv_sem):
                    copy.start()

    d_norm = dot_nt(d_qkv[mine, :], w_qkv[...])

    @pl.when(step == last)
    def _():
        for copy in tile_sends(3, depth, tile, recv, send_sem, recv_sem):
            copy.start()

    d_res, g_gain, g_shift = norm_back(h_ref[...].astype(F32), rows_ref[0:1, :], d_norm)
    out_ref[...] = (grad + d_res).astype(out_ref.dtype)
    add_rows(vec_ref, step, [g_gain, g_shift, jnp.sum(grad, axis=0, keepdims=True)])

    @pl.when(step == last)
    def _():
        finish_tiles(4, depth, 4 * depth, tile, recv, send_sem, recv_sem, far_ref, keep_ref)


def by_step(rows, columns):
    return pl.BlockSpec((rows, columns), lambda i: (i, 0))


def whole(rows, columns):
    return pl.BlockSpec((rows, columns), lambda i: (0, 0))


def shape(rows, columns, dtype):
    return jax.ShapeDtypeStruct((rows, columns), dtype)


def call(kernel, steps, in_specs, out_specs, out_shapes, scratch, flops, moved, kind=None):
    return pl.pallas_call(
        kernel, grid=(steps,), in_specs=in_specs, out_specs=out_specs, out_shape=out_shapes, scratch_shapes=scratch,
        cost_estimate=pl.CostEstimate(flops=int(flops), bytes_accessed=int(moved), transcendentals=0),
        compiler_params=pltpu.CompilerParams(dimension_semantics=('arbitrary',), vmem_limit_bytes=VMEM_LIMIT, collective_id=kind,
                                             has_side_effects=kind is not None))


def self_forward(h, rows, pieces, tokens):
    count, width = h.shape
    return call(
        functools.partial(self_forward_kernel, STEP // tokens, tokens), count // STEP,
        [by_step(STEP, width), whole(*rows.shape)] + [ANY] * 8,
        [by_step(STEP, width), by_step(STEP, 3 * width), by_step(STEP, width), by_step(STEP, width)],
        [shape(count, width, BF16), shape(count, 3 * width, BF16), shape(count, width, BF16), shape(count, width, F32)],
        [pltpu.VMEM((width, 3 * width), BF16), pltpu.VMEM((width, width), BF16), pltpu.SemaphoreType.DMA((2,))],
        count * width * width * 8 + count * tokens * width * 4, 2e7)(h, rows, *pieces)


def cross_forward(h, rows, ctx, pieces, tokens, valid):
    count, width = h.shape
    ctx_rows, ctx_width = ctx.shape
    return call(
        functools.partial(cross_forward_kernel, STEP // tokens, tokens, valid), count // STEP,
        [by_step(STEP, width), whole(*rows.shape), whole(ctx_rows, ctx_width)] + [ANY] * 8,
        [by_step(STEP, width), by_step(STEP, width), whole(ctx_rows, 2 * width), by_step(STEP, width), by_step(STEP, width)],
        [shape(count, width, BF16), shape(count, width, BF16), shape(ctx_rows, 2 * width, BF16), shape(count, width, BF16),
         shape(count, width, F32)],
        [pltpu.VMEM((ctx_width, 2 * width), BF16), pltpu.VMEM((width, width), BF16), pltpu.VMEM((width, width), BF16),
         pltpu.SemaphoreType.DMA((3,))],
        count * width * width * 4 + ctx_rows * ctx_width * width * 4 + count * 128 * width * 4, 2e7)(h, rows, ctx, *pieces)


def ff_forward(h, rows, bias, pieces, offset):
    count, width = h.shape
    half = bias.shape[1] // 2
    return call(
        functools.partial(ff_forward_kernel, offset), count // FF_STEP,
        [by_step(FF_STEP, width), whole(*rows.shape), whole(1, 2 * half)] + [ANY] * 16,
        [by_step(FF_STEP, width), by_step(FF_STEP, half), by_step(FF_STEP, half), by_step(FF_STEP, half), by_step(FF_STEP, width)],
        [shape(count, width, BF16), shape(count, half, BF16), shape(count, half, F32), shape(count, half, F32),
         shape(count, width, F32)],
        [pltpu.VMEM((width, 2 * half), BF16), pltpu.VMEM((half, width), BF16), pltpu.SemaphoreType.DMA((2,))],
        count * width * half * 6, 6e7)(h, rows, bias, *pieces)


def ff_up_forward(h, rows, bias, pieces):
    count, width = h.shape
    half = bias.shape[1] // 2
    return call(
        ff_up_kernel, count // FF_STEP,
        [by_step(FF_STEP, width), whole(*rows.shape), whole(1, 2 * half)] + [ANY] * 8,
        [by_step(FF_STEP, width), by_step(FF_STEP, half), by_step(FF_STEP, half), by_step(FF_STEP, half)],
        [shape(count, width, BF16), shape(count, half, BF16), shape(count, half, F32), shape(count, half, F32)],
        [pltpu.VMEM((width, 2 * half), BF16), pltpu.SemaphoreType.DMA((1,))],
        count * width * half * 4, 5e7)(h, rows, bias, *pieces)


def ff_down_forward(h, rows, gated, pieces):
    count, width = h.shape
    half = gated.shape[1]
    return call(
        ff_down_kernel, count // STEP,
        [by_step(STEP, width), whole(*rows.shape), by_step(STEP, half)] + [ANY] * 8,
        by_step(STEP, width), shape(count, width, BF16),
        [pltpu.VMEM((half, width), BF16), pltpu.SemaphoreType.DMA((1,))],
        count * width * half * 2, 2e7)(h, rows, gated, *pieces)


def cross_backward(grad, query, kv, h, rows, norm, mix, ctx_mine, ctx_other, pieces, tokens, valid):
    count, width = h.shape
    ctx_rows = kv.shape[0]
    steps = count // STEP
    group_rows = 2 * (width // 8) + ctx_mine.shape[0] // 2
    dma = pltpu.SemaphoreType.DMA
    big = pltpu.VMEM((count, width), BF16)
    kv_buf, ctx_buf = pltpu.VMEM((ctx_mine.shape[1], 2 * width), BF16), pltpu.VMEM(ctx_mine.shape, BF16)
    return call(
        functools.partial(cross_backward_kernel, STEP // tokens, tokens, valid), steps,
        [by_step(STEP, width), by_step(STEP, width), by_step(ctx_rows // steps, 2 * width), by_step(STEP, width),
         whole(*rows.shape)] + [ANY] * 12,
        [by_step(STEP, width), whole(8, width), whole(2 * group_rows, width), whole(2 * group_rows, width)],
        [shape(count, width, F32), shape(8, width, F32), shape(2 * group_rows, width, F32), shape(2 * group_rows, width, F32)],
        [pltpu.VMEM((STEP, width), BF16), pltpu.VMEM((width, width), BF16), pltpu.VMEM((width, width), BF16), big, big, kv_buf, kv_buf,
         big, big, ctx_buf, ctx_buf, pltpu.VMEM((2, width, width), F32), pltpu.VMEM((4, 2 * (width // 8), width), F32),
         dma((2,)), dma((4,)), dma, dma, dma((2, 4)), dma((2, 4))],
        count * width * width * 8 + count * 128 * width * 10 + ctx_mine.size * width * 8, 2e7, 3)(
            grad, query, kv, h, rows, norm, mix, ctx_mine, ctx_other, *pieces)


def self_backward(kind, grad, qkv, h, rows, norm, mix, pieces, tokens, out_dtype):
    count, width = h.shape
    group_rows = width // 2
    dma = pltpu.SemaphoreType.DMA
    big = pltpu.VMEM((count, width), BF16)
    return call(
        functools.partial(self_backward_kernel, STEP // tokens, tokens), count // STEP,
        [by_step(STEP, width), by_step(STEP, 3 * width), by_step(STEP, width), whole(*rows.shape)] + [ANY] * 10,
        [by_step(STEP, width), whole(8, width), whole(2 * group_rows, width), whole(2 * group_rows, width)],
        [shape(count, width, out_dtype), shape(8, width, F32), shape(2 * group_rows, width, F32), shape(2 * group_rows, width, F32)],
        [pltpu.VMEM((STEP, width), BF16), pltpu.VMEM((width, 3 * width), BF16), pltpu.VMEM((width, width), BF16),
         pltpu.VMEM((count, 3 * width), BF16), big, big, big, pltpu.VMEM((4, width, width), F32),
         pltpu.VMEM((4, group_rows, width), F32), dma((2,)), dma((2,)), dma((4, 4)), dma((4, 4))],
        count * width * width * 16 + count * tokens * width * 10, 3e7, kind)(grad, qkv, h, rows, norm, mix, *pieces)


def grad_kernel(tiles, group_rows, inputs, *refs):
    ins, refs = refs[:inputs], refs[inputs:]
    far_ref, keep_ref, x_buf, turned, y_buf, tile, own, recv, x_sem, y_sem, send_sem, recv_sem = refs[:12]
    width = tile.shape[1]
    me = lax.axis_index(AXIS)
    core, chip = lax.rem(me, 2), me // 2
    mate = me + 1 - 2 * core
    chip_x, chip_y = lax.rem(chip, 2), chip // 2

    xs, ys, x_of, y_of = [], [], [], []
    for x, x_col, y, y_col, *_ in tiles:
        if not xs or xs[-1] != (x, x_col):
            xs.append((x, x_col))
        if not ys or ys[-1] != (y, y_col):
            ys.append((y, y_col))
        x_of.append(len(xs) - 1)
        y_of.append(len(ys) - 1)

    def load(which, sequence, buf, sem):
        array, col = sequence[which]
        return pltpu.make_async_copy(ins[array].at[:, pl.ds(col, width)], buf.at[which % 2], sem.at[which % 2])

    for which in range(2):
        if which < len(xs):
            load(which, xs, x_buf, x_sem).start()
        if which < len(ys):
            load(which, ys, y_buf, y_sem).start()

    barrier = pltpu.get_barrier_semaphore()
    pl.semaphore_signal(barrier, inc=1, device_id=(mate,), device_id_type=pl.DeviceIdType.MESH)
    pl.semaphore_wait(barrier, 1)

    def sends(q):
        *_, first_row, rows, chips = tiles[q]
        copies = []
        for index, other in enumerate(chips):
            d_x, d_y = lax.rem(chip_x + other % 2, 2), lax.rem(chip_y + other // 2, 2)
            slot = d_x + 2 * d_y + core * (d_x - d_y)
            start = pl.multiple_of((2 * index + 1 - core) * rows, 16)
            copies.append(pltpu.make_async_remote_copy(
                src_ref=tile.at[q % 3, pl.ds(start, rows), :], dst_ref=recv.at[slot, pl.ds(first_row, rows), :],
                send_sem=send_sem.at[q % 3, index], recv_sem=recv_sem.at[q, index],
                device_id=(mate,), device_id_type=pl.DeviceIdType.MESH))
        return copies

    for q, (x, x_col, y, y_col, first_row, rows, chips) in enumerate(tiles):
        if q == 0 or x_of[q] != x_of[q - 1]:
            which = x_of[q]
            load(which, xs, x_buf, x_sem).wait()
            turned[...] = x_buf[which % 2].T
            if which + 2 < len(xs):
                load(which + 2, xs, x_buf, x_sem).start()
        if q == 0 or y_of[q] != y_of[q - 1]:
            load(y_of[q], ys, y_buf, y_sem).wait()
        if q >= 3:
            for copy in sends(q - 3):
                copy.wait_send()
        tile[q % 3] = dot_nn(turned[...], y_buf[y_of[q] % 2])
        if (q + 1 == len(tiles) or y_of[q + 1] != y_of[q]) and y_of[q] + 2 < len(ys):
            load(y_of[q] + 2, ys, y_buf, y_sem).start()
        for index, other in enumerate(chips):
            d_x, d_y = lax.rem(chip_x + other % 2, 2), lax.rem(chip_y + other // 2, 2)
            slot = 2 * d_x + d_y + core * (d_y - d_x)
            start = pl.multiple_of((2 * index + core) * rows, 16)
            own[slot, first_row:first_row + rows, :] = tile[q % 3, pl.ds(start, rows), :]
        if q >= 1:
            for copy in sends(q - 1):
                copy.start()
    last = len(tiles) - 1
    for copy in sends(last):
        copy.start()
    for q in range(max(0, last - 2), last + 1):
        for copy in sends(q):
            copy.wait_send()
    for q in range(last + 1):
        for copy in sends(q):
            copy.wait_recv()
    for slot in range(4):
        ref = keep_ref if slot < 2 else far_ref
        ref[(slot % 2) * group_rows:(slot % 2 + 1) * group_rows, :] = own[slot] + recv[slot]


def weight_grads(kind, arrays, tiles, group_rows):
    count, width = arrays[0].shape[0], 640
    chips = max(len(t[-1]) for t in tiles)
    dma = pltpu.SemaphoreType.DMA
    out = jax.ShapeDtypeStruct((2 * group_rows, width), F32)
    return pl.pallas_call(
        functools.partial(grad_kernel, tiles, group_rows, len(arrays)), in_specs=[ANY] * len(arrays),
        out_specs=[pl.BlockSpec(memory_space=pltpu.VMEM)] * 2, out_shape=[out, out],
        scratch_shapes=[pltpu.VMEM((2, count, width), BF16), pltpu.VMEM((width, count), BF16), pltpu.VMEM((2, count, width), BF16),
                        pltpu.VMEM((3, width, width), F32), pltpu.VMEM((4, group_rows, width), F32),
                        pltpu.VMEM((4, group_rows, width), F32), dma((2,)), dma((2,)), dma((3, chips)), dma((len(tiles), chips))],
        cost_estimate=pl.CostEstimate(flops=2 * count * width * width * len(tiles), bytes_accessed=int(2e7), transcendentals=0),
        compiler_params=pltpu.CompilerParams(collective_id=kind, has_side_effects=True, vmem_limit_bytes=VMEM_LIMIT))(*arrays)


def context_kernel(context_ref, ctx_ref, mine_ref, other_ref):
    batch, valid, _ = context_ref.shape
    padded = ctx_ref.shape[0] // batch
    me = lax.axis_index(AXIS)
    core, chip = lax.rem(me, 2), me // 2
    ctx_ref[...] = jnp.zeros_like(ctx_ref)
    for sample in range(batch):
        ctx_ref[sample * padded:sample * padded + valid, :] = context_ref[sample]
    each, rows = mine_ref.shape[0] // 4, ctx_ref.shape[0]
    mine_ref[...] = jnp.zeros_like(mine_ref)
    other_ref[...] = jnp.zeros_like(other_ref)
    x = jnp.bitwise_xor
    for of_core, ref in ((core, mine_ref), (1 - core, other_ref)):
        for slot, other in enumerate((chip, x(chip, 2 - of_core), x(chip, 1 + of_core), x(chip, 3))):
            column = pl.multiple_of((2 * other + of_core) * each, each)
            ref[slot * each:(slot + 1) * each, 0:rows] = ctx_ref[:, pl.ds(column, each)].T


def prepare_context(context, n_dev):
    batch, valid, ctx_width = context.shape
    rows = batch * ((valid + 15) // 16 * 16)
    vmem = pl.BlockSpec(memory_space=pltpu.VMEM)
    turned = shape(ctx_width // 2, (rows + 127) // 128 * 128, BF16)
    ctx, mine, other = pl.pallas_call(
        context_kernel, in_specs=[vmem], out_specs=[vmem] * 3, out_shape=[shape(rows, ctx_width, BF16), turned, turned],
        cost_estimate=pl.CostEstimate(flops=rows * ctx_width * 8, bytes_accessed=int(8e6), transcendentals=0),
        name='context')(context)
    return ctx, mine, permute(other, gather_perms(n_dev)[2])


def vec_pack_kernel(*refs):
    ins, out = refs[:-1], refs[-1]
    width = out.shape[1]
    out[...] = jnp.zeros_like(out)
    for layer in range(len(ins) // 4):
        first, second, third, bias = ins[4 * layer:4 * layer + 4]
        rows = [(first, 0), (first, 1), (second, 0), (second, 1), (third, 0), (third, 1), (first, 2), (second, 2), (third, 2)]
        for index, (ref, row) in enumerate(rows):
            out[17 * layer + index:17 * layer + index + 1, :] = ref[row:row + 1, :]
        for index in range(8):
            row = 17 * layer + 9 + index
            out[row:row + 1, :] = bias[0:1, index * width:(index + 1) * width]


def vec_total(parts, rows, n_dev):
    vmem = pl.BlockSpec(memory_space=pltpu.VMEM)
    width = parts[0].shape[1]
    total = pl.pallas_call(
        vec_pack_kernel, in_specs=[vmem] * len(parts), out_specs=vmem, out_shape=shape(rows, width, F32),
        cost_estimate=pl.CostEstimate(flops=rows * width, bytes_accessed=rows * width * 8, transcendentals=0),
        name='vec_pack')(*parts)
    near, far, core = gather_perms(n_dev)
    for perm in (core, far, near):
        total = total + permute(total, perm)
    return total


def ff_grad_kernel(offset, grad_ref, save_a, save_g, norm_ref, h_ref, rows_ref, *refs):
    pieces, refs = refs[:16], refs[16:]
    (out_ref, vec_ref, bias_ref, far_ref, keep_ref, grad, grad_bf, turned, acc, part_a, part_g, d_both, w_ff1, w_ff2, tile, recv, obuf,
     in_sem, part_sem, w1_sem, w2_sem, out_sem, send_sem, recv_sem) = refs
    count, width = grad.shape
    half = w_ff2.shape[0]
    chunks, depth = half // width, width // 8
    me = lax.axis_index(AXIS)
    core, mate, mate_slot, own_chip = chip_places(me)

    load_grad = pltpu.make_async_copy(grad_ref, grad, in_sem.at[0])
    load_norm = pltpu.make_async_copy(norm_ref, d_both.at[:, pl.ds(0, width)], in_sem.at[1])
    load_grad.start()
    load_norm.start()
    start_load(pieces[8:], offset, w_ff2, w2_sem)

    def parts(chunk):
        at = (slice(None), pl.ds(pl.multiple_of(chunk * width, width), width))
        return [pltpu.make_async_copy(ref.at[at], buf.at[lax.rem(chunk, 2)], part_sem.at[which, lax.rem(chunk, 2)])
                for which, (ref, buf) in enumerate(((save_a, part_a), (save_g, part_g)))]

    def load_h(step):
        return pltpu.make_async_copy(h_ref.at[pl.ds(step * STEP, STEP), :], part_a.at[0, pl.ds(step * STEP, STEP), :], part_sem.at[0, 0])

    for copy in parts(0):
        copy.start()
    devices = piece_devices(me)
    for chunk in range(chunks):
        for kind in range(2):
            for piece, device in zip(pieces[:8], devices):
                pltpu.make_async_copy(
                    piece.at[pl.ds((kind * chunks + chunk) * depth, depth), :],
                    w_ff1.at[pl.ds(pl.multiple_of(device * depth, 16), depth), pl.ds((2 * chunk + kind) * width, width)],
                    w1_sem.at[chunk]).start()
    greet(mate)

    def sends(chunk):
        copies = []
        for other in range(4):
            start = pl.multiple_of((2 * other + 1 - core) * depth, 16)
            to = pl.multiple_of(mate_slot(other) * depth, 16)
            copies.append(pltpu.make_async_remote_copy(
                src_ref=tile.at[pl.ds(start, depth), :], dst_ref=recv.at[chunk, pl.ds(to, depth), :], send_sem=send_sem.at[other],
                recv_sem=recv_sem.at[chunk, other], device_id=(mate,), device_id_type=pl.DeviceIdType.MESH))
        return copies

    def wait_write():
        pltpu.make_async_copy(obuf, obuf, out_sem).wait()

    def finish(chunk, first):
        for copy in sends(chunk):
            copy.wait_recv()

        @pl.when(jnp.logical_not(first))
        def _():
            wait_write()

        for slot in range(4):
            start = pl.multiple_of((2 * own_chip(slot) + core) * depth, 16)
            rows = slice(slot * depth, (slot + 1) * depth)
            obuf[rows, :] = tile[pl.ds(start, depth), :] + recv[chunk, rows, :]
        for slot in range(4):
            ref = keep_ref if slot < 2 else far_ref
            for kind in range(2):
                row = pl.multiple_of((slot % 2) * 8 * depth + (kind * chunks + chunk) * depth, 16)
                pltpu.make_async_copy(obuf.at[pl.ds(slot * depth, depth), pl.ds(kind * width, width)], ref.at[pl.ds(row, depth), :],
                                      out_sem).start()
        for copy in sends(chunk):
            copy.wait_send()

    load_grad.wait()
    grad_bf[...] = grad[...].astype(BF16)
    load_norm.wait()
    turned[...] = d_both[:, 0:width].T
    acc[...] = jnp.zeros_like(acc)
    bias_ref[...] = jnp.zeros_like(bias_ref)
    vec_ref[...] = jnp.zeros_like(vec_ref)
    wait_load(w_ff2, w2_sem)

    def one_chunk(chunk, carry):
        w_pair = w_ff1.at[:, pl.ds(pl.multiple_of(chunk * 2 * width, width), 2 * width)]
        pltpu.make_async_copy(w_pair, w_pair, w1_sem.at[chunk]).wait()
        for copy in parts(chunk):
            copy.wait()

        @pl.when(chunk + 1 < chunks)
        def _():
            for copy in parts(chunk + 1):
                copy.start()

        even = lax.rem(chunk, 2)
        w_down = w_ff2.at[pl.ds(pl.multiple_of(chunk * width, width), width), :]
        sums = [0.0, 0.0]
        ahead = dot_nt(grad_bf[0:FF_ROWS, :], w_down[...])
        for start in range(0, count, FF_ROWS):
            rows = slice(start, start + FF_ROWS)
            d_gated = ahead
            if start + FF_ROWS < count:
                ahead = dot_nt(grad_bf[start + FF_ROWS:start + 2 * FF_ROWS, :], w_down[...])
            for kind, saved in enumerate((part_a, part_g)):
                d_part = d_gated * saved[even, rows, :]
                sums[kind] = sums[kind] + jnp.sum(d_part, axis=0, keepdims=True)
                d_both[rows, kind * width:(kind + 1) * width] = d_part.astype(BF16)
            acc[rows, :] += dot_nt(d_both[rows, :], w_pair[...])
        for kind in range(2):
            bias_ref[0:1, pl.ds(pl.multiple_of(kind * half + chunk * width, 2 * HEAD), width)] += sums[kind]

        @pl.when(chunk > 0)
        def _():
            finish(jnp.maximum(chunk - 1, 0), chunk == 1)

        tile[...] = dot_nn(turned[...], d_both[...])
        for copy in sends(chunk):
            copy.start()
        return carry

    lax.fori_loop(0, chunks, one_chunk, 0)
    steps = count // STEP
    for step in range(steps):
        load_h(step).start()
    pltpu.make_async_copy(part_a.at[0], part_a.at[0], part_sem.at[0, 0]).wait()
    for step in range(steps):
        rows = slice(step * STEP, (step + 1) * STEP)
        mine = grad[rows, :].astype(F32)
        d_res, g_gain, g_shift = norm_back(part_a[0, rows, :], rows_ref[4:5, :], acc[rows, :])
        acc[rows, :] = mine + d_res
        pltpu.make_async_copy(acc.at[pl.ds(step * STEP, STEP), :], out_ref.at[pl.ds(step * STEP, STEP), :], in_sem.at[0]).start()
        for at, row in enumerate((g_gain, g_shift, jnp.sum(mine, axis=0, keepdims=True))):
            vec_ref[at:at + 1, :] += row
    finish(chunks - 1, False)
    wait_write()
    pltpu.make_async_copy(acc, out_ref, in_sem.at[0]).wait()


def ff_grads(kind, grad, save_a, save_g, norm, h, rows, pieces, offset):
    count, width = h.shape
    half = save_a.shape[1]
    vmem = pl.BlockSpec(memory_space=pltpu.VMEM)
    big = shape(2 * width, width, F32)
    dma = pltpu.SemaphoreType.DMA
    saved = pltpu.VMEM((2, count, width), F32)
    return pl.pallas_call(
        functools.partial(ff_grad_kernel, offset), in_specs=[ANY] * 5 + [vmem] + [ANY] * 16, out_specs=[ANY, vmem, vmem, ANY, ANY],
        out_shape=[shape(count, width, F32), shape(8, width, F32), shape(8, 2 * half, F32), big, big],
        scratch_shapes=[pltpu.VMEM((count, width), grad.dtype), pltpu.VMEM((count, width), BF16), pltpu.VMEM((width, count), BF16),
                        pltpu.VMEM((count, width), F32), saved, saved, pltpu.VMEM((count, 2 * width), BF16),
                        pltpu.VMEM((width, 2 * half), BF16), pltpu.VMEM((half, width), BF16), pltpu.VMEM((width, 2 * width), F32),
                        pltpu.VMEM((4, width // 2, 2 * width), F32), pltpu.VMEM((width // 2, 2 * width), F32),
                        dma((2,)), dma((2, 2)), dma((4,)), dma, dma, dma((4,)), dma((4, 4))],
        cost_estimate=pl.CostEstimate(flops=count * width * half * 10, bytes_accessed=int(6e7), transcendentals=0),
        compiler_params=pltpu.CompilerParams(collective_id=kind, has_side_effects=True, vmem_limit_bytes=VMEM_MOST))(grad, save_a, save_g, norm, h, rows, *pieces)


def finish_scatter(far, keep, n_dev):
    near_perm, far_perm, _ = gather_perms(n_dev)
    rows = keep.shape[0] // 2
    second = permute(far, far_perm)
    third = permute(keep[rows:] + second[rows:], near_perm)
    return keep[:rows] + second[:rows] + third


def solution(mesh):
    n_dev = mesh.shape[AXIS]

    def inner(tokens_x, context, cot_out, *shards):
        batch, tokens, width = tokens_x.shape
        _, valid, ctx_width = context.shape
        blocks = shards[0].shape[0]
        total = batch * n_dev
        depth = width // n_dev
        count = batch * tokens
        half = 4 * width

        views = []
        for shard, rows in zip(shards[:7], (depth, depth, depth, ctx_width // n_dev, depth, depth, half // n_dev)):
            views.append(shard.reshape(blocks, rows, -1))
        qkv_s, out_s = lax.optimization_barrier(views[:2])
        q2_s, kv2_s, out2_s = lax.optimization_barrier(views[2:5])
        ff1_s, ff2_s = lax.optimization_barrier(views[5:])
        me = lax.axis_index(AXIS)
        vec_len = shards[7].shape[1]
        vec_each = 17
        vec_rows = (blocks * vec_each + 15) // 16 * 16
        vec_block = lax.dynamic_update_slice(jnp.zeros((blocks, n_dev * vec_len), BF16), shards[7], (0, me * vec_len))
        vec_block = vec_block[:, :vec_each * width].reshape(blocks * vec_each, width)
        vec_block = jnp.pad(vec_block, ((0, vec_rows - blocks * vec_each), (0, 0)))

        members = []
        for layer in range(blocks):
            members += [(layer, [qkv_s, out_s]), (layer, [kv2_s, q2_s, out2_s])]
            members += [(layer, [ff1_s, ff2_s])] if layer < blocks - 1 else [(layer, [ff1_s]), (layer, [ff2_s])]
        groups = []
        for index, (layer, parts) in enumerate(members):
            block = pack(parts, layer, [vec_block] if index == 0 else [], width)
            groups.append(gather_group(block, n_dev))
        ff_groups = [groups[3 * layer + 2] * 2 if layer < blocks - 1 else groups[-2] + groups[-1] for layer in range(blocks)]
        ff_offsets = [8 * depth if layer < blocks - 1 else 0 for layer in range(blocks)]

        vecs = vec_sum(groups[0], vec_rows)
        vecs = vecs[:blocks * vec_each].reshape(blocks, vec_each, width)
        rows_all = jnp.pad(vecs[:, :9], ((0, 0), (0, 7), (0, 0)))
        bias_all = vecs[:, 9:].reshape(blocks, 1, 8 * width)

        ctx, ctx_mine, ctx_other = prepare_context(context, n_dev)

        h = tokens_x.reshape(count, width)
        saved = []
        for layer in range(blocks):
            rows, bias = rows_all[layer], bias_all[layer]
            group = groups[3 * layer:3 * layer + 2]
            norm1, qkv, mix1, h1 = self_forward(h, rows, group[0], tokens)
            norm2, query, kv, mix2, h2 = cross_forward(h1, rows, ctx, group[1], tokens, valid)
            if layer < blocks - 1:
                norm3, gated, save_a, save_g, h3 = ff_forward(h2, rows, bias, ff_groups[layer], ff_offsets[layer])
            else:
                norm3, gated, save_a, save_g = ff_up_forward(h2, rows, bias, groups[-2])
                out_tokens = ff_down_forward(h2, rows, gated, groups[-1])
            saved.append((h, norm1, qkv, mix1, h1, norm2, query, kv, mix2, h2, norm3, gated, save_a, save_g))
            h = h3 if layer < blocks - 1 else None

        grad = cot_out.reshape(count, width)
        results, vec_grads = [None] * blocks, [None] * blocks
        for layer in reversed(range(blocks)):
            turn = blocks - 1 - layer
            rows, group = rows_all[layer], groups[3 * layer:3 * layer + 2]
            h0, norm1, qkv, mix1, h1, norm2, query, kv, mix2, h2, norm3, gated, save_a, save_g = saved[layer]

            def reduce(pair):
                return finish_scatter(pair[0], pair[1], n_dev)

            r_ff2 = reduce(weight_grads(1, (gated, grad.astype(BF16)),
                                           [(0, c * width, 1, 0, 0, half // n_dev, (c,)) for c in range(half // width)], half // n_dev))
            grad, vec3, vec_b1, *pair = ff_grads(5 + turn, grad, save_a, save_g, norm3, h2, rows, ff_groups[layer],
                                                 ff_offsets[layer])
            r_ff1 = reduce(pair)
            grad, vec2, *pair = cross_backward(grad, query, kv, h1, rows, norm2, mix2, ctx_mine, ctx_other, group[1],
                                               tokens, valid)
            r_cross = reduce(pair)
            grad, vec1, *pair = self_backward(8 + turn, grad, qkv, h0, rows, norm1, mix1, group[0], tokens,
                                              BF16 if layer == 0 else F32)
            r_self = reduce(pair)
            side = lambda array, blocks_of: jnp.concatenate(jnp.split(array, blocks_of, 0), 1)
            results[layer] = [side(r_self[:3 * depth], 3), r_self[3 * depth:], r_cross[:depth], side(r_cross[2 * depth:], 2), r_cross[depth:2 * depth],
                              side(r_ff1, 8), r_ff2]
            vec_grads[layer] = [vec1, vec2, vec3, vec_b1]
        vec_out = vec_total([part for parts in vec_grads for part in parts], vec_rows, n_dev)
        vec_out = vec_out[:blocks * vec_each].reshape(blocks, vec_each * width)
        vec_out = jnp.pad(vec_out, ((0, 0), (0, vec_len * n_dev - vec_each * width)))
        vec_out = lax.dynamic_slice(vec_out, (0, me * vec_len), (blocks, vec_len))
        outs = []
        for index in range(7):
            stacked = jnp.stack([results[layer][index] for layer in range(blocks)]) / total
            stacked = lax.optimization_barrier(stacked)
            outs.append(stacked.reshape(blocks, -1))
        outs.append(vec_out / total)
        return tuple([out_tokens.reshape(tokens_x.shape), grad.reshape(tokens_x.shape)] + outs)

    param_spec = P(None, AXIS)
    in_specs = (P(AXIS), P(AXIS), P(AXIS)) + (param_spec,) * 8
    out_specs = (P(AXIS), P(AXIS)) + (param_spec,) * 8
    return jax.shard_map(inner, mesh=mesh, in_specs=in_specs, out_specs=out_specs, check_vma=False)
```

```python
import functools
import math
import jax
import jax.numpy as jnp
from jax import lax
from jax.experimental import pallas as pl
from jax.experimental.pallas import tpu as pltpu
from jax.sharding import PartitionSpec as P


HEAD = 64
AXIS = 'fsdp'
CHUNK = 1280
FF_ROWS = 256
FF_STEP = 256
STEP = 512
VMEM_LIMIT = 60 * 1024 * 1024
VMEM_MOST = 67043328
FORWARD_UNROLL = 10

F32 = jnp.float32
BF16 = jnp.bfloat16
ANY = pl.BlockSpec(memory_space=pl.ANY)


def gather_perms(n_dev):
    near = [(i, i ^ (4 if i % 2 == 0 else 2)) for i in range(n_dev)]
    far = [(i, i ^ (2 if i % 2 == 0 else 4)) for i in range(n_dev)]
    core = [(i, i ^ 1) for i in range(n_dev)]
    return near, far, core


def pack_kernel(*refs):
    ins, out = refs[:-1], refs[-1]
    width, row = out.shape[1], 0
    for ref in ins:
        depth = ref.shape[-2]
        for col in range(0, ref.shape[-1], width):
            piece = ref[0, :, col:col + width] if len(ref.shape) == 3 else ref[:, col:col + width]
            out[row:row + depth, :] = piece
            row += depth


def pack(views, layer, extra, width):
    rows = sum(v.shape[1] * v.shape[2] // width for v in views) + sum(e.shape[0] for e in extra)
    specs = [pl.BlockSpec((1,) + v.shape[1:], lambda i: (layer, 0, 0)) for v in views]
    specs += [pl.BlockSpec(e.shape, lambda i: (0, 0)) for e in extra]
    return pl.pallas_call(
        pack_kernel, grid=(1,), in_specs=specs, out_specs=pl.BlockSpec((rows, width), lambda i: (0, 0)),
        out_shape=jax.ShapeDtypeStruct((rows, width), BF16),
        cost_estimate=pl.CostEstimate(flops=rows * width, bytes_accessed=rows * width * 4, transcendentals=0),
        name='pack')(*views, *extra)


def vec_kernel(*refs):
    pieces, (out, buf, sem) = refs[:8], refs[8:]
    rows = out.shape[0]
    copies = [pltpu.make_async_copy(piece.at[pl.ds(piece.shape[0] - rows, rows), :], buf.at[index], sem.at[index])
              for index, piece in enumerate(pieces)]
    for copy in copies:
        copy.start()
    total = None
    for index, copy in enumerate(copies):
        copy.wait()
        total = buf[index].astype(F32) if total is None else total + buf[index].astype(F32)
    out[...] = total


def vec_sum(pieces, rows):
    width = pieces[0].shape[1]
    return pl.pallas_call(
        vec_kernel, in_specs=[ANY] * 8, out_specs=pl.BlockSpec(memory_space=pltpu.VMEM),
        out_shape=jax.ShapeDtypeStruct((rows, width), F32),
        scratch_shapes=[pltpu.VMEM((8, rows, width), BF16), pltpu.SemaphoreType.DMA((8,))],
        cost_estimate=pl.CostEstimate(flops=rows * width * 8, bytes_accessed=rows * width * 20, transcendentals=0),
        name='vec_sum')(*pieces)


def permute(array, perm):
    return lax.ppermute(array, AXIS, perm)


def gather_group(shard, n_dev):
    near, far, core = gather_perms(n_dev)
    first = permute(shard, near)
    second = permute(shard, far)
    third = permute(first, far)
    mine = [shard, first, second, third]
    return mine + [permute(piece, core) for piece in mine]


def piece_devices(me):
    core = lax.rem(me, 2)
    one, two = 4 - 2 * core, 2 + 2 * core
    x = jnp.bitwise_xor
    mate = x(me, 1)
    return [me, x(me, one), x(me, two), x(me, 6), mate, x(mate, two), x(mate, one), x(mate, 6)]


def start_load(pieces, offset, ref, sem):
    width = pieces[0].shape[1]
    depth = ref.shape[0] // 8
    devices = piece_devices(lax.axis_index(AXIS))
    for block in range(ref.shape[1] // width):
        for piece, device in zip(pieces, devices):
            src = piece.at[pl.ds(offset + block * depth, depth), :]
            dst = ref.at[pl.ds(pl.multiple_of(device * depth, 16), depth), pl.ds(block * width, width)]
            pltpu.make_async_copy(src, dst, sem).start()


def wait_load(ref, sem):
    pltpu.make_async_copy(ref, ref, sem).wait()


def dot_nn(a, b):
    return lax.dot_general(a, b, (((1,), (0,)), ((), ())), preferred_element_type=F32)


def dot_nt(a, b):
    return lax.dot_general(a, b, (((1,), (1,)), ((), ())), preferred_element_type=F32)


def dot_tn(a, b):
    return lax.dot_general(a, b, (((0,), (0,)), ((), ())), preferred_element_type=F32)


def norm_stats(x):
    average = jnp.mean(x, axis=-1, keepdims=True)
    centered = x - average
    variance = jnp.mean(centered * centered, axis=-1, keepdims=True)
    scale = lax.rsqrt(variance + 1e-5)
    return centered * scale, scale


def norm_back(x, gain, d_norm):
    unit, scale = norm_stats(x)
    d_unit = d_norm * gain
    inner = d_unit - jnp.mean(d_unit, axis=-1, keepdims=True) - unit * jnp.mean(d_unit * unit, axis=-1, keepdims=True)
    return scale * inner, jnp.sum(d_norm * unit, axis=0, keepdims=True), jnp.sum(d_norm, axis=0, keepdims=True)


def softmax_rows(scores):
    top = jnp.max(scores, axis=-1, keepdims=True)
    raised = jnp.exp(scores - top)
    return raised * (1.0 / jnp.sum(raised, axis=-1, keepdims=True))


def low_lanes(rows):
    return lax.broadcasted_iota(jnp.int32, (rows, 2 * HEAD), 1) < HEAD


def heads_of(pair):
    low, zero = low_lanes(pair.shape[0]), jnp.zeros_like(pair)
    return jnp.where(low, pair, zero), jnp.where(low, zero, pair)


def pair_forward(query, key, value, valid=None):
    mixed = []
    for q_head in heads_of(query * HEAD ** -0.5):
        scores = dot_nt(q_head, key)
        if valid is not None:
            column = lax.broadcasted_iota(jnp.int32, scores.shape, 1)
            scores = jnp.where(column < valid, scores, -1e30)
        mixed.append(dot_nn(softmax_rows(scores).astype(BF16), value))
    return jnp.where(low_lanes(query.shape[0]), mixed[0], mixed[1]).astype(BF16)


def backward_scores(query, key, value, d_out):
    q_heads, d_heads = heads_of(query * HEAD ** -0.5), heads_of(d_out)
    return q_heads, d_heads, [dot_nt(key, q) for q in q_heads], [dot_nt(value, d) for d in d_heads]


def backward_probs(scores, d_probs, valid):
    if valid is not None:
        row = lax.broadcasted_iota(jnp.int32, scores.shape, 0)
        scores = jnp.where(row < valid, scores, -1e30)
    raised = jnp.exp(scores - jnp.max(scores, axis=0, keepdims=True))
    probs = raised * (1.0 / jnp.sum(raised, axis=0, keepdims=True))
    inner = jnp.sum(d_probs * probs, axis=0, keepdims=True)
    return probs.astype(BF16), (probs * (d_probs - inner)).astype(BF16)


def pairs_backward(pairs, load, store, valid=None):
    ahead = load(0)
    ahead = ahead, backward_scores(*ahead)
    for pair in range(pairs):
        (query, key, value, d_out), (q_heads, d_heads, scores, d_probs) = ahead
        if pair + 1 < pairs:
            ahead = load(pair + 1)
            ahead = ahead, backward_scores(*ahead)
        turned = key.T
        d_query, d_key, d_value = [], 0.0, 0.0
        for head in range(2):
            probs, d_scores = backward_probs(scores[head], d_probs[head], valid)
            d_query.append(dot_nn(turned[head * HEAD:(head + 1) * HEAD, :], d_scores))
            d_key = d_key + dot_nn(d_scores, q_heads[head])
            d_value = d_value + dot_nn(probs, d_heads[head])
        d_query = (jnp.concatenate(d_query, 0) * HEAD ** -0.5).T
        store(pair, d_query.astype(BF16), d_key.astype(BF16), d_value.astype(BF16))


def chip_places(me):
    core, chip = lax.rem(me, 2), me // 2
    chip_x, chip_y = lax.rem(chip, 2), chip // 2

    def mate_slot(other):
        d_x, d_y = lax.rem(chip_x + other % 2, 2), lax.rem(chip_y + other // 2, 2)
        return d_x + 2 * d_y + core * (d_x - d_y)

    def own_chip(slot):
        one, two = slot // 2, slot % 2
        d_x, d_y = one + core * (two - one), two + core * (one - two)
        return 2 * lax.rem(chip_y + d_y, 2) + lax.rem(chip_x + d_x, 2)

    return core, me + 1 - 2 * core, mate_slot, own_chip


def greet(mate):
    barrier = pltpu.get_barrier_semaphore()
    pl.semaphore_signal(barrier, inc=1, device_id=(mate,), device_id_type=pl.DeviceIdType.MESH)
    pl.semaphore_wait(barrier, 1)


def tile_sends(q, rows, tile, recv, send_sem, recv_sem):
    core, mate, mate_slot, _ = chip_places(lax.axis_index(AXIS))
    copies = []
    for other in range(4):
        start = pl.multiple_of((2 * other + 1 - core) * rows, 16)
        copies.append(pltpu.make_async_remote_copy(
            src_ref=tile.at[q, pl.ds(start, rows), :], dst_ref=recv.at[mate_slot(other), pl.ds(q * rows, rows), :],
            send_sem=send_sem.at[q, other], recv_sem=recv_sem.at[q, other],
            device_id=(mate,), device_id_type=pl.DeviceIdType.MESH))
    return copies


def finish_tiles(tiles, rows, group_rows, tile, recv, send_sem, recv_sem, far_ref, keep_ref):
    core, _, _, own_chip = chip_places(lax.axis_index(AXIS))
    for q in range(tiles):
        for copy in tile_sends(q, rows, tile, recv, send_sem, recv_sem):
            copy.wait()
        for slot in range(4):
            ref = keep_ref if slot < 2 else far_ref
            start = pl.multiple_of((2 * own_chip(slot) + core) * rows, 16)
            at = (slot % 2) * group_rows + q * rows
            ref[at:at + rows, :] = tile[q, pl.ds(start, rows), :] + recv[slot, q * rows:(q + 1) * rows, :]


def add_rows(ref, step, rows):
    @pl.when(step == 0)
    def _():
        ref[...] = jnp.zeros_like(ref)

    for index, row in enumerate(rows):
        ref[pl.ds(index, 1), :] += row


def self_loads(pieces, w_qkv, w_out, sems):
    start_load(pieces, 0, w_qkv, sems.at[0])
    start_load(pieces, 3 * (w_out.shape[0] // 8), w_out, sems.at[1])


def cross_loads(pieces, offset, w_kv, w_query, w_out, sems):
    deep, depth = w_kv.shape[0] // 8, w_out.shape[0] // 8
    start_load(pieces, offset, w_kv, sems.at[0])
    start_load(pieces, offset + 2 * deep, w_query, sems.at[1])
    start_load(pieces, offset + 2 * deep + depth, w_out, sems.at[2])


def self_forward_kernel(samples, tokens, h_ref, rows_ref, *refs):
    @pl.when(pl.program_id(0) == 0)
    def _():
        self_loads(refs[:8], *refs[12:])

    self_forward_step(samples, tokens, h_ref, rows_ref, *refs[8:])


def cross_forward_kernel(samples, tokens, valid, h_ref, rows_ref, ctx_ref, *refs):
    @pl.when(pl.program_id(0) == 0)
    def _():
        cross_loads(refs[:8], 0, *refs[13:])

    cross_forward_step(samples, tokens, valid, h_ref, rows_ref, ctx_ref, *refs[8:])


def attention_forward_kernel(samples, tokens, valid, h_ref, rows_ref, ctx_ref, *refs):
    pieces, self_outs, cross_outs, self_scratch, cross_scratch = refs[:8], refs[8:12], refs[12:17], refs[17:20], refs[20:24]

    @pl.when(pl.program_id(0) == 0)
    def _():
        self_loads(pieces, *self_scratch)
        cross_loads(pieces, 4 * (h_ref.shape[1] // 8), *cross_scratch)

    self_forward_step(samples, tokens, h_ref, rows_ref, *self_outs, *self_scratch)
    cross_forward_step(samples, tokens, valid, self_outs[3], rows_ref, ctx_ref, *cross_outs, *cross_scratch)


def self_forward_step(samples, tokens, h_ref, rows_ref, norm_ref, qkv_ref, mix_ref, out_ref, w_qkv, w_out, sems):
    width = h_ref.shape[1]
    step = pl.program_id(0)
    x = h_ref[...].astype(F32)
    unit, _ = norm_stats(x)
    normed = (unit * rows_ref[0:1, :] + rows_ref[1:2, :]).astype(BF16)
    norm_ref[...] = normed

    @pl.when(step == 0)
    def _():
        wait_load(w_qkv, sems.at[0])
        wait_load(w_out, sems.at[1])

    qkv_ref[...] = dot_nn(normed, w_qkv[...]).astype(BF16)
    pairs = width // (2 * HEAD)

    def body(index, carry):
        row = pl.multiple_of((index // pairs) * tokens, tokens)
        col = pl.multiple_of((index % pairs) * 2 * HEAD, 2 * HEAD)
        part = lambda which: qkv_ref[pl.ds(row, tokens), pl.ds(which * width + col, 2 * HEAD)]
        mix_ref[pl.ds(row, tokens), pl.ds(col, 2 * HEAD)] = pair_forward(part(0), part(1), part(2))
        return carry

    lax.fori_loop(0, samples * pairs, body, 0, unroll=FORWARD_UNROLL)
    out_ref[...] = x + dot_nn(mix_ref[...], w_out[...]) + rows_ref[6:7, :]


def cross_forward_step(samples, tokens, valid, h_ref, rows_ref, ctx_ref, norm_ref, query_ref, kv_ref, mix_ref, out_ref, w_kv, w_query,
                       w_out, sems):
    width = h_ref.shape[1]
    step = pl.program_id(0)
    padded = ctx_ref.shape[0] // (samples * pl.num_programs(0))
    x = h_ref[...]
    unit, _ = norm_stats(x)
    normed = (unit * rows_ref[2:3, :] + rows_ref[3:4, :]).astype(BF16)
    norm_ref[...] = normed

    @pl.when(step == 0)
    def _():
        wait_load(w_kv, sems.at[0])
        wait_load(w_query, sems.at[1])
        wait_load(w_out, sems.at[2])
        kv_ref[...] = dot_nn(ctx_ref[...], w_kv[...]).astype(BF16)

    query_ref[...] = dot_nn(normed, w_query[...]).astype(BF16)
    pairs = width // (2 * HEAD)

    def body(index, carry):
        sample = index // pairs
        row = pl.multiple_of(sample * tokens, tokens)
        kv_row = pl.multiple_of((step * samples + sample) * padded, 16)
        col = pl.multiple_of((index % pairs) * 2 * HEAD, 2 * HEAD)
        query = query_ref[pl.ds(row, tokens), pl.ds(col, 2 * HEAD)]
        key = kv_ref[pl.ds(kv_row, padded), pl.ds(col, 2 * HEAD)]
        value = kv_ref[pl.ds(kv_row, padded), pl.ds(width + col, 2 * HEAD)]
        mix_ref[pl.ds(row, tokens), pl.ds(col, 2 * HEAD)] = pair_forward(query, key, value, valid)
        return carry

    lax.fori_loop(0, samples * pairs, body, 0, unroll=FORWARD_UNROLL)
    out_ref[...] = x + dot_nn(mix_ref[...], w_out[...]) + rows_ref[7:8, :]


def ff_loads(pieces, offset, w_ff1, w_ff2, sems):
    start_load(pieces[:8], 0, w_ff1, sems.at[0])
    start_load(pieces[8:], offset, w_ff2, sems.at[1])


def ff_up(normed, bias_ref, w_ff1, half, start, gated_ref, save_a, save_g):
    u_a = dot_nn(normed, w_ff1[:, start:start + CHUNK]) + bias_ref[:, start:start + CHUNK]
    u_g = dot_nn(normed, w_ff1[:, half + start:half + start + CHUNK]) + bias_ref[:, half + start:half + start + CHUNK]
    cumulative = 0.5 * (1.0 + lax.erf(u_g * math.sqrt(0.5)))
    gate = u_g * cumulative
    slope = cumulative + u_g * (jnp.exp(-0.5 * u_g * u_g) * (1.0 / math.sqrt(2.0 * math.pi)))
    gated = (u_a * gate).astype(BF16)
    gated_ref[:, start:start + CHUNK] = gated
    save_a[:, start:start + CHUNK] = gate
    save_g[:, start:start + CHUNK] = u_a * slope
    return gated


def ff_forward_kernel(offset, h_ref, rows_ref, bias_ref, *refs):
    pieces, (norm_ref, gated_ref, save_a, save_g, out_ref, w_ff1, w_ff2, sems) = refs[:16], refs[16:]
    half = w_ff2.shape[0]
    step = pl.program_id(0)

    @pl.when(step == 0)
    def _():
        ff_loads(pieces, offset, w_ff1, w_ff2, sems)

    x = h_ref[...]
    unit, _ = norm_stats(x)
    normed = (unit * rows_ref[4:5, :] + rows_ref[5:6, :]).astype(BF16)
    norm_ref[...] = normed

    @pl.when(step == 0)
    def _():
        wait_load(w_ff1, sems.at[0])
        wait_load(w_ff2, sems.at[1])

    total = x + rows_ref[8:9, :]
    for start in range(0, half, CHUNK):
        gated = ff_up(normed, bias_ref, w_ff1, half, start, gated_ref, save_a, save_g)
        total = total + dot_nn(gated, w_ff2[start:start + CHUNK, :])
    out_ref[...] = total


def ff_up_kernel(h_ref, rows_ref, bias_ref, *refs):
    pieces, (norm_ref, gated_ref, save_a, save_g, w_ff1, sems) = refs[:8], refs[8:]
    half = w_ff1.shape[1] // 2
    step = pl.program_id(0)

    @pl.when(step == 0)
    def _():
        start_load(pieces, 0, w_ff1, sems.at[0])

    unit, _ = norm_stats(h_ref[...])
    normed = (unit * rows_ref[4:5, :] + rows_ref[5:6, :]).astype(BF16)
    norm_ref[...] = normed

    @pl.when(step == 0)
    def _():
        wait_load(w_ff1, sems.at[0])

    for start in range(0, half, CHUNK):
        ff_up(normed, bias_ref, w_ff1, half, start, gated_ref, save_a, save_g)


def ff_down_kernel(h_ref, rows_ref, gated_ref, *refs):
    pieces, (out_ref, w_ff2, sems) = refs[:8], refs[8:]
    step = pl.program_id(0)

    @pl.when(step == 0)
    def _():
        start_load(pieces, 0, w_ff2, sems.at[0])
        wait_load(w_ff2, sems.at[0])

    out_ref[...] = (h_ref[...] + rows_ref[8:9, :] + dot_nn(gated_ref[...], w_ff2[...])).astype(BF16)


def cross_backward_kernel(samples, tokens, valid, grad_ref, query_ref, kv_ref, h_ref, rows_ref, norm_ref, mix_ref, ctx_mine_ref,
                          ctx_other_ref, *refs):
    pieces, refs = refs[:8], refs[8:]
    (out_ref, vec_ref, far_ref, keep_ref, d_mix, w_query, w_out, d_query, grad_bf, d_kv, kv_other, x_norm, x_mix, ctx_mine, ctx_other,
     tile, recv, sems, load_sem, kv_send, kv_recv, send_sem, recv_sem) = refs
    width = h_ref.shape[1]
    depth = width // 8
    step, last = pl.program_id(0), pl.num_programs(0) - 1
    padded = kv_ref.shape[0] // samples
    context_rows = kv_ref.shape[0] * (last + 1)
    mate = chip_places(lax.axis_index(AXIS))[1]
    loads = [pltpu.make_async_copy(src, dst, load_sem.at[index]) for index, (src, dst) in enumerate(
        ((norm_ref, x_norm), (mix_ref, x_mix), (ctx_mine_ref, ctx_mine), (ctx_other_ref, ctx_other)))]
    exchange = pltpu.make_async_remote_copy(
        src_ref=d_kv.at[pl.ds(0, context_rows), :], dst_ref=kv_other.at[pl.ds(0, context_rows), :], send_sem=kv_send, recv_sem=kv_recv,
        device_id=(mate,), device_id_type=pl.DeviceIdType.MESH)

    @pl.when(step == 0)
    def _():
        base = pieces[0].shape[0] - 2 * depth
        start_load(pieces, base, w_query, sems.at[0])
        start_load(pieces, base + depth, w_out, sems.at[1])
        for copy in loads:
            copy.start()
        for ref in (d_kv, kv_other):
            ref[context_rows:, :] = jnp.zeros((ref.shape[0] - context_rows, ref.shape[1]), BF16)
        greet(mate)

    grad = grad_ref[...]
    mine = pl.ds(pl.multiple_of(step * grad.shape[0], grad.shape[0]), grad.shape[0])
    grad_bf[mine, :] = grad.astype(BF16)

    @pl.when(step == 0)
    def _():
        wait_load(w_query, sems.at[0])
        wait_load(w_out, sems.at[1])

    d_mix[...] = dot_nt(grad.astype(BF16), w_out[...]).astype(BF16)
    pairs = width // (2 * HEAD)

    at = lambda which, pair: slice(which * width + pair * 2 * HEAD, which * width + (pair + 1) * 2 * HEAD)

    def load(index):
        sample, pair = index // pairs, index % pairs
        row, here = slice(sample * tokens, (sample + 1) * tokens), slice(sample * padded, (sample + 1) * padded)
        return query_ref[row, at(0, pair)], kv_ref[here, at(0, pair)], kv_ref[here, at(1, pair)], d_mix[row, at(0, pair)]

    def store(index, d_q, d_key, d_value):
        sample, pair = index // pairs, index % pairs
        d_query[pl.ds(pl.multiple_of((step * samples + sample) * tokens, tokens), tokens), at(0, pair)] = d_q
        there = pl.ds(pl.multiple_of((step * samples + sample) * padded, 16), padded)
        d_kv[there, at(0, pair)] = d_key
        d_kv[there, at(1, pair)] = d_value

    pairs_backward(samples * pairs, load, store, valid)
    rows, summed = depth, 2 * depth
    group_rows = keep_ref.shape[0] // 2
    deep = ctx_mine.shape[0] // 4

    def context_part(ctx, kv, slot, block):
        return dot_nn(ctx[slot * deep:(slot + 1) * deep, :], kv[:, block * width:(block + 1) * width])

    def context_at(slot, block):
        start = (slot % 2) * group_rows + summed + block * deep
        return slice(start, start + deep)

    @pl.when(step == last)
    def _():
        for copy in loads:
            copy.wait()
        tile[0] = dot_tn(x_norm[...], d_query[...])
        exchange.start()
        tile[1] = dot_tn(x_mix[...], grad_bf[...])
        for copy in tile_sends(0, rows, tile, recv, send_sem, recv_sem):
            copy.start()
        for slot in range(4):
            for block in range(2):
                (keep_ref if slot < 2 else far_ref)[context_at(slot, block), :] = context_part(ctx_mine, d_kv, slot, block)
        for copy in tile_sends(1, rows, tile, recv, send_sem, recv_sem):
            copy.start()

    d_norm = dot_nt(d_query[mine, :], w_query[...])
    d_res, g_gain, g_shift = norm_back(h_ref[...], rows_ref[2:3, :], d_norm)
    out_ref[...] = grad + d_res
    add_rows(vec_ref, step, [g_gain, g_shift, jnp.sum(grad, axis=0, keepdims=True)])

    @pl.when(step == last)
    def _():
        exchange.wait()
        for slot in range(4):
            for block in range(2):
                (keep_ref if slot < 2 else far_ref)[context_at(slot, block), :] += context_part(ctx_other, kv_other, slot, block)
        finish_tiles(2, rows, group_rows, tile, recv, send_sem, recv_sem, far_ref, keep_ref)


def self_backward_kernel(samples, tokens, grad_ref, qkv_ref, h_ref, rows_ref, norm_ref, mix_ref, *refs):
    pieces, refs = refs[:8], refs[8:]
    (out_ref, rounded_ref, vec_ref, far_ref, keep_ref, d_mix, w_qkv, w_out, d_qkv, grad_bf, x_norm, x_mix, tile, recv, sems, load_sem,
     send_sem, recv_sem) = refs
    width = h_ref.shape[1]
    depth = width // 8
    step, last = pl.program_id(0), pl.num_programs(0) - 1
    mate = chip_places(lax.axis_index(AXIS))[1]
    loads = [pltpu.make_async_copy(src, dst, load_sem.at[index]) for index, (src, dst) in enumerate(((norm_ref, x_norm), (mix_ref, x_mix)))]

    @pl.when(step == 0)
    def _():
        start_load(pieces, 0, w_qkv, sems.at[0])
        start_load(pieces, 3 * depth, w_out, sems.at[1])
        for copy in loads:
            copy.start()
        greet(mate)

    grad = grad_ref[...]
    mine = pl.ds(pl.multiple_of(step * grad.shape[0], grad.shape[0]), grad.shape[0])
    grad_bf[mine, :] = grad.astype(BF16)

    @pl.when(step == 0)
    def _():
        wait_load(w_qkv, sems.at[0])
        wait_load(w_out, sems.at[1])

    d_mix[...] = dot_nt(grad.astype(BF16), w_out[...]).astype(BF16)
    pairs = width // (2 * HEAD)

    at = lambda which, pair: slice(which * width + pair * 2 * HEAD, which * width + (pair + 1) * 2 * HEAD)
    rows_of = lambda sample: slice(sample * tokens, (sample + 1) * tokens)
    all_rows_of = lambda sample: pl.ds(pl.multiple_of((step * samples + sample) * tokens, tokens), tokens)

    def load(index):
        row, pair = rows_of(index // pairs), index % pairs
        return tuple(qkv_ref[row, at(which, pair)] for which in range(3)) + (d_mix[row, at(0, pair)],)

    def store(index, *parts):
        for which, part in enumerate(parts):
            d_qkv[all_rows_of(index // pairs), at(which, index % pairs)] = part

    pairs_backward(samples * pairs, load, store)

    @pl.when(step == last)
    def _():
        for copy in loads:
            copy.wait()
        for q in range(4):
            if q < 3:
                tile[q] = dot_tn(x_norm[...], d_qkv[:, q * width:(q + 1) * width])
            else:
                tile[q] = dot_tn(x_mix[...], grad_bf[...])
            if q > 0:
                for copy in tile_sends(q - 1, depth, tile, recv, send_sem, recv_sem):
                    copy.start()

    d_norm = dot_nt(d_qkv[mine, :], w_qkv[...])

    @pl.when(step == last)
    def _():
        for copy in tile_sends(3, depth, tile, recv, send_sem, recv_sem):
            copy.start()

    d_res, g_gain, g_shift = norm_back(h_ref[...].astype(F32), rows_ref[0:1, :], d_norm)
    out_ref[...] = grad + d_res
    rounded_ref[...] = (grad + d_res).astype(BF16)
    add_rows(vec_ref, step, [g_gain, g_shift, jnp.sum(grad, axis=0, keepdims=True)])

    @pl.when(step == last)
    def _():
        finish_tiles(4, depth, 4 * depth, tile, recv, send_sem, recv_sem, far_ref, keep_ref)


def by_step(rows, columns):
    return pl.BlockSpec((rows, columns), lambda i: (i, 0))


def whole(rows, columns):
    return pl.BlockSpec((rows, columns), lambda i: (0, 0))


def shape(rows, columns, dtype):
    return jax.ShapeDtypeStruct((rows, columns), dtype)


def call(kernel, steps, in_specs, out_specs, out_shapes, scratch, flops, moved, kind=None):
    return pl.pallas_call(
        kernel, grid=(steps,), in_specs=in_specs, out_specs=out_specs, out_shape=out_shapes, scratch_shapes=scratch,
        cost_estimate=pl.CostEstimate(flops=int(flops), bytes_accessed=int(moved), transcendentals=0),
        compiler_params=pltpu.CompilerParams(dimension_semantics=('arbitrary',), vmem_limit_bytes=VMEM_LIMIT, collective_id=kind,
                                             has_side_effects=kind is not None))


def self_forward(h, rows, pieces, tokens):
    count, width = h.shape
    return call(
        functools.partial(self_forward_kernel, STEP // tokens, tokens), count // STEP,
        [by_step(STEP, width), whole(*rows.shape)] + [ANY] * 8,
        [by_step(STEP, width), by_step(STEP, 3 * width), by_step(STEP, width), by_step(STEP, width)],
        [shape(count, width, BF16), shape(count, 3 * width, BF16), shape(count, width, BF16), shape(count, width, F32)],
        [pltpu.VMEM((width, 3 * width), BF16), pltpu.VMEM((width, width), BF16), pltpu.SemaphoreType.DMA((2,))],
        count * width * width * 8 + count * tokens * width * 4, 2e7)(h, rows, *pieces)


def cross_forward(h, rows, ctx, pieces, tokens, valid):
    count, width = h.shape
    ctx_rows, ctx_width = ctx.shape
    return call(
        functools.partial(cross_forward_kernel, STEP // tokens, tokens, valid), count // STEP,
        [by_step(STEP, width), whole(*rows.shape), whole(ctx_rows, ctx_width)] + [ANY] * 8,
        [by_step(STEP, width), by_step(STEP, width), whole(ctx_rows, 2 * width), by_step(STEP, width), by_step(STEP, width)],
        [shape(count, width, BF16), shape(count, width, BF16), shape(ctx_rows, 2 * width, BF16), shape(count, width, BF16),
         shape(count, width, F32)],
        [pltpu.VMEM((ctx_width, 2 * width), BF16), pltpu.VMEM((width, width), BF16), pltpu.VMEM((width, width), BF16),
         pltpu.SemaphoreType.DMA((3,))],
        count * width * width * 4 + ctx_rows * ctx_width * width * 4 + count * 128 * width * 4, 2e7)(h, rows, ctx, *pieces)


def attention_forward(h, rows, ctx, pieces, tokens, valid):
    count, width = h.shape
    ctx_rows, ctx_width = ctx.shape
    one, kv = by_step(STEP, width), whole(ctx_rows, 2 * width)
    thin, full = shape(count, width, BF16), shape(count, width, F32)
    square = pltpu.VMEM((width, width), BF16)
    return call(
        functools.partial(attention_forward_kernel, STEP // tokens, tokens, valid), count // STEP,
        [one, whole(*rows.shape), whole(ctx_rows, ctx_width)] + [ANY] * 8,
        [one, by_step(STEP, 3 * width), one, one, one, one, kv, one, one],
        [thin, shape(count, 3 * width, BF16), thin, full, thin, thin, shape(ctx_rows, 2 * width, BF16), thin, full],
        [pltpu.VMEM((width, 3 * width), BF16), square, pltpu.SemaphoreType.DMA((2,)), pltpu.VMEM((ctx_width, 2 * width), BF16), square,
         square, pltpu.SemaphoreType.DMA((3,))],
        count * width * width * 12 + ctx_rows * ctx_width * width * 4 + count * tokens * width * 6, 4e7)(h, rows, ctx, *pieces)


def ff_forward(h, rows, bias, pieces, offset):
    count, width = h.shape
    half = bias.shape[1] // 2
    return call(
        functools.partial(ff_forward_kernel, offset), count // FF_STEP,
        [by_step(FF_STEP, width), whole(*rows.shape), whole(1, 2 * half)] + [ANY] * 16,
        [by_step(FF_STEP, width), by_step(FF_STEP, half), by_step(FF_STEP, half), by_step(FF_STEP, half), by_step(FF_STEP, width)],
        [shape(count, width, BF16), shape(count, half, BF16), shape(count, half, F32), shape(count, half, F32),
         shape(count, width, F32)],
        [pltpu.VMEM((width, 2 * half), BF16), pltpu.VMEM((half, width), BF16), pltpu.SemaphoreType.DMA((2,))],
        count * width * half * 6, 6e7)(h, rows, bias, *pieces)


def ff_up_forward(h, rows, bias, pieces):
    count, width = h.shape
    half = bias.shape[1] // 2
    return call(
        ff_up_kernel, count // FF_STEP,
        [by_step(FF_STEP, width), whole(*rows.shape), whole(1, 2 * half)] + [ANY] * 8,
        [by_step(FF_STEP, width), by_step(FF_STEP, half), by_step(FF_STEP, half), by_step(FF_STEP, half)],
        [shape(count, width, BF16), shape(count, half, BF16), shape(count, half, F32), shape(count, half, F32)],
        [pltpu.VMEM((width, 2 * half), BF16), pltpu.SemaphoreType.DMA((1,))],
        count * width * half * 4, 5e7)(h, rows, bias, *pieces)


def ff_down_forward(h, rows, gated, pieces):
    count, width = h.shape
    half = gated.shape[1]
    return call(
        ff_down_kernel, count // STEP,
        [by_step(STEP, width), whole(*rows.shape), by_step(STEP, half)] + [ANY] * 8,
        by_step(STEP, width), shape(count, width, BF16),
        [pltpu.VMEM((half, width), BF16), pltpu.SemaphoreType.DMA((1,))],
        count * width * half * 2, 2e7)(h, rows, gated, *pieces)


def cross_backward(kind, grad, query, kv, h, rows, norm, mix, ctx_mine, ctx_other, pieces, tokens, valid):
    count, width = h.shape
    ctx_rows = kv.shape[0]
    steps = count // STEP
    group_rows = 2 * (width // 8) + ctx_mine.shape[0] // 2
    dma = pltpu.SemaphoreType.DMA
    big = pltpu.VMEM((count, width), BF16)
    kv_buf, ctx_buf = pltpu.VMEM((ctx_mine.shape[1], 2 * width), BF16), pltpu.VMEM(ctx_mine.shape, BF16)
    return call(
        functools.partial(cross_backward_kernel, STEP // tokens, tokens, valid), steps,
        [by_step(STEP, width), by_step(STEP, width), by_step(ctx_rows // steps, 2 * width), by_step(STEP, width),
         whole(*rows.shape)] + [ANY] * 12,
        [by_step(STEP, width), whole(8, width), whole(2 * group_rows, width), whole(2 * group_rows, width)],
        [shape(count, width, F32), shape(8, width, F32), shape(2 * group_rows, width, F32), shape(2 * group_rows, width, F32)],
        [pltpu.VMEM((STEP, width), BF16), pltpu.VMEM((width, width), BF16), pltpu.VMEM((width, width), BF16), big, big, kv_buf, kv_buf,
         big, big, ctx_buf, ctx_buf, pltpu.VMEM((2, width, width), F32), pltpu.VMEM((4, 2 * (width // 8), width), F32),
         dma((2,)), dma((4,)), dma, dma, dma((2, 4)), dma((2, 4))],
        count * width * width * 8 + count * 128 * width * 10 + ctx_mine.size * width * 8, 2e7, kind)(
            grad, query, kv, h, rows, norm, mix, ctx_mine, ctx_other, *pieces)


def self_backward(kind, grad, qkv, h, rows, norm, mix, pieces, tokens):
    count, width = h.shape
    group_rows = width // 2
    dma = pltpu.SemaphoreType.DMA
    big = pltpu.VMEM((count, width), BF16)
    return call(
        functools.partial(self_backward_kernel, STEP // tokens, tokens), count // STEP,
        [by_step(STEP, width), by_step(STEP, 3 * width), by_step(STEP, width), whole(*rows.shape)] + [ANY] * 10,
        [by_step(STEP, width), by_step(STEP, width), whole(8, width), whole(2 * group_rows, width), whole(2 * group_rows, width)],
        [shape(count, width, F32), shape(count, width, BF16), shape(8, width, F32), shape(2 * group_rows, width, F32), shape(2 * group_rows, width, F32)],
        [pltpu.VMEM((STEP, width), BF16), pltpu.VMEM((width, 3 * width), BF16), pltpu.VMEM((width, width), BF16),
         pltpu.VMEM((count, 3 * width), BF16), big, big, big, pltpu.VMEM((4, width, width), F32),
         pltpu.VMEM((4, group_rows, width), F32), dma((2,)), dma((2,)), dma((4, 4)), dma((4, 4))],
        count * width * width * 16 + count * tokens * width * 10, 3e7, kind)(grad, qkv, h, rows, norm, mix, *pieces)


def grad_kernel(tiles, group_rows, inputs, *refs):
    ins, refs = refs[:inputs], refs[inputs:]
    far_ref, keep_ref, x_buf, turned, y_buf, tile, own, recv, x_sem, y_sem, send_sem, recv_sem = refs[:12]
    width = tile.shape[1]
    me = lax.axis_index(AXIS)
    core, chip = lax.rem(me, 2), me // 2
    mate = me + 1 - 2 * core
    chip_x, chip_y = lax.rem(chip, 2), chip // 2

    xs, ys, x_of, y_of = [], [], [], []
    for x, x_col, y, y_col, *_ in tiles:
        if not xs or xs[-1] != (x, x_col):
            xs.append((x, x_col))
        if not ys or ys[-1] != (y, y_col):
            ys.append((y, y_col))
        x_of.append(len(xs) - 1)
        y_of.append(len(ys) - 1)

    def load(which, sequence, buf, sem):
        array, col = sequence[which]
        return pltpu.make_async_copy(ins[array].at[:, pl.ds(col, width)], buf.at[which % 2], sem.at[which % 2])

    for which in range(2):
        if which < len(xs):
            load(which, xs, x_buf, x_sem).start()
        if which < len(ys):
            load(which, ys, y_buf, y_sem).start()

    barrier = pltpu.get_barrier_semaphore()
    pl.semaphore_signal(barrier, inc=1, device_id=(mate,), device_id_type=pl.DeviceIdType.MESH)
    pl.semaphore_wait(barrier, 1)

    def sends(q):
        *_, first_row, rows, chips = tiles[q]
        copies = []
        for index, other in enumerate(chips):
            d_x, d_y = lax.rem(chip_x + other % 2, 2), lax.rem(chip_y + other // 2, 2)
            slot = d_x + 2 * d_y + core * (d_x - d_y)
            start = pl.multiple_of((2 * index + 1 - core) * rows, 16)
            copies.append(pltpu.make_async_remote_copy(
                src_ref=tile.at[q % 3, pl.ds(start, rows), :], dst_ref=recv.at[slot, pl.ds(first_row, rows), :],
                send_sem=send_sem.at[q % 3, index], recv_sem=recv_sem.at[q, index],
                device_id=(mate,), device_id_type=pl.DeviceIdType.MESH))
        return copies

    for q, (x, x_col, y, y_col, first_row, rows, chips) in enumerate(tiles):
        if q == 0 or x_of[q] != x_of[q - 1]:
            which = x_of[q]
            load(which, xs, x_buf, x_sem).wait()
            turned[...] = x_buf[which % 2].T
            if which + 2 < len(xs):
                load(which + 2, xs, x_buf, x_sem).start()
        if q == 0 or y_of[q] != y_of[q - 1]:
            load(y_of[q], ys, y_buf, y_sem).wait()
        if q >= 3:
            for copy in sends(q - 3):
                copy.wait_send()
        tile[q % 3] = dot_nn(turned[...], y_buf[y_of[q] % 2])
        if (q + 1 == len(tiles) or y_of[q + 1] != y_of[q]) and y_of[q] + 2 < len(ys):
            load(y_of[q] + 2, ys, y_buf, y_sem).start()
        for index, other in enumerate(chips):
            d_x, d_y = lax.rem(chip_x + other % 2, 2), lax.rem(chip_y + other // 2, 2)
            slot = 2 * d_x + d_y + core * (d_y - d_x)
            start = pl.multiple_of((2 * index + core) * rows, 16)
            own[slot, first_row:first_row + rows, :] = tile[q % 3, pl.ds(start, rows), :]
        if q >= 1:
            for copy in sends(q - 1):
                copy.start()
    last = len(tiles) - 1
    for copy in sends(last):
        copy.start()
    for q in range(max(0, last - 2), last + 1):
        for copy in sends(q):
            copy.wait_send()
    for q in range(last + 1):
        for copy in sends(q):
            copy.wait_recv()
    for slot in range(4):
        ref = keep_ref if slot < 2 else far_ref
        ref[(slot % 2) * group_rows:(slot % 2 + 1) * group_rows, :] = own[slot] + recv[slot]


def weight_grads(kind, arrays, tiles, group_rows):
    count, width = arrays[0].shape[0], 640
    chips = max(len(t[-1]) for t in tiles)
    dma = pltpu.SemaphoreType.DMA
    out = jax.ShapeDtypeStruct((2 * group_rows, width), F32)
    return pl.pallas_call(
        functools.partial(grad_kernel, tiles, group_rows, len(arrays)), in_specs=[ANY] * len(arrays),
        out_specs=[pl.BlockSpec(memory_space=pltpu.VMEM)] * 2, out_shape=[out, out],
        scratch_shapes=[pltpu.VMEM((2, count, width), BF16), pltpu.VMEM((width, count), BF16), pltpu.VMEM((2, count, width), BF16),
                        pltpu.VMEM((3, width, width), F32), pltpu.VMEM((4, group_rows, width), F32),
                        pltpu.VMEM((4, group_rows, width), F32), dma((2,)), dma((2,)), dma((3, chips)), dma((len(tiles), chips))],
        cost_estimate=pl.CostEstimate(flops=2 * count * width * width * len(tiles), bytes_accessed=int(2e7), transcendentals=0),
        compiler_params=pltpu.CompilerParams(collective_id=kind, has_side_effects=True, vmem_limit_bytes=VMEM_LIMIT))(*arrays)


def context_kernel(context_ref, ctx_ref, mine_ref, other_ref):
    batch, valid, _ = context_ref.shape
    padded = ctx_ref.shape[0] // batch
    me = lax.axis_index(AXIS)
    core, chip = lax.rem(me, 2), me // 2
    ctx_ref[...] = jnp.zeros_like(ctx_ref)
    for sample in range(batch):
        ctx_ref[sample * padded:sample * padded + valid, :] = context_ref[sample]
    each, rows = mine_ref.shape[0] // 4, ctx_ref.shape[0]
    mine_ref[...] = jnp.zeros_like(mine_ref)
    other_ref[...] = jnp.zeros_like(other_ref)
    x = jnp.bitwise_xor
    for of_core, ref in ((core, mine_ref), (1 - core, other_ref)):
        for slot, other in enumerate((chip, x(chip, 2 - of_core), x(chip, 1 + of_core), x(chip, 3))):
            column = pl.multiple_of((2 * other + of_core) * each, each)
            ref[slot * each:(slot + 1) * each, 0:rows] = ctx_ref[:, pl.ds(column, each)].T


def prepare_context(context, n_dev):
    batch, valid, ctx_width = context.shape
    rows = batch * ((valid + 15) // 16 * 16)
    vmem = pl.BlockSpec(memory_space=pltpu.VMEM)
    turned = shape(ctx_width // 2, (rows + 127) // 128 * 128, BF16)
    ctx, mine, other = pl.pallas_call(
        context_kernel, in_specs=[vmem], out_specs=[vmem] * 3, out_shape=[shape(rows, ctx_width, BF16), turned, turned],
        cost_estimate=pl.CostEstimate(flops=rows * ctx_width * 8, bytes_accessed=int(8e6), transcendentals=0),
        name='context')(context)
    return ctx, mine, permute(other, gather_perms(n_dev)[2])


def vec_pack_kernel(biases, *refs):
    ins, out = list(refs[:-1]), refs[-1]
    width = out.shape[1]
    out[...] = jnp.zeros_like(out)
    for layer, parts in enumerate(biases):
        first, second, third = ins[:3]
        rows = [(first, 0), (first, 1), (second, 0), (second, 1), (third, 0), (third, 1), (first, 2), (second, 2), (third, 2)]
        for index, (ref, row) in enumerate(rows):
            out[17 * layer + index:17 * layer + index + 1, :] = ref[row:row + 1, :]
        for (start, chunks), bias in zip(parts, ins[3:]):
            for kind in range(2):
                for chunk in range(chunks):
                    row, column = 17 * layer + 9 + 4 * kind + start + chunk, (kind * chunks + chunk) * width
                    out[row:row + 1, :] = bias[0:1, column:column + width]
        ins = ins[3 + len(parts):]


def vec_total(parts, biases, rows, n_dev):
    vmem = pl.BlockSpec(memory_space=pltpu.VMEM)
    width = parts[0].shape[1]
    total = pl.pallas_call(
        functools.partial(vec_pack_kernel, biases), in_specs=[vmem] * len(parts), out_specs=vmem, out_shape=shape(rows, width, F32),
        cost_estimate=pl.CostEstimate(flops=rows * width, bytes_accessed=rows * width * 8, transcendentals=0),
        name='vec_pack')(*parts)
    near, far, core = gather_perms(n_dev)
    for perm in (core, far, near):
        total = total + permute(total, perm)
    return total


def ff_grad_kernel(offset, first, resumed, final, grad_ref, save_a, save_g, norm_ref, h_ref, rows_ref, *refs):
    before_ref, refs = (refs[0], refs[1:]) if resumed else (None, refs)
    pieces, refs = refs[:16], refs[16:]
    out_ref, refs = refs[0], refs[1:]
    vec_ref, refs = (refs[0], refs[1:]) if final else (None, refs)
    (bias_ref, far_ref, keep_ref, grad, grad_bf, turned, acc, part_a, part_g, d_both, w_ff1, w_ff2, tile, recv, obuf,
     in_sem, part_sem, w1_sem, w2_sem, out_sem, send_sem, recv_sem) = refs
    count, width = grad.shape
    every, chunks, depth = w_ff2.shape[0] // width, recv.shape[0], width // 8
    me = lax.axis_index(AXIS)
    core, mate, mate_slot, own_chip = chip_places(me)

    load_grad = pltpu.make_async_copy(grad_ref, grad, in_sem.at[0])
    load_norm = pltpu.make_async_copy(norm_ref, d_both.at[:, pl.ds(0, width)], in_sem.at[1])
    load_before = pltpu.make_async_copy(before_ref, acc, in_sem.at[2]) if resumed else None
    load_grad.start()
    load_norm.start()
    if resumed:
        load_before.start()
    start_load(pieces[8:], offset, w_ff2, w2_sem)

    def parts(chunk):
        at = (slice(None), pl.ds(pl.multiple_of((first + chunk) * width, width), width))
        return [pltpu.make_async_copy(ref.at[at], buf.at[lax.rem(chunk, 2)], part_sem.at[which, lax.rem(chunk, 2)])
                for which, (ref, buf) in enumerate(((save_a, part_a), (save_g, part_g)))]

    def load_h(step):
        return pltpu.make_async_copy(h_ref.at[pl.ds(step * STEP, STEP), :], part_a.at[0, pl.ds(step * STEP, STEP), :], part_sem.at[0, 0])

    for copy in parts(0):
        copy.start()
    devices = piece_devices(me)
    for chunk in range(chunks):
        for kind in range(2):
            for piece, device in zip(pieces[:8], devices):
                pltpu.make_async_copy(
                    piece.at[pl.ds((kind * every + first + chunk) * depth, depth), :],
                    w_ff1.at[pl.ds(pl.multiple_of(device * depth, 16), depth), pl.ds((2 * chunk + kind) * width, width)],
                    w1_sem.at[chunk]).start()
    greet(mate)

    def sends(chunk):
        copies = []
        for other in range(4):
            start = pl.multiple_of((2 * other + 1 - core) * depth, 16)
            to = pl.multiple_of(mate_slot(other) * depth, 16)
            copies.append(pltpu.make_async_remote_copy(
                src_ref=tile.at[pl.ds(start, depth), :], dst_ref=recv.at[chunk, pl.ds(to, depth), :], send_sem=send_sem.at[other],
                recv_sem=recv_sem.at[chunk, other], device_id=(mate,), device_id_type=pl.DeviceIdType.MESH))
        return copies

    def wait_write():
        pltpu.make_async_copy(obuf, obuf, out_sem).wait()

    def finish(chunk, first):
        for copy in sends(chunk):
            copy.wait_recv()

        @pl.when(jnp.logical_not(first))
        def _():
            wait_write()

        for slot in range(4):
            start = pl.multiple_of((2 * own_chip(slot) + core) * depth, 16)
            rows = slice(slot * depth, (slot + 1) * depth)
            obuf[rows, :] = tile[pl.ds(start, depth), :] + recv[chunk, rows, :]
        for slot in range(4):
            ref = keep_ref if slot < 2 else far_ref
            for kind in range(2):
                row = pl.multiple_of((slot % 2) * 2 * chunks * depth + (kind * chunks + chunk) * depth, 16)
                pltpu.make_async_copy(obuf.at[pl.ds(slot * depth, depth), pl.ds(kind * width, width)], ref.at[pl.ds(row, depth), :],
                                      out_sem).start()
        for copy in sends(chunk):
            copy.wait_send()

    load_grad.wait()
    grad_bf[...] = grad[...].astype(BF16)
    load_norm.wait()
    turned[...] = d_both[:, 0:width].T
    if resumed:
        load_before.wait()
    else:
        acc[...] = jnp.zeros_like(acc)
    bias_ref[...] = jnp.zeros_like(bias_ref)
    wait_load(w_ff2, w2_sem)

    def one_chunk(chunk, carry):
        w_pair = w_ff1.at[:, pl.ds(pl.multiple_of(chunk * 2 * width, width), 2 * width)]
        pltpu.make_async_copy(w_pair, w_pair, w1_sem.at[chunk]).wait()
        for copy in parts(chunk):
            copy.wait()

        @pl.when(chunk + 1 < chunks)
        def _():
            for copy in parts(chunk + 1):
                copy.start()

        even = lax.rem(chunk, 2)
        w_down = w_ff2.at[pl.ds(pl.multiple_of((first + chunk) * width, width), width), :]
        sums = [0.0, 0.0]
        ahead = dot_nt(grad_bf[0:FF_ROWS, :], w_down[...])
        for start in range(0, count, FF_ROWS):
            rows = slice(start, start + FF_ROWS)
            d_gated = ahead
            if start + FF_ROWS < count:
                ahead = dot_nt(grad_bf[start + FF_ROWS:start + 2 * FF_ROWS, :], w_down[...])
            for kind, saved in enumerate((part_a, part_g)):
                d_part = d_gated * saved[even, rows, :]
                sums[kind] = sums[kind] + jnp.sum(d_part, axis=0, keepdims=True)
                d_both[rows, kind * width:(kind + 1) * width] = d_part.astype(BF16)
            acc[rows, :] += dot_nt(d_both[rows, :], w_pair[...])
        for kind in range(2):
            bias_ref[0:1, pl.ds(pl.multiple_of((kind * chunks + chunk) * width, 2 * HEAD), width)] += sums[kind]

        @pl.when(chunk > 0)
        def _():
            finish(jnp.maximum(chunk - 1, 0), chunk == 1)

        tile[...] = dot_nn(turned[...], d_both[...])
        for copy in sends(chunk):
            copy.start()
        return carry

    lax.fori_loop(0, chunks, one_chunk, 0)
    if final:
        steps = count // STEP
        vec_ref[...] = jnp.zeros_like(vec_ref)
        for step in range(steps):
            load_h(step).start()
        pltpu.make_async_copy(part_a.at[0], part_a.at[0], part_sem.at[0, 0]).wait()
        for step in range(steps):
            rows = slice(step * STEP, (step + 1) * STEP)
            mine = grad[rows, :].astype(F32)
            d_res, g_gain, g_shift = norm_back(part_a[0, rows, :], rows_ref[4:5, :], acc[rows, :])
            acc[rows, :] = mine + d_res
            pltpu.make_async_copy(acc.at[pl.ds(step * STEP, STEP), :], out_ref.at[pl.ds(step * STEP, STEP), :], in_sem.at[0]).start()
            for at, row in enumerate((g_gain, g_shift, jnp.sum(mine, axis=0, keepdims=True))):
                vec_ref[at:at + 1, :] += row
    else:
        pltpu.make_async_copy(acc, out_ref, in_sem.at[0]).start()
    finish(chunks - 1, chunks == 1)
    wait_write()
    pltpu.make_async_copy(acc, out_ref, in_sem.at[0]).wait()


def ff_grads(kind, grad, save_a, save_g, norm, h, rows, pieces, offset, first, chunks, before):
    count, width = h.shape
    half = save_a.shape[1]
    final = first + chunks == half // width
    vmem = pl.BlockSpec(memory_space=pltpu.VMEM)
    big = shape(4 * chunks * (width // 8), width, F32)
    dma = pltpu.SemaphoreType.DMA
    saved = pltpu.VMEM((2, count, width), F32)
    resumed = before is not None
    return pl.pallas_call(
        functools.partial(ff_grad_kernel, offset, first, resumed, final), in_specs=[ANY] * 5 + [vmem] + [ANY] * (16 + resumed),
        out_specs=[ANY] + [vmem] * final + [vmem, ANY, ANY],
        out_shape=[shape(count, width, F32)] + [shape(8, width, F32)] * final + [shape(8, 2 * chunks * width, F32), big, big],
        scratch_shapes=[pltpu.VMEM((count, width), grad.dtype), pltpu.VMEM((count, width), BF16), pltpu.VMEM((width, count), BF16),
                        pltpu.VMEM((count, width), F32), saved, saved, pltpu.VMEM((count, 2 * width), BF16),
                        pltpu.VMEM((width, 2 * chunks * width), BF16), pltpu.VMEM((half, width), BF16),
                        pltpu.VMEM((width, 2 * width), F32), pltpu.VMEM((chunks, width // 2, 2 * width), F32),
                        pltpu.VMEM((width // 2, 2 * width), F32),
                        dma((3,)), dma((2, 2)), dma((chunks,)), dma, dma, dma((4,)), dma((chunks, 4))],
        cost_estimate=pl.CostEstimate(flops=count * width * width * chunks * 10, bytes_accessed=int(6e7), transcendentals=0),
        compiler_params=pltpu.CompilerParams(collective_id=kind, has_side_effects=True, vmem_limit_bytes=VMEM_MOST))(grad, save_a, save_g, norm, h, rows, *([before] if resumed else []), *pieces)


def scatter(far, keep, n_dev):
    near_perm, far_perm, _ = gather_perms(n_dev)
    rows = keep.shape[0] // 2
    second = permute(far, far_perm)
    third = permute(keep[rows:] + second[rows:], near_perm)
    return keep, second, third


def total_kernel(plans, counts, depths, scale, *refs):
    ins, outs = refs[:3 * sum(counts)], refs[3 * sum(counts):]
    width, lanes, layers = ins[0].shape[1], outs[0].shape[1], len(plans)
    for layer, plan in enumerate(plans):
        base = 3 * sum(counts[:layer])
        for out, blocks, depth in zip(outs, plan, depths):
            stride = layers * len(blocks) * width // lanes
            for index, (part, row) in enumerate(blocks):
                keep, second, third = (ref[row:row + depth, :] for ref in ins[base + 3 * part:base + 3 * part + 3])
                block = ((keep + second) + third) * scale
                for column in range(0, width, lanes):
                    start = layers * ((index * width + column) // lanes) + layer
                    out[pl.ds(start, depth, stride), :] = block[:, column:column + lanes]


def totals(layers, plans, depths, scale):
    width, lanes = layers[0][0][0].shape[1], 128
    arrays, specs = [], []
    for parts in layers:
        for terms in parts:
            rows = terms[2].shape[0]
            arrays += list(terms)
            specs += [whole(rows, width)] * 3
    sizes = [depth * len(blocks) * width for depth, blocks in zip(depths, plans[0])]
    shapes = [shape(len(layers) * size // lanes, lanes, F32) for size in sizes]
    sums = pl.pallas_call(
        functools.partial(total_kernel, plans, [len(parts) for parts in layers], depths, scale), grid=(1,), in_specs=specs,
        out_specs=[whole(*out.shape) for out in shapes], out_shape=shapes,
        cost_estimate=pl.CostEstimate(flops=sum(a.size for a in arrays), bytes_accessed=4 * sum(a.size for a in arrays),
                                      transcendentals=0),
        compiler_params=pltpu.CompilerParams(vmem_limit_bytes=VMEM_LIMIT), name='totals')(*arrays)
    result = []
    for total, size in zip(sums, sizes):
        total = lax.optimization_barrier(total.reshape(size // lanes, len(layers), lanes))
        result.append(jnp.swapaxes(total, 0, 1).reshape(len(layers), size))
    return result


def solution(mesh):
    n_dev = mesh.shape[AXIS]

    def inner(tokens_x, context, cot_out, *shards):
        batch, tokens, width = tokens_x.shape
        _, valid, ctx_width = context.shape
        blocks = shards[0].shape[0]
        total = batch * n_dev
        depth = width // n_dev
        count = batch * tokens
        half = 4 * width

        views = []
        for shard, rows in zip(shards[:7], (depth, depth, depth, ctx_width // n_dev, depth, depth, half // n_dev)):
            views.append(shard.reshape(blocks, rows, -1))
        qkv_s, out_s = lax.optimization_barrier(views[:2])
        q2_s, kv2_s, out2_s = lax.optimization_barrier(views[2:5])
        ff1_s, ff2_s = lax.optimization_barrier(views[5:])
        me = lax.axis_index(AXIS)
        vec_len = shards[7].shape[1]
        vec_each = 17
        vec_rows = (blocks * vec_each + 15) // 16 * 16
        vec_block = lax.dynamic_update_slice(jnp.zeros((blocks, n_dev * vec_len), BF16), shards[7], (0, me * vec_len))
        vec_block = vec_block[:, :vec_each * width].reshape(blocks * vec_each, width)
        vec_block = jnp.pad(vec_block, ((0, vec_rows - blocks * vec_each), (0, 0)))

        members = []
        for layer in range(blocks):
            if layer < blocks - 1:
                members += [(layer, [qkv_s, out_s]), (layer, [kv2_s, q2_s, out2_s]), (layer, [ff1_s, ff2_s])]
            else:
                members += [(layer, [qkv_s, out_s, kv2_s, q2_s, out2_s]), (layer, [ff1_s]), (layer, [ff2_s])]
        groups = []
        for index, (layer, parts) in enumerate(members):
            block = pack(parts, layer, [vec_block] if index == 0 else [], width)
            groups.append(gather_group(block, n_dev))
        ff_groups = [groups[3 * layer + 2] * 2 if layer < blocks - 1 else groups[-2] + groups[-1] for layer in range(blocks)]
        ff_offsets = [8 * depth if layer < blocks - 1 else 0 for layer in range(blocks)]

        vecs = vec_sum(groups[0], vec_rows)
        vecs = vecs[:blocks * vec_each].reshape(blocks, vec_each, width)
        rows_all = jnp.pad(vecs[:, :9], ((0, 0), (0, 7), (0, 0)))
        bias_all = vecs[:, 9:].reshape(blocks, 1, 8 * width)

        ctx, ctx_mine, ctx_other = prepare_context(context, n_dev)

        h = tokens_x.reshape(count, width)
        saved, attention_groups = [], []
        for layer in range(blocks):
            rows, bias = rows_all[layer], bias_all[layer]
            group = groups[3 * layer:3 * layer + 2] if layer < blocks - 1 else [groups[3 * layer]] * 2
            attention_groups.append(group)
            if layer < blocks - 1:
                norm1, qkv, mix1, h1 = self_forward(h, rows, group[0], tokens)
                norm2, query, kv, mix2, h2 = cross_forward(h1, rows, ctx, group[1], tokens, valid)
                norm3, gated, save_a, save_g, h3 = ff_forward(h2, rows, bias, ff_groups[layer], ff_offsets[layer])
            else:
                norm1, qkv, mix1, h1, norm2, query, kv, mix2, h2 = attention_forward(h, rows, ctx, group[0], tokens, valid)
                norm3, gated, save_a, save_g = ff_up_forward(h2, rows, bias, groups[-2])
                out_tokens = ff_down_forward(h2, rows, gated, groups[-1])
            saved.append((h, norm1, qkv, mix1, h1, norm2, query, kv, mix2, h2, norm3, gated, save_a, save_g))
            h = h3 if layer < blocks - 1 else None

        grad = rounded = cot_out.reshape(count, width)
        results, vec_grads = [None] * blocks, [None] * blocks
        for layer in reversed(range(blocks)):
            turn = blocks - 1 - layer
            rows, group = rows_all[layer], attention_groups[layer]
            h0, norm1, qkv, mix1, h1, norm2, query, kv, mix2, h2, norm3, gated, save_a, save_g = saved[layer]

            def reduce(pair):
                return scatter(pair[0], pair[1], n_dev)

            r_ff2 = reduce(weight_grads(1, (gated, rounded),
                                           [(0, c * width, 1, 0, 0, half // n_dev, (c,)) for c in range(half // width)], half // n_dev))
            sizes = (4,) if turn == 0 else (2, 2)
            d_norm, r_ff1, bias_grads, first_chunk = None, [], [], 0
            for index, chunks in enumerate(sizes):
                *out, vec_b1, far, keep = ff_grads(5 + turn + index, grad, save_a, save_g, norm3, h2, rows,
                                                   ff_groups[layer], ff_offsets[layer], first_chunk, chunks, d_norm)
                d_norm = out[0]
                bias_grads.append(((first_chunk, chunks), vec_b1))
                r_ff1.append(reduce((far, keep)))
                first_chunk += chunks
            grad, vec3 = out
            grad, vec2, *pair = cross_backward(3 + turn, grad, query, kv, h1, rows, norm2, mix2, ctx_mine, ctx_other, group[1],
                                               tokens, valid)
            r_cross = reduce(pair)
            grad, rounded, vec1, *pair = self_backward(8 + turn, grad, qkv, h0, rows, norm1, mix1, group[0], tokens)
            r_self = reduce(pair)
            results[layer] = [r_self], [r_cross], r_ff1, [r_ff2], sizes
            vec_grads[layer] = ([vec1, vec2, vec3] + [array for _, array in bias_grads], tuple(where for where, _ in bias_grads))
        vec_out = vec_total([part for parts, _ in vec_grads for part in parts], tuple(where for _, where in vec_grads), vec_rows, n_dev)
        vec_out = vec_out[:blocks * vec_each].reshape(blocks, vec_each * width)
        vec_out = jnp.pad(vec_out, ((0, 0), (0, vec_len * n_dev - vec_each * width)))
        vec_out = lax.dynamic_slice(vec_out, (0, me * vec_len), (blocks, vec_len))
        ff1_plans = []
        for layer in range(blocks):
            size = results[layer][4][0]
            ff1_plans.append([[(chunk // size, (kind * size + chunk % size) * depth) for kind in range(2) for chunk in range(4)]])
        deep = ctx_width // n_dev
        plans = ([[[(0, 0), (0, depth), (0, 2 * depth)], [(0, 3 * depth)]]] * blocks,
                 [[[(0, 0)], [(0, depth)], [(0, 2 * depth), (0, 2 * depth + deep)]]] * blocks, ff1_plans, [[[(0, 0)]]] * blocks)
        depths = ((depth, depth), (depth, depth, deep), (depth,), (half // n_dev,))
        summed = []
        for index in range(4):
            summed += totals([results[layer][index] for layer in range(blocks)], plans[index], depths[index], 1.0 / total)
        g_qkv, g_out, g_q2, g_out2, g_kv2, g_ff1, g_ff2 = summed
        outs = [g_qkv, g_out, g_q2, g_kv2, g_out2, g_ff1, g_ff2]
        outs.append(vec_out / total)
        return tuple([out_tokens.reshape(tokens_x.shape), rounded.reshape(tokens_x.shape)] + outs)

    param_spec = P(None, AXIS)
    in_specs = (P(AXIS), P(AXIS), P(AXIS)) + (param_spec,) * 8
    out_specs = (P(AXIS), P(AXIS)) + (param_spec,) * 8
    return jax.shard_map(inner, mesh=mesh, in_specs=in_specs, out_specs=out_specs, check_vma=False)
```

```python
import functools
import math
import jax
import jax.numpy as jnp
from jax import lax
from jax.experimental import pallas as pl
from jax.experimental.pallas import tpu as pltpu
from jax.sharding import PartitionSpec as P


HEAD = 64
AXIS = 'fsdp'
CHUNK = 256
FF_ROWS = 256
FF_STEP = 256
STEP = 512
VMEM_LIMIT = 60 * 1024 * 1024
VMEM_MOST = 67043328
FORWARD_UNROLL = 10

F32 = jnp.float32
BF16 = jnp.bfloat16
ANY = pl.BlockSpec(memory_space=pl.ANY)


def gather_perms(n_dev):
    near = [(i, i ^ (4 if i % 2 == 0 else 2)) for i in range(n_dev)]
    far = [(i, i ^ (2 if i % 2 == 0 else 4)) for i in range(n_dev)]
    core = [(i, i ^ 1) for i in range(n_dev)]
    return near, far, core


def pack_kernel(*refs):
    ins, out = refs[:-1], refs[-1]
    width, row = out.shape[1], 0
    for ref in ins:
        depth = ref.shape[-2]
        for col in range(0, ref.shape[-1], width):
            piece = ref[0, :, col:col + width] if len(ref.shape) == 3 else ref[:, col:col + width]
            out[row:row + depth, :] = piece
            row += depth


def pack(views, layer, extra, width):
    rows = sum(v.shape[1] * v.shape[2] // width for v in views) + sum(e.shape[0] for e in extra)
    specs = [pl.BlockSpec((1,) + v.shape[1:], lambda i: (layer, 0, 0)) for v in views]
    specs += [pl.BlockSpec(e.shape, lambda i: (0, 0)) for e in extra]
    return pl.pallas_call(
        pack_kernel, grid=(1,), in_specs=specs, out_specs=pl.BlockSpec((rows, width), lambda i: (0, 0)),
        out_shape=jax.ShapeDtypeStruct((rows, width), BF16),
        cost_estimate=pl.CostEstimate(flops=rows * width, bytes_accessed=rows * width * 4, transcendentals=0),
        name='pack')(*views, *extra)


def vec_kernel(*refs):
    pieces, (out, buf, sem) = refs[:8], refs[8:]
    rows = out.shape[0]
    copies = [pltpu.make_async_copy(piece.at[pl.ds(piece.shape[0] - rows, rows), :], buf.at[index], sem.at[index])
              for index, piece in enumerate(pieces)]
    for copy in copies:
        copy.start()
    total = None
    for index, copy in enumerate(copies):
        copy.wait()
        total = buf[index].astype(F32) if total is None else total + buf[index].astype(F32)
    out[...] = total


def vec_sum(pieces, rows):
    width = pieces[0].shape[1]
    return pl.pallas_call(
        vec_kernel, in_specs=[ANY] * 8, out_specs=pl.BlockSpec(memory_space=pltpu.VMEM),
        out_shape=jax.ShapeDtypeStruct((rows, width), F32),
        scratch_shapes=[pltpu.VMEM((8, rows, width), BF16), pltpu.SemaphoreType.DMA((8,))],
        cost_estimate=pl.CostEstimate(flops=rows * width * 8, bytes_accessed=rows * width * 20, transcendentals=0),
        name='vec_sum')(*pieces)


def permute(array, perm):
    return lax.ppermute(array, AXIS, perm)


def gather_group(shard, n_dev):
    near, far, core = gather_perms(n_dev)
    first = permute(shard, near)
    second = permute(shard, far)
    third = permute(first, far)
    mine = [shard, first, second, third]
    return mine + [permute(piece, core) for piece in mine]


def piece_devices(me):
    core = lax.rem(me, 2)
    one, two = 4 - 2 * core, 2 + 2 * core
    x = jnp.bitwise_xor
    mate = x(me, 1)
    return [me, x(me, one), x(me, two), x(me, 6), mate, x(mate, two), x(mate, one), x(mate, 6)]


def start_load(pieces, offset, ref, sem):
    width = pieces[0].shape[1]
    depth = ref.shape[0] // 8
    devices = piece_devices(lax.axis_index(AXIS))
    for block in range(ref.shape[1] // width):
        for piece, device in zip(pieces, devices):
            src = piece.at[pl.ds(offset + block * depth, depth), :]
            dst = ref.at[pl.ds(pl.multiple_of(device * depth, 16), depth), pl.ds(block * width, width)]
            pltpu.make_async_copy(src, dst, sem).start()


def wait_load(ref, sem):
    pltpu.make_async_copy(ref, ref, sem).wait()


def dot_nn(a, b):
    return lax.dot_general(a, b, (((1,), (0,)), ((), ())), preferred_element_type=F32)


def dot_nt(a, b):
    return lax.dot_general(a, b, (((1,), (1,)), ((), ())), preferred_element_type=F32)


def dot_tn(a, b):
    return lax.dot_general(a, b, (((0,), (0,)), ((), ())), preferred_element_type=F32)


def norm_stats(x):
    average = jnp.mean(x, axis=-1, keepdims=True)
    centered = x - average
    variance = jnp.mean(centered * centered, axis=-1, keepdims=True)
    scale = lax.rsqrt(variance + 1e-5)
    return centered * scale, scale


def norm_back(x, gain, d_norm):
    unit, scale = norm_stats(x)
    d_unit = d_norm * gain
    inner = d_unit - jnp.mean(d_unit, axis=-1, keepdims=True) - unit * jnp.mean(d_unit * unit, axis=-1, keepdims=True)
    return scale * inner, jnp.sum(d_norm * unit, axis=0, keepdims=True), jnp.sum(d_norm, axis=0, keepdims=True)


def softmax_rows(scores):
    top = jnp.max(scores, axis=-1, keepdims=True)
    raised = jnp.exp(scores - top)
    return raised * (1.0 / jnp.sum(raised, axis=-1, keepdims=True))


def low_lanes(rows):
    return lax.broadcasted_iota(jnp.int32, (rows, 2 * HEAD), 1) < HEAD


def heads_of(pair):
    low, zero = low_lanes(pair.shape[0]), jnp.zeros_like(pair)
    return jnp.where(low, pair, zero), jnp.where(low, zero, pair)


def pair_forward(query, key, value, valid=None):
    mixed = []
    for q_head in heads_of(query * HEAD ** -0.5):
        scores = dot_nt(q_head, key)
        if valid is not None:
            column = lax.broadcasted_iota(jnp.int32, scores.shape, 1)
            scores = jnp.where(column < valid, scores, -1e30)
        mixed.append(dot_nn(softmax_rows(scores).astype(BF16), value))
    return jnp.where(low_lanes(query.shape[0]), mixed[0], mixed[1]).astype(BF16)


def backward_scores(query, key, value, d_out):
    q_heads, d_heads = heads_of(query * HEAD ** -0.5), heads_of(d_out)
    return q_heads, d_heads, [dot_nt(key, q) for q in q_heads], [dot_nt(value, d) for d in d_heads]


def backward_probs(scores, d_probs, valid):
    if valid is not None:
        row = lax.broadcasted_iota(jnp.int32, scores.shape, 0)
        scores = jnp.where(row < valid, scores, -1e30)
    raised = jnp.exp(scores - jnp.max(scores, axis=0, keepdims=True))
    probs = raised * (1.0 / jnp.sum(raised, axis=0, keepdims=True))
    inner = jnp.sum(d_probs * probs, axis=0, keepdims=True)
    return probs.astype(BF16), (probs * (d_probs - inner)).astype(BF16)


def pairs_backward(pairs, load, store, valid=None):
    ahead = load(0)
    ahead = ahead, backward_scores(*ahead)
    for pair in range(pairs):
        (query, key, value, d_out), (q_heads, d_heads, scores, d_probs) = ahead
        if pair + 1 < pairs:
            ahead = load(pair + 1)
            ahead = ahead, backward_scores(*ahead)
        turned = key.T
        d_query, d_key, d_value = [], 0.0, 0.0
        for head in range(2):
            probs, d_scores = backward_probs(scores[head], d_probs[head], valid)
            d_query.append(dot_nn(turned[head * HEAD:(head + 1) * HEAD, :], d_scores))
            d_key = d_key + dot_nn(d_scores, q_heads[head])
            d_value = d_value + dot_nn(probs, d_heads[head])
        d_query = (jnp.concatenate(d_query, 0) * HEAD ** -0.5).T
        store(pair, d_query.astype(BF16), d_key.astype(BF16), d_value.astype(BF16))


def chip_places(me):
    core, chip = lax.rem(me, 2), me // 2
    chip_x, chip_y = lax.rem(chip, 2), chip // 2

    def mate_slot(other):
        d_x, d_y = lax.rem(chip_x + other % 2, 2), lax.rem(chip_y + other // 2, 2)
        return d_x + 2 * d_y + core * (d_x - d_y)

    def own_chip(slot):
        one, two = slot // 2, slot % 2
        d_x, d_y = one + core * (two - one), two + core * (one - two)
        return 2 * lax.rem(chip_y + d_y, 2) + lax.rem(chip_x + d_x, 2)

    return core, me + 1 - 2 * core, mate_slot, own_chip


def greet(mate):
    barrier = pltpu.get_barrier_semaphore()
    pl.semaphore_signal(barrier, inc=1, device_id=(mate,), device_id_type=pl.DeviceIdType.MESH)
    pl.semaphore_wait(barrier, 1)


def tile_sends(q, rows, tile, recv, send_sem, recv_sem):
    core, mate, mate_slot, _ = chip_places(lax.axis_index(AXIS))
    copies = []
    for other in range(4):
        start = pl.multiple_of((2 * other + 1 - core) * rows, 16)
        copies.append(pltpu.make_async_remote_copy(
            src_ref=tile.at[q, pl.ds(start, rows), :], dst_ref=recv.at[mate_slot(other), pl.ds(q * rows, rows), :],
            send_sem=send_sem.at[q, other], recv_sem=recv_sem.at[q, other],
            device_id=(mate,), device_id_type=pl.DeviceIdType.MESH))
    return copies


def finish_tiles(tiles, rows, group_rows, tile, recv, send_sem, recv_sem, far_ref, keep_ref):
    core, _, _, own_chip = chip_places(lax.axis_index(AXIS))
    for q in range(tiles):
        for copy in tile_sends(q, rows, tile, recv, send_sem, recv_sem):
            copy.wait()
        for slot in range(4):
            ref = keep_ref if slot < 2 else far_ref
            start = pl.multiple_of((2 * own_chip(slot) + core) * rows, 16)
            at = (slot % 2) * group_rows + q * rows
            ref[at:at + rows, :] = tile[q, pl.ds(start, rows), :] + recv[slot, q * rows:(q + 1) * rows, :]


def down_send(chip, tile, recv, send_sem, recv_sem):
    core, mate, _, _ = chip_places(lax.axis_index(AXIS))
    rows = recv.shape[1]
    return pltpu.make_async_remote_copy(
        src_ref=tile.at[chip, pl.ds(pl.multiple_of((1 - core) * rows, rows), rows), :], dst_ref=recv.at[chip],
        send_sem=send_sem.at[chip], recv_sem=recv_sem.at[chip], device_id=(mate,), device_id_type=pl.DeviceIdType.MESH)


def down_finish(tile, recv, send_sem, recv_sem, far_ref, keep_ref):
    core, _, _, own_chip = chip_places(lax.axis_index(AXIS))
    rows = recv.shape[1]
    for chip in range(4):
        down_send(chip, tile, recv, send_sem, recv_sem).wait()
    for slot in range(4):
        chip = own_chip(slot)
        ref = keep_ref if slot < 2 else far_ref
        at = (slot % 2) * rows
        ref[at:at + rows, :] = tile[chip, pl.ds(pl.multiple_of(core * rows, rows), rows), :] + recv[chip]


def add_rows(ref, step, rows):
    @pl.when(step == 0)
    def _():
        ref[...] = jnp.zeros_like(ref)

    for index, row in enumerate(rows):
        ref[pl.ds(index, 1), :] += row


def self_loads(pieces, w_qkv, w_out, sems):
    start_load(pieces, 0, w_qkv, sems.at[0])
    start_load(pieces, 3 * (w_out.shape[0] // 8), w_out, sems.at[1])


def cross_loads(pieces, offset, w_kv, w_query, w_out, sems):
    deep, depth = w_kv.shape[0] // 8, w_out.shape[0] // 8
    start_load(pieces, offset, w_kv, sems.at[0])
    start_load(pieces, offset + 2 * deep, w_query, sems.at[1])
    start_load(pieces, offset + 2 * deep + depth, w_out, sems.at[2])


def self_forward_kernel(samples, tokens, h_ref, rows_ref, *refs):
    @pl.when(pl.program_id(0) == 0)
    def _():
        self_loads(refs[:8], *refs[12:])

    self_forward_step(samples, tokens, h_ref, rows_ref, *refs[8:])


def cross_forward_kernel(samples, tokens, valid, h_ref, rows_ref, ctx_ref, *refs):
    @pl.when(pl.program_id(0) == 0)
    def _():
        cross_loads(refs[:8], 0, *refs[13:])

    cross_forward_step(samples, tokens, valid, h_ref, rows_ref, ctx_ref, *refs[8:])


def attention_forward_kernel(samples, tokens, valid, h_ref, rows_ref, ctx_ref, *refs):
    pieces, self_outs, cross_outs, self_scratch, cross_scratch = refs[:8], refs[8:12], refs[12:17], refs[17:20], refs[20:24]

    @pl.when(pl.program_id(0) == 0)
    def _():
        self_loads(pieces, *self_scratch)
        cross_loads(pieces, 4 * (h_ref.shape[1] // 8), *cross_scratch)

    self_forward_step(samples, tokens, h_ref, rows_ref, *self_outs, *self_scratch)
    cross_forward_step(samples, tokens, valid, self_outs[3], rows_ref, ctx_ref, *cross_outs, *cross_scratch)


def self_forward_step(samples, tokens, h_ref, rows_ref, norm_ref, qkv_ref, mix_ref, out_ref, w_qkv, w_out, sems):
    width = h_ref.shape[1]
    step = pl.program_id(0)
    x = h_ref[...].astype(F32)
    unit, _ = norm_stats(x)
    normed = (unit * rows_ref[0:1, :] + rows_ref[1:2, :]).astype(BF16)
    norm_ref[...] = normed

    @pl.when(step == 0)
    def _():
        wait_load(w_qkv, sems.at[0])
        wait_load(w_out, sems.at[1])

    qkv_ref[...] = dot_nn(normed, w_qkv[...]).astype(BF16)
    pairs = width // (2 * HEAD)

    def body(index, carry):
        row = pl.multiple_of((index // pairs) * tokens, tokens)
        col = pl.multiple_of((index % pairs) * 2 * HEAD, 2 * HEAD)
        part = lambda which: qkv_ref[pl.ds(row, tokens), pl.ds(which * width + col, 2 * HEAD)]
        mix_ref[pl.ds(row, tokens), pl.ds(col, 2 * HEAD)] = pair_forward(part(0), part(1), part(2))
        return carry

    lax.fori_loop(0, samples * pairs, body, 0, unroll=FORWARD_UNROLL)
    out_ref[...] = x + dot_nn(mix_ref[...], w_out[...]) + rows_ref[6:7, :]


def cross_forward_step(samples, tokens, valid, h_ref, rows_ref, ctx_ref, norm_ref, query_ref, kv_ref, mix_ref, out_ref, w_kv, w_query,
                       w_out, sems):
    width = h_ref.shape[1]
    step = pl.program_id(0)
    padded = ctx_ref.shape[0] // (samples * pl.num_programs(0))
    x = h_ref[...]
    unit, _ = norm_stats(x)
    normed = (unit * rows_ref[2:3, :] + rows_ref[3:4, :]).astype(BF16)
    norm_ref[...] = normed

    @pl.when(step == 0)
    def _():
        wait_load(w_kv, sems.at[0])
        wait_load(w_query, sems.at[1])
        wait_load(w_out, sems.at[2])
        kv_ref[...] = dot_nn(ctx_ref[...], w_kv[...]).astype(BF16)

    query_ref[...] = dot_nn(normed, w_query[...]).astype(BF16)
    pairs = width // (2 * HEAD)

    def body(index, carry):
        sample = index // pairs
        row = pl.multiple_of(sample * tokens, tokens)
        kv_row = pl.multiple_of((step * samples + sample) * padded, 16)
        col = pl.multiple_of((index % pairs) * 2 * HEAD, 2 * HEAD)
        query = query_ref[pl.ds(row, tokens), pl.ds(col, 2 * HEAD)]
        key = kv_ref[pl.ds(kv_row, padded), pl.ds(col, 2 * HEAD)]
        value = kv_ref[pl.ds(kv_row, padded), pl.ds(width + col, 2 * HEAD)]
        mix_ref[pl.ds(row, tokens), pl.ds(col, 2 * HEAD)] = pair_forward(query, key, value, valid)
        return carry

    lax.fori_loop(0, samples * pairs, body, 0, unroll=FORWARD_UNROLL)
    out_ref[...] = x + dot_nn(mix_ref[...], w_out[...]) + rows_ref[7:8, :]


def ff_loads(pieces, offset, w_ff1, w_ff2, sems):
    start_load(pieces[:8], 0, w_ff1, sems.at[0])
    start_load(pieces[8:], offset, w_ff2, sems.at[1])


def ff_hidden(normed, bias_ref, w_ff1, start):
    return dot_nn(normed, w_ff1[:, start:start + CHUNK]) + bias_ref[:, start:start + CHUNK]


def ff_up(normed, bias_ref, w_ff1, half, gated_ref, save_a, save_g, each=None):
    starts = list(range(0, half, CHUNK))
    ahead = (ff_hidden(normed, bias_ref, w_ff1, 0), ff_hidden(normed, bias_ref, w_ff1, half))
    for start in starts:
        u_a, u_g = ahead
        if start + CHUNK < half:
            ahead = tuple(ff_hidden(normed, bias_ref, w_ff1, base + start + CHUNK) for base in (0, half))
        cumulative = 0.5 * (1.0 + lax.erf(u_g * math.sqrt(0.5)))
        gate = u_g * cumulative
        slope = cumulative + u_g * (jnp.exp(-0.5 * u_g * u_g) * (1.0 / math.sqrt(2.0 * math.pi)))
        gated = (u_a * gate).astype(BF16)
        gated_ref[:, start:start + CHUNK] = gated
        save_a[:, start:start + CHUNK] = gate
        save_g[:, start:start + CHUNK] = u_a * slope
        if each is not None:
            each(start, gated)


def ff_forward_kernel(offset, h_ref, rows_ref, bias_ref, *refs):
    pieces, (norm_ref, gated_ref, save_a, save_g, out_ref, w_ff1, w_ff2, sems) = refs[:16], refs[16:]
    half = w_ff2.shape[0]
    step = pl.program_id(0)

    @pl.when(step == 0)
    def _():
        ff_loads(pieces, offset, w_ff1, w_ff2, sems)

    x = h_ref[...]
    unit, _ = norm_stats(x)
    normed = (unit * rows_ref[4:5, :] + rows_ref[5:6, :]).astype(BF16)
    norm_ref[...] = normed

    @pl.when(step == 0)
    def _():
        wait_load(w_ff1, sems.at[0])
        wait_load(w_ff2, sems.at[1])

    out_ref[...] = x + rows_ref[8:9, :]

    def down(start, gated):
        out_ref[...] += dot_nn(gated, w_ff2[start:start + CHUNK, :])

    ff_up(normed, bias_ref, w_ff1, half, gated_ref, save_a, save_g, down)


def ff_up_kernel(h_ref, rows_ref, bias_ref, cot_ref, *refs):
    pieces, refs = refs[:8], refs[8:]
    (norm_ref, gated_ref, save_a, save_g, far_ref, keep_ref, w_ff1, every, grad, tile, recv, sems, grad_sem, send_sem, recv_sem) = refs
    half, width = w_ff1.shape[1] // 2, grad.shape[1]
    step, last = pl.program_id(0), pl.num_programs(0) - 1
    load_grad = pltpu.make_async_copy(cot_ref, grad, grad_sem)

    @pl.when(step == 0)
    def _():
        start_load(pieces, 0, w_ff1, sems.at[0])
        load_grad.start()
        greet(chip_places(lax.axis_index(AXIS))[1])

    unit, _ = norm_stats(h_ref[...])
    normed = (unit * rows_ref[4:5, :] + rows_ref[5:6, :]).astype(BF16)
    norm_ref[...] = normed

    @pl.when(step == 0)
    def _():
        wait_load(w_ff1, sems.at[0])

    mine = pl.ds(pl.multiple_of(step * normed.shape[0], normed.shape[0]), normed.shape[0])

    def keep_gated(start, gated):
        every[mine, start:start + CHUNK] = gated

    ff_up(normed, bias_ref, w_ff1, half, gated_ref, save_a, save_g, keep_gated)

    @pl.when(step == last)
    def _():
        load_grad.wait()
        for chip in range(4):
            tile[chip] = dot_tn(every[:, chip * width:(chip + 1) * width], grad[...])
            down_send(chip, tile, recv, send_sem, recv_sem).start()
        down_finish(tile, recv, send_sem, recv_sem, far_ref, keep_ref)


def ff_down_kernel(h_ref, rows_ref, gated_ref, *refs):
    pieces, (out_ref, w_ff2, sems) = refs[:8], refs[8:]
    step = pl.program_id(0)

    @pl.when(step == 0)
    def _():
        start_load(pieces, 0, w_ff2, sems.at[0])
        wait_load(w_ff2, sems.at[0])

    out_ref[...] = (h_ref[...] + rows_ref[8:9, :] + dot_nn(gated_ref[...], w_ff2[...])).astype(BF16)


def cross_backward_kernel(samples, tokens, valid, grad_ref, query_ref, kv_ref, h_ref, rows_ref, norm_ref, mix_ref, ctx_mine_ref,
                          ctx_other_ref, *refs):
    pieces, refs = refs[:8], refs[8:]
    (out_ref, vec_ref, far_ref, keep_ref, d_mix, w_query, w_out, d_query, grad_bf, d_kv, kv_other, x_norm, x_mix, ctx_mine, ctx_other,
     tile, recv, sems, load_sem, kv_send, kv_recv, send_sem, recv_sem) = refs
    width = h_ref.shape[1]
    depth = width // 8
    step, last = pl.program_id(0), pl.num_programs(0) - 1
    padded = kv_ref.shape[0] // samples
    context_rows = kv_ref.shape[0] * (last + 1)
    mate = chip_places(lax.axis_index(AXIS))[1]
    loads = [pltpu.make_async_copy(src, dst, load_sem.at[index]) for index, (src, dst) in enumerate(
        ((norm_ref, x_norm), (mix_ref, x_mix), (ctx_mine_ref, ctx_mine), (ctx_other_ref, ctx_other)))]
    exchange = pltpu.make_async_remote_copy(
        src_ref=d_kv.at[pl.ds(0, context_rows), :], dst_ref=kv_other.at[pl.ds(0, context_rows), :], send_sem=kv_send, recv_sem=kv_recv,
        device_id=(mate,), device_id_type=pl.DeviceIdType.MESH)

    @pl.when(step == 0)
    def _():
        base = pieces[0].shape[0] - 2 * depth
        start_load(pieces, base, w_query, sems.at[0])
        start_load(pieces, base + depth, w_out, sems.at[1])
        for copy in loads:
            copy.start()
        for ref in (d_kv, kv_other):
            ref[context_rows:, :] = jnp.zeros((ref.shape[0] - context_rows, ref.shape[1]), BF16)
        greet(mate)

    grad = grad_ref[...]
    mine = pl.ds(pl.multiple_of(step * grad.shape[0], grad.shape[0]), grad.shape[0])
    grad_bf[mine, :] = grad.astype(BF16)

    @pl.when(step == 0)
    def _():
        wait_load(w_query, sems.at[0])
        wait_load(w_out, sems.at[1])

    d_mix[...] = dot_nt(grad.astype(BF16), w_out[...]).astype(BF16)
    pairs = width // (2 * HEAD)

    at = lambda which, pair: slice(which * width + pair * 2 * HEAD, which * width + (pair + 1) * 2 * HEAD)

    def load(index):
        sample, pair = index // pairs, index % pairs
        row, here = slice(sample * tokens, (sample + 1) * tokens), slice(sample * padded, (sample + 1) * padded)
        return query_ref[row, at(0, pair)], kv_ref[here, at(0, pair)], kv_ref[here, at(1, pair)], d_mix[row, at(0, pair)]

    def store(index, d_q, d_key, d_value):
        sample, pair = index // pairs, index % pairs
        d_query[pl.ds(pl.multiple_of((step * samples + sample) * tokens, tokens), tokens), at(0, pair)] = d_q
        there = pl.ds(pl.multiple_of((step * samples + sample) * padded, 16), padded)
        d_kv[there, at(0, pair)] = d_key
        d_kv[there, at(1, pair)] = d_value

    pairs_backward(samples * pairs, load, store, valid)
    rows, summed = depth, 2 * depth
    group_rows = keep_ref.shape[0] // 2
    deep = ctx_mine.shape[0] // 4

    def context_part(ctx, kv, slot, block):
        return dot_nn(ctx[slot * deep:(slot + 1) * deep, :], kv[:, block * width:(block + 1) * width])

    def context_at(slot, block):
        start = (slot % 2) * group_rows + summed + block * deep
        return slice(start, start + deep)

    @pl.when(step == last)
    def _():
        for copy in loads:
            copy.wait()
        tile[0] = dot_tn(x_norm[...], d_query[...])
        exchange.start()
        tile[1] = dot_tn(x_mix[...], grad_bf[...])
        for copy in tile_sends(0, rows, tile, recv, send_sem, recv_sem):
            copy.start()
        for slot in range(4):
            for block in range(2):
                (keep_ref if slot < 2 else far_ref)[context_at(slot, block), :] = context_part(ctx_mine, d_kv, slot, block)
        for copy in tile_sends(1, rows, tile, recv, send_sem, recv_sem):
            copy.start()

    d_norm = dot_nt(d_query[mine, :], w_query[...])
    d_res, g_gain, g_shift = norm_back(h_ref[...], rows_ref[2:3, :], d_norm)
    out_ref[...] = grad + d_res
    add_rows(vec_ref, step, [g_gain, g_shift, jnp.sum(grad, axis=0, keepdims=True)])

    @pl.when(step == last)
    def _():
        exchange.wait()
        for slot in range(4):
            for block in range(2):
                (keep_ref if slot < 2 else far_ref)[context_at(slot, block), :] += context_part(ctx_other, kv_other, slot, block)
        finish_tiles(2, rows, group_rows, tile, recv, send_sem, recv_sem, far_ref, keep_ref)


def self_backward_kernel(samples, tokens, grad_ref, qkv_ref, h_ref, rows_ref, norm_ref, mix_ref, *refs):
    pieces, refs = refs[:8], refs[8:]
    (out_ref, rounded_ref, vec_ref, far_ref, keep_ref, d_mix, w_qkv, w_out, d_qkv, grad_bf, x_norm, x_mix, tile, recv, sems, load_sem,
     send_sem, recv_sem) = refs
    width = h_ref.shape[1]
    depth = width // 8
    step, last = pl.program_id(0), pl.num_programs(0) - 1
    mate = chip_places(lax.axis_index(AXIS))[1]
    loads = [pltpu.make_async_copy(src, dst, load_sem.at[index]) for index, (src, dst) in enumerate(((norm_ref, x_norm), (mix_ref, x_mix)))]

    @pl.when(step == 0)
    def _():
        start_load(pieces, 0, w_qkv, sems.at[0])
        start_load(pieces, 3 * depth, w_out, sems.at[1])
        for copy in loads:
            copy.start()
        greet(mate)

    grad = grad_ref[...]
    mine = pl.ds(pl.multiple_of(step * grad.shape[0], grad.shape[0]), grad.shape[0])
    grad_bf[mine, :] = grad.astype(BF16)

    @pl.when(step == 0)
    def _():
        wait_load(w_qkv, sems.at[0])
        wait_load(w_out, sems.at[1])

    d_mix[...] = dot_nt(grad.astype(BF16), w_out[...]).astype(BF16)
    pairs = width // (2 * HEAD)

    at = lambda which, pair: slice(which * width + pair * 2 * HEAD, which * width + (pair + 1) * 2 * HEAD)
    rows_of = lambda sample: slice(sample * tokens, (sample + 1) * tokens)
    all_rows_of = lambda sample: pl.ds(pl.multiple_of((step * samples + sample) * tokens, tokens), tokens)

    def load(index):
        row, pair = rows_of(index // pairs), index % pairs
        return tuple(qkv_ref[row, at(which, pair)] for which in range(3)) + (d_mix[row, at(0, pair)],)

    def store(index, *parts):
        for which, part in enumerate(parts):
            d_qkv[all_rows_of(index // pairs), at(which, index % pairs)] = part

    pairs_backward(samples * pairs, load, store)

    @pl.when(step == last)
    def _():
        for copy in loads:
            copy.wait()
        for q in range(4):
            if q < 3:
                tile[q] = dot_tn(x_norm[...], d_qkv[:, q * width:(q + 1) * width])
            else:
                tile[q] = dot_tn(x_mix[...], grad_bf[...])
            if q > 0:
                for copy in tile_sends(q - 1, depth, tile, recv, send_sem, recv_sem):
                    copy.start()
        for copy in tile_sends(3, depth, tile, recv, send_sem, recv_sem):
            copy.start()

    d_norm = dot_nt(d_qkv[mine, :], w_qkv[...])
    d_res, g_gain, g_shift = norm_back(h_ref[...].astype(F32), rows_ref[0:1, :], d_norm)
    out_ref[...] = grad + d_res
    rounded_ref[...] = (grad + d_res).astype(BF16)
    add_rows(vec_ref, step, [g_gain, g_shift, jnp.sum(grad, axis=0, keepdims=True)])

    @pl.when(step == last)
    def _():
        finish_tiles(4, depth, 4 * depth, tile, recv, send_sem, recv_sem, far_ref, keep_ref)


def by_step(rows, columns):
    return pl.BlockSpec((rows, columns), lambda i: (i, 0))


def whole(rows, columns):
    return pl.BlockSpec((rows, columns), lambda i: (0, 0))


def shape(rows, columns, dtype):
    return jax.ShapeDtypeStruct((rows, columns), dtype)


def call(kernel, steps, in_specs, out_specs, out_shapes, scratch, flops, moved, kind=None):
    return pl.pallas_call(
        kernel, grid=(steps,), in_specs=in_specs, out_specs=out_specs, out_shape=out_shapes, scratch_shapes=scratch,
        cost_estimate=pl.CostEstimate(flops=int(flops), bytes_accessed=int(moved), transcendentals=0),
        compiler_params=pltpu.CompilerParams(dimension_semantics=('arbitrary',), vmem_limit_bytes=VMEM_LIMIT, collective_id=kind,
                                             has_side_effects=kind is not None))


def self_forward(h, rows, pieces, tokens):
    count, width = h.shape
    return call(
        functools.partial(self_forward_kernel, STEP // tokens, tokens), count // STEP,
        [by_step(STEP, width), whole(*rows.shape)] + [ANY] * 8,
        [by_step(STEP, width), by_step(STEP, 3 * width), by_step(STEP, width), by_step(STEP, width)],
        [shape(count, width, BF16), shape(count, 3 * width, BF16), shape(count, width, BF16), shape(count, width, F32)],
        [pltpu.VMEM((width, 3 * width), BF16), pltpu.VMEM((width, width), BF16), pltpu.SemaphoreType.DMA((2,))],
        count * width * width * 8 + count * tokens * width * 4, 2e7)(h, rows, *pieces)


def cross_forward(h, rows, ctx, pieces, tokens, valid):
    count, width = h.shape
    ctx_rows, ctx_width = ctx.shape
    return call(
        functools.partial(cross_forward_kernel, STEP // tokens, tokens, valid), count // STEP,
        [by_step(STEP, width), whole(*rows.shape), whole(ctx_rows, ctx_width)] + [ANY] * 8,
        [by_step(STEP, width), by_step(STEP, width), whole(ctx_rows, 2 * width), by_step(STEP, width), by_step(STEP, width)],
        [shape(count, width, BF16), shape(count, width, BF16), shape(ctx_rows, 2 * width, BF16), shape(count, width, BF16),
         shape(count, width, F32)],
        [pltpu.VMEM((ctx_width, 2 * width), BF16), pltpu.VMEM((width, width), BF16), pltpu.VMEM((width, width), BF16),
         pltpu.SemaphoreType.DMA((3,))],
        count * width * width * 4 + ctx_rows * ctx_width * width * 4 + count * 128 * width * 4, 2e7)(h, rows, ctx, *pieces)


def attention_forward(h, rows, ctx, pieces, tokens, valid):
    count, width = h.shape
    ctx_rows, ctx_width = ctx.shape
    one, kv = by_step(STEP, width), whole(ctx_rows, 2 * width)
    thin, full = shape(count, width, BF16), shape(count, width, F32)
    square = pltpu.VMEM((width, width), BF16)
    return call(
        functools.partial(attention_forward_kernel, STEP // tokens, tokens, valid), count // STEP,
        [one, whole(*rows.shape), whole(ctx_rows, ctx_width)] + [ANY] * 8,
        [one, by_step(STEP, 3 * width), one, one, one, one, kv, one, one],
        [thin, shape(count, 3 * width, BF16), thin, full, thin, thin, shape(ctx_rows, 2 * width, BF16), thin, full],
        [pltpu.VMEM((width, 3 * width), BF16), square, pltpu.SemaphoreType.DMA((2,)), pltpu.VMEM((ctx_width, 2 * width), BF16), square,
         square, pltpu.SemaphoreType.DMA((3,))],
        count * width * width * 12 + ctx_rows * ctx_width * width * 4 + count * tokens * width * 6, 4e7)(h, rows, ctx, *pieces)


def ff_forward(h, rows, bias, pieces, offset):
    count, width = h.shape
    half = bias.shape[1] // 2
    return call(
        functools.partial(ff_forward_kernel, offset), count // FF_STEP,
        [by_step(FF_STEP, width), whole(*rows.shape), whole(1, 2 * half)] + [ANY] * 16,
        [by_step(FF_STEP, width), by_step(FF_STEP, half), by_step(FF_STEP, half), by_step(FF_STEP, half), by_step(FF_STEP, width)],
        [shape(count, width, BF16), shape(count, half, BF16), shape(count, half, F32), shape(count, half, F32),
         shape(count, width, F32)],
        [pltpu.VMEM((width, 2 * half), BF16), pltpu.VMEM((half, width), BF16), pltpu.SemaphoreType.DMA((2,))],
        count * width * half * 6, 6e7)(h, rows, bias, *pieces)


def ff_up_forward(kind, h, rows, bias, cot, pieces):
    count, width = h.shape
    half = bias.shape[1] // 2
    dma = pltpu.SemaphoreType.DMA
    return call(
        ff_up_kernel, count // FF_STEP,
        [by_step(FF_STEP, width), whole(*rows.shape), whole(1, 2 * half)] + [ANY] * 9,
        [by_step(FF_STEP, width), by_step(FF_STEP, half), by_step(FF_STEP, half), by_step(FF_STEP, half), whole(width, width),
         whole(width, width)],
        [shape(count, width, BF16), shape(count, half, BF16), shape(count, half, F32), shape(count, half, F32), shape(width, width, F32),
         shape(width, width, F32)],
        [pltpu.VMEM((width, 2 * half), BF16), pltpu.VMEM((count, half), BF16), pltpu.VMEM((count, width), BF16),
         pltpu.VMEM((4, width, width), F32), pltpu.VMEM((4, width // 2, width), F32), dma((1,)), dma, dma((4,)), dma((4,))],
        count * width * half * 6, 5e7, kind)(h, rows, bias, cot, *pieces)


def ff_down_forward(h, rows, gated, pieces):
    count, width = h.shape
    half = gated.shape[1]
    return call(
        ff_down_kernel, count // STEP,
        [by_step(STEP, width), whole(*rows.shape), by_step(STEP, half)] + [ANY] * 8,
        by_step(STEP, width), shape(count, width, BF16),
        [pltpu.VMEM((half, width), BF16), pltpu.SemaphoreType.DMA((1,))],
        count * width * half * 2, 2e7)(h, rows, gated, *pieces)


def cross_backward(kind, grad, query, kv, h, rows, norm, mix, ctx_mine, ctx_other, pieces, tokens, valid):
    count, width = h.shape
    ctx_rows = kv.shape[0]
    steps = count // STEP
    group_rows = 2 * (width // 8) + ctx_mine.shape[0] // 2
    dma = pltpu.SemaphoreType.DMA
    big = pltpu.VMEM((count, width), BF16)
    kv_buf, ctx_buf = pltpu.VMEM((ctx_mine.shape[1], 2 * width), BF16), pltpu.VMEM(ctx_mine.shape, BF16)
    return call(
        functools.partial(cross_backward_kernel, STEP // tokens, tokens, valid), steps,
        [by_step(STEP, width), by_step(STEP, width), by_step(ctx_rows // steps, 2 * width), by_step(STEP, width),
         whole(*rows.shape)] + [ANY] * 12,
        [by_step(STEP, width), whole(8, width), whole(2 * group_rows, width), whole(2 * group_rows, width)],
        [shape(count, width, F32), shape(8, width, F32), shape(2 * group_rows, width, F32), shape(2 * group_rows, width, F32)],
        [pltpu.VMEM((STEP, width), BF16), pltpu.VMEM((width, width), BF16), pltpu.VMEM((width, width), BF16), big, big, kv_buf, kv_buf,
         big, big, ctx_buf, ctx_buf, pltpu.VMEM((2, width, width), F32), pltpu.VMEM((4, 2 * (width // 8), width), F32),
         dma((2,)), dma((4,)), dma, dma, dma((2, 4)), dma((2, 4))],
        count * width * width * 8 + count * 128 * width * 10 + ctx_mine.size * width * 8, 2e7, kind)(
            grad, query, kv, h, rows, norm, mix, ctx_mine, ctx_other, *pieces)


def self_backward(kind, grad, qkv, h, rows, norm, mix, pieces, tokens):
    count, width = h.shape
    group_rows = width // 2
    dma = pltpu.SemaphoreType.DMA
    big = pltpu.VMEM((count, width), BF16)
    return call(
        functools.partial(self_backward_kernel, STEP // tokens, tokens), count // STEP,
        [by_step(STEP, width), by_step(STEP, 3 * width), by_step(STEP, width), whole(*rows.shape)] + [ANY] * 10,
        [by_step(STEP, width), by_step(STEP, width), whole(8, width), whole(2 * group_rows, width), whole(2 * group_rows, width)],
        [shape(count, width, F32), shape(count, width, BF16), shape(8, width, F32), shape(2 * group_rows, width, F32), shape(2 * group_rows, width, F32)],
        [pltpu.VMEM((STEP, width), BF16), pltpu.VMEM((width, 3 * width), BF16), pltpu.VMEM((width, width), BF16),
         pltpu.VMEM((count, 3 * width), BF16), big, big, big, pltpu.VMEM((4, width, width), F32),
         pltpu.VMEM((4, group_rows, width), F32), dma((2,)), dma((2,)), dma((4, 4)), dma((4, 4))],
        count * width * width * 16 + count * tokens * width * 10, 3e7, kind)(grad, qkv, h, rows, norm, mix, *pieces)


def grad_kernel(tiles, group_rows, inputs, *refs):
    ins, refs = refs[:inputs], refs[inputs:]
    far_ref, keep_ref, x_buf, turned, y_buf, tile, own, recv, x_sem, y_sem, send_sem, recv_sem = refs[:12]
    width = tile.shape[1]
    me = lax.axis_index(AXIS)
    core, chip = lax.rem(me, 2), me // 2
    mate = me + 1 - 2 * core
    chip_x, chip_y = lax.rem(chip, 2), chip // 2

    xs, ys, x_of, y_of = [], [], [], []
    for x, x_col, y, y_col, *_ in tiles:
        if not xs or xs[-1] != (x, x_col):
            xs.append((x, x_col))
        if not ys or ys[-1] != (y, y_col):
            ys.append((y, y_col))
        x_of.append(len(xs) - 1)
        y_of.append(len(ys) - 1)

    def load(which, sequence, buf, sem):
        array, col = sequence[which]
        return pltpu.make_async_copy(ins[array].at[:, pl.ds(col, width)], buf.at[which % 2], sem.at[which % 2])

    for which in range(2):
        if which < len(xs):
            load(which, xs, x_buf, x_sem).start()
        if which < len(ys):
            load(which, ys, y_buf, y_sem).start()

    barrier = pltpu.get_barrier_semaphore()
    pl.semaphore_signal(barrier, inc=1, device_id=(mate,), device_id_type=pl.DeviceIdType.MESH)
    pl.semaphore_wait(barrier, 1)

    def sends(q):
        *_, first_row, rows, chips = tiles[q]
        copies = []
        for index, other in enumerate(chips):
            d_x, d_y = lax.rem(chip_x + other % 2, 2), lax.rem(chip_y + other // 2, 2)
            slot = d_x + 2 * d_y + core * (d_x - d_y)
            start = pl.multiple_of((2 * index + 1 - core) * rows, 16)
            copies.append(pltpu.make_async_remote_copy(
                src_ref=tile.at[q % 3, pl.ds(start, rows), :], dst_ref=recv.at[slot, pl.ds(first_row, rows), :],
                send_sem=send_sem.at[q % 3, index], recv_sem=recv_sem.at[q, index],
                device_id=(mate,), device_id_type=pl.DeviceIdType.MESH))
        return copies

    for q, (x, x_col, y, y_col, first_row, rows, chips) in enumerate(tiles):
        if q == 0 or x_of[q] != x_of[q - 1]:
            which = x_of[q]
            load(which, xs, x_buf, x_sem).wait()
            turned[...] = x_buf[which % 2].T
            if which + 2 < len(xs):
                load(which + 2, xs, x_buf, x_sem).start()
        if q == 0 or y_of[q] != y_of[q - 1]:
            load(y_of[q], ys, y_buf, y_sem).wait()
        if q >= 3:
            for copy in sends(q - 3):
                copy.wait_send()
        tile[q % 3] = dot_nn(turned[...], y_buf[y_of[q] % 2])
        if (q + 1 == len(tiles) or y_of[q + 1] != y_of[q]) and y_of[q] + 2 < len(ys):
            load(y_of[q] + 2, ys, y_buf, y_sem).start()
        for index, other in enumerate(chips):
            d_x, d_y = lax.rem(chip_x + other % 2, 2), lax.rem(chip_y + other // 2, 2)
            slot = 2 * d_x + d_y + core * (d_y - d_x)
            start = pl.multiple_of((2 * index + core) * rows, 16)
            own[slot, first_row:first_row + rows, :] = tile[q % 3, pl.ds(start, rows), :]
        if q >= 1:
            for copy in sends(q - 1):
                copy.start()
    last = len(tiles) - 1
    for copy in sends(last):
        copy.start()
    for q in range(max(0, last - 2), last + 1):
        for copy in sends(q):
            copy.wait_send()
    for q in range(last + 1):
        for copy in sends(q):
            copy.wait_recv()
    for slot in range(4):
        ref = keep_ref if slot < 2 else far_ref
        ref[(slot % 2) * group_rows:(slot % 2 + 1) * group_rows, :] = own[slot] + recv[slot]


def weight_grads(kind, arrays, tiles, group_rows):
    count, width = arrays[0].shape[0], 640
    chips = max(len(t[-1]) for t in tiles)
    dma = pltpu.SemaphoreType.DMA
    out = jax.ShapeDtypeStruct((2 * group_rows, width), F32)
    return pl.pallas_call(
        functools.partial(grad_kernel, tiles, group_rows, len(arrays)), in_specs=[ANY] * len(arrays),
        out_specs=[pl.BlockSpec(memory_space=pltpu.VMEM)] * 2, out_shape=[out, out],
        scratch_shapes=[pltpu.VMEM((2, count, width), BF16), pltpu.VMEM((width, count), BF16), pltpu.VMEM((2, count, width), BF16),
                        pltpu.VMEM((3, width, width), F32), pltpu.VMEM((4, group_rows, width), F32),
                        pltpu.VMEM((4, group_rows, width), F32), dma((2,)), dma((2,)), dma((3, chips)), dma((len(tiles), chips))],
        cost_estimate=pl.CostEstimate(flops=2 * count * width * width * len(tiles), bytes_accessed=int(2e7), transcendentals=0),
        compiler_params=pltpu.CompilerParams(collective_id=kind, has_side_effects=True, vmem_limit_bytes=VMEM_LIMIT))(*arrays)


def context_kernel(context_ref, ctx_ref, mine_ref, other_ref):
    batch, valid, _ = context_ref.shape
    padded = ctx_ref.shape[0] // batch
    me = lax.axis_index(AXIS)
    core, chip = lax.rem(me, 2), me // 2
    ctx_ref[...] = jnp.zeros_like(ctx_ref)
    for sample in range(batch):
        ctx_ref[sample * padded:sample * padded + valid, :] = context_ref[sample]
    each, rows = mine_ref.shape[0] // 4, ctx_ref.shape[0]
    mine_ref[...] = jnp.zeros_like(mine_ref)
    other_ref[...] = jnp.zeros_like(other_ref)
    x = jnp.bitwise_xor
    for of_core, ref in ((core, mine_ref), (1 - core, other_ref)):
        for slot, other in enumerate((chip, x(chip, 2 - of_core), x(chip, 1 + of_core), x(chip, 3))):
            column = pl.multiple_of((2 * other + of_core) * each, each)
            ref[slot * each:(slot + 1) * each, 0:rows] = ctx_ref[:, pl.ds(column, each)].T


def prepare_context(context, n_dev):
    batch, valid, ctx_width = context.shape
    rows = batch * ((valid + 15) // 16 * 16)
    vmem = pl.BlockSpec(memory_space=pltpu.VMEM)
    turned = shape(ctx_width // 2, (rows + 127) // 128 * 128, BF16)
    ctx, mine, other = pl.pallas_call(
        context_kernel, in_specs=[vmem], out_specs=[vmem] * 3, out_shape=[shape(rows, ctx_width, BF16), turned, turned],
        cost_estimate=pl.CostEstimate(flops=rows * ctx_width * 8, bytes_accessed=int(8e6), transcendentals=0),
        name='context')(context)
    return ctx, mine, permute(other, gather_perms(n_dev)[2])


def vec_pack_kernel(biases, *refs):
    ins, out = list(refs[:-1]), refs[-1]
    width = out.shape[1]
    out[...] = jnp.zeros_like(out)
    for layer, parts in enumerate(biases):
        first, second, third = ins[:3]
        rows = [(first, 0), (first, 1), (second, 0), (second, 1), (third, 0), (third, 1), (first, 2), (second, 2), (third, 2)]
        for index, (ref, row) in enumerate(rows):
            out[17 * layer + index:17 * layer + index + 1, :] = ref[row:row + 1, :]
        for (start, chunks), bias in zip(parts, ins[3:]):
            for kind in range(2):
                for chunk in range(chunks):
                    row, column = 17 * layer + 9 + 4 * kind + start + chunk, (kind * chunks + chunk) * width
                    out[row:row + 1, :] = bias[0:1, column:column + width]
        ins = ins[3 + len(parts):]


def vec_total(parts, biases, rows, n_dev):
    vmem = pl.BlockSpec(memory_space=pltpu.VMEM)
    width = parts[0].shape[1]
    total = pl.pallas_call(
        functools.partial(vec_pack_kernel, biases), in_specs=[vmem] * len(parts), out_specs=vmem, out_shape=shape(rows, width, F32),
        cost_estimate=pl.CostEstimate(flops=rows * width, bytes_accessed=rows * width * 8, transcendentals=0),
        name='vec_pack')(*parts)
    near, far, core = gather_perms(n_dev)
    for perm in (core, far, near):
        total = total + permute(total, perm)
    return total


def ff_grad_kernel(offset, first, resumed, final, rounded_ref, grad_ref, save_a, save_g, norm_ref, h_ref, rows_ref, *refs):
    before_ref, refs = (refs[0], refs[1:]) if resumed else (None, refs)
    pieces, refs = refs[:16], refs[16:]
    out_ref, refs = refs[0], refs[1:]
    vec_ref, refs = (refs[0], refs[1:]) if final else (None, refs)
    (bias_ref, far_ref, keep_ref, grad, grad_bf, norm_buf, turned, acc, part_a, part_g, d_both, w_ff1, w_ff2, tile, recv, obuf,
     in_sem, part_sem, w1_sem, w2_sem, out_sem, send_sem, recv_sem) = refs
    count, width = grad.shape
    every, chunks, depth = w_ff2.shape[0] // width, recv.shape[0], width // 8
    me = lax.axis_index(AXIS)
    core, mate, mate_slot, own_chip = chip_places(me)

    load_rounded = pltpu.make_async_copy(rounded_ref, grad_bf, in_sem.at[3])
    load_grad = pltpu.make_async_copy(grad_ref, grad, in_sem.at[0])
    load_norm = pltpu.make_async_copy(norm_ref, norm_buf, in_sem.at[1])
    load_before = pltpu.make_async_copy(before_ref, acc, in_sem.at[2]) if resumed else None
    load_rounded.start()
    start_load(pieces[8:], offset, w_ff2, w2_sem)

    blocks = count // STEP

    def parts(chunk, block):
        rows = pl.ds(block * STEP, STEP)
        at = (rows, pl.ds(pl.multiple_of((first + chunk) * width, width), width))
        return [pltpu.make_async_copy(ref.at[at], buf.at[lax.rem(chunk, 2), rows, :], part_sem.at[which, lax.rem(chunk, 2), block])
                for which, (ref, buf) in enumerate(((save_a, part_a), (save_g, part_g)))]

    def load_h(step):
        return pltpu.make_async_copy(h_ref.at[pl.ds(step * STEP, STEP), :], part_a.at[0, pl.ds(step * STEP, STEP), :], part_sem.at[0, 0, step])

    for copy in parts(0, 0):
        copy.start()
    devices = piece_devices(me)

    def load_w1(chunk):
        for kind in range(2):
            for piece, device in zip(pieces[:8], devices):
                pltpu.make_async_copy(
                    piece.at[pl.ds((kind * every + first + chunk) * depth, depth), :],
                    w_ff1.at[pl.ds(pl.multiple_of(device * depth, 16), depth), pl.ds((2 * chunk + kind) * width, width)],
                    w1_sem.at[chunk]).start()

    load_w1(0)
    for block in range(1, blocks):
        for copy in parts(0, block):
            copy.start()
    load_norm.start()
    if resumed:
        load_before.start()
    for chunk in range(1, chunks):
        load_w1(chunk)
    if final:
        load_grad.start()
    greet(mate)

    def sends(chunk):
        copies = []
        for other in range(4):
            start = pl.multiple_of((2 * other + 1 - core) * depth, 16)
            to = pl.multiple_of(mate_slot(other) * depth, 16)
            copies.append(pltpu.make_async_remote_copy(
                src_ref=tile.at[pl.ds(start, depth), :], dst_ref=recv.at[chunk, pl.ds(to, depth), :], send_sem=send_sem.at[other],
                recv_sem=recv_sem.at[chunk, other], device_id=(mate,), device_id_type=pl.DeviceIdType.MESH))
        return copies

    def wait_write():
        pltpu.make_async_copy(obuf, obuf, out_sem).wait()

    def finish(chunk, first):
        for copy in sends(chunk):
            copy.wait_recv()

        @pl.when(jnp.logical_not(first))
        def _():
            wait_write()

        for slot in range(4):
            start = pl.multiple_of((2 * own_chip(slot) + core) * depth, 16)
            rows = slice(slot * depth, (slot + 1) * depth)
            obuf[rows, :] = tile[pl.ds(start, depth), :] + recv[chunk, rows, :]
        for slot in range(4):
            ref = keep_ref if slot < 2 else far_ref
            for kind in range(2):
                row = pl.multiple_of((slot % 2) * 2 * chunks * depth + (kind * chunks + chunk) * depth, 16)
                pltpu.make_async_copy(obuf.at[pl.ds(slot * depth, depth), pl.ds(kind * width, width)], ref.at[pl.ds(row, depth), :],
                                      out_sem).start()
        for copy in sends(chunk):
            copy.wait_send()

    load_rounded.wait()
    load_norm.wait()
    turned[...] = norm_buf[...].T
    if resumed:
        load_before.wait()
    else:
        acc[...] = jnp.zeros_like(acc)
    bias_ref[...] = jnp.zeros_like(bias_ref)
    wait_load(w_ff2, w2_sem)

    def one_chunk(chunk, carry):
        w_pair = w_ff1.at[:, pl.ds(pl.multiple_of(chunk * 2 * width, width), 2 * width)]
        pltpu.make_async_copy(w_pair, w_pair, w1_sem.at[chunk]).wait()

        @pl.when(chunk + 1 < chunks)
        def _():
            for block in range(blocks):
                for copy in parts(chunk + 1, block):
                    copy.start()

        for block in range(blocks):
            for copy in parts(chunk, block):
                copy.wait()
        even = lax.rem(chunk, 2)
        w_down = w_ff2.at[pl.ds(pl.multiple_of((first + chunk) * width, width), width), :]
        sums = [0.0, 0.0]
        ahead = dot_nt(grad_bf[0:FF_ROWS, :], w_down[...])
        for start in range(0, count, FF_ROWS):
            rows = slice(start, start + FF_ROWS)
            d_gated = ahead
            if start + FF_ROWS < count:
                ahead = dot_nt(grad_bf[start + FF_ROWS:start + 2 * FF_ROWS, :], w_down[...])
            for kind, saved in enumerate((part_a, part_g)):
                d_part = d_gated * saved[even, rows, :]
                sums[kind] = sums[kind] + jnp.sum(d_part, axis=0, keepdims=True)
                d_both[rows, kind * width:(kind + 1) * width] = d_part.astype(BF16)
            acc[rows, :] += dot_nt(d_both[rows, :], w_pair[...])
        for kind in range(2):
            bias_ref[0:1, pl.ds(pl.multiple_of((kind * chunks + chunk) * width, 2 * HEAD), width)] += sums[kind]

        @pl.when(chunk > 0)
        def _():
            finish(jnp.maximum(chunk - 1, 0), chunk == 1)

        tile[...] = dot_nn(turned[...], d_both[...])
        for copy in sends(chunk):
            copy.start()
        return carry

    lax.fori_loop(0, chunks, one_chunk, 0)
    if final:
        steps = count // STEP
        vec_ref[...] = jnp.zeros_like(vec_ref)
        for step in range(steps):
            load_h(step).start()
        load_grad.wait()
        for step in range(steps):
            rows = slice(step * STEP, (step + 1) * STEP)
            load_h(step).wait()
            mine = grad[rows, :].astype(F32)
            d_res, g_gain, g_shift = norm_back(part_a[0, rows, :], rows_ref[4:5, :], acc[rows, :])
            acc[rows, :] = mine + d_res
            pltpu.make_async_copy(acc.at[pl.ds(step * STEP, STEP), :], out_ref.at[pl.ds(step * STEP, STEP), :], in_sem.at[0]).start()
            for at, row in enumerate((g_gain, g_shift, jnp.sum(mine, axis=0, keepdims=True))):
                vec_ref[at:at + 1, :] += row
    else:
        pltpu.make_async_copy(acc, out_ref, in_sem.at[0]).start()
    finish(chunks - 1, chunks == 1)
    wait_write()
    pltpu.make_async_copy(acc, out_ref, in_sem.at[0]).wait()


def ff_grads(kind, rounded, grad, save_a, save_g, norm, h, rows, pieces, offset, first, chunks, before):
    count, width = h.shape
    half = save_a.shape[1]
    final = first + chunks == half // width
    vmem = pl.BlockSpec(memory_space=pltpu.VMEM)
    big = shape(4 * chunks * (width // 8), width, F32)
    dma = pltpu.SemaphoreType.DMA
    saved = pltpu.VMEM((2, count, width), F32)
    resumed = before is not None
    return pl.pallas_call(
        functools.partial(ff_grad_kernel, offset, first, resumed, final), in_specs=[ANY] * 6 + [vmem] + [ANY] * (16 + resumed),
        out_specs=[ANY] + [vmem] * final + [vmem, ANY, ANY],
        out_shape=[shape(count, width, F32)] + [shape(8, width, F32)] * final + [shape(8, 2 * chunks * width, F32), big, big],
        scratch_shapes=[pltpu.VMEM((count, width), grad.dtype), pltpu.VMEM((count, width), BF16), pltpu.VMEM((count, width), BF16),
                        pltpu.VMEM((width, count), BF16),
                        pltpu.VMEM((count, width), F32), saved, saved, pltpu.VMEM((count, 2 * width), BF16),
                        pltpu.VMEM((width, 2 * chunks * width), BF16), pltpu.VMEM((half, width), BF16),
                        pltpu.VMEM((width, 2 * width), F32), pltpu.VMEM((chunks, width // 2, 2 * width), F32),
                        pltpu.VMEM((width // 2, 2 * width), F32),
                        dma((4,)), dma((2, 2, count // STEP)), dma((chunks,)), dma, dma, dma((4,)), dma((chunks, 4))],
        cost_estimate=pl.CostEstimate(flops=count * width * width * chunks * 10, bytes_accessed=int(6e7), transcendentals=0),
        compiler_params=pltpu.CompilerParams(collective_id=kind, has_side_effects=True, vmem_limit_bytes=VMEM_MOST))(rounded, grad, save_a, save_g, norm, h, rows, *([before] if resumed else []), *pieces)


def scatter(far, keep, n_dev):
    near_perm, far_perm, _ = gather_perms(n_dev)
    rows = keep.shape[0] // 2
    second = permute(far, far_perm)
    third = permute(keep[rows:] + second[rows:], near_perm)
    return keep, second, third


def total_kernel(plans, counts, depths, scale, *refs):
    ins, outs = refs[:3 * sum(counts)], refs[3 * sum(counts):]
    width, lanes, layers = ins[0].shape[1], outs[0].shape[1], len(plans)
    for layer, plan in enumerate(plans):
        base = 3 * sum(counts[:layer])
        for out, blocks, depth in zip(outs, plan, depths):
            stride = layers * len(blocks) * width // lanes
            for index, (part, row) in enumerate(blocks):
                keep, second, third = (ref[row:row + depth, :] for ref in ins[base + 3 * part:base + 3 * part + 3])
                block = ((keep + second) + third) * scale
                for column in range(0, width, lanes):
                    start = layers * ((index * width + column) // lanes) + layer
                    out[pl.ds(start, depth, stride), :] = block[:, column:column + lanes]


def totals(layers, plans, depths, scale):
    width, lanes = layers[0][0][0].shape[1], 128
    arrays, specs = [], []
    for parts in layers:
        for terms in parts:
            rows = terms[2].shape[0]
            arrays += list(terms)
            specs += [whole(rows, width)] * 3
    sizes = [depth * len(blocks) * width for depth, blocks in zip(depths, plans[0])]
    shapes = [shape(len(layers) * size // lanes, lanes, F32) for size in sizes]
    sums = pl.pallas_call(
        functools.partial(total_kernel, plans, [len(parts) for parts in layers], depths, scale), grid=(1,), in_specs=specs,
        out_specs=[whole(*out.shape) for out in shapes], out_shape=shapes,
        cost_estimate=pl.CostEstimate(flops=sum(a.size for a in arrays), bytes_accessed=4 * sum(a.size for a in arrays),
                                      transcendentals=0),
        compiler_params=pltpu.CompilerParams(vmem_limit_bytes=VMEM_LIMIT), name='totals')(*arrays)
    result = []
    for total, size in zip(sums, sizes):
        total = lax.optimization_barrier(total.reshape(size // lanes, len(layers), lanes))
        result.append(jnp.swapaxes(total, 0, 1).reshape(len(layers), size))
    return result


def solution(mesh):
    n_dev = mesh.shape[AXIS]

    def inner(tokens_x, context, cot_out, *shards):
        batch, tokens, width = tokens_x.shape
        _, valid, ctx_width = context.shape
        blocks = shards[0].shape[0]
        total = batch * n_dev
        depth = width // n_dev
        count = batch * tokens
        half = 4 * width

        views = []
        for shard, rows in zip(shards[:7], (depth, depth, depth, ctx_width // n_dev, depth, depth, half // n_dev)):
            views.append(shard.reshape(blocks, rows, -1))
        qkv_s, out_s = lax.optimization_barrier(views[:2])
        q2_s, kv2_s, out2_s = lax.optimization_barrier(views[2:5])
        ff1_s, ff2_s = lax.optimization_barrier(views[5:])
        me = lax.axis_index(AXIS)
        vec_len = shards[7].shape[1]
        vec_each = 17
        vec_rows = (blocks * vec_each + 15) // 16 * 16
        vec_block = lax.dynamic_update_slice(jnp.zeros((blocks, n_dev * vec_len), BF16), shards[7], (0, me * vec_len))
        vec_block = vec_block[:, :vec_each * width].reshape(blocks * vec_each, width)
        vec_block = jnp.pad(vec_block, ((0, vec_rows - blocks * vec_each), (0, 0)))

        members = []
        for layer in range(blocks):
            if layer < blocks - 1:
                members += [(layer, [qkv_s, out_s]), (layer, [kv2_s, q2_s, out2_s]), (layer, [ff1_s, ff2_s])]
            else:
                members += [(layer, [qkv_s, out_s, kv2_s, q2_s, out2_s]), (layer, [ff1_s]), (layer, [ff2_s])]
        groups = []
        for index, (layer, parts) in enumerate(members):
            block = pack(parts, layer, [vec_block] if index == 0 else [], width)
            groups.append(gather_group(block, n_dev))
        ff_groups = [groups[3 * layer + 2] * 2 if layer < blocks - 1 else groups[-2] + groups[-1] for layer in range(blocks)]
        ff_offsets = [8 * depth if layer < blocks - 1 else 0 for layer in range(blocks)]

        vecs = vec_sum(groups[0], vec_rows)
        vecs = vecs[:blocks * vec_each].reshape(blocks, vec_each, width)
        rows_all = jnp.pad(vecs[:, :9], ((0, 0), (0, 7), (0, 0)))
        bias_all = vecs[:, 9:].reshape(blocks, 1, 8 * width)

        ctx, ctx_mine, ctx_other = prepare_context(context, n_dev)

        h = tokens_x.reshape(count, width)
        cot = cot_out.reshape(count, width)
        saved, attention_groups = [], []
        for layer in range(blocks):
            rows, bias = rows_all[layer], bias_all[layer]
            group = groups[3 * layer:3 * layer + 2] if layer < blocks - 1 else [groups[3 * layer]] * 2
            attention_groups.append(group)
            if layer < blocks - 1:
                norm1, qkv, mix1, h1 = self_forward(h, rows, group[0], tokens)
                norm2, query, kv, mix2, h2 = cross_forward(h1, rows, ctx, group[1], tokens, valid)
                norm3, gated, save_a, save_g, h3 = ff_forward(h2, rows, bias, ff_groups[layer], ff_offsets[layer])
            else:
                norm1, qkv, mix1, h1, norm2, query, kv, mix2, h2 = attention_forward(h, rows, ctx, group[0], tokens, valid)
                norm3, gated, save_a, save_g, *down_pair = ff_up_forward(2, h2, rows, bias, cot, groups[-2])
                out_tokens = ff_down_forward(h2, rows, gated, groups[-1])
            saved.append((h, norm1, qkv, mix1, h1, norm2, query, kv, mix2, h2, norm3, gated, save_a, save_g))
            h = h3 if layer < blocks - 1 else None

        grad = rounded = cot
        results, vec_grads = [None] * blocks, [None] * blocks
        for layer in reversed(range(blocks)):
            turn = blocks - 1 - layer
            rows, group = rows_all[layer], attention_groups[layer]
            h0, norm1, qkv, mix1, h1, norm2, query, kv, mix2, h2, norm3, gated, save_a, save_g = saved[layer]

            def reduce(pair):
                return scatter(pair[0], pair[1], n_dev)

            if turn > 0:
                down_pair = weight_grads(1, (gated, rounded),
                                               [(0, c * width, 1, 0, 0, half // n_dev, (c,)) for c in range(half // width)], half // n_dev)
            r_ff2 = reduce(down_pair)
            sizes = (4,) if turn == 0 else (2, 2)
            d_norm, r_ff1, bias_grads, first_chunk = None, [], [], 0
            for index, chunks in enumerate(sizes):
                *out, vec_b1, far, keep = ff_grads(10 + 2 * turn + index, rounded, grad, save_a, save_g, norm3, h2, rows,
                                                   ff_groups[layer], ff_offsets[layer], first_chunk, chunks, d_norm)
                d_norm = out[0]
                bias_grads.append(((first_chunk, chunks), vec_b1))
                r_ff1.append(reduce((far, keep)))
                first_chunk += chunks
            grad, vec3 = out
            grad, vec2, *pair = cross_backward(3 + turn, grad, query, kv, h1, rows, norm2, mix2, ctx_mine, ctx_other, group[1],
                                               tokens, valid)
            r_cross = reduce(pair)
            grad, rounded, vec1, *pair = self_backward(8 + turn, grad, qkv, h0, rows, norm1, mix1, group[0], tokens)
            r_self = reduce(pair)
            results[layer] = [r_self], [r_cross], r_ff1, [r_ff2], sizes
            vec_grads[layer] = ([vec1, vec2, vec3] + [array for _, array in bias_grads], tuple(where for where, _ in bias_grads))
        vec_out = vec_total([part for parts, _ in vec_grads for part in parts], tuple(where for _, where in vec_grads), vec_rows, n_dev)
        vec_out = vec_out[:blocks * vec_each].reshape(blocks, vec_each * width)
        vec_out = jnp.pad(vec_out, ((0, 0), (0, vec_len * n_dev - vec_each * width)))
        vec_out = lax.dynamic_slice(vec_out, (0, me * vec_len), (blocks, vec_len))
        ff1_plans = []
        for layer in range(blocks):
            size = results[layer][4][0]
            ff1_plans.append([[(chunk // size, (kind * size + chunk % size) * depth) for kind in range(2) for chunk in range(4)]])
        deep = ctx_width // n_dev
        plans = ([[[(0, 0), (0, depth), (0, 2 * depth)], [(0, 3 * depth)]]] * blocks,
                 [[[(0, 0)], [(0, depth)], [(0, 2 * depth), (0, 2 * depth + deep)]]] * blocks, ff1_plans, [[[(0, 0)]]] * blocks)
        depths = ((depth, depth), (depth, depth, deep), (depth,), (half // n_dev,))
        summed = []
        for index in range(4):
            summed += totals([results[layer][index] for layer in range(blocks)], plans[index], depths[index], 1.0 / total)
        g_qkv, g_out, g_q2, g_out2, g_kv2, g_ff1, g_ff2 = summed
        outs = [g_qkv, g_out, g_q2, g_kv2, g_out2, g_ff1, g_ff2]
        outs.append(vec_out / total)
        return tuple([out_tokens.reshape(tokens_x.shape), rounded.reshape(tokens_x.shape)] + outs)

    param_spec = P(None, AXIS)
    in_specs = (P(AXIS), P(AXIS), P(AXIS)) + (param_spec,) * 8
    out_specs = (P(AXIS), P(AXIS)) + (param_spec,) * 8
    return jax.shard_map(inner, mesh=mesh, in_specs=in_specs, out_specs=out_specs, check_vma=False)
```

```python
import functools
import math
import jax
import jax.numpy as jnp
from jax import lax
from jax.experimental import pallas as pl
from jax.experimental.pallas import tpu as pltpu
from jax.sharding import PartitionSpec as P


HEAD = 64
AXIS = 'fsdp'
CHUNK = 256
FF_ROWS = 256
FF_STEP = 256
STEP = 512
VMEM_LIMIT = 60 * 1024 * 1024
VMEM_MOST = 67043328
FORWARD_UNROLL = 10

F32 = jnp.float32
BF16 = jnp.bfloat16
ANY = pl.BlockSpec(memory_space=pl.ANY)


def gather_perms(n_dev):
    near = [(i, i ^ (4 if i % 2 == 0 else 2)) for i in range(n_dev)]
    far = [(i, i ^ (2 if i % 2 == 0 else 4)) for i in range(n_dev)]
    core = [(i, i ^ 1) for i in range(n_dev)]
    return near, far, core


def pack_kernel(*refs):
    ins, out = refs[:-1], refs[-1]
    width, row = out.shape[1], 0
    for ref in ins:
        depth = ref.shape[-2]
        for col in range(0, ref.shape[-1], width):
            piece = ref[0, :, col:col + width] if len(ref.shape) == 3 else ref[:, col:col + width]
            out[row:row + depth, :] = piece
            row += depth


def pack(views, layer, extra, width):
    rows = sum(v.shape[1] * v.shape[2] // width for v in views) + sum(e.shape[0] for e in extra)
    specs = [pl.BlockSpec((1,) + v.shape[1:], lambda i: (layer, 0, 0)) for v in views]
    specs += [pl.BlockSpec(e.shape, lambda i: (0, 0)) for e in extra]
    return pl.pallas_call(
        pack_kernel, grid=(1,), in_specs=specs, out_specs=pl.BlockSpec((rows, width), lambda i: (0, 0)),
        out_shape=jax.ShapeDtypeStruct((rows, width), BF16),
        cost_estimate=pl.CostEstimate(flops=rows * width, bytes_accessed=rows * width * 4, transcendentals=0),
        name='pack')(*views, *extra)


def vec_kernel(*refs):
    pieces, (out, buf, sem) = refs[:8], refs[8:]
    rows = out.shape[0]
    copies = [pltpu.make_async_copy(piece.at[pl.ds(piece.shape[0] - rows, rows), :], buf.at[index], sem.at[index])
              for index, piece in enumerate(pieces)]
    for copy in copies:
        copy.start()
    total = None
    for index, copy in enumerate(copies):
        copy.wait()
        total = buf[index].astype(F32) if total is None else total + buf[index].astype(F32)
    out[...] = total


def vec_sum(pieces, rows):
    width = pieces[0].shape[1]
    return pl.pallas_call(
        vec_kernel, in_specs=[ANY] * 8, out_specs=pl.BlockSpec(memory_space=pltpu.VMEM),
        out_shape=jax.ShapeDtypeStruct((rows, width), F32),
        scratch_shapes=[pltpu.VMEM((8, rows, width), BF16), pltpu.SemaphoreType.DMA((8,))],
        cost_estimate=pl.CostEstimate(flops=rows * width * 8, bytes_accessed=rows * width * 20, transcendentals=0),
        name='vec_sum')(*pieces)


def permute(array, perm):
    return lax.ppermute(array, AXIS, perm)


def gather_group(shard, n_dev):
    near, far, core = gather_perms(n_dev)
    first = permute(shard, near)
    second = permute(shard, far)
    third = permute(first, far)
    mine = [shard, first, second, third]
    return mine + [permute(piece, core) for piece in mine]


def piece_devices(me):
    core = lax.rem(me, 2)
    one, two = 4 - 2 * core, 2 + 2 * core
    x = jnp.bitwise_xor
    mate = x(me, 1)
    return [me, x(me, one), x(me, two), x(me, 6), mate, x(mate, two), x(mate, one), x(mate, 6)]


def start_load(pieces, offset, ref, sem):
    width = pieces[0].shape[1]
    depth = ref.shape[0] // 8
    devices = piece_devices(lax.axis_index(AXIS))
    for block in range(ref.shape[1] // width):
        for piece, device in zip(pieces, devices):
            src = piece.at[pl.ds(offset + block * depth, depth), :]
            dst = ref.at[pl.ds(pl.multiple_of(device * depth, 16), depth), pl.ds(block * width, width)]
            pltpu.make_async_copy(src, dst, sem).start()


def wait_load(ref, sem):
    pltpu.make_async_copy(ref, ref, sem).wait()


def dot_nn(a, b):
    return lax.dot_general(a, b, (((1,), (0,)), ((), ())), preferred_element_type=F32)


def dot_nt(a, b):
    return lax.dot_general(a, b, (((1,), (1,)), ((), ())), preferred_element_type=F32)


def dot_tn(a, b):
    return lax.dot_general(a, b, (((0,), (0,)), ((), ())), preferred_element_type=F32)


def norm_stats(x):
    average = jnp.mean(x, axis=-1, keepdims=True)
    centered = x - average
    variance = jnp.mean(centered * centered, axis=-1, keepdims=True)
    scale = lax.rsqrt(variance + 1e-5)
    return centered * scale, scale


def norm_back(x, gain, d_norm):
    unit, scale = norm_stats(x)
    d_unit = d_norm * gain
    inner = d_unit - jnp.mean(d_unit, axis=-1, keepdims=True) - unit * jnp.mean(d_unit * unit, axis=-1, keepdims=True)
    return scale * inner, jnp.sum(d_norm * unit, axis=0, keepdims=True), jnp.sum(d_norm, axis=0, keepdims=True)


def softmax_rows(scores):
    top = jnp.max(scores, axis=-1, keepdims=True)
    raised = jnp.exp(scores - top)
    return raised * (1.0 / jnp.sum(raised, axis=-1, keepdims=True))


def low_lanes(rows):
    return lax.broadcasted_iota(jnp.int32, (rows, 2 * HEAD), 1) < HEAD


def heads_of(pair):
    low, zero = low_lanes(pair.shape[0]), jnp.zeros_like(pair)
    return jnp.where(low, pair, zero), jnp.where(low, zero, pair)


def pair_forward(query, key, value, valid=None):
    mixed = []
    for q_head in heads_of(query * HEAD ** -0.5):
        scores = dot_nt(q_head, key)
        if valid is not None:
            column = lax.broadcasted_iota(jnp.int32, scores.shape, 1)
            scores = jnp.where(column < valid, scores, -jnp.inf)
        mixed.append(dot_nn(softmax_rows(scores).astype(BF16), value))
    return jnp.where(low_lanes(query.shape[0]), mixed[0], mixed[1]).astype(BF16)


def backward_scores(query, key, value, d_out):
    q_heads, d_heads = heads_of(query * HEAD ** -0.5), heads_of(d_out)
    return q_heads, d_heads, [dot_nt(key, q) for q in q_heads], [dot_nt(value, d) for d in d_heads]


def backward_probs(scores, d_probs, valid):
    if valid is not None:
        row = lax.broadcasted_iota(jnp.int32, scores.shape, 0)
        scores = jnp.where(row < valid, scores, -jnp.inf)
    raised = jnp.exp(scores - jnp.max(scores, axis=0, keepdims=True))
    probs = raised * (1.0 / jnp.sum(raised, axis=0, keepdims=True))
    inner = jnp.sum(d_probs * probs, axis=0, keepdims=True)
    return probs.astype(BF16), (probs * (d_probs - inner)).astype(BF16)


def pairs_backward(pairs, load, store, valid=None):
    ahead = load(0)
    ahead = ahead, backward_scores(*ahead)
    for pair in range(pairs):
        (query, key, value, d_out), (q_heads, d_heads, scores, d_probs) = ahead
        if pair + 1 < pairs:
            ahead = load(pair + 1)
            ahead = ahead, backward_scores(*ahead)
        turned = key.T
        d_query, d_key, d_value = [], 0.0, 0.0
        for head in range(2):
            probs, d_scores = backward_probs(scores[head], d_probs[head], valid)
            d_query.append(dot_nn(turned[head * HEAD:(head + 1) * HEAD, :], d_scores))
            d_key = d_key + dot_nn(d_scores, q_heads[head])
            d_value = d_value + dot_nn(probs, d_heads[head])
        d_query = (jnp.concatenate(d_query, 0) * HEAD ** -0.5).T
        store(pair, d_query.astype(BF16), d_key.astype(BF16), d_value.astype(BF16))


def chip_places(me):
    core, chip = lax.rem(me, 2), me // 2
    chip_x, chip_y = lax.rem(chip, 2), chip // 2

    def mate_slot(other):
        d_x, d_y = lax.rem(chip_x + other % 2, 2), lax.rem(chip_y + other // 2, 2)
        return d_x + 2 * d_y + core * (d_x - d_y)

    def own_chip(slot):
        one, two = slot // 2, slot % 2
        d_x, d_y = one + core * (two - one), two + core * (one - two)
        return 2 * lax.rem(chip_y + d_y, 2) + lax.rem(chip_x + d_x, 2)

    return core, me + 1 - 2 * core, mate_slot, own_chip


def greet(mate):
    barrier = pltpu.get_barrier_semaphore()
    pl.semaphore_signal(barrier, inc=1, device_id=(mate,), device_id_type=pl.DeviceIdType.MESH)
    pl.semaphore_wait(barrier, 1)


def tile_sends(q, rows, tile, recv, send_sem, recv_sem):
    core, mate, mate_slot, _ = chip_places(lax.axis_index(AXIS))
    copies = []
    for other in range(4):
        start = pl.multiple_of((2 * other + 1 - core) * rows, 16)
        copies.append(pltpu.make_async_remote_copy(
            src_ref=tile.at[q, pl.ds(start, rows), :], dst_ref=recv.at[mate_slot(other), pl.ds(q * rows, rows), :],
            send_sem=send_sem.at[q, other], recv_sem=recv_sem.at[q, other],
            device_id=(mate,), device_id_type=pl.DeviceIdType.MESH))
    return copies


def finish_tiles(tiles, rows, group_rows, tile, recv, send_sem, recv_sem, far_ref, keep_ref):
    core, _, _, own_chip = chip_places(lax.axis_index(AXIS))
    for q in range(tiles):
        for copy in tile_sends(q, rows, tile, recv, send_sem, recv_sem):
            copy.wait()
        for slot in range(4):
            ref = keep_ref if slot < 2 else far_ref
            start = pl.multiple_of((2 * own_chip(slot) + core) * rows, 16)
            at = (slot % 2) * group_rows + q * rows
            ref[at:at + rows, :] = tile[q, pl.ds(start, rows), :] + recv[slot, q * rows:(q + 1) * rows, :]


def down_send(chip, tile, recv, send_sem, recv_sem):
    core, mate, _, _ = chip_places(lax.axis_index(AXIS))
    rows = recv.shape[1]
    return pltpu.make_async_remote_copy(
        src_ref=tile.at[chip, pl.ds(pl.multiple_of((1 - core) * rows, rows), rows), :], dst_ref=recv.at[chip],
        send_sem=send_sem.at[chip], recv_sem=recv_sem.at[chip], device_id=(mate,), device_id_type=pl.DeviceIdType.MESH)


def down_finish(tile, recv, send_sem, recv_sem, far_ref, keep_ref):
    core, _, _, own_chip = chip_places(lax.axis_index(AXIS))
    rows = recv.shape[1]
    for chip in range(4):
        down_send(chip, tile, recv, send_sem, recv_sem).wait()
    for slot in range(4):
        chip = own_chip(slot)
        ref = keep_ref if slot < 2 else far_ref
        at = (slot % 2) * rows
        ref[at:at + rows, :] = tile[chip, pl.ds(pl.multiple_of(core * rows, rows), rows), :] + recv[chip]


def add_rows(ref, step, rows):
    @pl.when(step == 0)
    def _():
        ref[...] = jnp.zeros_like(ref)

    for index, row in enumerate(rows):
        ref[pl.ds(index, 1), :] += row


def self_loads(pieces, w_qkv, w_out, sems):
    start_load(pieces, 0, w_qkv, sems.at[0])
    start_load(pieces, 3 * (w_out.shape[0] // 8), w_out, sems.at[1])


def cross_loads(pieces, offset, w_kv, w_query, w_out, sems):
    deep, depth = w_kv.shape[0] // 8, w_out.shape[0] // 8
    start_load(pieces, offset, w_kv, sems.at[0])
    start_load(pieces, offset + 2 * deep, w_query, sems.at[1])
    start_load(pieces, offset + 2 * deep + depth, w_out, sems.at[2])


def self_forward_kernel(samples, tokens, h_ref, rows_ref, *refs):
    @pl.when(pl.program_id(0) == 0)
    def _():
        self_loads(refs[:8], *refs[12:])

    self_forward_step(samples, tokens, h_ref, rows_ref, *refs[8:])


def cross_forward_kernel(samples, tokens, valid, h_ref, rows_ref, ctx_ref, *refs):
    @pl.when(pl.program_id(0) == 0)
    def _():
        cross_loads(refs[:8], 0, *refs[13:])

    cross_forward_step(samples, tokens, valid, h_ref, rows_ref, ctx_ref, *refs[8:])


def attention_forward_kernel(samples, tokens, valid, h_ref, rows_ref, ctx_ref, *refs):
    pieces, self_outs, cross_outs, self_scratch, cross_scratch = refs[:8], refs[8:12], refs[12:17], refs[17:20], refs[20:24]

    @pl.when(pl.program_id(0) == 0)
    def _():
        self_loads(pieces, *self_scratch)
        cross_loads(pieces, 4 * (h_ref.shape[1] // 8), *cross_scratch)

    self_forward_step(samples, tokens, h_ref, rows_ref, *self_outs, *self_scratch)
    cross_forward_step(samples, tokens, valid, self_outs[3], rows_ref, ctx_ref, *cross_outs, *cross_scratch)


def self_forward_step(samples, tokens, h_ref, rows_ref, norm_ref, qkv_ref, mix_ref, out_ref, w_qkv, w_out, sems):
    width = h_ref.shape[1]
    step = pl.program_id(0)
    x = h_ref[...].astype(F32)
    unit, _ = norm_stats(x)
    normed = (unit * rows_ref[0:1, :] + rows_ref[1:2, :]).astype(BF16)
    norm_ref[...] = normed

    @pl.when(step == 0)
    def _():
        wait_load(w_qkv, sems.at[0])
        wait_load(w_out, sems.at[1])

    qkv_ref[...] = dot_nn(normed, w_qkv[...]).astype(BF16)
    pairs = width // (2 * HEAD)

    def body(index, carry):
        row = pl.multiple_of((index // pairs) * tokens, tokens)
        col = pl.multiple_of((index % pairs) * 2 * HEAD, 2 * HEAD)
        part = lambda which: qkv_ref[pl.ds(row, tokens), pl.ds(which * width + col, 2 * HEAD)]
        mix_ref[pl.ds(row, tokens), pl.ds(col, 2 * HEAD)] = pair_forward(part(0), part(1), part(2))
        return carry

    lax.fori_loop(0, samples * pairs, body, 0, unroll=FORWARD_UNROLL)
    out_ref[...] = x + dot_nn(mix_ref[...], w_out[...]) + rows_ref[6:7, :]


def cross_forward_step(samples, tokens, valid, h_ref, rows_ref, ctx_ref, norm_ref, query_ref, kv_ref, mix_ref, out_ref, w_kv, w_query,
                       w_out, sems):
    width = h_ref.shape[1]
    step = pl.program_id(0)
    padded = ctx_ref.shape[0] // (samples * pl.num_programs(0))
    x = h_ref[...]
    unit, _ = norm_stats(x)
    normed = (unit * rows_ref[2:3, :] + rows_ref[3:4, :]).astype(BF16)
    norm_ref[...] = normed

    @pl.when(step == 0)
    def _():
        wait_load(w_kv, sems.at[0])
        wait_load(w_query, sems.at[1])
        wait_load(w_out, sems.at[2])
        kv_ref[...] = dot_nn(ctx_ref[...], w_kv[...]).astype(BF16)

    query_ref[...] = dot_nn(normed, w_query[...]).astype(BF16)
    pairs = width // (2 * HEAD)

    def body(index, carry):
        sample = index // pairs
        row = pl.multiple_of(sample * tokens, tokens)
        kv_row = pl.multiple_of((step * samples + sample) * padded, 16)
        col = pl.multiple_of((index % pairs) * 2 * HEAD, 2 * HEAD)
        query = query_ref[pl.ds(row, tokens), pl.ds(col, 2 * HEAD)]
        key = kv_ref[pl.ds(kv_row, padded), pl.ds(col, 2 * HEAD)]
        value = kv_ref[pl.ds(kv_row, padded), pl.ds(width + col, 2 * HEAD)]
        mix_ref[pl.ds(row, tokens), pl.ds(col, 2 * HEAD)] = pair_forward(query, key, value, valid)
        return carry

    lax.fori_loop(0, samples * pairs, body, 0, unroll=FORWARD_UNROLL)
    out_ref[...] = x + dot_nn(mix_ref[...], w_out[...]) + rows_ref[7:8, :]


def ff_loads(pieces, offset, w_ff1, w_ff2, sems):
    start_load(pieces[:8], 0, w_ff1, sems.at[0])
    start_load(pieces[8:], offset, w_ff2, sems.at[1])


def ff_hidden(normed, bias_ref, w_ff1, start):
    return dot_nn(normed, w_ff1[:, start:start + CHUNK]) + bias_ref[:, start:start + CHUNK]


def ff_up(normed, bias_ref, w_ff1, half, gated_ref, save_a, save_g, each=None):
    starts = list(range(0, half, CHUNK))
    ahead = (ff_hidden(normed, bias_ref, w_ff1, 0), ff_hidden(normed, bias_ref, w_ff1, half))
    for start in starts:
        u_a, u_g = ahead
        if start + CHUNK < half:
            ahead = tuple(ff_hidden(normed, bias_ref, w_ff1, base + start + CHUNK) for base in (0, half))
        cumulative = 0.5 * (1.0 + lax.erf(u_g * math.sqrt(0.5)))
        gate = u_g * cumulative
        slope = cumulative + u_g * (jnp.exp(-0.5 * u_g * u_g) * (1.0 / math.sqrt(2.0 * math.pi)))
        gated = (u_a * gate).astype(BF16)
        gated_ref[:, start:start + CHUNK] = gated
        save_a[:, start:start + CHUNK] = gate
        save_g[:, start:start + CHUNK] = u_a * slope
        if each is not None:
            each(start, gated)


def ff_forward_kernel(offset, h_ref, rows_ref, bias_ref, *refs):
    pieces, (norm_ref, gated_ref, save_a, save_g, out_ref, w_ff1, w_ff2, sems) = refs[:16], refs[16:]
    half = w_ff2.shape[0]
    step = pl.program_id(0)

    @pl.when(step == 0)
    def _():
        ff_loads(pieces, offset, w_ff1, w_ff2, sems)

    x = h_ref[...]
    unit, _ = norm_stats(x)
    normed = (unit * rows_ref[4:5, :] + rows_ref[5:6, :]).astype(BF16)
    norm_ref[...] = normed

    @pl.when(step == 0)
    def _():
        wait_load(w_ff1, sems.at[0])
        wait_load(w_ff2, sems.at[1])

    out_ref[...] = x + rows_ref[8:9, :]

    def down(start, gated):
        out_ref[...] += dot_nn(gated, w_ff2[start:start + CHUNK, :])

    ff_up(normed, bias_ref, w_ff1, half, gated_ref, save_a, save_g, down)


def ff_up_kernel(h_ref, rows_ref, bias_ref, cot_ref, *refs):
    pieces, refs = refs[:8], refs[8:]
    (norm_ref, gated_ref, save_a, save_g, far_ref, keep_ref, w_ff1, every, grad, tile, recv, sems, grad_sem, send_sem, recv_sem) = refs
    half, width = w_ff1.shape[1] // 2, grad.shape[1]
    step, last = pl.program_id(0), pl.num_programs(0) - 1
    load_grad = pltpu.make_async_copy(cot_ref, grad, grad_sem)

    @pl.when(step == 0)
    def _():
        start_load(pieces, 0, w_ff1, sems.at[0])
        load_grad.start()
        greet(chip_places(lax.axis_index(AXIS))[1])

    unit, _ = norm_stats(h_ref[...])
    normed = (unit * rows_ref[4:5, :] + rows_ref[5:6, :]).astype(BF16)
    norm_ref[...] = normed

    @pl.when(step == 0)
    def _():
        wait_load(w_ff1, sems.at[0])

    mine = pl.ds(pl.multiple_of(step * normed.shape[0], normed.shape[0]), normed.shape[0])

    def keep_gated(start, gated):
        every[mine, start:start + CHUNK] = gated

    ff_up(normed, bias_ref, w_ff1, half, gated_ref, save_a, save_g, keep_gated)

    @pl.when(step == last)
    def _():
        load_grad.wait()
        for chip in range(4):
            tile[chip] = dot_tn(every[:, chip * width:(chip + 1) * width], grad[...])
            down_send(chip, tile, recv, send_sem, recv_sem).start()
        down_finish(tile, recv, send_sem, recv_sem, far_ref, keep_ref)


def ff_down_kernel(h_ref, rows_ref, gated_ref, *refs):
    pieces, (out_ref, w_ff2, sems) = refs[:8], refs[8:]
    step = pl.program_id(0)

    @pl.when(step == 0)
    def _():
        start_load(pieces, 0, w_ff2, sems.at[0])
        wait_load(w_ff2, sems.at[0])

    out_ref[...] = (h_ref[...] + rows_ref[8:9, :] + dot_nn(gated_ref[...], w_ff2[...])).astype(BF16)


def cross_backward_kernel(samples, tokens, valid, grad_ref, query_ref, kv_ref, h_ref, rows_ref, norm_ref, mix_ref, ctx_mine_ref,
                          ctx_other_ref, *refs):
    pieces, refs = refs[:8], refs[8:]
    (out_ref, vec_ref, far_ref, keep_ref, d_mix, w_query, w_out, d_query, grad_bf, d_kv, kv_other, x_norm, x_mix, ctx_mine, ctx_other,
     tile, recv, sems, load_sem, kv_send, kv_recv, send_sem, recv_sem) = refs
    width = h_ref.shape[1]
    depth = width // 8
    step, last = pl.program_id(0), pl.num_programs(0) - 1
    padded = kv_ref.shape[0] // samples
    context_rows = kv_ref.shape[0] * (last + 1)
    mate = chip_places(lax.axis_index(AXIS))[1]
    loads = [pltpu.make_async_copy(src, dst, load_sem.at[index]) for index, (src, dst) in enumerate(
        ((norm_ref, x_norm), (mix_ref, x_mix), (ctx_mine_ref, ctx_mine), (ctx_other_ref, ctx_other)))]
    exchange = pltpu.make_async_remote_copy(
        src_ref=d_kv.at[pl.ds(0, context_rows), :], dst_ref=kv_other.at[pl.ds(0, context_rows), :], send_sem=kv_send, recv_sem=kv_recv,
        device_id=(mate,), device_id_type=pl.DeviceIdType.MESH)

    @pl.when(step == 0)
    def _():
        base = pieces[0].shape[0] - 2 * depth
        start_load(pieces, base, w_query, sems.at[0])
        start_load(pieces, base + depth, w_out, sems.at[1])
        for copy in loads:
            copy.start()
        for ref in (d_kv, kv_other):
            ref[context_rows:, :] = jnp.zeros((ref.shape[0] - context_rows, ref.shape[1]), BF16)
        greet(mate)

    grad = grad_ref[...]
    mine = pl.ds(pl.multiple_of(step * grad.shape[0], grad.shape[0]), grad.shape[0])
    grad_bf[mine, :] = grad.astype(BF16)

    @pl.when(step == 0)
    def _():
        wait_load(w_query, sems.at[0])
        wait_load(w_out, sems.at[1])

    d_mix[...] = dot_nt(grad.astype(BF16), w_out[...]).astype(BF16)
    pairs = width // (2 * HEAD)

    at = lambda which, pair: slice(which * width + pair * 2 * HEAD, which * width + (pair + 1) * 2 * HEAD)

    def load(index):
        sample, pair = index // pairs, index % pairs
        row, here = slice(sample * tokens, (sample + 1) * tokens), slice(sample * padded, (sample + 1) * padded)
        return query_ref[row, at(0, pair)], kv_ref[here, at(0, pair)], kv_ref[here, at(1, pair)], d_mix[row, at(0, pair)]

    def store(index, d_q, d_key, d_value):
        sample, pair = index // pairs, index % pairs
        d_query[pl.ds(pl.multiple_of((step * samples + sample) * tokens, tokens), tokens), at(0, pair)] = d_q
        there = pl.ds(pl.multiple_of((step * samples + sample) * padded, 16), padded)
        d_kv[there, at(0, pair)] = d_key
        d_kv[there, at(1, pair)] = d_value

    pairs_backward(samples * pairs, load, store, valid)
    rows, summed = depth, 2 * depth
    group_rows = keep_ref.shape[0] // 2
    deep = ctx_mine.shape[0] // 4

    def context_part(ctx, kv, slot, block):
        return dot_nn(ctx[slot * deep:(slot + 1) * deep, :], kv[:, block * width:(block + 1) * width])

    def context_at(slot, block):
        start = (slot % 2) * group_rows + summed + block * deep
        return slice(start, start + deep)

    @pl.when(step == last)
    def _():
        for copy in loads:
            copy.wait()
        tile[0] = dot_tn(x_norm[...], d_query[...])
        exchange.start()
        tile[1] = dot_tn(x_mix[...], grad_bf[...])
        for copy in tile_sends(0, rows, tile, recv, send_sem, recv_sem):
            copy.start()
        for slot in range(4):
            for block in range(2):
                (keep_ref if slot < 2 else far_ref)[context_at(slot, block), :] = context_part(ctx_mine, d_kv, slot, block)
        for copy in tile_sends(1, rows, tile, recv, send_sem, recv_sem):
            copy.start()

    d_norm = dot_nt(d_query[mine, :], w_query[...])
    d_res, g_gain, g_shift = norm_back(h_ref[...], rows_ref[2:3, :], d_norm)
    out_ref[...] = grad + d_res
    add_rows(vec_ref, step, [g_gain, g_shift, jnp.sum(grad, axis=0, keepdims=True)])

    @pl.when(step == last)
    def _():
        exchange.wait()
        for slot in range(4):
            for block in range(2):
                (keep_ref if slot < 2 else far_ref)[context_at(slot, block), :] += context_part(ctx_other, kv_other, slot, block)
        finish_tiles(2, rows, group_rows, tile, recv, send_sem, recv_sem, far_ref, keep_ref)


def self_backward_kernel(samples, tokens, grad_ref, qkv_ref, h_ref, rows_ref, norm_ref, mix_ref, *refs):
    pieces, refs = refs[:8], refs[8:]
    (out_ref, rounded_ref, vec_ref, far_ref, keep_ref, d_mix, w_qkv, w_out, d_qkv, grad_bf, x_norm, x_mix, tile, recv, sems, load_sem,
     send_sem, recv_sem) = refs
    width = h_ref.shape[1]
    depth = width // 8
    step, last = pl.program_id(0), pl.num_programs(0) - 1
    mate = chip_places(lax.axis_index(AXIS))[1]
    loads = [pltpu.make_async_copy(src, dst, load_sem.at[index]) for index, (src, dst) in enumerate(((norm_ref, x_norm), (mix_ref, x_mix)))]

    @pl.when(step == 0)
    def _():
        start_load(pieces, 0, w_qkv, sems.at[0])
        start_load(pieces, 3 * depth, w_out, sems.at[1])
        for copy in loads:
            copy.start()
        greet(mate)

    grad = grad_ref[...]
    mine = pl.ds(pl.multiple_of(step * grad.shape[0], grad.shape[0]), grad.shape[0])
    grad_bf[mine, :] = grad.astype(BF16)

    @pl.when(step == 0)
    def _():
        wait_load(w_qkv, sems.at[0])
        wait_load(w_out, sems.at[1])

    d_mix[...] = dot_nt(grad.astype(BF16), w_out[...]).astype(BF16)
    pairs = width // (2 * HEAD)

    at = lambda which, pair: slice(which * width + pair * 2 * HEAD, which * width + (pair + 1) * 2 * HEAD)
    rows_of = lambda sample: slice(sample * tokens, (sample + 1) * tokens)
    all_rows_of = lambda sample: pl.ds(pl.multiple_of((step * samples + sample) * tokens, tokens), tokens)

    def load(index):
        row, pair = rows_of(index // pairs), index % pairs
        return tuple(qkv_ref[row, at(which, pair)] for which in range(3)) + (d_mix[row, at(0, pair)],)

    def store(index, *parts):
        for which, part in enumerate(parts):
            d_qkv[all_rows_of(index // pairs), at(which, index % pairs)] = part

    pairs_backward(samples * pairs, load, store)

    @pl.when(step == last)
    def _():
        for copy in loads:
            copy.wait()
        for q in range(4):
            if q < 3:
                tile[q] = dot_tn(x_norm[...], d_qkv[:, q * width:(q + 1) * width])
            else:
                tile[q] = dot_tn(x_mix[...], grad_bf[...])
            if q > 0:
                for copy in tile_sends(q - 1, depth, tile, recv, send_sem, recv_sem):
                    copy.start()
        for copy in tile_sends(3, depth, tile, recv, send_sem, recv_sem):
            copy.start()

    d_norm = dot_nt(d_qkv[mine, :], w_qkv[...])
    d_res, g_gain, g_shift = norm_back(h_ref[...].astype(F32), rows_ref[0:1, :], d_norm)
    out_ref[...] = grad + d_res
    rounded_ref[...] = (grad + d_res).astype(BF16)
    add_rows(vec_ref, step, [g_gain, g_shift, jnp.sum(grad, axis=0, keepdims=True)])

    @pl.when(step == last)
    def _():
        finish_tiles(4, depth, 4 * depth, tile, recv, send_sem, recv_sem, far_ref, keep_ref)


def by_step(rows, columns):
    return pl.BlockSpec((rows, columns), lambda i: (i, 0))


def whole(rows, columns):
    return pl.BlockSpec((rows, columns), lambda i: (0, 0))


def shape(rows, columns, dtype):
    return jax.ShapeDtypeStruct((rows, columns), dtype)


def call(kernel, steps, in_specs, out_specs, out_shapes, scratch, flops, moved, kind=None):
    return pl.pallas_call(
        kernel, grid=(steps,), in_specs=in_specs, out_specs=out_specs, out_shape=out_shapes, scratch_shapes=scratch,
        cost_estimate=pl.CostEstimate(flops=int(flops), bytes_accessed=int(moved), transcendentals=0),
        compiler_params=pltpu.CompilerParams(dimension_semantics=('arbitrary',), vmem_limit_bytes=VMEM_LIMIT, collective_id=kind,
                                             has_side_effects=kind is not None))


def self_forward(h, rows, pieces, tokens):
    count, width = h.shape
    return call(
        functools.partial(self_forward_kernel, STEP // tokens, tokens), count // STEP,
        [by_step(STEP, width), whole(*rows.shape)] + [ANY] * 8,
        [by_step(STEP, width), by_step(STEP, 3 * width), by_step(STEP, width), by_step(STEP, width)],
        [shape(count, width, BF16), shape(count, 3 * width, BF16), shape(count, width, BF16), shape(count, width, F32)],
        [pltpu.VMEM((width, 3 * width), BF16), pltpu.VMEM((width, width), BF16), pltpu.SemaphoreType.DMA((2,))],
        count * width * width * 8 + count * tokens * width * 4, 2e7)(h, rows, *pieces)


def cross_forward(h, rows, ctx, pieces, tokens, valid):
    count, width = h.shape
    ctx_rows, ctx_width = ctx.shape
    return call(
        functools.partial(cross_forward_kernel, STEP // tokens, tokens, valid), count // STEP,
        [by_step(STEP, width), whole(*rows.shape), whole(ctx_rows, ctx_width)] + [ANY] * 8,
        [by_step(STEP, width), by_step(STEP, width), whole(ctx_rows, 2 * width), by_step(STEP, width), by_step(STEP, width)],
        [shape(count, width, BF16), shape(count, width, BF16), shape(ctx_rows, 2 * width, BF16), shape(count, width, BF16),
         shape(count, width, F32)],
        [pltpu.VMEM((ctx_width, 2 * width), BF16), pltpu.VMEM((width, width), BF16), pltpu.VMEM((width, width), BF16),
         pltpu.SemaphoreType.DMA((3,))],
        count * width * width * 4 + ctx_rows * ctx_width * width * 4 + count * 128 * width * 4, 2e7)(h, rows, ctx, *pieces)


def attention_forward(h, rows, ctx, pieces, tokens, valid):
    count, width = h.shape
    ctx_rows, ctx_width = ctx.shape
    one, kv = by_step(STEP, width), whole(ctx_rows, 2 * width)
    thin, full = shape(count, width, BF16), shape(count, width, F32)
    square = pltpu.VMEM((width, width), BF16)
    return call(
        functools.partial(attention_forward_kernel, STEP // tokens, tokens, valid), count // STEP,
        [one, whole(*rows.shape), whole(ctx_rows, ctx_width)] + [ANY] * 8,
        [one, by_step(STEP, 3 * width), one, one, one, one, kv, one, one],
        [thin, shape(count, 3 * width, BF16), thin, full, thin, thin, shape(ctx_rows, 2 * width, BF16), thin, full],
        [pltpu.VMEM((width, 3 * width), BF16), square, pltpu.SemaphoreType.DMA((2,)), pltpu.VMEM((ctx_width, 2 * width), BF16), square,
         square, pltpu.SemaphoreType.DMA((3,))],
        count * width * width * 12 + ctx_rows * ctx_width * width * 4 + count * tokens * width * 6, 4e7)(h, rows, ctx, *pieces)


def ff_forward(h, rows, bias, pieces, offset):
    count, width = h.shape
    half = bias.shape[1] // 2
    return call(
        functools.partial(ff_forward_kernel, offset), count // FF_STEP,
        [by_step(FF_STEP, width), whole(*rows.shape), whole(1, 2 * half)] + [ANY] * 16,
        [by_step(FF_STEP, width), by_step(FF_STEP, half), by_step(FF_STEP, half), by_step(FF_STEP, half), by_step(FF_STEP, width)],
        [shape(count, width, BF16), shape(count, half, BF16), shape(count, half, F32), shape(count, half, F32),
         shape(count, width, F32)],
        [pltpu.VMEM((width, 2 * half), BF16), pltpu.VMEM((half, width), BF16), pltpu.SemaphoreType.DMA((2,))],
        count * width * half * 6, 6e7)(h, rows, bias, *pieces)


def ff_up_forward(kind, h, rows, bias, cot, pieces):
    count, width = h.shape
    half = bias.shape[1] // 2
    dma = pltpu.SemaphoreType.DMA
    return call(
        ff_up_kernel, count // FF_STEP,
        [by_step(FF_STEP, width), whole(*rows.shape), whole(1, 2 * half)] + [ANY] * 9,
        [by_step(FF_STEP, width), by_step(FF_STEP, half), by_step(FF_STEP, half), by_step(FF_STEP, half), whole(width, width),
         whole(width, width)],
        [shape(count, width, BF16), shape(count, half, BF16), shape(count, half, F32), shape(count, half, F32), shape(width, width, F32),
         shape(width, width, F32)],
        [pltpu.VMEM((width, 2 * half), BF16), pltpu.VMEM((count, half), BF16), pltpu.VMEM((count, width), BF16),
         pltpu.VMEM((4, width, width), F32), pltpu.VMEM((4, width // 2, width), F32), dma((1,)), dma, dma((4,)), dma((4,))],
        count * width * half * 6, 5e7, kind)(h, rows, bias, cot, *pieces)


def ff_down_forward(h, rows, gated, pieces):
    count, width = h.shape
    half = gated.shape[1]
    return call(
        ff_down_kernel, count // STEP,
        [by_step(STEP, width), whole(*rows.shape), by_step(STEP, half)] + [ANY] * 8,
        by_step(STEP, width), shape(count, width, BF16),
        [pltpu.VMEM((half, width), BF16), pltpu.SemaphoreType.DMA((1,))],
        count * width * half * 2, 2e7)(h, rows, gated, *pieces)


def cross_backward(kind, grad, query, kv, h, rows, norm, mix, ctx_mine, ctx_other, pieces, tokens, valid):
    count, width = h.shape
    ctx_rows = kv.shape[0]
    steps = count // STEP
    group_rows = 2 * (width // 8) + ctx_mine.shape[0] // 2
    dma = pltpu.SemaphoreType.DMA
    big = pltpu.VMEM((count, width), BF16)
    kv_buf, ctx_buf = pltpu.VMEM((ctx_mine.shape[1], 2 * width), BF16), pltpu.VMEM(ctx_mine.shape, BF16)
    return call(
        functools.partial(cross_backward_kernel, STEP // tokens, tokens, valid), steps,
        [by_step(STEP, width), by_step(STEP, width), by_step(ctx_rows // steps, 2 * width), by_step(STEP, width),
         whole(*rows.shape)] + [ANY] * 12,
        [by_step(STEP, width), whole(8, width), whole(2 * group_rows, width), whole(2 * group_rows, width)],
        [shape(count, width, F32), shape(8, width, F32), shape(2 * group_rows, width, F32), shape(2 * group_rows, width, F32)],
        [pltpu.VMEM((STEP, width), BF16), pltpu.VMEM((width, width), BF16), pltpu.VMEM((width, width), BF16), big, big, kv_buf, kv_buf,
         big, big, ctx_buf, ctx_buf, pltpu.VMEM((2, width, width), F32), pltpu.VMEM((4, 2 * (width // 8), width), F32),
         dma((2,)), dma((4,)), dma, dma, dma((2, 4)), dma((2, 4))],
        count * width * width * 8 + count * 128 * width * 10 + ctx_mine.size * width * 8, 2e7, kind)(
            grad, query, kv, h, rows, norm, mix, ctx_mine, ctx_other, *pieces)


def self_backward(kind, grad, qkv, h, rows, norm, mix, pieces, tokens):
    count, width = h.shape
    group_rows = width // 2
    dma = pltpu.SemaphoreType.DMA
    big = pltpu.VMEM((count, width), BF16)
    return call(
        functools.partial(self_backward_kernel, STEP // tokens, tokens), count // STEP,
        [by_step(STEP, width), by_step(STEP, 3 * width), by_step(STEP, width), whole(*rows.shape)] + [ANY] * 10,
        [by_step(STEP, width), by_step(STEP, width), whole(8, width), whole(2 * group_rows, width), whole(2 * group_rows, width)],
        [shape(count, width, F32), shape(count, width, BF16), shape(8, width, F32), shape(2 * group_rows, width, F32), shape(2 * group_rows, width, F32)],
        [pltpu.VMEM((STEP, width), BF16), pltpu.VMEM((width, 3 * width), BF16), pltpu.VMEM((width, width), BF16),
         pltpu.VMEM((count, 3 * width), BF16), big, big, big, pltpu.VMEM((4, width, width), F32),
         pltpu.VMEM((4, group_rows, width), F32), dma((2,)), dma((2,)), dma((4, 4)), dma((4, 4))],
        count * width * width * 16 + count * tokens * width * 10, 3e7, kind)(grad, qkv, h, rows, norm, mix, *pieces)


def grad_kernel(tiles, group_rows, inputs, *refs):
    ins, refs = refs[:inputs], refs[inputs:]
    far_ref, keep_ref, x_buf, turned, y_buf, tile, own, recv, x_sem, y_sem, send_sem, recv_sem = refs[:12]
    width = tile.shape[1]
    me = lax.axis_index(AXIS)
    core, chip = lax.rem(me, 2), me // 2
    mate = me + 1 - 2 * core
    chip_x, chip_y = lax.rem(chip, 2), chip // 2

    xs, ys, x_of, y_of = [], [], [], []
    for x, x_col, y, y_col, *_ in tiles:
        if not xs or xs[-1] != (x, x_col):
            xs.append((x, x_col))
        if not ys or ys[-1] != (y, y_col):
            ys.append((y, y_col))
        x_of.append(len(xs) - 1)
        y_of.append(len(ys) - 1)

    def load(which, sequence, buf, sem):
        array, col = sequence[which]
        return pltpu.make_async_copy(ins[array].at[:, pl.ds(col, width)], buf.at[which % 2], sem.at[which % 2])

    for which in range(2):
        if which < len(xs):
            load(which, xs, x_buf, x_sem).start()
        if which < len(ys):
            load(which, ys, y_buf, y_sem).start()

    barrier = pltpu.get_barrier_semaphore()
    pl.semaphore_signal(barrier, inc=1, device_id=(mate,), device_id_type=pl.DeviceIdType.MESH)
    pl.semaphore_wait(barrier, 1)

    def sends(q):
        *_, first_row, rows, chips = tiles[q]
        copies = []
        for index, other in enumerate(chips):
            d_x, d_y = lax.rem(chip_x + other % 2, 2), lax.rem(chip_y + other // 2, 2)
            slot = d_x + 2 * d_y + core * (d_x - d_y)
            start = pl.multiple_of((2 * index + 1 - core) * rows, 16)
            copies.append(pltpu.make_async_remote_copy(
                src_ref=tile.at[q % 3, pl.ds(start, rows), :], dst_ref=recv.at[slot, pl.ds(first_row, rows), :],
                send_sem=send_sem.at[q % 3, index], recv_sem=recv_sem.at[q, index],
                device_id=(mate,), device_id_type=pl.DeviceIdType.MESH))
        return copies

    for q, (x, x_col, y, y_col, first_row, rows, chips) in enumerate(tiles):
        if q == 0 or x_of[q] != x_of[q - 1]:
            which = x_of[q]
            load(which, xs, x_buf, x_sem).wait()
            turned[...] = x_buf[which % 2].T
            if which + 2 < len(xs):
                load(which + 2, xs, x_buf, x_sem).start()
        if q == 0 or y_of[q] != y_of[q - 1]:
            load(y_of[q], ys, y_buf, y_sem).wait()
        if q >= 3:
            for copy in sends(q - 3):
                copy.wait_send()
        tile[q % 3] = dot_nn(turned[...], y_buf[y_of[q] % 2])
        if (q + 1 == len(tiles) or y_of[q + 1] != y_of[q]) and y_of[q] + 2 < len(ys):
            load(y_of[q] + 2, ys, y_buf, y_sem).start()
        for index, other in enumerate(chips):
            d_x, d_y = lax.rem(chip_x + other % 2, 2), lax.rem(chip_y + other // 2, 2)
            slot = 2 * d_x + d_y + core * (d_y - d_x)
            start = pl.multiple_of((2 * index + core) * rows, 16)
            own[slot, first_row:first_row + rows, :] = tile[q % 3, pl.ds(start, rows), :]
        if q >= 1:
            for copy in sends(q - 1):
                copy.start()
    last = len(tiles) - 1
    for copy in sends(last):
        copy.start()
    for q in range(max(0, last - 2), last + 1):
        for copy in sends(q):
            copy.wait_send()
    for q in range(last + 1):
        for copy in sends(q):
            copy.wait_recv()
    for slot in range(4):
        ref = keep_ref if slot < 2 else far_ref
        ref[(slot % 2) * group_rows:(slot % 2 + 1) * group_rows, :] = own[slot] + recv[slot]


def weight_grads(kind, arrays, tiles, group_rows):
    count, width = arrays[0].shape[0], 640
    chips = max(len(t[-1]) for t in tiles)
    dma = pltpu.SemaphoreType.DMA
    out = jax.ShapeDtypeStruct((2 * group_rows, width), F32)
    return pl.pallas_call(
        functools.partial(grad_kernel, tiles, group_rows, len(arrays)), in_specs=[ANY] * len(arrays),
        out_specs=[pl.BlockSpec(memory_space=pltpu.VMEM)] * 2, out_shape=[out, out],
        scratch_shapes=[pltpu.VMEM((2, count, width), BF16), pltpu.VMEM((width, count), BF16), pltpu.VMEM((2, count, width), BF16),
                        pltpu.VMEM((3, width, width), F32), pltpu.VMEM((4, group_rows, width), F32),
                        pltpu.VMEM((4, group_rows, width), F32), dma((2,)), dma((2,)), dma((3, chips)), dma((len(tiles), chips))],
        cost_estimate=pl.CostEstimate(flops=2 * count * width * width * len(tiles), bytes_accessed=int(2e7), transcendentals=0),
        compiler_params=pltpu.CompilerParams(collective_id=kind, has_side_effects=True, vmem_limit_bytes=VMEM_LIMIT))(*arrays)


def context_kernel(context_ref, ctx_ref, mine_ref, other_ref):
    batch, valid, _ = context_ref.shape
    padded = ctx_ref.shape[0] // batch
    me = lax.axis_index(AXIS)
    core, chip = lax.rem(me, 2), me // 2
    ctx_ref[...] = jnp.zeros_like(ctx_ref)
    for sample in range(batch):
        ctx_ref[sample * padded:sample * padded + valid, :] = context_ref[sample]
    each, rows = mine_ref.shape[0] // 4, ctx_ref.shape[0]
    mine_ref[...] = jnp.zeros_like(mine_ref)
    other_ref[...] = jnp.zeros_like(other_ref)
    x = jnp.bitwise_xor
    for of_core, ref in ((core, mine_ref), (1 - core, other_ref)):
        for slot, other in enumerate((chip, x(chip, 2 - of_core), x(chip, 1 + of_core), x(chip, 3))):
            column = pl.multiple_of((2 * other + of_core) * each, each)
            ref[slot * each:(slot + 1) * each, 0:rows] = ctx_ref[:, pl.ds(column, each)].T


def prepare_context(context, n_dev):
    batch, valid, ctx_width = context.shape
    rows = batch * ((valid + 15) // 16 * 16)
    vmem = pl.BlockSpec(memory_space=pltpu.VMEM)
    turned = shape(ctx_width // 2, (rows + 127) // 128 * 128, BF16)
    ctx, mine, other = pl.pallas_call(
        context_kernel, in_specs=[vmem], out_specs=[vmem] * 3, out_shape=[shape(rows, ctx_width, BF16), turned, turned],
        cost_estimate=pl.CostEstimate(flops=rows * ctx_width * 8, bytes_accessed=int(8e6), transcendentals=0),
        name='context')(context)
    return ctx, mine, permute(other, gather_perms(n_dev)[2])


def vec_pack_kernel(biases, *refs):
    ins, out = list(refs[:-1]), refs[-1]
    width = out.shape[1]
    out[...] = jnp.zeros_like(out)
    for layer, parts in enumerate(biases):
        first, second, third = ins[:3]
        rows = [(first, 0), (first, 1), (second, 0), (second, 1), (third, 0), (third, 1), (first, 2), (second, 2), (third, 2)]
        for index, (ref, row) in enumerate(rows):
            out[17 * layer + index:17 * layer + index + 1, :] = ref[row:row + 1, :]
        for (start, chunks), bias in zip(parts, ins[3:]):
            for kind in range(2):
                for chunk in range(chunks):
                    row, column = 17 * layer + 9 + 4 * kind + start + chunk, (kind * chunks + chunk) * width
                    out[row:row + 1, :] = bias[0:1, column:column + width]
        ins = ins[3 + len(parts):]


def vec_total(parts, biases, rows, n_dev):
    vmem = pl.BlockSpec(memory_space=pltpu.VMEM)
    width = parts[0].shape[1]
    total = pl.pallas_call(
        functools.partial(vec_pack_kernel, biases), in_specs=[vmem] * len(parts), out_specs=vmem, out_shape=shape(rows, width, F32),
        cost_estimate=pl.CostEstimate(flops=rows * width, bytes_accessed=rows * width * 8, transcendentals=0),
        name='vec_pack')(*parts)
    near, far, core = gather_perms(n_dev)
    for perm in (core, far, near):
        total = total + permute(total, perm)
    return total


def ff_grad_kernel(offset, first, resumed, final, rounded_ref, grad_ref, save_a, save_g, norm_ref, h_ref, rows_ref, *refs):
    before_ref, refs = (refs[0], refs[1:]) if resumed else (None, refs)
    pieces, refs = refs[:16], refs[16:]
    out_ref, refs = refs[0], refs[1:]
    vec_ref, refs = (refs[0], refs[1:]) if final else (None, refs)
    (bias_ref, far_ref, keep_ref, grad, grad_bf, norm_buf, turned, acc, part_a, part_g, d_both, w_ff1, w_ff2, tile, recv, obuf,
     in_sem, part_sem, w1_sem, w2_sem, out_sem, send_sem, recv_sem) = refs
    count, width = grad.shape
    every, chunks, depth = w_ff2.shape[0] // width, recv.shape[0], width // 8
    me = lax.axis_index(AXIS)
    core, mate, mate_slot, own_chip = chip_places(me)

    load_rounded = pltpu.make_async_copy(rounded_ref, grad_bf, in_sem.at[3])
    load_grad = pltpu.make_async_copy(grad_ref, grad, in_sem.at[0])
    load_norm = pltpu.make_async_copy(norm_ref, norm_buf, in_sem.at[1])
    load_before = pltpu.make_async_copy(before_ref, acc, in_sem.at[2]) if resumed else None
    load_rounded.start()
    start_load(pieces[8:], offset, w_ff2, w2_sem)

    blocks = count // STEP

    def parts(chunk, block):
        rows = pl.ds(block * STEP, STEP)
        at = (rows, pl.ds(pl.multiple_of((first + chunk) * width, width), width))
        return [pltpu.make_async_copy(ref.at[at], buf.at[lax.rem(chunk, 2), rows, :], part_sem.at[which, lax.rem(chunk, 2), block])
                for which, (ref, buf) in enumerate(((save_a, part_a), (save_g, part_g)))]

    def load_h(step):
        return pltpu.make_async_copy(h_ref.at[pl.ds(step * STEP, STEP), :], part_a.at[0, pl.ds(step * STEP, STEP), :], part_sem.at[0, 0, step])

    for copy in parts(0, 0):
        copy.start()
    devices = piece_devices(me)

    def load_w1(chunk):
        for kind in range(2):
            for piece, device in zip(pieces[:8], devices):
                pltpu.make_async_copy(
                    piece.at[pl.ds((kind * every + first + chunk) * depth, depth), :],
                    w_ff1.at[pl.ds(pl.multiple_of(device * depth, 16), depth), pl.ds((2 * chunk + kind) * width, width)],
                    w1_sem.at[chunk]).start()

    load_w1(0)
    for block in range(1, blocks):
        for copy in parts(0, block):
            copy.start()
    load_norm.start()
    if resumed:
        load_before.start()
    for chunk in range(1, chunks):
        load_w1(chunk)
    if final:
        load_grad.start()
    greet(mate)

    def sends(chunk):
        copies = []
        for other in range(4):
            start = pl.multiple_of((2 * other + 1 - core) * depth, 16)
            to = pl.multiple_of(mate_slot(other) * depth, 16)
            copies.append(pltpu.make_async_remote_copy(
                src_ref=tile.at[pl.ds(start, depth), :], dst_ref=recv.at[chunk, pl.ds(to, depth), :], send_sem=send_sem.at[other],
                recv_sem=recv_sem.at[chunk, other], device_id=(mate,), device_id_type=pl.DeviceIdType.MESH))
        return copies

    def wait_write():
        pltpu.make_async_copy(obuf, obuf, out_sem).wait()

    def finish(chunk, first):
        for copy in sends(chunk):
            copy.wait_recv()

        @pl.when(jnp.logical_not(first))
        def _():
            wait_write()

        for slot in range(4):
            start = pl.multiple_of((2 * own_chip(slot) + core) * depth, 16)
            rows = slice(slot * depth, (slot + 1) * depth)
            obuf[rows, :] = tile[pl.ds(start, depth), :] + recv[chunk, rows, :]
        for slot in range(4):
            ref = keep_ref if slot < 2 else far_ref
            for kind in range(2):
                row = pl.multiple_of((slot % 2) * 2 * chunks * depth + (kind * chunks + chunk) * depth, 16)
                pltpu.make_async_copy(obuf.at[pl.ds(slot * depth, depth), pl.ds(kind * width, width)], ref.at[pl.ds(row, depth), :],
                                      out_sem).start()
        for copy in sends(chunk):
            copy.wait_send()

    load_rounded.wait()
    load_norm.wait()
    turned[...] = norm_buf[...].T
    if resumed:
        load_before.wait()
    else:
        acc[...] = jnp.zeros_like(acc)
    bias_ref[...] = jnp.zeros_like(bias_ref)
    wait_load(w_ff2, w2_sem)

    def one_chunk(chunk, carry):
        w_pair = w_ff1.at[:, pl.ds(pl.multiple_of(chunk * 2 * width, width), 2 * width)]
        pltpu.make_async_copy(w_pair, w_pair, w1_sem.at[chunk]).wait()

        @pl.when(chunk + 1 < chunks)
        def _():
            for block in range(blocks):
                for copy in parts(chunk + 1, block):
                    copy.start()

        for block in range(blocks):
            for copy in parts(chunk, block):
                copy.wait()
        even = lax.rem(chunk, 2)
        w_down = w_ff2.at[pl.ds(pl.multiple_of((first + chunk) * width, width), width), :]
        sums = [0.0, 0.0]
        ahead = dot_nt(grad_bf[0:FF_ROWS, :], w_down[...])
        for start in range(0, count, FF_ROWS):
            rows = slice(start, start + FF_ROWS)
            d_gated = ahead
            if start + FF_ROWS < count:
                ahead = dot_nt(grad_bf[start + FF_ROWS:start + 2 * FF_ROWS, :], w_down[...])
            for kind, saved in enumerate((part_a, part_g)):
                d_part = d_gated * saved[even, rows, :]
                sums[kind] = sums[kind] + jnp.sum(d_part, axis=0, keepdims=True)
                d_both[rows, kind * width:(kind + 1) * width] = d_part.astype(BF16)
            acc[rows, :] += dot_nt(d_both[rows, :], w_pair[...])
        for kind in range(2):
            bias_ref[0:1, pl.ds(pl.multiple_of((kind * chunks + chunk) * width, 2 * HEAD), width)] += sums[kind]

        @pl.when(chunk > 0)
        def _():
            finish(jnp.maximum(chunk - 1, 0), chunk == 1)

        tile[...] = dot_nn(turned[...], d_both[...])
        for copy in sends(chunk):
            copy.start()
        return carry

    lax.fori_loop(0, chunks, one_chunk, 0)
    if final:
        steps = count // STEP
        vec_ref[...] = jnp.zeros_like(vec_ref)
        for step in range(steps):
            load_h(step).start()
        load_grad.wait()
        for step in range(steps):
            rows = slice(step * STEP, (step + 1) * STEP)
            load_h(step).wait()
            mine = grad[rows, :].astype(F32)
            d_res, g_gain, g_shift = norm_back(part_a[0, rows, :], rows_ref[4:5, :], acc[rows, :])
            acc[rows, :] = mine + d_res
            pltpu.make_async_copy(acc.at[pl.ds(step * STEP, STEP), :], out_ref.at[pl.ds(step * STEP, STEP), :], in_sem.at[0]).start()
            for at, row in enumerate((g_gain, g_shift, jnp.sum(mine, axis=0, keepdims=True))):
                vec_ref[at:at + 1, :] += row
    else:
        pltpu.make_async_copy(acc, out_ref, in_sem.at[0]).start()
    finish(chunks - 1, chunks == 1)
    wait_write()
    pltpu.make_async_copy(acc, out_ref, in_sem.at[0]).wait()


def ff_grads(kind, rounded, grad, save_a, save_g, norm, h, rows, pieces, offset, first, chunks, before):
    count, width = h.shape
    half = save_a.shape[1]
    final = first + chunks == half // width
    vmem = pl.BlockSpec(memory_space=pltpu.VMEM)
    big = shape(4 * chunks * (width // 8), width, F32)
    dma = pltpu.SemaphoreType.DMA
    saved = pltpu.VMEM((2, count, width), F32)
    resumed = before is not None
    return pl.pallas_call(
        functools.partial(ff_grad_kernel, offset, first, resumed, final), in_specs=[ANY] * 6 + [vmem] + [ANY] * (16 + resumed),
        out_specs=[ANY] + [vmem] * final + [vmem, ANY, ANY],
        out_shape=[shape(count, width, F32)] + [shape(8, width, F32)] * final + [shape(8, 2 * chunks * width, F32), big, big],
        scratch_shapes=[pltpu.VMEM((count, width), grad.dtype), pltpu.VMEM((count, width), BF16), pltpu.VMEM((count, width), BF16),
                        pltpu.VMEM((width, count), BF16),
                        pltpu.VMEM((count, width), F32), saved, saved, pltpu.VMEM((count, 2 * width), BF16),
                        pltpu.VMEM((width, 2 * chunks * width), BF16), pltpu.VMEM((half, width), BF16),
                        pltpu.VMEM((width, 2 * width), F32), pltpu.VMEM((chunks, width // 2, 2 * width), F32),
                        pltpu.VMEM((width // 2, 2 * width), F32),
                        dma((4,)), dma((2, 2, count // STEP)), dma((chunks,)), dma, dma, dma((4,)), dma((chunks, 4))],
        cost_estimate=pl.CostEstimate(flops=count * width * width * chunks * 10, bytes_accessed=int(6e7), transcendentals=0),
        compiler_params=pltpu.CompilerParams(collective_id=kind, has_side_effects=True, vmem_limit_bytes=VMEM_MOST))(rounded, grad, save_a, save_g, norm, h, rows, *([before] if resumed else []), *pieces)


def scatter(far, keep, n_dev):
    near_perm, far_perm, _ = gather_perms(n_dev)
    rows = keep.shape[0] // 2
    second = permute(far, far_perm)
    third = permute(keep[rows:] + second[rows:], near_perm)
    return keep, second, third


def total_kernel(plans, counts, depths, scale, *refs):
    ins, outs = refs[:3 * sum(counts)], refs[3 * sum(counts):]
    width, lanes, layers = ins[0].shape[1], outs[0].shape[1], len(plans)
    for layer, plan in enumerate(plans):
        base = 3 * sum(counts[:layer])
        for out, blocks, depth in zip(outs, plan, depths):
            stride = layers * len(blocks) * width // lanes
            for index, (part, row) in enumerate(blocks):
                keep, second, third = (ref[row:row + depth, :] for ref in ins[base + 3 * part:base + 3 * part + 3])
                block = ((keep + second) + third) * scale
                for column in range(0, width, lanes):
                    start = layers * ((index * width + column) // lanes) + layer
                    out[pl.ds(start, depth, stride), :] = block[:, column:column + lanes]


def totals(layers, plans, depths, scale):
    width, lanes = layers[0][0][0].shape[1], 128
    arrays, specs = [], []
    for parts in layers:
        for terms in parts:
            rows = terms[2].shape[0]
            arrays += list(terms)
            specs += [whole(rows, width)] * 3
    sizes = [depth * len(blocks) * width for depth, blocks in zip(depths, plans[0])]
    shapes = [shape(len(layers) * size // lanes, lanes, F32) for size in sizes]
    sums = pl.pallas_call(
        functools.partial(total_kernel, plans, [len(parts) for parts in layers], depths, scale), grid=(1,), in_specs=specs,
        out_specs=[whole(*out.shape) for out in shapes], out_shape=shapes,
        cost_estimate=pl.CostEstimate(flops=sum(a.size for a in arrays), bytes_accessed=4 * sum(a.size for a in arrays),
                                      transcendentals=0),
        compiler_params=pltpu.CompilerParams(vmem_limit_bytes=VMEM_LIMIT), name='totals')(*arrays)
    result = []
    for total, size in zip(sums, sizes):
        total = lax.optimization_barrier(total.reshape(size // lanes, len(layers), lanes))
        result.append(jnp.swapaxes(total, 0, 1).reshape(len(layers), size))
    return result


def solution(mesh):
    n_dev = mesh.shape[AXIS]

    def inner(tokens_x, context, cot_out, *shards):
        batch, tokens, width = tokens_x.shape
        _, valid, ctx_width = context.shape
        blocks = shards[0].shape[0]
        total = batch * n_dev
        depth = width // n_dev
        count = batch * tokens
        half = 4 * width

        views = []
        for shard, rows in zip(shards[:7], (depth, depth, depth, ctx_width // n_dev, depth, depth, half // n_dev)):
            views.append(shard.reshape(blocks, rows, -1))
        qkv_s, out_s = lax.optimization_barrier(views[:2])
        q2_s, kv2_s, out2_s = lax.optimization_barrier(views[2:5])
        ff1_s, ff2_s = lax.optimization_barrier(views[5:])
        me = lax.axis_index(AXIS)
        vec_len = shards[7].shape[1]
        vec_each = 17
        vec_rows = (blocks * vec_each + 15) // 16 * 16
        vec_block = lax.dynamic_update_slice(jnp.zeros((blocks, n_dev * vec_len), BF16), shards[7], (0, me * vec_len))
        vec_block = vec_block[:, :vec_each * width].reshape(blocks * vec_each, width)
        vec_block = jnp.pad(vec_block, ((0, vec_rows - blocks * vec_each), (0, 0)))

        members = []
        for layer in range(blocks):
            if layer < blocks - 1:
                members += [(layer, [qkv_s, out_s]), (layer, [kv2_s, q2_s, out2_s]), (layer, [ff1_s, ff2_s])]
            else:
                members += [(layer, [qkv_s, out_s, kv2_s, q2_s, out2_s]), (layer, [ff1_s]), (layer, [ff2_s])]
        groups = []
        for index, (layer, parts) in enumerate(members):
            block = pack(parts, layer, [vec_block] if index == 0 else [], width)
            groups.append(gather_group(block, n_dev))
        ff_groups = [groups[3 * layer + 2] * 2 if layer < blocks - 1 else groups[-2] + groups[-1] for layer in range(blocks)]
        ff_offsets = [8 * depth if layer < blocks - 1 else 0 for layer in range(blocks)]

        vecs = vec_sum(groups[0], vec_rows)
        vecs = vecs[:blocks * vec_each].reshape(blocks, vec_each, width)
        rows_all = jnp.pad(vecs[:, :9], ((0, 0), (0, 7), (0, 0)))
        bias_all = vecs[:, 9:].reshape(blocks, 1, 8 * width)

        ctx, ctx_mine, ctx_other = prepare_context(context, n_dev)

        h = tokens_x.reshape(count, width)
        cot = cot_out.reshape(count, width)
        saved, attention_groups = [], []
        for layer in range(blocks):
            rows, bias = rows_all[layer], bias_all[layer]
            group = groups[3 * layer:3 * layer + 2] if layer < blocks - 1 else [groups[3 * layer]] * 2
            attention_groups.append(group)
            if layer < blocks - 1:
                norm1, qkv, mix1, h1 = self_forward(h, rows, group[0], tokens)
                norm2, query, kv, mix2, h2 = cross_forward(h1, rows, ctx, group[1], tokens, valid)
                norm3, gated, save_a, save_g, h3 = ff_forward(h2, rows, bias, ff_groups[layer], ff_offsets[layer])
            else:
                norm1, qkv, mix1, h1, norm2, query, kv, mix2, h2 = attention_forward(h, rows, ctx, group[0], tokens, valid)
                norm3, gated, save_a, save_g, *down_pair = ff_up_forward(2, h2, rows, bias, cot, groups[-2])
                out_tokens = ff_down_forward(h2, rows, gated, groups[-1])
            saved.append((h, norm1, qkv, mix1, h1, norm2, query, kv, mix2, h2, norm3, gated, save_a, save_g))
            h = h3 if layer < blocks - 1 else None

        grad = rounded = cot
        results, vec_grads = [None] * blocks, [None] * blocks
        for layer in reversed(range(blocks)):
            turn = blocks - 1 - layer
            rows, group = rows_all[layer], attention_groups[layer]
            h0, norm1, qkv, mix1, h1, norm2, query, kv, mix2, h2, norm3, gated, save_a, save_g = saved[layer]

            def reduce(pair):
                return scatter(pair[0], pair[1], n_dev)

            if turn > 0:
                down_pair = weight_grads(1, (gated, rounded),
                                               [(0, c * width, 1, 0, 0, half // n_dev, (c,)) for c in range(half // width)], half // n_dev)
            r_ff2 = reduce(down_pair)
            sizes = (4,)
            d_norm, r_ff1, bias_grads, first_chunk = None, [], [], 0
            for index, chunks in enumerate(sizes):
                *out, vec_b1, far, keep = ff_grads(10 + 2 * turn + index, rounded, grad, save_a, save_g, norm3, h2, rows,
                                                   ff_groups[layer], ff_offsets[layer], first_chunk, chunks, d_norm)
                d_norm = out[0]
                bias_grads.append(((first_chunk, chunks), vec_b1))
                r_ff1.append(reduce((far, keep)))
                first_chunk += chunks
            grad, vec3 = out
            grad, vec2, *pair = cross_backward(3 + turn, grad, query, kv, h1, rows, norm2, mix2, ctx_mine, ctx_other, group[1],
                                               tokens, valid)
            r_cross = reduce(pair)
            grad, rounded, vec1, *pair = self_backward(8 + turn, grad, qkv, h0, rows, norm1, mix1, group[0], tokens)
            r_self = reduce(pair)
            results[layer] = [r_self], [r_cross], r_ff1, [r_ff2], sizes
            vec_grads[layer] = ([vec1, vec2, vec3] + [array for _, array in bias_grads], tuple(where for where, _ in bias_grads))
        vec_out = vec_total([part for parts, _ in vec_grads for part in parts], tuple(where for _, where in vec_grads), vec_rows, n_dev)
        vec_out = vec_out[:blocks * vec_each].reshape(blocks, vec_each * width)
        vec_out = jnp.pad(vec_out, ((0, 0), (0, vec_len * n_dev - vec_each * width)))
        vec_out = lax.dynamic_slice(vec_out, (0, me * vec_len), (blocks, vec_len))
        ff1_plans = []
        for layer in range(blocks):
            size = results[layer][4][0]
            ff1_plans.append([[(chunk // size, (kind * size + chunk % size) * depth) for kind in range(2) for chunk in range(4)]])
        deep = ctx_width // n_dev
        plans = ([[[(0, 0), (0, depth), (0, 2 * depth)], [(0, 3 * depth)]]] * blocks,
                 [[[(0, 0)], [(0, depth)], [(0, 2 * depth), (0, 2 * depth + deep)]]] * blocks, ff1_plans, [[[(0, 0)]]] * blocks)
        depths = ((depth, depth), (depth, depth, deep), (depth,), (half // n_dev,))
        summed = []
        for index in range(4):
            summed += totals([results[layer][index] for layer in range(blocks)], plans[index], depths[index], 1.0 / total)
        g_qkv, g_out, g_q2, g_out2, g_kv2, g_ff1, g_ff2 = summed
        outs = [g_qkv, g_out, g_q2, g_kv2, g_out2, g_ff1, g_ff2]
        outs.append(vec_out / total)
        return tuple([out_tokens.reshape(tokens_x.shape), rounded.reshape(tokens_x.shape)] + outs)

    param_spec = P(None, AXIS)
    in_specs = (P(AXIS), P(AXIS), P(AXIS)) + (param_spec,) * 8
    out_specs = (P(AXIS), P(AXIS)) + (param_spec,) * 8
    return jax.shard_map(inner, mesh=mesh, in_specs=in_specs, out_specs=out_specs, check_vma=False)
```
